8 devices in a mesh: dp: 1 (over z), tp: 2 (over y), cp: 4 (over x, core).
Axes of the slice: x: 2, y: 2, z: 1, core: 2. Of those that a mesh axis runs over, the one named last changes fastest.
Arguments:
- hidden: bfloat16 [16, 512, 6144], P('dp', 'cp')
- alphas: float32 [2], replicated
- wq_attn: bfloat16 [6144, 8192], P(None, 'tp')
- wk_attn: bfloat16 [6144, 1024], P(None, 'tp')
- wv_attn: bfloat16 [6144, 1024], P(None, 'tp')
- wo_attn: bfloat16 [8192, 6144], P('tp')
- gain_attn: float32 [6144], replicated
- wq_lin: bfloat16 [6144, 8192], P(None, 'tp')
- wk_lin: bfloat16 [6144, 8192], P(None, 'tp')
- wv_lin: bfloat16 [6144, 8192], P(None, 'tp')
- wg_lin: bfloat16 [6144, 8192], P(None, 'tp')
- slopes: float32 [64], P('tp')
- gain_inner: float32 [8192], P('tp')
- wo_lin: bfloat16 [8192, 6144], P('tp')
- gain_lin: float32 [6144], replicated
Outputs:
- output: bfloat16 [16, 512, 6144], P('dp', 'cp')
All inputs are finite; a program needn't handle non-finite values.
Results may differ from the reference program's by a relative error of at most 0.0125434.
Values are sent between devices in bfloat16 or wider.
A program may use at most 1.75 GiB of HBM per device.

```python
import math
import jax
import jax.numpy as jnp
from jax import lax

BATCH = 16
SEQ = 512
D = 6144
HEADS = 64
KV_HEADS = 8
HEAD = 128
CHUNK = 128

GROUP = HEADS // KV_HEADS
ROT = HEAD // 2
WIDTH = HEADS * HEAD
KV_WIDTH = KV_HEADS * HEAD
ROPE_BASE = 10000000.0
NORM_EPS = 1e-5


def setup_inputs(seed: int = 0, part: int = 0) -> dict:
    base_key = jax.random.key(seed)
    part_key = jax.random.fold_in(base_key, part)
    keys = jax.random.split(base_key, 16)
    logit_std = math.sqrt(max(math.log(SEQ / 8.0), 1.0))
    qk_scale = math.sqrt(logit_std / D)
    in_scale = 1.0 / math.sqrt(D)
    out_scale = 3.0 / math.sqrt(WIDTH)

    def normal_w(slot, shape, scale):
        return jax.random.normal(keys[slot], shape, jnp.float32) * scale

    head_scale = jnp.exp(jax.random.uniform(keys[0], (HEADS,), jnp.float32, -math.log(3.0), math.log(3.0)))
    rates = jnp.exp(jax.random.uniform(keys[1], (HEADS,), jnp.float32, math.log(0.25), math.log(8.0)))
    return {
        'hidden': jax.random.normal(part_key, (BATCH, SEQ, D), jnp.float32).astype(jnp.bfloat16),
        'alphas': jax.random.uniform(keys[2], (2,), jnp.float32, 1.5, 3.0),
        'wq_attn': normal_w(3, (D, WIDTH), qk_scale).astype(jnp.bfloat16),
        'wk_attn': normal_w(4, (D, KV_WIDTH), qk_scale).astype(jnp.bfloat16),
        'wv_attn': normal_w(5, (D, KV_WIDTH), in_scale).astype(jnp.bfloat16),
        'wo_attn': normal_w(6, (WIDTH, D), out_scale).astype(jnp.bfloat16),
        'gain_attn': jax.random.uniform(keys[7], (D,), jnp.float32, 0.5, 1.5),
        'wq_lin': normal_w(8, (D, WIDTH), in_scale).astype(jnp.bfloat16),
        'wk_lin': normal_w(9, (D, WIDTH), in_scale).astype(jnp.bfloat16),
        'wv_lin': (normal_w(10, (D, WIDTH), in_scale) * jnp.repeat(head_scale, HEAD)[None, :]).astype(jnp.bfloat16),
        'wg_lin': normal_w(11, (D, WIDTH), in_scale).astype(jnp.bfloat16),
        'slopes': rates / SEQ,
        'gain_inner': jax.random.uniform(keys[12], (WIDTH,), jnp.float32, 0.5, 1.5),
        'wo_lin': normal_w(13, (WIDTH, D), out_scale).astype(jnp.bfloat16),
        'gain_lin': jax.random.uniform(keys[14], (D,), jnp.float32, 0.5, 1.5),
    }


def rms_norm(values, gain_vec):
    return values * lax.rsqrt(jnp.mean(values * values, axis=-1, keepdims=True) + NORM_EPS) * gain_vec


def project(inputs, weight):
    flat_in = inputs.reshape(-1, inputs.shape[-1])
    product = jnp.dot(flat_in, weight, preferred_element_type=jnp.float32)
    return product.reshape(inputs.shape[:-1] + (weight.shape[-1],))


def rotary(values, positions):
    half = ROT // 2
    inv_freq = jnp.power(ROPE_BASE, -jnp.arange(half, dtype=jnp.float32) * 2.0 / ROT)
    angles = positions.astype(jnp.float32)[:, None] * inv_freq[None, :]
    cosine = jnp.cos(angles)[:, None, :]
    sine = jnp.sin(angles)[:, None, :]
    first = values[..., :half]
    second = values[..., half:ROT]
    return jnp.concatenate([first * cosine - second * sine, second * cosine + first * sine, values[..., ROT:]], axis=-1)


def softmax_layer(hidden, alphas, wq_attn, wk_attn, wv_attn, wo_attn, gain_attn):
    positions = jnp.arange(SEQ)
    keys_all = rotary(project(hidden, wk_attn).reshape(BATCH, SEQ, KV_HEADS, HEAD), positions).astype(jnp.bfloat16)
    values_all = project(hidden, wv_attn).astype(jnp.bfloat16).reshape(BATCH, SEQ, KV_HEADS, HEAD)
    keys_heads = jnp.moveaxis(keys_all, 2, 0)
    values_heads = jnp.moveaxis(values_all, 2, 0)
    blocks = jnp.moveaxis(hidden.reshape(BATCH, SEQ // CHUNK, CHUNK, D), 1, 0)
    starts = jnp.arange(SEQ // CHUNK) * CHUNK
    scale = 1.0 / math.sqrt(HEAD)

    def query_block(inputs):
        block, start = inputs
        q_pos = start + jnp.arange(CHUNK)
        queries = rotary(project(block, wq_attn).reshape(BATCH, CHUNK, HEADS, HEAD), q_pos).astype(jnp.bfloat16)
        queries = jnp.moveaxis(queries.reshape(BATCH, CHUNK, KV_HEADS, GROUP, HEAD), 2, 0)
        mask = q_pos[:, None] >= positions[None, :]

        def per_head(head_in):
            q_head, k_head, v_head = head_in
            scores = jnp.einsum('bqgd,bsd->bgqs', q_head.astype(jnp.float32), k_head.astype(jnp.float32)) * scale
            scores = jnp.where(mask, scores, -jnp.inf)
            prob_vals = jax.nn.softmax(scores, axis=-1).astype(jnp.bfloat16)
            return jnp.einsum('bgqs,bsd->bqgd', prob_vals.astype(jnp.float32), v_head.astype(jnp.float32))

        head_out = lax.map(per_head, (queries, keys_heads, values_heads))
        attn_out = jnp.moveaxis(head_out, 0, 2).astype(jnp.bfloat16).reshape(BATCH, CHUNK, WIDTH)
        mixed = project(attn_out, wo_attn)
        return rms_norm(alphas[0] * block.astype(jnp.float32) + mixed, gain_attn).astype(jnp.bfloat16)

    out_blocks = lax.map(query_block, (blocks, starts))
    return jnp.moveaxis(out_blocks, 0, 1).reshape(BATCH, SEQ, D)


def lightning_layer(mid_hidden, alphas, wq_lin, wk_lin, wv_lin, wg_lin, slopes, gain_inner, wo_lin, gain_lin):
    offsets = jnp.arange(CHUNK).astype(jnp.float32)
    tok_gap = offsets[:, None] - offsets[None, :]
    intra_w = jnp.where(tok_gap[None] >= 0, jnp.exp(-slopes[:, None, None] * jnp.maximum(tok_gap, 0.0)[None]), 0.0)
    query_decay = jnp.exp(-slopes[None, :] * (offsets[:, None] + 1.0))
    key_decay = jnp.exp(-slopes[None, :] * (CHUNK - 1.0 - offsets[:, None]))
    tile_decay = jnp.exp(-slopes * CHUNK)
    blocks = jnp.moveaxis(mid_hidden.reshape(BATCH, SEQ // CHUNK, CHUNK, D), 1, 0)

    def heads_of(block, weight):
        return jax.nn.silu(project(block, weight)).astype(jnp.bfloat16).astype(jnp.float32).reshape(BATCH, CHUNK, HEADS, HEAD)

    def step(state, block):
        queries = heads_of(block, wq_lin)
        keys_c = heads_of(block, wk_lin)
        values_c = heads_of(block, wv_lin)
        gate_vals = jax.nn.sigmoid(project(block, wg_lin))
        scores = jnp.einsum('bqhd,bshd->bhqs', queries, keys_c) * intra_w[None]
        inside = jnp.einsum('bhqs,bshe->bqhe', scores, values_c)
        carried = jnp.einsum('bqhd,bhde->bqhe', queries, state) * query_decay[None, :, :, None]
        mixed = (inside + carried).reshape(BATCH, CHUNK, WIDTH)
        inner_vals = (rms_norm(mixed, gain_inner) * gate_vals).astype(jnp.bfloat16)
        new_state = tile_decay[None, :, None, None] * state + jnp.einsum('bshd,bshe->bhde', keys_c * key_decay[None, :, :, None], values_c)
        lin_out = project(inner_vals, wo_lin)
        out_block = rms_norm(alphas[1] * block.astype(jnp.float32) + lin_out, gain_lin).astype(jnp.bfloat16)
        return new_state, out_block

    init_state = jnp.zeros((BATCH, HEADS, HEAD, HEAD), jnp.float32)
    out_blocks = lax.scan(step, init_state, blocks)[1]
    return jnp.moveaxis(out_blocks, 0, 1).reshape(BATCH, SEQ, D)


def reference(hidden, alphas, wq_attn, wk_attn, wv_attn, wo_attn, gain_attn, wq_lin, wk_lin, wv_lin, wg_lin, slopes, gain_inner, wo_lin, gain_lin):
    mid_hidden = softmax_layer(hidden, alphas, wq_attn, wk_attn, wv_attn, wo_attn, gain_attn)
    return lightning_layer(mid_hidden, alphas, wq_lin, wk_lin, wv_lin, wg_lin, slopes, gain_inner, wo_lin, gain_lin)
```

```python
import math

import jax
import jax.numpy as jnp
import numpy as np
from jax import lax
from jax.experimental import pallas as pl
from jax.experimental.pallas import tpu as pltpu
from jax.sharding import PartitionSpec as P

MESH = pl.DeviceIdType.MESH
F32 = jnp.float32
BF = jnp.bfloat16
ROPE_BASE = 10000000.0
EPS = 1e-5

TOK = 128
HD = 128
TN = 512
DM = 6144
W = 4096
KVW = 1024
OWN_KV = W - KVW
N_SEQ = 4
N_CH = 4
N_CP = 4
N_G = 8
ROWS = N_SEQ * TOK
OWN = ROWS // 2
RB = 64
LA, LB = 0, 1
K, V, Q = 0, 1, 2
NT_DIMS = (((1,), (1,)), ((), ()))
TN_DIMS = (((0,), (0,)), ((), ()))


def rope_tables(n_cp):
    half = HD // 4
    inv = ROPE_BASE ** (-np.arange(half, dtype=np.float64) * 2.0 / (2 * half))
    pos = np.arange(n_cp * TOK, dtype=np.float64)
    ang = pos[:, None] * inv[None, :]
    tab = np.zeros((3, n_cp * TOK, HD), np.float32)
    tab[0] = 1.0
    tab[0, :, :half] = np.cos(ang)
    tab[0, :, half : 2 * half] = np.cos(ang)
    tab[1, :, :half] = -np.sin(ang)
    tab[2, :, half : 2 * half] = np.sin(ang)
    return np.ascontiguousarray(tab.reshape(3, n_cp, TOK, HD).transpose(1, 0, 2, 3))


def mo(v, m):
    return pl.multiple_of(v, m)


def parity(j):
    return lax.rem(j, 2)


def blk(b):
    return pl.ds(mo(b * TOK, TOK), TOK)


def hcol(g, hh):
    return pl.ds(mo((4 * g + hh) * HD, HD), HD)


def dot(a, b, dims=(((1,), (0,)), ((), ()))):
    return lax.dot_general(a, b, dims, preferred_element_type=F32)


def sigmoid(z):
    return 1.0 / (1.0 + jnp.exp(-z))


def kernel(
    hid, wqa, wka, wva, woa, wql, wkl, wvl, wgl, wol, rope_hbm, alphas, slopes, gains, ginner,
    out, pt, prec, h1own, h1oth, kvh, kvr, sth, str_,
    wbuf, x, kvq, gbuf, u, acc, ost, stg, pst, nb_p, nb_r, nb_h, nout, ss, rsb, rope, ssx, ssr, wtab,
    w_sem, x_sem, o_sem, kvo_sem, kvl_sem, sto_sem, stl_sem, nl_sem, no_sem,
    rs_send, rs_recv, ag_send, ag_recv, kv_send, kv_recv, st_send, st_recv, ss_send, ss_recv,
):
    cp = lax.axis_index("cp")
    tp = lax.axis_index("tp")
    mate = 1 - tp
    is0, is1, is2, is3 = (cp == c for c in range(N_CP))

    bar = pltpu.get_barrier_semaphore()
    pl.semaphore_signal(bar, inc=1, device_id={"tp": mate}, device_id_type=MESH)
    for d in range(1, 4):
        pl.semaphore_signal(bar, inc=1, device_id={"cp": lax.rem(cp + d, 4)}, device_id_type=MESH)

    def wcopy(src, col, slot, rows):
        dst = wbuf.at[slot] if rows == DM else wbuf.at[slot, pl.ds(0, rows)]
        return pltpu.make_async_copy(src.at[:, pl.ds(col, TN)], dst, w_sem.at[slot])

    def wcol(j):
        return mo(j * TN, TN)

    def issue_a(j, slot):
        @pl.when(j == 0)
        def _():
            wcopy(wka, 0, slot, DM).start()

        @pl.when(j == 1)
        def _():
            wcopy(wva, 0, slot, DM).start()

        @pl.when(j >= 2)
        def _():
            wcopy(wqa, wcol(j - 2), slot, DM).start()

    def issue_b(j, slot):
        for n, w in enumerate((wkl, wvl, wql, wgl)):

            @pl.when(j // 8 == n)
            def _(n=n, w=w):
                wcopy(w, wcol(j - 8 * n), slot, DM).start()

    def wait_w(slot, rows=DM):
        wcopy(wqa if rows == DM else woa, 0, slot, rows).wait()

    def own_row(i):
        return mo((tp * 8 + 2 * i) * TOK, TOK)

    def oth_row(i):
        return mo((mate * 8 + 2 * i) * TOK, TOK)

    def load_x(top, bot):
        a = pltpu.make_async_copy(top, x.at[pl.ds(0, OWN)], x_sem.at[0])
        b = pltpu.make_async_copy(bot, x.at[pl.ds(OWN, OWN)], x_sem.at[1])
        a.start()
        b.start()
        a.wait()
        b.wait()

    def rs_copy(n, i, col, width):
        return pltpu.make_async_remote_copy(
            src_ref=pt.at[n, i, pl.ds(OWN, OWN), pl.ds(col, width)],
            dst_ref=prec.at[n, i, :, pl.ds(col, width)],
            send_sem=rs_send.at[n, i],
            recv_sem=rs_recv.at[n, i],
            device_id={"tp": mate},
            device_id_type=MESH,
        )

    def ag_copy(n, i, row, rows):
        if n == 0:
            src = h1own.at[i, pl.ds(row, rows)]
            dst = h1oth.at[i, pl.ds(row, rows)]
        else:
            src = out.at[pl.ds(mo(own_row(i) + row, RB), rows)]
            dst = src
        return pltpu.make_async_remote_copy(
            src_ref=src,
            dst_ref=dst,
            send_sem=ag_send.at[n, i],
            recv_sem=ag_recv.at[n, i],
            device_id={"tp": mate},
            device_id_type=MESH,
        )

    def ag_wait_recv(n, i):
        if n == 0:
            ag_copy(0, i, 0, OWN).wait_recv()
        else:
            oth = out.at[pl.ds(oth_row(i), OWN)]
            pltpu.make_async_remote_copy(
                src_ref=oth,
                dst_ref=oth,
                send_sem=ag_send.at[n, i],
                recv_sem=ag_recv.at[n, i],
                device_id={"tp": mate},
                device_id_type=MESH,
            ).wait_recv()

    def kv_copy(i, src, own, dst_cp, send):
        return pltpu.make_async_remote_copy(
            src_ref=kvh.at[i] if own else kvr.at[i, src],
            dst_ref=kvr.at[i, src],
            send_sem=kv_send.at[i, send],
            recv_sem=kv_recv.at[i, src],
            device_id={"cp": dst_cp},
            device_id_type=MESH,
        )

    def st_copy(i, g):
        return pltpu.make_async_remote_copy(
            src_ref=sth.at[i, g],
            dst_ref=str_.at[i, g],
            send_sem=st_send.at[i, g],
            recv_sem=st_recv.at[i, g],
            device_id={"cp": lax.rem(cp + 1, 4)},
            device_id_type=MESH,
        )

    def ss_copy(i):
        return pltpu.make_async_remote_copy(
            src_ref=ssx.at[i],
            dst_ref=ssr.at[i],
            send_sem=ss_send.at[i],
            recv_sem=ss_recv.at[i],
            device_id={"tp": mate},
            device_id_type=MESH,
        )

    def norm(n, i):
        with jax.named_scope("norm_wait"):
            rs_copy(n, i, 0, DM).wait_recv()
        wait_n = n

        def loads(r, slot):
            rows = pl.ds(mo(r * RB, RB), RB)
            if wait_n == 0:
                res = hid.at[pl.ds(mo(own_row(i) + r * RB, RB), RB)]
            else:
                res = h1own.at[i, rows]
            return (
                pltpu.make_async_copy(pt.at[n, i, rows], nb_p.at[slot], nl_sem.at[slot, 0]),
                pltpu.make_async_copy(prec.at[n, i, rows], nb_r.at[slot], nl_sem.at[slot, 1]),
                pltpu.make_async_copy(res, nb_h.at[slot], nl_sem.at[slot, 2]),
            )

        def store(r, slot):
            rows = pl.ds(mo(r * RB, RB), RB)
            if n == 0:
                dst = h1own.at[i, rows]
            else:
                dst = out.at[pl.ds(mo(own_row(i) + r * RB, RB), RB)]
            return pltpu.make_async_copy(nout.at[slot], dst, no_sem.at[slot])

        with jax.named_scope("norm"):
            for c in loads(0, 0):
                c.start()
            alpha = alphas[n]

            @pl.loop(0, 4)
            def _(r):
                slot = parity(r)

                @pl.when(r + 1 < 4)
                def _():
                    for c in loads(r + 1, 1 - slot):
                        c.start()

                for c in loads(r, slot):
                    c.wait()

                @pl.loop(0, 4)
                def _(q):
                    rows = pl.ds(mo(q * 16, 16), 16)
                    both = nb_p[slot, rows, :].astype(F32) + nb_r[slot, rows, :].astype(F32)
                    h = alpha * nb_h[slot, rows, :].astype(F32) + both
                    inv = lax.rsqrt(jnp.mean(h * h, axis=-1, keepdims=True) + EPS)
                    nout[slot, rows, :] = (h * inv * gains[n : n + 1, :]).astype(BF)

                @pl.when(r >= 1)
                def _():
                    store(r - 1, 1 - slot).wait()
                    ag_copy(n, i, mo((r - 1) * RB, RB), RB).start()

                store(r, slot).start()

            store(3, 1).wait()
            ag_copy(n, i, OWN - RB, RB).start()

    def out_proj(n, i, wo, then):
        def put(j, slot):
            return pltpu.make_async_copy(ost.at[slot], pt.at[n, i, :, pl.ds(wcol(j), TN)], o_sem.at[slot])

        with jax.named_scope("out_proj"):
            @pl.loop(0, 12)
            def _(j):
                slot = parity(j)
                wait_w(slot, W)

                @pl.when(j + 1 < 12)
                def _():
                    wcopy(wo, wcol(j + 1), 1 - slot, W).start()

                @pl.when(j == 11)
                def _():
                    then()

                ost[slot] = dot(u[...], wbuf[slot, 0:W, :]).astype(BF)

                @pl.when(j >= 1)
                def _():
                    put(j - 1, 1 - slot).wait()
                    rs_copy(n, i, wcol(j - 1), TN).start()

                put(j, slot).start()

            put(11, 1).wait()
            rs_copy(n, i, 11 * TN, TN).start()

    def layer_a(i, then):
        with jax.named_scope("x_a"):
            load_x(hid.at[pl.ds(own_row(i), OWN)], hid.at[pl.ds(oth_row(i), OWN)])
        kv_out = pltpu.make_async_copy(kvq.at[K, :, pl.ds(OWN_KV, KVW)], kvh.at[i], kvo_sem)

        def finish(j, slot):
            kind = jnp.where(j == 1, 1, 0)
            dst = jnp.where(j < 2, 0, 2)
            col = mo(jnp.where(j < 2, OWN_KV + j * TN, (j - 2) * TN), TN)
            for b in range(N_SEQ):
                for h in range(N_SEQ):
                    a = acc[slot, blk(b), h * HD : (h + 1) * HD]
                    a = (
                        a * rope[kind, 0]
                        + pltpu.roll(a, HD - 32, 1) * rope[kind, 1]
                        + pltpu.roll(a, 32, 1) * rope[kind, 2]
                    )
                    kvq[dst, blk(b), pl.ds(col + h * HD, HD)] = a.astype(BF)

        with jax.named_scope("qkv_a"):
            @pl.loop(0, 10)
            def _(j):
                slot = parity(j)
                wait_w(slot)

                @pl.when(j + 1 < 10)
                def _():
                    issue_a(j + 1, 1 - slot)

                @pl.when(j == 9)
                def _():
                    wcopy(woa, 0, 0, W).start()

                finish(jnp.maximum(j - 1, 0), 1 - slot)
                acc[slot] = dot(x[...], wbuf[slot])

                @pl.when(j == 2)
                def _():
                    kv_out.start()

                @pl.when(j == 3)
                def _():
                    kv_out.wait()

                    @pl.when(is0)
                    def _():
                        kv_copy(i, 0, True, 2, 0).start()
                        kv_copy(i, 0, True, 1, 1).start()

                    @pl.when(is1)
                    def _():
                        kv_copy(i, 1, True, 3, 0).start()

                    @pl.when(is2)
                    def _():
                        kv_copy(i, 2, True, 3, 0).start()

        finish(9, 1)

        with jax.named_scope("kv_wait"):
            @pl.when(is2)
            def _():
                kv_copy(i, 0, False, 3, 1).wait_recv()
                kv_copy(i, 0, False, 3, 1).start()

            @pl.when(is3)
            def _():
                kv_copy(i, 1, False, 2, 0).wait_recv()
                kv_copy(i, 1, False, 2, 0).start()
                kv_copy(i, 2, False, 2, 0).wait_recv()
                kv_copy(i, 0, False, 2, 0).wait_recv()

            @pl.when(is2)
            def _():
                kv_copy(i, 1, False, 3, 1).wait_recv()

            @pl.when(is1)
            def _():
                kv_copy(i, 0, False, 3, 1).wait_recv()

            def kv_load(s):
                return pltpu.make_async_copy(kvr.at[i, s], kvq.at[K, :, pl.ds(s * KVW, KVW)], kvl_sem.at[s])

            for s in range(3):

                @pl.when(cp > s)
                def _(s=s):
                    kv_load(s).start()

            for s in range(3):

                @pl.when(cp > s)
                def _(s=s):
                    kv_load(s).wait()

        with jax.named_scope("attn"):
            scale = math.log2(math.e) / math.sqrt(HD)
            for c in range(N_SEQ):

                @pl.when(cp == c)
                def _(c=c):
                    cols = [OWN_KV] + [s * KVW for s in range(c)]

                    @pl.loop(0, 16)
                    def _(t):
                        b = t // 4
                        g = lax.rem(t, 4)
                        rows = blk(b)
                        ks = [kvq[K, rows, pl.ds(mo(o + g * HD, HD), HD)] for o in cols]
                        vs = [kvq[K, rows, pl.ds(mo(o + TN + g * HD, HD), HD)] for o in cols]
                        keys = jnp.concatenate(ks, axis=0) if c else ks[0]
                        vals = jnp.concatenate(vs, axis=0) if c else vs[0]
                        key_id = lax.broadcasted_iota(jnp.int32, (TOK, 2 * TOK), 0)
                        tok_id = lax.rem(lax.broadcasted_iota(jnp.int32, (TOK, 2 * TOK), 1), TOK)
                        causal = key_id <= tok_id
                        for p in range(N_SEQ):
                            hc = [mo((g * 8 + 2 * p + e) * HD, HD) for e in range(2)]
                            qs = jnp.concatenate([kvq[Q, rows, pl.ds(o, HD)] for o in hc], axis=0)
                            s = dot(keys, qs, NT_DIMS)
                            own = jnp.where(causal, s[:TOK], -jnp.inf)
                            s = jnp.concatenate([own, s[TOK:]], axis=0) if c else own
                            m = jnp.max(s, axis=0, keepdims=True)
                            e = jnp.exp2((s - m) * scale)
                            inv = 1.0 / jnp.sum(e, axis=0, keepdims=True)
                            o = dot(vals, e.astype(BF), TN_DIMS) * inv
                            for z in range(2):
                                u[rows, pl.ds(hc[z], HD)] = o[:, z * TOK : (z + 1) * TOK].T.astype(BF)

        out_proj(0, i, woa, then)

    def key_decay(h):
        back = lax.broadcasted_iota(jnp.int32, (TOK, HD), 0).astype(F32) - (TOK - 1.0)
        return jnp.exp(slopes[h] * back)

    def state_of(g, b, hh, kd):
        rows = blk(b)
        col = hcol(g, hh)
        k = (kvq[K, rows, col].astype(F32) * kd).astype(BF)
        return dot(k, kvq[V, rows, col], TN_DIMS)

    def block_decay(h):
        return jnp.exp(jnp.full((8, HD), -float(TOK), F32) * slopes[h])[0:1, :]

    def st_store(i, g, slot):
        return pltpu.make_async_copy(stg.at[slot], sth.at[i, g], sto_sem.at[slot])

    def st_load(i, g, slot):
        return pltpu.make_async_copy(str_.at[i, g], pst.at[slot], stl_sem.at[slot])

    def local_state(i, g):
        slot = parity(g)

        @pl.when(is1)
        def _():
            st_copy(i, g).wait_recv()
            st_load(i, g, slot).start()
            st_load(i, g, slot).wait()

        @pl.when(is0)
        def _():
            for hh in range(N_SEQ):
                kd = key_decay(4 * g + hh)
                for b in range(N_SEQ):
                    stg[slot, b * 4 + hh] = state_of(g, b, hh, kd)

        @pl.when(is1)
        def _():
            for hh in range(N_SEQ):
                kd = key_decay(4 * g + hh)
                bd = block_decay(4 * g + hh)
                for b in range(N_SEQ):
                    stg[slot, b * 4 + hh] = state_of(g, b, hh, kd) + bd * pst[slot, b * 4 + hh]

        st_store(i, g, slot).start()

    def st_send_on(i, g):
        st_store(i, g, parity(g)).wait()
        st_copy(i, g).start()

    def layer_b(i, middle, then):
        with jax.named_scope("h1_wait"):
            ag_wait_recv(0, i)
        with jax.named_scope("x_b"):
            load_x(h1own.at[i], h1oth.at[i])

        def finish(j, a):
            kvq[j // 8, :, pl.ds(wcol(lax.rem(j, 8)), TN)] = (a * sigmoid(a)).astype(BF)

        with jax.named_scope("qkv_b"):
            @pl.loop(0, 24)
            def _(j):
                slot = parity(j)
                wait_w(slot)
                issue_b(j + 1, 1 - slot)
                finish(j, dot(x[...], wbuf[slot]))

                @pl.when((cp <= 1) & (j >= 9) & (j < 17))
                def _():
                    local_state(i, j - 9)

                    @pl.when(j >= 10)
                    def _():
                        st_send_on(i, j - 10)

                @pl.when((cp <= 1) & (j == 17))
                def _():
                    st_send_on(i, 7)

        middle()

        with jax.named_scope("gate"):
            @pl.loop(0, 8)
            def _(j):
                slot = parity(j)
                wait_w(slot)

                @pl.when(j + 1 < 8)
                def _():
                    issue_b(25 + j, 1 - slot)

                @pl.when(j == 7)
                def _():
                    wcopy(wol, 0, 0, W).start()

                gbuf[:, pl.ds(wcol(j), TN)] = sigmoid(dot(x[...], wbuf[slot]))

        with jax.named_scope("lin"):
            ss[...] = jnp.zeros_like(ss)

            @pl.when(is0)
            def _():
                pst[...] = jnp.zeros_like(pst)

            @pl.loop(0, 8)
            def _(g):
                slot = parity(g)

                @pl.when(is1)
                def _():
                    st_load(i, g, slot).start()

                @pl.when(cp >= 2)
                def _():
                    st_copy(i, g).wait_recv()
                    st_load(i, g, slot).start()

                for hh in range(N_SEQ):
                    lam = slopes[4 * g + hh]
                    row = lax.broadcasted_iota(jnp.int32, (TOK, HD), 0).astype(F32)
                    lane = lax.broadcasted_iota(jnp.int32, (TOK, HD), 1).astype(F32)
                    gap = row - lane
                    wtab[hh, 0] = jnp.where(gap >= 0, jnp.exp(-lam * jnp.maximum(gap, 0.0)), 0.0)
                    wtab[hh, 1] = jnp.exp(-lam * (row + 1.0))

                @pl.when(cp >= 1)
                def _():
                    st_load(i, g, slot).wait()

                @pl.when(is2)
                def _():
                    for hh in range(N_SEQ):
                        kd = key_decay(4 * g + hh)
                        bd = block_decay(4 * g + hh)
                        for b in range(N_SEQ):
                            stg[slot, b * 4 + hh] = state_of(g, b, hh, kd) + bd * pst[slot, b * 4 + hh]
                    st_store(i, g, slot).start()

                @pl.loop(0, 4)
                def _(b):
                    rows = blk(b)
                    sq = None
                    res = []
                    for hh in range(N_SEQ):
                        col = hcol(g, hh)
                        q = kvq[Q, rows, col]
                        w = (dot(q, kvq[K, rows, col], NT_DIMS) * wtab[hh, 0]).astype(BF)
                        o = dot(w, kvq[V, rows, col])
                        o = o + dot(q, pst[slot, b * 4 + hh].astype(BF)) * wtab[hh, 1]
                        sq = o * o if sq is None else sq + o * o
                        res.append(o * ginner[0:1, col] * gbuf[rows, col])
                    for hh in range(N_SEQ):
                        gbuf[rows, hcol(g, hh)] = res[hh]
                    ss[rows, :] += sq

                @pl.when(is2)
                def _():
                    st_send_on(i, g)

        with jax.named_scope("ss_swap"):
            sums = [jnp.sum(ss[blk(b), :].T, axis=0, keepdims=True) for b in range(N_SEQ)]
            ssx[i] = jnp.concatenate(sums + sums, axis=0)
            ss_copy(i).start()
            ss_copy(i).wait_recv()
            for b in range(N_SEQ):
                whole = ssx[i, b : b + 1, :] + ssr[i, b ^ 2 : (b ^ 2) + 1, :]
                inv = lax.rsqrt(whole / 8192.0 + EPS)
                rsb[b] = jnp.broadcast_to(inv, (TOK, TOK)).T

        with jax.named_scope("scale"):
            @pl.loop(0, 8)
            def _(g):
                for b in range(N_SEQ):
                    rsv = rsb[b]
                    for hh in range(N_SEQ):
                        col = hcol(g, hh)
                        u[blk(b), col] = (gbuf[blk(b), col] * rsv).astype(BF)

        out_proj(1, i, wol, then)

    issue_a(0, 0)
    rope_in = pltpu.make_async_copy(rope_hbm.at[cp], rope.at[0], kvo_sem)
    rope_in.start()
    rope[1, 0] = jnp.ones((TOK, HD), F32)
    rope[1, 1] = jnp.zeros((TOK, HD), F32)
    rope[1, 2] = jnp.zeros((TOK, HD), F32)
    rope_in.wait()
    pl.semaphore_wait(bar, 4)

    @pl.loop(0, 7)
    def _(s):
        @pl.when((s < 3) | (s == 4))
        def _():
            def then_a():
                @pl.when(s < 2)
                def _():
                    issue_a(0, 0)

                @pl.when(s >= 2)
                def _():
                    issue_b(0, 0)

            layer_a(jnp.where(s < 3, s, 3), then_a)

        @pl.when((s == 1) | (s == 2))
        def _():
            norm(0, s - 1)

        @pl.when(s == 4)
        def _():
            norm(1, 0)

        @pl.when(s >= 3)
        def _():
            def middle():
                @pl.when(s <= 4)
                def _():
                    norm(0, s - 1)

                @pl.when(s >= 5)
                def _():
                    norm(1, s - 4)

            def then_b():
                @pl.when(s == 3)
                def _():
                    issue_a(0, 0)

                @pl.when((s > 3) & (s < 6))
                def _():
                    issue_b(0, 0)

            layer_b(s - 3, middle, then_b)

    norm(1, 3)

    for i in range(N_SEQ):
        for n in range(2):
            rs_copy(n, i, 0, DM).wait_send()
            ag_copy(n, i, 0, OWN).wait_send()
        ag_wait_recv(1, i)
        ss_copy(i).wait_send()

        @pl.when(is0)
        def _(i=i):
            kv_copy(i, 0, True, 2, 0).wait_send()
            kv_copy(i, 0, True, 1, 1).wait_send()

        @pl.when(is1)
        def _(i=i):
            kv_copy(i, 1, True, 3, 0).wait_send()

        @pl.when(is2)
        def _(i=i):
            kv_copy(i, 2, True, 3, 0).wait_send()
            kv_copy(i, 0, False, 3, 1).wait_send()

        @pl.when(is3)
        def _(i=i):
            kv_copy(i, 1, False, 2, 0).wait_send()

        @pl.when(cp <= 2)
        def _(i=i):
            @pl.loop(0, 8)
            def _(g):
                st_copy(i, g).wait_send()


def solution(mesh):
    n_cp = mesh.shape["cp"]
    table = rope_tables(n_cp)
    any_ = pl.BlockSpec(memory_space=pl.ANY)
    smem = pl.BlockSpec(memory_space=pltpu.SMEM)
    vmem = pl.BlockSpec(memory_space=pltpu.VMEM)
    dma = pltpu.SemaphoreType.DMA
    two = (2,)

    def body(hidden, alphas, wqa, wka, wva, woa, gain_attn, wql, wkl, wvl, wgl, slopes, gain_inner, wol, gain_lin):
        shape = hidden.shape
        hid = hidden.reshape(shape[0] * shape[1], shape[2])
        gains = jnp.stack([gain_attn, gain_lin])
        sds = jax.ShapeDtypeStruct
        outs = (
            sds(hid.shape, BF),
            sds((2, N_CH, ROWS, DM), BF),
            sds((2, N_CH, OWN, DM), BF),
            sds((N_CH, OWN, DM), BF),
            sds((N_CH, OWN, DM), BF),
            sds((N_CH, ROWS, KVW), BF),
            sds((N_CH, 3, ROWS, KVW), BF),
            sds((N_CH, N_G, 16, HD, HD), F32),
            sds((N_CH, N_G, 16, HD, HD), F32),
        )
        scratch = [
            pltpu.VMEM((2, DM, TN), BF),
            pltpu.VMEM((ROWS, DM), BF),
            pltpu.VMEM((3, ROWS, W), BF),
            pltpu.VMEM((ROWS, W), F32),
            pltpu.VMEM((ROWS, W), BF),
            pltpu.VMEM((2, ROWS, TN), F32),
            pltpu.VMEM((2, ROWS, TN), BF),
            pltpu.VMEM((2, 16, HD, HD), F32),
            pltpu.VMEM((2, 16, HD, HD), F32),
            pltpu.VMEM((2, RB, DM), BF),
            pltpu.VMEM((2, RB, DM), BF),
            pltpu.VMEM((2, RB, DM), BF),
            pltpu.VMEM((2, RB, DM), BF),
            pltpu.VMEM((ROWS, HD), F32),
            pltpu.VMEM((N_SEQ, TOK, HD), F32),
            pltpu.VMEM((2, 3, TOK, HD), F32),
            pltpu.VMEM((N_CH, 8, HD), F32),
            pltpu.VMEM((N_CH, 8, HD), F32),
            pltpu.VMEM((4, 2, TOK, HD), F32),
            dma(two), dma(two), dma(two), dma(()), dma((3,)), dma(two), dma(two), dma((2, 3)), dma(two),
            dma((2, N_CH)), dma((2, N_CH)), dma((2, N_CH)), dma((2, N_CH)), dma((N_CH, 2)), dma((N_CH, 3)), dma((N_CH, N_G)), dma((N_CH, N_G)),
            dma((N_CH,)), dma((N_CH,)),
        ]
        res = pl.pallas_call(
            kernel,
            out_shape=outs,
            in_specs=[any_] * 11 + [smem, smem, vmem, vmem],
            out_specs=tuple(any_ for _ in outs),
            scratch_shapes=scratch,
            compiler_params=pltpu.CompilerParams(
                collective_id=0, has_side_effects=True, vmem_limit_bytes=67043328
            ),
            name="layers",
        )(
            hid, wqa, wka, wva, woa, wql, wkl, wvl, wgl, wol, jnp.asarray(table), alphas, slopes, gains,
            gain_inner.reshape(1, -1),
        )
        return res[0].reshape(shape)

    act = P("dp", "cp", None)
    rep = P()
    col = P(None, "tp")
    row = P("tp", None)
    vec = P("tp")
    in_specs = (act, rep, col, col, col, row, rep, col, col, col, col, vec, vec, row, rep)
    return jax.shard_map(body, mesh=mesh, in_specs=in_specs, out_specs=act, check_vma=False)
```

```python
import math

import jax
import jax.numpy as jnp
import numpy as np
from jax import lax
from jax.experimental import pallas as pl
from jax.experimental.pallas import tpu as pltpu
from jax.sharding import PartitionSpec as P

MESH = pl.DeviceIdType.MESH
F32 = jnp.float32
BF = jnp.bfloat16
ROPE_BASE = 10000000.0
EPS = 1e-5

TOK = 128
HD = 128
TN = 512
DM = 6144
W = 4096
KVW = 1024
OWN_KV = W - KVW
N_SEQ = 4
N_CH = 4
N_CP = 4
N_G = 8
ROWS = N_SEQ * TOK
OWN = ROWS // 2
RB = 32
N_RB = OWN // RB
LA, LB = 0, 1
K, V, Q = 0, 1, 2
NT_DIMS = (((1,), (1,)), ((), ()))
TN_DIMS = (((0,), (0,)), ((), ()))


def rope_tables(n_cp):
    half = HD // 4
    inv = ROPE_BASE ** (-np.arange(half, dtype=np.float64) * 2.0 / (2 * half))
    pos = np.arange(n_cp * TOK, dtype=np.float64)
    ang = pos[:, None] * inv[None, :]
    tab = np.zeros((3, n_cp * TOK, HD), np.float32)
    tab[0] = 1.0
    tab[0, :, :half] = np.cos(ang)
    tab[0, :, half : 2 * half] = np.cos(ang)
    tab[1, :, :half] = -np.sin(ang)
    tab[2, :, half : 2 * half] = np.sin(ang)
    return np.ascontiguousarray(tab.reshape(3, n_cp, TOK, HD).transpose(1, 0, 2, 3))


def mo(v, m):
    return pl.multiple_of(v, m)


def parity(j):
    return lax.rem(j, 2)


def blk(b):
    return pl.ds(mo(b * TOK, TOK), TOK)


def hcol(g, hh):
    return pl.ds(mo((4 * g + hh) * HD, HD), HD)


def dot(a, b, dims=(((1,), (0,)), ((), ()))):
    return lax.dot_general(a, b, dims, preferred_element_type=F32)


def sigmoid(z):
    return 1.0 / (1.0 + jnp.exp(-z))


def kernel(
    hid, wqa, wka, wva, woa, wql, wkl, wvl, wgl, wol, rope_hbm, alphas, slopes, gains, ginner,
    out, pt, prec, h1own, h1oth, kvh, kvr, sth, str_,
    wbuf, x, kvq, gbuf, u, acc, ost, stg, pst, nb_p, nb_r, nb_h, nout, ss, rsb, rope, ssx, ssr, wtab,
    w_sem, x_sem, o_sem, kvo_sem, kvl_sem, sto_sem, stl_sem, nl_sem, no_sem,
    rs_send, rs_recv, ag_send, ag_recv, kv_send, kv_recv, st_send, st_recv, ss_send, ss_recv,
):
    cp = lax.axis_index("cp")
    tp = lax.axis_index("tp")
    mate = 1 - tp
    is0, is1, is2, is3 = (cp == c for c in range(N_CP))

    bar = pltpu.get_barrier_semaphore()
    pl.semaphore_signal(bar, inc=1, device_id={"tp": mate}, device_id_type=MESH)
    for d in range(1, 4):
        pl.semaphore_signal(bar, inc=1, device_id={"cp": lax.rem(cp + d, 4)}, device_id_type=MESH)

    def wcopy(src, col, slot, rows):
        dst = wbuf.at[slot] if rows == DM else wbuf.at[slot, pl.ds(0, rows)]
        return pltpu.make_async_copy(src.at[:, pl.ds(col, TN)], dst, w_sem.at[slot])

    def wcol(j):
        return mo(j * TN, TN)

    def issue_a(j, slot):
        @pl.when(j == 0)
        def _():
            wcopy(wka, 0, slot, DM).start()

        @pl.when(j == 1)
        def _():
            wcopy(wva, 0, slot, DM).start()

        @pl.when(j >= 2)
        def _():
            wcopy(wqa, wcol(j - 2), slot, DM).start()

    def issue_b(j, slot):
        for n, w in enumerate((wkl, wvl, wql, wgl)):

            @pl.when(j // 8 == n)
            def _(n=n, w=w):
                wcopy(w, wcol(j - 8 * n), slot, DM).start()

    def wait_w(slot, rows=DM):
        wcopy(wqa if rows == DM else woa, 0, slot, rows).wait()

    def own_row(i):
        return mo((tp * 8 + 2 * i) * TOK, TOK)

    def oth_row(i):
        return mo((mate * 8 + 2 * i) * TOK, TOK)

    def x_copies(top, bot):
        return (
            pltpu.make_async_copy(top, x.at[pl.ds(0, OWN)], x_sem.at[0]),
            pltpu.make_async_copy(bot, x.at[pl.ds(OWN, OWN)], x_sem.at[1]),
        )

    def x_from_hid(i):
        return x_copies(hid.at[pl.ds(own_row(i), OWN)], hid.at[pl.ds(oth_row(i), OWN)])

    def x_from_h1(i):
        return x_copies(h1own.at[i], h1oth.at[i])

    def start_x_a(i):
        for c in x_from_hid(i):
            c.start()

    def start_x_b(i):
        ag_wait_recv(LA, i)
        for c in x_from_h1(i):
            c.start()

    def rs_copy(n, i, col, width):
        return pltpu.make_async_remote_copy(
            src_ref=pt.at[n, i, pl.ds(OWN, OWN), pl.ds(col, width)],
            dst_ref=prec.at[n, i, :, pl.ds(col, width)],
            send_sem=rs_send.at[n, i],
            recv_sem=rs_recv.at[n, i],
            device_id={"tp": mate},
            device_id_type=MESH,
        )

    def ag_copy(n, i, row, rows):
        if n == 0:
            src = h1own.at[i, pl.ds(row, rows)]
            dst = h1oth.at[i, pl.ds(row, rows)]
        else:
            src = out.at[pl.ds(mo(own_row(i) + row, RB), rows)]
            dst = src
        return pltpu.make_async_remote_copy(
            src_ref=src,
            dst_ref=dst,
            send_sem=ag_send.at[n, i],
            recv_sem=ag_recv.at[n, i],
            device_id={"tp": mate},
            device_id_type=MESH,
        )

    def ag_wait_recv(n, i):
        if n == 0:
            ag_copy(0, i, 0, OWN).wait_recv()
        else:
            oth = out.at[pl.ds(oth_row(i), OWN)]
            pltpu.make_async_remote_copy(
                src_ref=oth,
                dst_ref=oth,
                send_sem=ag_send.at[n, i],
                recv_sem=ag_recv.at[n, i],
                device_id={"tp": mate},
                device_id_type=MESH,
            ).wait_recv()

    def kv_copy(i, src, own, dst_cp, send):
        return pltpu.make_async_remote_copy(
            src_ref=kvh.at[i] if own else kvr.at[i, src],
            dst_ref=kvr.at[i, src],
            send_sem=kv_send.at[i, send],
            recv_sem=kv_recv.at[i, src],
            device_id={"cp": dst_cp},
            device_id_type=MESH,
        )

    def st_copy(i, g):
        return pltpu.make_async_remote_copy(
            src_ref=sth.at[i, g],
            dst_ref=str_.at[i, g],
            send_sem=st_send.at[i, g],
            recv_sem=st_recv.at[i, g],
            device_id={"cp": lax.rem(cp + 1, 4)},
            device_id_type=MESH,
        )

    def ss_copy(i):
        return pltpu.make_async_remote_copy(
            src_ref=ssx.at[i],
            dst_ref=ssr.at[i],
            send_sem=ss_send.at[i],
            recv_sem=ss_recv.at[i],
            device_id={"tp": mate},
            device_id_type=MESH,
        )

    def norm_loads(n, i, r, start):
        slot = parity(r)
        rows = pl.ds(mo(r * RB, RB), RB)
        copies = [
            pltpu.make_async_copy(pt.at[n, i, rows], nb_p.at[slot], nl_sem.at[slot, 0]),
            pltpu.make_async_copy(prec.at[n, i, rows], nb_r.at[slot], nl_sem.at[slot, 1]),
        ]
        res_a = hid.at[pl.ds(mo(own_row(i) + r * RB, RB), RB)]
        res_b = h1own.at[i, rows]
        for layer, res in ((LA, res_a), (LB, res_b)):

            @pl.when(n == layer)
            def _(res=res):
                c = pltpu.make_async_copy(res, nb_h.at[slot], nl_sem.at[slot, 2])
                c.start() if start else c.wait()

        for c in copies:
            c.start() if start else c.wait()

    def norm_begin(n, i):
        with jax.named_scope("norm_wait"):
            rs_copy(n, i, 0, DM).wait_recv()

            @pl.when(n == LB)
            def _():
                ss_copy(i).wait_recv()
                for b in range(2):
                    whole = ssx[i, b : b + 1, :] + ssr[i, b + 2 : b + 3, :]
                    inv = lax.rsqrt(whole / float(2 * W) + EPS)
                    rsb[blk(b), :] = jnp.broadcast_to(inv, (TOK, TOK)).T

            @pl.when(n == LA)
            def _():
                rsb[...] = jnp.ones_like(rsb)

            norm_loads(n, i, 0, True)

    def norm_ready(n, i, r):
        @pl.when(r + 1 < N_RB)
        def _():
            norm_loads(n, i, r + 1, True)

        norm_loads(n, i, r, False)

    def norm_rows(n, r):
        slot = parity(r)
        alpha = alphas[n]
        for q in range(RB // 16):
            rows = slice(q * 16, (q + 1) * 16)
            both = nb_p[slot, rows, :].astype(F32) + nb_r[slot, rows, :].astype(F32)
            both = both * rsb[pl.ds(mo(r * RB + q * 16, 16), 16), 0:1]
            h = alpha * nb_h[slot, rows, :].astype(F32) + both
            inv = lax.rsqrt(jnp.mean(h * h, axis=-1, keepdims=True) + EPS)
            nout[slot, rows, :] = (h * inv * gains[pl.ds(n, 1), :]).astype(BF)

    def norm_store(n, i, r, start):
        slot = parity(r)
        dst_a = h1own.at[i, pl.ds(mo(r * RB, RB), RB)]
        dst_b = out.at[pl.ds(mo(own_row(i) + r * RB, RB), RB)]
        for layer, dst in ((LA, dst_a), (LB, dst_b)):

            @pl.when(n == layer)
            def _(layer=layer, dst=dst):
                c = pltpu.make_async_copy(nout.at[slot], dst, no_sem.at[slot])
                if start:
                    c.start()
                else:
                    c.wait()
                    ag_copy(layer, i, mo(r * RB, RB), RB).start()

    def norm_out(n, i, r):
        @pl.when(r >= 1)
        def _():
            norm_store(n, i, r - 1, False)

        norm_store(n, i, r, True)

    def norm_end(n, i):
        norm_store(n, i, N_RB - 1, False)

    def norm(n, i):
        norm_begin(n, i)
        with jax.named_scope("norm"):

            @pl.loop(0, N_RB)
            def _(r):
                norm_ready(n, i, r)
                norm_rows(n, r)
                norm_out(n, i, r)

            norm_end(n, i)

    def out_proj(n, i, wo, then, pre):
        def put(j, slot):
            return pltpu.make_async_copy(ost.at[slot], pt.at[n, i, :, pl.ds(wcol(j), TN)], o_sem.at[slot])

        with jax.named_scope("out_proj"):
            @pl.loop(0, 12)
            def _(j):
                slot = parity(j)
                wait_w(slot, W)

                @pl.when(j + 1 < 12)
                def _():
                    wcopy(wo, wcol(j + 1), 1 - slot, W).start()

                @pl.when(j == 11)
                def _():
                    then()

                @pl.when(j == 8)
                def _():
                    pre()

                ost[slot] = dot(u[...], wbuf[slot, 0:W, :]).astype(BF)

                @pl.when(j >= 1)
                def _():
                    put(j - 1, 1 - slot).wait()
                    rs_copy(n, i, wcol(j - 1), TN).start()

                put(j, slot).start()

            put(11, 1).wait()
            rs_copy(n, i, 11 * TN, TN).start()

    def layer_a(i, mid, then, pre):
        with jax.named_scope("x_a"):
            for c in x_from_hid(i):
                c.wait()
        kv_out = pltpu.make_async_copy(kvq.at[K, :, pl.ds(OWN_KV, KVW)], kvh.at[i], kvo_sem)

        def finish(j, slot):
            kind = jnp.where(j == 1, 1, 0)
            dst = jnp.where(j < 2, 0, 2)
            col = mo(jnp.where(j < 2, OWN_KV + j * TN, (j - 2) * TN), TN)
            for b in range(N_SEQ):
                for h in range(N_SEQ):
                    a = acc[slot, blk(b), h * HD : (h + 1) * HD]
                    a = (
                        a * rope[kind, 0]
                        + pltpu.roll(a, HD - 32, 1) * rope[kind, 1]
                        + pltpu.roll(a, 32, 1) * rope[kind, 2]
                    )
                    kvq[dst, blk(b), pl.ds(col + h * HD, HD)] = a.astype(BF)

        with jax.named_scope("qkv_a"):
            @pl.loop(0, 10)
            def _(j):
                slot = parity(j)
                wait_w(slot)

                @pl.when(j + 1 < 10)
                def _():
                    issue_a(j + 1, 1 - slot)

                @pl.when(j == 9)
                def _():
                    wcopy(woa, 0, 0, W).start()

                finish(jnp.maximum(j - 1, 0), 1 - slot)
                acc[slot] = dot(x[...], wbuf[slot])
                mid(j)

                @pl.when(j == 2)
                def _():
                    kv_out.start()

                @pl.when(j == 3)
                def _():
                    kv_out.wait()

                    @pl.when(is0)
                    def _():
                        kv_copy(i, 0, True, 2, 0).start()
                        kv_copy(i, 0, True, 1, 1).start()

                    @pl.when(is1)
                    def _():
                        kv_copy(i, 1, True, 3, 0).start()

                    @pl.when(is2)
                    def _():
                        kv_copy(i, 2, True, 3, 0).start()

        finish(9, 1)

        with jax.named_scope("kv_wait"):
            @pl.when(is2)
            def _():
                kv_copy(i, 0, False, 3, 1).wait_recv()
                kv_copy(i, 0, False, 3, 1).start()

            @pl.when(is3)
            def _():
                kv_copy(i, 1, False, 2, 0).wait_recv()
                kv_copy(i, 1, False, 2, 0).start()
                kv_copy(i, 2, False, 2, 0).wait_recv()
                kv_copy(i, 0, False, 2, 0).wait_recv()

            @pl.when(is2)
            def _():
                kv_copy(i, 1, False, 3, 1).wait_recv()

            @pl.when(is1)
            def _():
                kv_copy(i, 0, False, 3, 1).wait_recv()

            def kv_load(s):
                return pltpu.make_async_copy(kvr.at[i, s], kvq.at[K, :, pl.ds(s * KVW, KVW)], kvl_sem.at[s])

            for s in range(3):

                @pl.when(cp > s)
                def _(s=s):
                    kv_load(s).start()

            for s in range(3):

                @pl.when(cp > s)
                def _(s=s):
                    kv_load(s).wait()

        with jax.named_scope("attn"):
            scale = math.log2(math.e) / math.sqrt(HD)
            for c in range(N_SEQ):

                @pl.when(cp == c)
                def _(c=c):
                    cols = [OWN_KV] + [s * KVW for s in range(c)]

                    @pl.loop(0, 16)
                    def _(t):
                        b = t // 4
                        g = lax.rem(t, 4)
                        rows = blk(b)
                        ks = [kvq[K, rows, pl.ds(mo(o + g * HD, HD), HD)] for o in cols]
                        vs = [kvq[K, rows, pl.ds(mo(o + TN + g * HD, HD), HD)] for o in cols]
                        keys = jnp.concatenate(ks, axis=0) if c else ks[0]
                        vals = jnp.concatenate(vs, axis=0) if c else vs[0]
                        row = lax.rem(lax.broadcasted_iota(jnp.int32, (2 * TOK, TOK), 0), TOK)
                        causal = lax.broadcasted_iota(jnp.int32, (2 * TOK, TOK), 1) <= row

                        def heads(p):
                            return [pl.ds(mo((g * 8 + 2 * p + z) * HD, HD), HD) for z in range(2)]

                        scores = []
                        for p in range(N_SEQ):
                            qs = jnp.concatenate([kvq[Q, rows, o] for o in heads(p)], axis=0)
                            scores.append(dot(qs, keys, NT_DIMS))
                        for p in range(N_SEQ):
                            s = scores[p]
                            own = jnp.where(causal, s[:, :TOK], -jnp.inf)
                            s = jnp.concatenate([own, s[:, TOK:]], axis=1) if c else own
                            m = jnp.max(s, axis=1, keepdims=True)
                            e = jnp.exp2((s - m) * scale)
                            o = dot(e.astype(BF), vals) * (1.0 / jnp.sum(e, axis=1, keepdims=True))
                            for z in range(2):
                                u[rows, heads(p)[z]] = o[z * TOK : (z + 1) * TOK].astype(BF)

        out_proj(0, i, woa, then, pre)

    def key_decay(h):
        back = lax.broadcasted_iota(jnp.int32, (TOK, HD), 0).astype(F32) - (TOK - 1.0)
        return jnp.exp(slopes[h] * back)

    def state_of(g, b, hh, kd):
        rows = blk(b)
        col = hcol(g, hh)
        k = (kvq[K, rows, col].astype(F32) * kd).astype(BF)
        return dot(k, kvq[V, rows, col], TN_DIMS)

    def block_decay(h):
        return jnp.exp(jnp.full((8, HD), -float(TOK), F32) * slopes[h])[0:1, :]

    def st_store(i, g, slot):
        return pltpu.make_async_copy(stg.at[slot], sth.at[i, g], sto_sem.at[slot])

    def st_load(i, g, slot):
        return pltpu.make_async_copy(str_.at[i, g], pst.at[slot], stl_sem.at[slot])

    def next_state(g):
        slot = parity(g)
        for hh in range(4):
            kd = key_decay(4 * g + hh)
            bd = block_decay(4 * g + hh)
            for b in range(N_SEQ):
                stg[slot, b * 4 + hh] = state_of(g, b, hh, kd) + bd * pst[slot, b * 4 + hh]

    def local_state(i, g):
        slot = parity(g)

        @pl.when(is1)
        def _():
            st_copy(i, g).wait_recv()
            st_load(i, g, slot).start()
            st_load(i, g, slot).wait()

        @pl.when(is0)
        def _():
            for hh in range(N_SEQ):
                kd = key_decay(4 * g + hh)
                for b in range(N_SEQ):
                    stg[slot, b * 4 + hh] = state_of(g, b, hh, kd)

        @pl.when(is1)
        def _():
            for hh in range(N_SEQ):
                kd = key_decay(4 * g + hh)
                bd = block_decay(4 * g + hh)
                for b in range(N_SEQ):
                    stg[slot, b * 4 + hh] = state_of(g, b, hh, kd) + bd * pst[slot, b * 4 + hh]

        st_store(i, g, slot).start()

    def st_send_on(i, g):
        st_store(i, g, parity(g)).wait()
        st_copy(i, g).start()

    def layer_b(i, mid, then, pre):
        with jax.named_scope("x_b"):
            for c in x_from_h1(i):
                c.wait()

        def finish(j, a):
            kvq[j // 8, :, pl.ds(wcol(lax.rem(j, 8)), TN)] = (a * sigmoid(a)).astype(BF)

        with jax.named_scope("qkv_b"):
            @pl.loop(0, 24)
            def _(j):
                slot = parity(j)
                wait_w(slot)
                issue_b(j + 1, 1 - slot)
                finish(j, dot(x[...], wbuf[slot]))

                @pl.when((cp <= 1) & (j >= 9) & (j < 17))
                def _():
                    local_state(i, j - 9)

                    @pl.when(j >= 10)
                    def _():
                        st_send_on(i, j - 10)

                @pl.when((cp <= 1) & (j == 17))
                def _():
                    st_send_on(i, 7)

                mid(j)

        with jax.named_scope("gate"):

            @pl.loop(0, 8)
            def _(j):
                slot = parity(j)
                wait_w(slot)

                @pl.when(j + 1 < 8)
                def _():
                    issue_b(25 + j, 1 - slot)

                @pl.when(j == 7)
                def _():
                    wcopy(wol, 0, 0, W).start()

                @pl.when(is2)
                def _():
                    st_copy(i, j).wait_recv()
                    st_load(i, j, slot).start()

                gbuf[:, pl.ds(wcol(j), TN)] = sigmoid(dot(x[...], wbuf[slot]))

                @pl.when(is2)
                def _():
                    st_load(i, j, slot).wait()
                    next_state(j)
                    st_store(i, j, slot).start()

                    @pl.when(j >= 1)
                    def _():
                        st_send_on(i, j - 1)

        with jax.named_scope("lin"):

            @pl.when(is2)
            def _():
                st_send_on(i, N_G - 1)

            ss[...] = jnp.zeros_like(ss)

            def fetch(g):
                @pl.when(is3)
                def _():
                    st_copy(i, g).wait_recv()

                @pl.when(cp >= 1)
                def _():
                    st_load(i, g, parity(g)).start()

            @pl.when(is0)
            def _():
                pst[...] = jnp.zeros_like(pst)

            fetch(0)

            @pl.loop(0, N_G)
            def _(g):
                slot = parity(g)

                @pl.when(g + 1 < N_G)
                def _():
                    fetch(g + 1)

                for hh in range(4):
                    lam = slopes[4 * g + hh]
                    row = lax.broadcasted_iota(jnp.int32, (TOK, HD), 0).astype(F32)
                    lane = lax.broadcasted_iota(jnp.int32, (TOK, HD), 1).astype(F32)
                    gap = row - lane
                    wtab[hh, 0] = jnp.where(gap >= 0, jnp.exp(-lam * jnp.maximum(gap, 0.0)), 0.0)
                    wtab[hh, 1] = jnp.exp(-lam * (row + 1.0))

                @pl.when(cp >= 1)
                def _():
                    st_load(i, g, slot).wait()

                @pl.loop(0, 2)
                def _(half):
                    pairs = [(half * 2 + z, hh) for z in range(2) for hh in range(4)]
                    at = [(blk(b), hcol(g, hh)) for b, hh in pairs]
                    qs = [kvq[Q, r, c] for r, c in at]
                    inner = [dot(q, kvq[K, r, c], NT_DIMS) for q, (r, c) in zip(qs, at)]
                    prior = [dot(q, pst[slot, b * 4 + hh].astype(BF)) for q, (b, hh) in zip(qs, pairs)]
                    o = [
                        dot((s * wtab[hh, 0]).astype(BF), kvq[V, r, c]) + p * wtab[hh, 1]
                        for s, p, (r, c), (b, hh) in zip(inner, prior, at, pairs)
                    ]
                    for v, (r, c) in zip(o, at):
                        u[r, c] = (v * ginner[0:1, c] * gbuf[r, c]).astype(BF)
                    for z in range(2):
                        ss[at[4 * z][0], :] += sum(v * v for v in o[4 * z : 4 * z + 4])

            sums = [jnp.sum(ss[blk(b), :].T, axis=0, keepdims=True) for b in range(N_SEQ)]
            ssx[i] = jnp.concatenate(sums + sums, axis=0)

        def then_ss():
            ss_copy(i).start()
            pre()

        out_proj(1, i, wol, then, then_ss)

    issue_a(0, 0)
    start_x_a(0)
    rope_in = pltpu.make_async_copy(rope_hbm.at[cp], rope.at[0], kvo_sem)
    rope_in.start()
    rope[1, 0] = jnp.ones((TOK, HD), F32)
    rope[1, 1] = jnp.zeros((TOK, HD), F32)
    rope[1, 2] = jnp.zeros((TOK, HD), F32)
    rope_in.wait()
    pl.semaphore_wait(bar, 4)

    @pl.loop(0, 7)
    def _(s):
        @pl.when((s < 3) | (s == 4))
        def _():
            def mid_a(j):
                @pl.when((s == 1) & (j == 6))
                def _():
                    norm(LA, 0)

            def then_a():
                @pl.when(s < 2)
                def _():
                    issue_a(0, 0)

                @pl.when(s >= 2)
                def _():
                    issue_b(0, 0)

            def pre_a():
                @pl.when(s < 2)
                def _():
                    start_x_a(s + 1)

                @pl.when(s >= 2)
                def _():
                    start_x_b(jnp.where(s == 2, 0, 1))

            layer_a(jnp.where(s < 3, s, 3), mid_a, then_a, pre_a)

        @pl.when(s == 2)
        def _():
            norm(LA, 1)

        @pl.when(s >= 3)
        def _():
            def mid_b(j):
                now = jnp.where(s == 4, 0, jnp.where(s == 6, 19, 15))

                @pl.when(j == now)
                def _():
                    norm(jnp.where(s == 3, LA, LB), jnp.where(s == 3, 2, s - 4))

            def then_b():
                @pl.when(s == 3)
                def _():
                    issue_a(0, 0)

                @pl.when((s > 3) & (s < 6))
                def _():
                    issue_b(0, 0)

            def pre_b():
                @pl.when(s == 3)
                def _():
                    start_x_a(3)

                @pl.when((s > 3) & (s < 6))
                def _():
                    start_x_b(s - 2)

            layer_b(s - 3, mid_b, then_b, pre_b)

        @pl.when(s == 4)
        def _():
            norm(LA, 3)

    norm(LB, 3)

    for i in range(N_SEQ):
        for n in range(2):
            rs_copy(n, i, 0, DM).wait_send()
            ag_copy(n, i, 0, OWN).wait_send()
        ag_wait_recv(1, i)
        ss_copy(i).wait_send()

        @pl.when(is0)
        def _(i=i):
            kv_copy(i, 0, True, 2, 0).wait_send()
            kv_copy(i, 0, True, 1, 1).wait_send()

        @pl.when(is1)
        def _(i=i):
            kv_copy(i, 1, True, 3, 0).wait_send()

        @pl.when(is2)
        def _(i=i):
            kv_copy(i, 2, True, 3, 0).wait_send()
            kv_copy(i, 0, False, 3, 1).wait_send()

        @pl.when(is3)
        def _(i=i):
            kv_copy(i, 1, False, 2, 0).wait_send()

        @pl.when(cp <= 2)
        def _(i=i):
            @pl.loop(0, 8)
            def _(g):
                st_copy(i, g).wait_send()


def solution(mesh):
    n_cp = mesh.shape["cp"]
    table = rope_tables(n_cp)
    any_ = pl.BlockSpec(memory_space=pl.ANY)
    smem = pl.BlockSpec(memory_space=pltpu.SMEM)
    vmem = pl.BlockSpec(memory_space=pltpu.VMEM)
    dma = pltpu.SemaphoreType.DMA
    two = (2,)

    def body(hidden, alphas, wqa, wka, wva, woa, gain_attn, wql, wkl, wvl, wgl, slopes, gain_inner, wol, gain_lin):
        shape = hidden.shape
        hid = hidden.reshape(shape[0] * shape[1], shape[2])
        gains = jnp.stack([gain_attn, gain_lin])
        sds = jax.ShapeDtypeStruct
        outs = (
            sds(hid.shape, BF),
            sds((2, N_CH, ROWS, DM), BF),
            sds((2, N_CH, OWN, DM), BF),
            sds((N_CH, OWN, DM), BF),
            sds((N_CH, OWN, DM), BF),
            sds((N_CH, ROWS, KVW), BF),
            sds((N_CH, 3, ROWS, KVW), BF),
            sds((N_CH, N_G, 16, HD, HD), F32),
            sds((N_CH, N_G, 16, HD, HD), F32),
        )
        scratch = [
            pltpu.VMEM((2, DM, TN), BF),
            pltpu.VMEM((ROWS, DM), BF),
            pltpu.VMEM((3, ROWS, W), BF),
            pltpu.VMEM((ROWS, W), F32),
            pltpu.VMEM((ROWS, W), BF),
            pltpu.VMEM((2, ROWS, TN), F32),
            pltpu.VMEM((2, ROWS, TN), BF),
            pltpu.VMEM((2, 16, HD, HD), F32),
            pltpu.VMEM((2, 16, HD, HD), F32),
            pltpu.VMEM((2, RB, DM), BF),
            pltpu.VMEM((2, RB, DM), BF),
            pltpu.VMEM((2, RB, DM), BF),
            pltpu.VMEM((2, RB, DM), BF),
            pltpu.VMEM((ROWS, HD), F32),
            pltpu.VMEM((OWN, HD), F32),
            pltpu.VMEM((2, 3, TOK, HD), F32),
            pltpu.VMEM((N_CH, 8, HD), F32),
            pltpu.VMEM((N_CH, 8, HD), F32),
            pltpu.VMEM((4, 2, TOK, HD), F32),
            dma(two), dma(two), dma(two), dma(()), dma((3,)), dma(two), dma(two), dma((2, 3)), dma(two),
            dma((2, N_CH)), dma((2, N_CH)), dma((2, N_CH)), dma((2, N_CH)), dma((N_CH, 2)), dma((N_CH, 3)), dma((N_CH, N_G)), dma((N_CH, N_G)),
            dma((N_CH,)), dma((N_CH,)),
        ]
        res = pl.pallas_call(
            kernel,
            out_shape=outs,
            in_specs=[any_] * 11 + [smem, smem, vmem, vmem],
            out_specs=tuple(any_ for _ in outs),
            scratch_shapes=scratch,
            compiler_params=pltpu.CompilerParams(
                collective_id=0, has_side_effects=True, vmem_limit_bytes=67043328
            ),
            name="layers",
        )(
            hid, wqa, wka, wva, woa, wql, wkl, wvl, wgl, wol, jnp.asarray(table), alphas, slopes, gains,
            gain_inner.reshape(1, -1),
        )
        return res[0].reshape(shape)

    act = P("dp", "cp", None)
    rep = P()
    col = P(None, "tp")
    row = P("tp", None)
    vec = P("tp")
    in_specs = (act, rep, col, col, col, row, rep, col, col, col, col, vec, vec, row, rep)
    return jax.shard_map(body, mesh=mesh, in_specs=in_specs, out_specs=act, check_vma=False)
```

```python
import math

import jax
import jax.numpy as jnp
import numpy as np
from jax import lax
from jax.experimental import pallas as pl
from jax.experimental.pallas import tpu as pltpu
from jax.sharding import PartitionSpec as P

MESH = pl.DeviceIdType.MESH
F32 = jnp.float32
BF = jnp.bfloat16
ROPE_BASE = 10000000.0
EPS = 1e-5

VMEM_BYTES = 67043328
TOK = 128
HD = 128
TN = 512
DM = 6144
W = 4096
KVW = 1024
OWN_KV = W - KVW
N_SEQ = 4
N_CH = 4
N_CP = 4
N_G = 8
ROWS = N_SEQ * TOK
OWN = ROWS // 2
RB = 32
N_RB = OWN // RB
N_BUF = 4
LA, LB = 0, 1
K, V, Q = 0, 1, 2
NT_DIMS = (((1,), (1,)), ((), ()))
TN_DIMS = (((0,), (0,)), ((), ()))


def rope_tables(n_cp):
    half = HD // 4
    inv = ROPE_BASE ** (-np.arange(half, dtype=np.float64) * 2.0 / (2 * half))
    pos = np.arange(n_cp * TOK, dtype=np.float64)
    ang = pos[:, None] * inv[None, :]
    tab = np.zeros((3, n_cp * TOK, HD), np.float32)
    tab[0] = 1.0
    tab[0, :, :half] = np.cos(ang)
    tab[0, :, half : 2 * half] = np.cos(ang)
    tab[1, :, :half] = -np.sin(ang)
    tab[2, :, half : 2 * half] = np.sin(ang)
    return np.ascontiguousarray(tab.reshape(3, n_cp, TOK, HD).transpose(1, 0, 2, 3))


def mo(v, m):
    return pl.multiple_of(v, m)


def parity(j):
    return lax.rem(j, 2)


def blk(b):
    return pl.ds(mo(b * TOK, TOK), TOK)


def hcol(g, hh):
    return pl.ds(mo((4 * g + hh) * HD, HD), HD)


def dot(a, b, dims=(((1,), (0,)), ((), ()))):
    return lax.dot_general(a, b, dims, preferred_element_type=F32)


def sigmoid(z):
    return 1.0 / (1.0 + jnp.exp(-z))


def kernel(
    hid, wqa, wka, wva, woa, wql, wkl, wvl, wgl, wol, rope_hbm, alphas, slopes, gain_a, gain_b, ginner,
    out, last, pt, prec, h1own, h1oth, kvh, kvr, sth, str_,
    wbuf, x, kvq, gbuf, u, acc, ost, stg, pst, nb_p, nb_r, nb_h, nout, ss, rsb, rope, ssx, ssr, wtab, gains,
    w_sem, x_sem, o_sem, kvo_sem, kvl_sem, sto_sem, stl_sem, nl_sem, no_sem,
    rs_send, rs_recv, ag_send, ag_recv, kv_send, kv_recv, st_send, st_recv, ss_send, ss_recv,
):
    cp = lax.axis_index("cp")
    tp = lax.axis_index("tp")
    mate = 1 - tp
    is0, is1, is2, is3 = (cp == c for c in range(N_CP))

    bar = pltpu.get_barrier_semaphore()
    pl.semaphore_signal(bar, inc=1, device_id={"tp": mate}, device_id_type=MESH)
    for d in range(1, 4):
        pl.semaphore_signal(bar, inc=1, device_id={"cp": lax.rem(cp + d, 4)}, device_id_type=MESH)

    def wcopy(src, col, slot, rows):
        dst = wbuf.at[slot] if rows == DM else wbuf.at[slot, pl.ds(0, rows)]
        return pltpu.make_async_copy(src.at[:, pl.ds(col, TN)], dst, w_sem.at[slot])

    def wcol(j):
        return mo(j * TN, TN)

    def issue_a(j, slot):
        @pl.when(j == 0)
        def _():
            wcopy(wka, 0, slot, DM).start()

        @pl.when(j == 1)
        def _():
            wcopy(wva, 0, slot, DM).start()

        @pl.when(j >= 2)
        def _():
            wcopy(wqa, wcol(j - 2), slot, DM).start()

    def issue_b(j, slot):
        kv = j < 16
        for cond, w, tile in (
            (kv & (parity(j) == 0), wkl, j // 2),
            (kv & (parity(j) == 1), wvl, j // 2),
            ((j >= 16) & (j < 24), wql, j - 16),
            (j >= 24, wgl, j - 24),
        ):

            @pl.when(cond)
            def _(w=w, tile=tile):
                wcopy(w, wcol(tile), slot, DM).start()

    def wait_w(slot, rows=DM):
        wcopy(wqa if rows == DM else woa, 0, slot, rows).wait()

    def own_row(i):
        return mo((tp * 8 + 2 * i) * TOK, TOK)

    def oth_row(i):
        return mo((mate * 8 + 2 * i) * TOK, TOK)

    def x_copies(top, bot):
        return (
            pltpu.make_async_copy(top, x.at[pl.ds(0, OWN)], x_sem.at[0]),
            pltpu.make_async_copy(bot, x.at[pl.ds(OWN, OWN)], x_sem.at[1]),
        )

    def x_from_hid(i):
        return x_copies(hid.at[pl.ds(own_row(i), OWN)], hid.at[pl.ds(oth_row(i), OWN)])

    def x_from_h1(i):
        return x_copies(h1own.at[i], h1oth.at[i])

    def start_x_a(i):
        for c in x_from_hid(i):
            c.start()

    def start_x_b(i):
        ag_wait_recv(LA, i)
        for c in x_from_h1(i):
            c.start()

    def rs_copy(n, i, col, width):
        return pltpu.make_async_remote_copy(
            src_ref=pt.at[n, i, pl.ds(OWN, OWN), pl.ds(col, width)],
            dst_ref=prec.at[n, i, :, pl.ds(col, width)],
            send_sem=rs_send.at[n, i],
            recv_sem=rs_recv.at[n, i],
            device_id={"tp": mate},
            device_id_type=MESH,
        )

    def ag_copy(n, i, row, rows):
        if n == 0:
            src = h1own.at[i, pl.ds(row, rows)]
            dst = h1oth.at[i, pl.ds(row, rows)]
        else:
            src = out.at[pl.ds(mo(own_row(i) + row, RB), rows)]
            dst = src
        return pltpu.make_async_remote_copy(
            src_ref=src,
            dst_ref=dst,
            send_sem=ag_send.at[n, i],
            recv_sem=ag_recv.at[n, i],
            device_id={"tp": mate},
            device_id_type=MESH,
        )

    def ag_wait_recv(n, i):
        if n == 0:
            ag_copy(0, i, 0, OWN).wait_recv()
        else:
            oth = out.at[pl.ds(oth_row(i), OWN)]
            pltpu.make_async_remote_copy(
                src_ref=oth,
                dst_ref=oth,
                send_sem=ag_send.at[n, i],
                recv_sem=ag_recv.at[n, i],
                device_id={"tp": mate},
                device_id_type=MESH,
            ).wait_recv()

    def kv_copy(i, src, own, dst_cp, send):
        return pltpu.make_async_remote_copy(
            src_ref=kvh.at[i] if own else kvr.at[i, src],
            dst_ref=kvr.at[i, src],
            send_sem=kv_send.at[i, send],
            recv_sem=kv_recv.at[i, src],
            device_id={"cp": dst_cp},
            device_id_type=MESH,
        )

    def st_copy(i, g):
        return pltpu.make_async_remote_copy(
            src_ref=sth.at[i, g],
            dst_ref=str_.at[i, g],
            send_sem=st_send.at[i, g],
            recv_sem=st_recv.at[i, g],
            device_id={"cp": lax.rem(cp + 1, 4)},
            device_id_type=MESH,
        )

    def ss_copy(i):
        return pltpu.make_async_remote_copy(
            src_ref=ssx.at[i],
            dst_ref=ssr.at[i],
            send_sem=ss_send.at[i],
            recv_sem=ss_recv.at[i],
            device_id={"tp": mate},
            device_id_type=MESH,
        )

    def norm_loads(n, i, r, start):
        slot = lax.rem(r, N_BUF)
        rows = pl.ds(mo(r * RB, RB), RB)
        copies = [
            pltpu.make_async_copy(pt.at[n, i, rows], nb_p.at[slot], nl_sem.at[slot, 0]),
            pltpu.make_async_copy(prec.at[n, i, rows], nb_r.at[slot], nl_sem.at[slot, 1]),
        ]
        res_a = hid.at[pl.ds(mo(own_row(i) + r * RB, RB), RB)]
        res_b = h1own.at[i, rows]
        for layer, res in ((LA, res_a), (LB, res_b)):

            @pl.when(n == layer)
            def _(res=res):
                c = pltpu.make_async_copy(res, nb_h.at[slot], nl_sem.at[slot, 2])
                c.start() if start else c.wait()

        for c in copies:
            c.start() if start else c.wait()

    def norm_begin(n, i):
        with jax.named_scope("norm_wait"):
            rs_copy(n, i, 0, DM).wait_recv()

            @pl.when(n == LB)
            def _():
                ss_copy(i).wait_recv()
                for b in range(2):
                    whole = ssx[i, b : b + 1, :] + ssr[i, b + 2 : b + 3, :]
                    inv = lax.rsqrt(whole / float(2 * W) + EPS)
                    rsb[blk(b), :] = jnp.broadcast_to(inv, (TOK, TOK)).T

            @pl.when(n == LA)
            def _():
                rsb[...] = jnp.ones_like(rsb)

            for r in range(N_BUF - 1):
                norm_loads(n, i, r, True)

    def norm_ready(n, i, r):
        @pl.when(r + N_BUF - 1 < N_RB)
        def _():
            norm_loads(n, i, r + N_BUF - 1, True)

        norm_loads(n, i, r, False)

    def norm_rows(n, r):
        slot = lax.rem(r, N_BUF)
        alpha = alphas[n]
        for q in range(RB // 16):
            rows = slice(q * 16, (q + 1) * 16)
            both = nb_p[slot, rows, :].astype(F32) + nb_r[slot, rows, :].astype(F32)
            both = both * rsb[pl.ds(mo(r * RB + q * 16, 16), 16), 0:1]
            h = alpha * nb_h[slot, rows, :].astype(F32) + both
            inv = lax.rsqrt(jnp.mean(h * h, axis=-1, keepdims=True) + EPS)
            nout[slot, rows, :] = (h * inv * gains[pl.ds(n, 1), :]).astype(BF)

    def norm_store(n, i, r, start, end):
        slot = lax.rem(r, N_BUF)
        if end:
            c = pltpu.make_async_copy(nout.at[slot], last.at[pl.ds(mo(r * RB, RB), RB)], no_sem.at[slot])
            c.start() if start else c.wait()
            return
        dst_a = h1own.at[i, pl.ds(mo(r * RB, RB), RB)]
        dst_b = out.at[pl.ds(mo(own_row(i) + r * RB, RB), RB)]
        for layer, dst in ((LA, dst_a), (LB, dst_b)):

            @pl.when(n == layer)
            def _(layer=layer, dst=dst):
                c = pltpu.make_async_copy(nout.at[slot], dst, no_sem.at[slot])
                if start:
                    c.start()
                else:
                    c.wait()
                    ag_copy(layer, i, mo(r * RB, RB), RB).start()

    def norm_out(n, i, r, end):
        @pl.when(r >= 2)
        def _():
            norm_store(n, i, r - 2, False, end)

        norm_store(n, i, r, True, end)

    def norm_end(n, i, end):
        for r in range(N_RB - 2, N_RB):
            norm_store(n, i, r, False, end)

    def norm(n, i, end=False):
        norm_begin(n, i)
        with jax.named_scope("norm"):

            @pl.loop(0, N_RB)
            def _(r):
                norm_ready(n, i, r)
                norm_rows(n, r)
                norm_out(n, i, r, end)

            norm_end(n, i, end)

    def out_proj(n, i, wo, then, pre):
        def put(j, slot):
            return pltpu.make_async_copy(ost.at[slot], pt.at[n, i, :, pl.ds(wcol(j), TN)], o_sem.at[slot])

        with jax.named_scope("out_proj"):
            @pl.loop(0, 12)
            def _(j):
                slot = parity(j)
                wait_w(slot, W)

                @pl.when(j + 1 < 12)
                def _():
                    wcopy(wo, wcol(j + 1), 1 - slot, W).start()

                @pl.when(j == 11)
                def _():
                    then()

                @pl.when(j == 8)
                def _():
                    pre()

                ost[slot] = dot(u[...], wbuf[slot, 0:W, :]).astype(BF)

                @pl.when(j >= 1)
                def _():
                    put(j - 1, 1 - slot).wait()
                    rs_copy(n, i, wcol(j - 1), TN).start()

                put(j, slot).start()

            put(11, 1).wait()
            rs_copy(n, i, 11 * TN, TN).start()

    def layer_a(i, mid, then, pre):
        with jax.named_scope("x_a"):
            for c in x_from_hid(i):
                c.wait()
        kv_out = pltpu.make_async_copy(kvq.at[K, :, pl.ds(OWN_KV, KVW)], kvh.at[i], kvo_sem)

        def finish(j, slot):
            kind = jnp.where(j == 1, 1, 0)
            dst = jnp.where(j < 2, 0, 2)
            col = mo(jnp.where(j < 2, OWN_KV + j * TN, (j - 2) * TN), TN)
            for b in range(N_SEQ):
                for h in range(N_SEQ):
                    a = acc[slot, blk(b), h * HD : (h + 1) * HD]
                    a = (
                        a * rope[kind, 0]
                        + pltpu.roll(a, HD - 32, 1) * rope[kind, 1]
                        + pltpu.roll(a, 32, 1) * rope[kind, 2]
                    )
                    kvq[dst, blk(b), pl.ds(col + h * HD, HD)] = a.astype(BF)

        with jax.named_scope("qkv_a"):
            @pl.loop(0, 10)
            def _(j):
                slot = parity(j)
                wait_w(slot)

                @pl.when(j + 1 < 10)
                def _():
                    issue_a(j + 1, 1 - slot)

                @pl.when(j == 9)
                def _():
                    wcopy(woa, 0, 0, W).start()

                @pl.when(j == 3)
                def _():
                    kv_out.wait()

                    @pl.when(is0)
                    def _():
                        kv_copy(i, 0, True, 2, 0).start()
                        kv_copy(i, 0, True, 1, 1).start()

                    @pl.when(is1)
                    def _():
                        kv_copy(i, 1, True, 3, 0).start()

                    @pl.when(is2)
                    def _():
                        kv_copy(i, 2, True, 3, 0).start()

                finish(jnp.maximum(j - 1, 0), 1 - slot)
                acc[slot] = dot(x[...], wbuf[slot])
                mid(j)

                @pl.when(j == 2)
                def _():
                    kv_out.start()

        finish(9, 1)

        with jax.named_scope("kv_wait"):
            @pl.when(is2)
            def _():
                kv_copy(i, 0, False, 3, 1).wait_recv()
                kv_copy(i, 0, False, 3, 1).start()

            @pl.when(is3)
            def _():
                kv_copy(i, 1, False, 2, 0).wait_recv()
                kv_copy(i, 1, False, 2, 0).start()
                kv_copy(i, 2, False, 2, 0).wait_recv()
                kv_copy(i, 0, False, 2, 0).wait_recv()

            @pl.when(is2)
            def _():
                kv_copy(i, 1, False, 3, 1).wait_recv()

            @pl.when(is1)
            def _():
                kv_copy(i, 0, False, 3, 1).wait_recv()

            def kv_load(s):
                return pltpu.make_async_copy(kvr.at[i, s], kvq.at[K, :, pl.ds(s * KVW, KVW)], kvl_sem.at[s])

            for s in range(3):

                @pl.when(cp > s)
                def _(s=s):
                    kv_load(s).start()

            for s in range(3):

                @pl.when(cp > s)
                def _(s=s):
                    kv_load(s).wait()

        with jax.named_scope("attn"):
            scale = math.log2(math.e) / math.sqrt(HD)
            for c in range(N_SEQ):

                @pl.when(cp == c)
                def _(c=c):
                    cols = [OWN_KV] + [s * KVW for s in range(c)]

                    @pl.loop(0, 16)
                    def _(t):
                        b = t // 4
                        g = lax.rem(t, 4)
                        rows = blk(b)
                        ks = [kvq[K, rows, pl.ds(mo(o + g * HD, HD), HD)] for o in cols]
                        vs = [kvq[K, rows, pl.ds(mo(o + TN + g * HD, HD), HD)] for o in cols]
                        keys = jnp.concatenate(ks, axis=0) if c else ks[0]
                        vals = jnp.concatenate(vs, axis=0) if c else vs[0]
                        row = lax.rem(lax.broadcasted_iota(jnp.int32, (2 * TOK, TOK), 0), TOK)
                        causal = lax.broadcasted_iota(jnp.int32, (2 * TOK, TOK), 1) <= row

                        def heads(p):
                            return [pl.ds(mo((g * 8 + 2 * p + z) * HD, HD), HD) for z in range(2)]

                        scores = []
                        for p in range(N_SEQ):
                            qs = jnp.concatenate([kvq[Q, rows, o] for o in heads(p)], axis=0)
                            scores.append(dot(qs, keys, NT_DIMS))
                        for p in range(N_SEQ):
                            s = scores[p]
                            own = jnp.where(causal, s[:, :TOK], -jnp.inf)
                            s = jnp.concatenate([own, s[:, TOK:]], axis=1) if c else own
                            m = jnp.max(s, axis=1, keepdims=True)
                            e = jnp.exp2((s - m) * scale)
                            o = dot(e.astype(BF), vals) * (1.0 / jnp.sum(e, axis=1, keepdims=True))
                            for z in range(2):
                                u[rows, heads(p)[z]] = o[z * TOK : (z + 1) * TOK].astype(BF)

        out_proj(0, i, woa, then, pre)

    def key_decay(h):
        back = lax.broadcasted_iota(jnp.int32, (TOK, HD), 0).astype(F32) - (TOK - 1.0)
        return jnp.exp(slopes[h] * back)

    def state_of(g, b, hh, kd):
        rows = blk(b)
        col = hcol(g, hh)
        k = (kvq[K, rows, col].astype(F32) * kd).astype(BF)
        return dot(k, kvq[V, rows, col], TN_DIMS)

    def block_decay(h):
        return jnp.exp(jnp.full((8, HD), -float(TOK), F32) * slopes[h])[0:1, :]

    def st_store(i, g, slot):
        return pltpu.make_async_copy(stg.at[slot], sth.at[i, g], sto_sem.at[slot])

    def st_load(i, g, slot):
        return pltpu.make_async_copy(str_.at[i, g], pst.at[slot], stl_sem.at[slot])

    def next_state(g):
        slot = parity(g)
        for hh in range(4):
            kd = key_decay(4 * g + hh)
            bd = block_decay(4 * g + hh)
            for b in range(N_SEQ):
                stg[slot, b * 4 + hh] = state_of(g, b, hh, kd) + bd * pst[slot, b * 4 + hh]

    def local_state(i, g):
        slot = parity(g)

        @pl.when(is1)
        def _():
            st_load(i, g, slot).wait()

        @pl.when(is0)
        def _():
            for hh in range(N_SEQ):
                kd = key_decay(4 * g + hh)
                for b in range(N_SEQ):
                    stg[slot, b * 4 + hh] = state_of(g, b, hh, kd)

        @pl.when(is1)
        def _():
            for hh in range(N_SEQ):
                kd = key_decay(4 * g + hh)
                bd = block_decay(4 * g + hh)
                for b in range(N_SEQ):
                    stg[slot, b * 4 + hh] = state_of(g, b, hh, kd) + bd * pst[slot, b * 4 + hh]

        st_store(i, g, slot).start()

    def st_send_on(i, g):
        st_store(i, g, parity(g)).wait()
        st_copy(i, g).start()

    def layer_b(i, mid, then, pre):
        with jax.named_scope("x_b"):
            for c in x_from_h1(i):
                c.wait()

        def finish(j, a):
            kv = j < 16
            dst = jnp.where(kv, parity(j), Q)
            kvq[dst, :, pl.ds(wcol(jnp.where(kv, j // 2, j - 16)), TN)] = (a * sigmoid(a)).astype(BF)

        with jax.named_scope("qkv_b"):
            @pl.loop(0, 24)
            def _(j):
                slot = parity(j)
                wait_w(slot)
                issue_b(j + 1, 1 - slot)
                e = j - jnp.where(is0, 0, 2)
                busy = (cp <= 1) & (e >= 1) & (e <= 16)
                g = e // 2

                @pl.when(busy & (parity(e) == 0))
                def _():
                    st_send_on(i, g - 1)

                @pl.when(busy & (parity(e) == 1) & is1)
                def _():
                    st_copy(i, g).wait_recv()
                    st_load(i, g, parity(g)).start()

                finish(j, dot(x[...], wbuf[slot]))

                @pl.when(busy & (parity(e) == 1))
                def _():
                    local_state(i, g)

                mid(j)

        with jax.named_scope("gate"):

            @pl.loop(0, 8)
            def _(j):
                slot = parity(j)
                wait_w(slot)

                @pl.when(j + 1 < 8)
                def _():
                    issue_b(25 + j, 1 - slot)

                @pl.when(j == 7)
                def _():
                    wcopy(wol, 0, 0, W).start()

                @pl.when(is2)
                def _():
                    st_copy(i, j).wait_recv()
                    st_load(i, j, slot).start()

                gbuf[:, pl.ds(wcol(j), TN)] = sigmoid(dot(x[...], wbuf[slot]))

                @pl.when(is2)
                def _():
                    st_load(i, j, slot).wait()
                    next_state(j)
                    st_store(i, j, slot).start()

                    @pl.when(j >= 1)
                    def _():
                        st_send_on(i, j - 1)

        with jax.named_scope("lin"):

            @pl.when(is2)
            def _():
                st_send_on(i, N_G - 1)

            ss[...] = jnp.zeros_like(ss)

            def fetch(g):
                @pl.when(is3)
                def _():
                    st_copy(i, g).wait_recv()

                @pl.when(cp >= 1)
                def _():
                    st_load(i, g, parity(g)).start()

            @pl.when(is0)
            def _():
                pst[...] = jnp.zeros_like(pst)

            fetch(0)

            @pl.loop(0, N_G)
            def _(g):
                slot = parity(g)

                @pl.when(g + 1 < N_G)
                def _():
                    fetch(g + 1)

                for hh in range(4):
                    lam = slopes[4 * g + hh]
                    row = lax.broadcasted_iota(jnp.int32, (TOK, HD), 0).astype(F32)
                    lane = lax.broadcasted_iota(jnp.int32, (TOK, HD), 1).astype(F32)
                    gap = row - lane
                    wtab[hh, 0] = jnp.where(gap >= 0, jnp.exp(-lam * jnp.maximum(gap, 0.0)), 0.0)
                    wtab[hh, 1] = jnp.exp(-lam * (row + 1.0))

                @pl.when(cp >= 1)
                def _():
                    st_load(i, g, slot).wait()

                @pl.loop(0, 2)
                def _(half):
                    pairs = [(half * 2 + z, hh) for z in range(2) for hh in range(4)]
                    at = [(blk(b), hcol(g, hh)) for b, hh in pairs]
                    qs = [kvq[Q, r, c] for r, c in at]
                    inner = [dot(q, kvq[K, r, c], NT_DIMS) for q, (r, c) in zip(qs, at)]
                    prior = [dot(q, pst[slot, b * 4 + hh].astype(BF)) for q, (b, hh) in zip(qs, pairs)]
                    o = [
                        dot((s * wtab[hh, 0]).astype(BF), kvq[V, r, c]) + p * wtab[hh, 1]
                        for s, p, (r, c), (b, hh) in zip(inner, prior, at, pairs)
                    ]
                    for v, (r, c) in zip(o, at):
                        u[r, c] = (v * ginner[0:1, c] * gbuf[r, c]).astype(BF)
                    for z in range(2):
                        ss[at[4 * z][0], :] += sum(v * v for v in o[4 * z : 4 * z + 4])

            sums = [jnp.sum(ss[blk(b), :].T, axis=0, keepdims=True) for b in range(N_SEQ)]
            ssx[i] = jnp.concatenate(sums + sums, axis=0)

        def then_ss():
            ss_copy(i).start()
            pre()

        out_proj(1, i, wol, then, then_ss)

    wcopy(wka, 0, 0, DM).start()
    start_x_a(0)
    rope_in = pltpu.make_async_copy(rope_hbm.at[cp], rope.at[0], kvo_sem)
    rope_in.start()
    gains[0:1, :] = gain_a[...]
    gains[1:2, :] = gain_b[...]
    rope[1, 0] = jnp.ones((TOK, HD), F32)
    rope[1, 1] = jnp.zeros((TOK, HD), F32)
    rope[1, 2] = jnp.zeros((TOK, HD), F32)
    rope_in.wait()
    pl.semaphore_wait(bar, 4)

    @pl.loop(0, 7)
    def _(s):
        @pl.when((s < 3) | (s == 4))
        def _():
            def mid_a(j):
                @pl.when((s == 1) & (j == 9))
                def _():
                    norm(LA, 0)

            def then_a():
                @pl.when(s < 2)
                def _():
                    wcopy(wka, 0, 0, DM).start()

                @pl.when(s >= 2)
                def _():
                    wcopy(wkl, 0, 0, DM).start()

            def pre_a():
                @pl.when(s < 2)
                def _():
                    start_x_a(s + 1)

                @pl.when(s >= 2)
                def _():
                    start_x_b(jnp.where(s == 2, 0, 1))

            layer_a(jnp.where(s < 3, s, 3), mid_a, then_a, pre_a)

        @pl.when(s == 2)
        def _():
            norm(LA, 1)

        @pl.when(s >= 3)
        def _():
            def mid_b(j):
                now = jnp.where(s == 4, 3, jnp.where(s == 6, 19, 15))

                @pl.when(j == now)
                def _():
                    norm(jnp.where(s == 3, LA, LB), jnp.where(s == 3, 2, s - 4))

            def then_b():
                @pl.when(s == 3)
                def _():
                    wcopy(wka, 0, 0, DM).start()

                @pl.when((s > 3) & (s < 6))
                def _():
                    wcopy(wkl, 0, 0, DM).start()

            def pre_b():
                @pl.when(s == 3)
                def _():
                    start_x_a(3)

                @pl.when((s > 3) & (s < 6))
                def _():
                    start_x_b(s - 2)

            layer_b(s - 3, mid_b, then_b, pre_b)

        @pl.when(s == 4)
        def _():
            norm(LA, 3)

    norm(LB, 3, end=True)

    for i in range(N_CH):
        for n in range(2):
            rs_copy(n, i, 0, DM).wait_send()
            if n == LA or i < N_CH - 1:
                ag_copy(n, i, 0, OWN).wait_send()
        if i < N_CH - 1:
            ag_wait_recv(LB, i)
        ss_copy(i).wait_send()

        @pl.when(is0)
        def _(i=i):
            kv_copy(i, 0, True, 2, 0).wait_send()
            kv_copy(i, 0, True, 1, 1).wait_send()

        @pl.when(is1)
        def _(i=i):
            kv_copy(i, 1, True, 3, 0).wait_send()

        @pl.when(is2)
        def _(i=i):
            kv_copy(i, 2, True, 3, 0).wait_send()
            kv_copy(i, 0, False, 3, 1).wait_send()

        @pl.when(is3)
        def _(i=i):
            kv_copy(i, 1, False, 2, 0).wait_send()

        @pl.when(cp <= 2)
        def _(i=i):
            @pl.loop(0, 8)
            def _(g):
                st_copy(i, g).wait_send()


def assemble(rows, last, res, buf, in_sem, out_sem):
    tp = lax.axis_index("tp")
    n = 2 * N_CH - 1

    def block(k):
        half = jnp.where(k < N_CH, tp, 1 - tp)
        return pl.ds(mo((half * N_CH + lax.rem(k, N_CH)) * OWN, OWN), OWN)

    def load(k):
        src = last if k == N_CH - 1 else rows.at[block(k)]
        return pltpu.make_async_copy(src, buf.at[k % N_CH], in_sem.at[k % N_CH])

    def store(k):
        return pltpu.make_async_copy(buf.at[k % N_CH], res.at[block(k)], out_sem.at[k % N_CH])

    for k in range(N_CH):
        load(k).start()
    for k in range(n):
        load(k).wait()
        store(k).start()
        if k >= 1 and k + N_CH - 1 < n:
            store(k - 1).wait()
            load(k + N_CH - 1).start()
    for k in range(n - N_CH, n):
        store(k).wait()


def solution(mesh):
    n_cp = mesh.shape["cp"]
    table = rope_tables(n_cp)
    any_ = pl.BlockSpec(memory_space=pl.ANY)
    smem = pl.BlockSpec(memory_space=pltpu.SMEM)
    vmem = pl.BlockSpec(memory_space=pltpu.VMEM)
    dma = pltpu.SemaphoreType.DMA
    two = (2,)

    def body(hidden, alphas, wqa, wka, wva, woa, gain_attn, wql, wkl, wvl, wgl, slopes, gain_inner, wol, gain_lin):
        shape = hidden.shape
        hid = hidden.reshape(shape[0] * shape[1], shape[2])
        sds = jax.ShapeDtypeStruct
        outs = (
            sds(hid.shape, BF),
            sds((OWN, DM), BF),
            sds((2, N_CH, ROWS, DM), BF),
            sds((2, N_CH, OWN, DM), BF),
            sds((N_CH, OWN, DM), BF),
            sds((N_CH, OWN, DM), BF),
            sds((N_CH, ROWS, KVW), BF),
            sds((N_CH, 3, ROWS, KVW), BF),
            sds((N_CH, N_G, 16, HD, HD), F32),
            sds((N_CH, N_G, 16, HD, HD), F32),
        )
        scratch = [
            pltpu.VMEM((2, DM, TN), BF),
            pltpu.VMEM((ROWS, DM), BF),
            pltpu.VMEM((3, ROWS, W), BF),
            pltpu.VMEM((ROWS, W), F32),
            pltpu.VMEM((ROWS, W), BF),
            pltpu.VMEM((2, ROWS, TN), F32),
            pltpu.VMEM((2, ROWS, TN), BF),
            pltpu.VMEM((2, 16, HD, HD), F32),
            pltpu.VMEM((2, 16, HD, HD), F32),
            pltpu.VMEM((N_BUF, RB, DM), BF),
            pltpu.VMEM((N_BUF, RB, DM), BF),
            pltpu.VMEM((N_BUF, RB, DM), BF),
            pltpu.VMEM((N_BUF, RB, DM), BF),
            pltpu.VMEM((ROWS, HD), F32),
            pltpu.VMEM((OWN, HD), F32),
            pltpu.VMEM((2, 3, TOK, HD), F32),
            pltpu.VMEM((N_CH, 8, HD), F32),
            pltpu.VMEM((N_CH, 8, HD), F32),
            pltpu.VMEM((4, 2, TOK, HD), F32),
            pltpu.VMEM((2, DM), F32),
            dma(two), dma(two), dma(two), dma(()), dma((3,)), dma(two), dma(two), dma((N_BUF, 3)), dma((N_BUF,)),
            dma((2, N_CH)), dma((2, N_CH)), dma((2, N_CH)), dma((2, N_CH)), dma((N_CH, 2)), dma((N_CH, 3)), dma((N_CH, N_G)), dma((N_CH, N_G)),
            dma((N_CH,)), dma((N_CH,)),
        ]
        res = pl.pallas_call(
            kernel,
            out_shape=outs,
            in_specs=[any_] * 11 + [smem, smem, vmem, vmem, vmem],
            out_specs=tuple(any_ for _ in outs),
            scratch_shapes=scratch,
            compiler_params=pltpu.CompilerParams(
                collective_id=0, has_side_effects=True, vmem_limit_bytes=VMEM_BYTES
            ),
            name="layers",
        )(
            hid, wqa, wka, wva, woa, wql, wkl, wvl, wgl, wol, jnp.asarray(table), alphas, slopes, gain_attn.reshape(1, -1),
            gain_lin.reshape(1, -1), gain_inner.reshape(1, -1),
        )
        got = lax.ppermute(res[1], "tp", [(0, 1), (1, 0)])
        rows = pl.pallas_call(
            assemble,
            out_shape=sds(hid.shape, BF),
            in_specs=[any_, any_],
            out_specs=any_,
            scratch_shapes=[pltpu.VMEM((N_CH, OWN, DM), BF), dma((N_CH,)), dma((N_CH,))],
            compiler_params=pltpu.CompilerParams(vmem_limit_bytes=VMEM_BYTES),
            cost_estimate=pl.CostEstimate(flops=10**11, bytes_accessed=2 * hid.size * 2, transcendentals=0),
            name="assemble",
        )(res[0], res[1])
        row = ((1 - lax.axis_index("tp")) * N_CH + N_CH - 1) * OWN
        return lax.dynamic_update_slice(rows, got, (row, 0)).reshape(shape)

    act = P("dp", "cp", None)
    rep = P()
    col = P(None, "tp")
    row = P("tp", None)
    vec = P("tp")
    in_specs = (act, rep, col, col, col, row, rep, col, col, col, col, vec, vec, row, rep)
    return jax.shard_map(body, mesh=mesh, in_specs=in_specs, out_specs=act, check_vma=False)
```

```python
import math

import jax
import jax.numpy as jnp
import numpy as np
from jax import lax
from jax.experimental import pallas as pl
from jax.experimental.pallas import tpu as pltpu
from jax.sharding import PartitionSpec as P

MESH = pl.DeviceIdType.MESH
F32 = jnp.float32
BF = jnp.bfloat16
ROPE_BASE = 10000000.0
EPS = 1e-5

VMEM_BYTES = 67043328
TOK = 128
HD = 128
TN = 512
DM = 6144
W = 4096
KVW = 1024
OWN_KV = W - KVW
N_SEQ = 4
N_CH = 4
N_CP = 4
N_G = 8
ROWS = N_SEQ * TOK
OWN = ROWS // 2
RB = 32
N_RB = OWN // RB
N_QKV = (KVW + W) // TN
N_WO = DM // TN
N_BUF = 4
LA, LB = 0, 1
K, V, Q = 0, 1, 2
NT_DIMS = (((1,), (1,)), ((), ()))
TN_DIMS = (((0,), (0,)), ((), ()))


def rope_tables(n_cp):
    half = HD // 4
    inv = ROPE_BASE ** (-np.arange(half, dtype=np.float64) * 2.0 / (2 * half))
    pos = np.arange(n_cp * TOK, dtype=np.float64)
    ang = pos[:, None] * inv[None, :]
    tab = np.zeros((3, n_cp * TOK, HD), np.float32)
    tab[0] = 1.0
    tab[0, :, :half] = np.cos(ang)
    tab[0, :, half : 2 * half] = np.cos(ang)
    tab[1, :, :half] = -np.sin(ang)
    tab[2, :, half : 2 * half] = np.sin(ang)
    return np.ascontiguousarray(tab.reshape(3, n_cp, TOK, HD).transpose(1, 0, 2, 3))


def mo(v, m):
    return pl.multiple_of(v, m)


def parity(j):
    return lax.rem(j, 2)


def blk(b):
    return pl.ds(mo(b * TOK, TOK), TOK)


def hcol(g, hh):
    return pl.ds(mo((4 * g + hh) * HD, HD), HD)


def dot(a, b, dims=(((1,), (0,)), ((), ()))):
    return lax.dot_general(a, b, dims, preferred_element_type=F32)


def sigmoid(z):
    return 1.0 / (1.0 + jnp.exp(-z))


def kernel(
    hid, wqa, wka, wva, woa, wql, wkl, wvl, wgl, wol, rope_hbm, alphas, slopes, gain_a, gain_b, ginner,
    out, last, pt, prec, h1own, h1oth, kvh, kvr, sth, str_,
    wbuf, x, kvq, gbuf, u, acc, ost, stg, pst, nb_p, nb_r, nb_h, nout, ss, rsb, rope, ssx, ssr, wtab, gains,
    w_sem, x_sem, o_sem, kvo_sem, kvl_sem, sto_sem, stl_sem, nl_sem, no_sem,
    rs_send, rs_recv, ag_send, ag_recv, kv_send, kv_recv, st_send, st_recv, ss_send, ss_recv,
):
    cp = lax.axis_index("cp")
    tp = lax.axis_index("tp")
    mate = 1 - tp
    is0, is1, is2, is3 = (cp == c for c in range(N_CP))

    bar = pltpu.get_barrier_semaphore()
    pl.semaphore_signal(bar, inc=1, device_id={"tp": mate}, device_id_type=MESH)
    for d in range(1, 4):
        pl.semaphore_signal(bar, inc=1, device_id={"cp": lax.rem(cp + d, 4)}, device_id_type=MESH)

    def wcopy(src, col, slot, rows):
        dst = wbuf.at[slot] if rows == DM else wbuf.at[slot, pl.ds(0, rows)]
        return pltpu.make_async_copy(src.at[:, pl.ds(col, TN)], dst, w_sem.at[slot])

    def wcol(j):
        return mo(j * TN, TN)

    def issue_b(j, slot):
        kv = j < 16
        for cond, w, tile in (
            (kv & (parity(j) == 0), wkl, j // 2),
            (kv & (parity(j) == 1), wvl, j // 2),
            ((j >= 16) & (j < 24), wql, j - 16),
            (j >= 24, wgl, j - 24),
        ):

            @pl.when(cond)
            def _(w=w, tile=tile):
                wcopy(w, wcol(tile), slot, DM).start()

    def wait_w(slot, rows=DM):
        wcopy(wqa if rows == DM else woa, 0, slot, rows).wait()

    def own_row(i):
        return mo((tp * 8 + 2 * i) * TOK, TOK)

    def oth_row(i):
        return mo((mate * 8 + 2 * i) * TOK, TOK)

    def x_copies(top, bot):
        return (
            pltpu.make_async_copy(top, x.at[pl.ds(0, OWN)], x_sem.at[0]),
            pltpu.make_async_copy(bot, x.at[pl.ds(OWN, OWN)], x_sem.at[1]),
        )

    def x_from_hid(i):
        return x_copies(hid.at[pl.ds(own_row(i), OWN)], hid.at[pl.ds(oth_row(i), OWN)])

    def x_from_h1(i):
        return x_copies(h1own.at[i], h1oth.at[i])

    def start_x_a(i):
        for c in x_from_hid(i):
            c.start()

    def start_x_b(i):
        ag_wait_recv(LA, i)
        for c in x_from_h1(i):
            c.start()

    def rs_copy(n, i, col, width):
        return pltpu.make_async_remote_copy(
            src_ref=pt.at[n, i, pl.ds(OWN, OWN), pl.ds(col, width)],
            dst_ref=prec.at[n, i, :, pl.ds(col, width)],
            send_sem=rs_send.at[n, i],
            recv_sem=rs_recv.at[n, i],
            device_id={"tp": mate},
            device_id_type=MESH,
        )

    def ag_copy(n, i, row, rows):
        if n == 0:
            src = h1own.at[i, pl.ds(row, rows)]
            dst = h1oth.at[i, pl.ds(row, rows)]
        else:
            src = out.at[pl.ds(mo(own_row(i) + row, RB), rows)]
            dst = src
        return pltpu.make_async_remote_copy(
            src_ref=src,
            dst_ref=dst,
            send_sem=ag_send.at[n, i],
            recv_sem=ag_recv.at[n, i],
            device_id={"tp": mate},
            device_id_type=MESH,
        )

    def ag_wait_recv(n, i):
        if n == 0:
            ag_copy(0, i, 0, OWN).wait_recv()
        else:
            oth = out.at[pl.ds(oth_row(i), OWN)]
            pltpu.make_async_remote_copy(
                src_ref=oth,
                dst_ref=oth,
                send_sem=ag_send.at[n, i],
                recv_sem=ag_recv.at[n, i],
                device_id={"tp": mate},
                device_id_type=MESH,
            ).wait_recv()

    def half_rows(h):
        return pl.ds(mo(OWN * (1 - h), OWN), OWN)

    def kv_copy(i, h, src, own, dst_cp, send):
        rows = half_rows(h)
        return pltpu.make_async_remote_copy(
            src_ref=kvh.at[i, rows] if own else kvr.at[i, src, rows],
            dst_ref=kvr.at[i, src, rows],
            send_sem=kv_send.at[i, h, send],
            recv_sem=kv_recv.at[i, h, src],
            device_id={"cp": dst_cp},
            device_id_type=MESH,
        )

    def kv_sends(i, h, go):
        @pl.when(is0)
        def _():
            go(kv_copy(i, h, 0, True, 2, 0))
            go(kv_copy(i, h, 0, True, 1, 1))

        @pl.when(is1)
        def _():
            go(kv_copy(i, h, 1, True, 3, 0))

        @pl.when(is2)
        def _():
            go(kv_copy(i, h, 2, True, 3, 0))

    def st_copy(i, g):
        return pltpu.make_async_remote_copy(
            src_ref=sth.at[i, g],
            dst_ref=str_.at[i, g],
            send_sem=st_send.at[i, g],
            recv_sem=st_recv.at[i, g],
            device_id={"cp": lax.rem(cp + 1, 4)},
            device_id_type=MESH,
        )

    def ss_copy(i):
        return pltpu.make_async_remote_copy(
            src_ref=ssx.at[i],
            dst_ref=ssr.at[i],
            send_sem=ss_send.at[i],
            recv_sem=ss_recv.at[i],
            device_id={"tp": mate},
            device_id_type=MESH,
        )

    def norm_loads(n, i, r, start):
        slot = lax.rem(r, N_BUF)
        rows = pl.ds(mo(r * RB, RB), RB)
        copies = [
            pltpu.make_async_copy(pt.at[n, i, rows], nb_p.at[slot], nl_sem.at[slot, 0]),
            pltpu.make_async_copy(prec.at[n, i, rows], nb_r.at[slot], nl_sem.at[slot, 1]),
        ]
        res_a = hid.at[pl.ds(mo(own_row(i) + r * RB, RB), RB)]
        res_b = h1own.at[i, rows]
        for layer, res in ((LA, res_a), (LB, res_b)):

            @pl.when(n == layer)
            def _(res=res):
                c = pltpu.make_async_copy(res, nb_h.at[slot], nl_sem.at[slot, 2])
                c.start() if start else c.wait()

        for c in copies:
            c.start() if start else c.wait()

    def norm_begin(n, i):
        with jax.named_scope("norm_wait"):
            rs_copy(n, i, 0, DM).wait_recv()

            @pl.when(n == LB)
            def _():
                ss_copy(i).wait_recv()
                for b in range(2):
                    whole = ssx[i, b : b + 1, :] + ssr[i, b + 2 : b + 3, :]
                    inv = lax.rsqrt(whole / float(2 * W) + EPS)
                    rsb[blk(b), :] = jnp.broadcast_to(inv, (TOK, TOK)).T

            @pl.when(n == LA)
            def _():
                rsb[...] = jnp.ones_like(rsb)

            for r in range(N_BUF - 1):
                norm_loads(n, i, r, True)

    def norm_ready(n, i, r):
        @pl.when(r + N_BUF - 1 < N_RB)
        def _():
            norm_loads(n, i, r + N_BUF - 1, True)

        norm_loads(n, i, r, False)

    def norm_rows(n, r):
        slot = lax.rem(r, N_BUF)
        alpha = alphas[n]
        for q in range(RB // 16):
            rows = slice(q * 16, (q + 1) * 16)
            both = nb_p[slot, rows, :].astype(F32) + nb_r[slot, rows, :].astype(F32)
            both = both * rsb[pl.ds(mo(r * RB + q * 16, 16), 16), 0:1]
            h = alpha * nb_h[slot, rows, :].astype(F32) + both
            inv = lax.rsqrt(jnp.mean(h * h, axis=-1, keepdims=True) + EPS)
            nout[slot, rows, :] = (h * inv * gains[pl.ds(n, 1), :]).astype(BF)

    def norm_store(n, i, r, start, end):
        slot = lax.rem(r, N_BUF)
        if end:
            c = pltpu.make_async_copy(nout.at[slot], last.at[pl.ds(mo(r * RB, RB), RB)], no_sem.at[slot])
            c.start() if start else c.wait()
            return
        dst_a = h1own.at[i, pl.ds(mo(r * RB, RB), RB)]
        dst_b = out.at[pl.ds(mo(own_row(i) + r * RB, RB), RB)]
        for layer, dst in ((LA, dst_a), (LB, dst_b)):

            @pl.when(n == layer)
            def _(layer=layer, dst=dst):
                c = pltpu.make_async_copy(nout.at[slot], dst, no_sem.at[slot])
                if start:
                    c.start()
                else:
                    c.wait()
                    ag_copy(layer, i, mo(r * RB, RB), RB).start()

    def norm_out(n, i, r, end):
        @pl.when(r >= 2)
        def _():
            norm_store(n, i, r - 2, False, end)

        norm_store(n, i, r, True, end)

    def norm_end(n, i, end):
        for r in range(N_RB - 2, N_RB):
            norm_store(n, i, r, False, end)

    def norm(n, i, end=False):
        norm_begin(n, i)
        with jax.named_scope("norm"):

            @pl.loop(0, N_RB)
            def _(r):
                norm_ready(n, i, r)
                norm_rows(n, r)
                norm_out(n, i, r, end)

            norm_end(n, i, end)

    def out_proj(n, i, wo, then, pre, rows, send):
        def put(j, slot):
            size = pl.ds(0, rows.size)
            return pltpu.make_async_copy(ost.at[slot, size], pt.at[n, i, rows, pl.ds(wcol(j), TN)], o_sem.at[slot])

        def send_on(j, slot):
            put(j, slot).wait()

            @pl.when(send)
            def _():
                rs_copy(n, i, wcol(j), TN).start()

        with jax.named_scope("out_proj"):

            @pl.loop(0, N_WO)
            def _(j):
                slot = parity(j)
                wait_w(slot, W)

                @pl.when(j + 1 < N_WO)
                def _():
                    wcopy(wo, wcol(j + 1), 1 - slot, W).start()

                @pl.when(j == N_WO - 1)
                def _():
                    then()

                @pl.when(j == 8)
                def _():
                    pre()

                ost[slot, 0 : rows.size, :] = dot(u[rows, :], wbuf[slot, 0:W, :]).astype(BF)

                @pl.when(j >= 1)
                def _():
                    send_on(j - 1, 1 - slot)

                put(j, slot).start()

            send_on(N_WO - 1, 1)

    def rotate(a, kind, dst, row, col):
        for b in range(a.shape[0] // TOK):
            for h in range(TN // HD):
                v = a[b * TOK : (b + 1) * TOK, h * HD : (h + 1) * HD]
                v = v * rope[kind, 0] + pltpu.roll(v, HD - 32, 1) * rope[kind, 1] + pltpu.roll(v, 32, 1) * rope[kind, 2]
                kvq[dst, pl.ds(mo(row + b * TOK, TOK), TOK), pl.ds(mo(col + h * HD, HD), HD)] = v.astype(BF)

    def kv_wait(i, halves):
        def got(h, src):
            kv_copy(i, h, src, False, 0, 0).wait_recv()

        def fetch(c, h):
            rows = half_rows(h)
            dst = kvq.at[K, rows, pl.ds(c * KVW, KVW)]
            return pltpu.make_async_copy(kvr.at[i, c, rows], dst, kvl_sem.at[c, h])

        with jax.named_scope("kv_wait"):
            for h in halves:

                @pl.when(is2)
                def _(h=h):
                    got(h, 0)
                    kv_copy(i, h, 0, False, 3, 1).start()

                @pl.when(is3)
                def _(h=h):
                    got(h, 1)
                    kv_copy(i, h, 1, False, 2, 0).start()

            for h in halves:

                @pl.when(is1)
                def _(h=h):
                    got(h, 0)

                @pl.when(is2)
                def _(h=h):
                    got(h, 1)

                @pl.when(is3)
                def _(h=h):
                    got(h, 2)
                    got(h, 0)

            for go in (lambda c: c.start(), lambda c: c.wait()):
                for c in range(N_CP - 1):

                    @pl.when(cp > c)
                    def _(c=c, go=go):
                        for h in halves:
                            go(fetch(c, h))

    def attention(first, count):
        scale = math.log2(math.e) / math.sqrt(HD)
        with jax.named_scope("attn"):
            for c in range(N_CP):

                @pl.when(cp == c)
                def _(c=c):
                    cols = [OWN_KV] + [b * KVW for b in range(c)]

                    @pl.loop(0, 4 * count)
                    def _(t):
                        g = lax.rem(t, 4)
                        seq = pl.ds(mo(first + t // 4 * TOK, TOK), TOK)
                        ks = [kvq[K, seq, pl.ds(mo(o + g * HD, HD), HD)] for o in cols]
                        vs = [kvq[K, seq, pl.ds(mo(o + TN + g * HD, HD), HD)] for o in cols]
                        keys = jnp.concatenate(ks, axis=0) if c else ks[0]
                        vals = jnp.concatenate(vs, axis=0) if c else vs[0]
                        row = lax.rem(lax.broadcasted_iota(jnp.int32, (2 * TOK, TOK), 0), TOK)
                        causal = lax.broadcasted_iota(jnp.int32, (2 * TOK, TOK), 1) <= row

                        def heads(p):
                            return [pl.ds(mo((g * 8 + 2 * p + z) * HD, HD), HD) for z in range(2)]

                        scores = []
                        for p in range(4):
                            qs = jnp.concatenate([kvq[Q, seq, o] for o in heads(p)], axis=0)
                            scores.append(dot(qs, keys, NT_DIMS))
                        for p in range(4):
                            s = scores[p]
                            own = jnp.where(causal, s[:, :TOK], -jnp.inf)
                            s = jnp.concatenate([own, s[:, TOK:]], axis=1) if c else own
                            m = jnp.max(s, axis=1, keepdims=True)
                            e = jnp.exp2((s - m) * scale)
                            o = dot(e.astype(BF), vals) * (1.0 / jnp.sum(e, axis=1, keepdims=True))
                            for z in range(2):
                                u[seq, heads(p)[z]] = o[z * TOK : (z + 1) * TOK].astype(BF)

    kv_own = kvq.at[K, :, pl.ds(OWN_KV, KVW)]

    def layer_a_first(then, pre):
        with jax.named_scope("x_a"):
            for c in x_from_hid(0):
                c.wait()

        with jax.named_scope("kv_a"):

            @pl.loop(0, 2)
            def _(j):
                wait_w(j)

                @pl.when(j == 0)
                def _():
                    wcopy(wva, 0, 1, DM).start()

                @pl.when(j == 1)
                def _():
                    wcopy(wqa, 0, 0, DM).start()

                rotate(dot(x[...], wbuf[j]), j, K, 0, OWN_KV + j * TN)

            kv_out = pltpu.make_async_copy(kv_own, kvh.at[0], kvo_sem)
            kv_out.start()
            kv_out.wait()
            for h in range(2):
                kv_sends(0, h, lambda c: c.start())

        @pl.loop(0, 2)
        def _(h):
            rows = half_rows(h)
            first = OWN * (1 - h)

            with jax.named_scope("q_a"):

                @pl.loop(0, 8)
                def _(j):
                    slot = parity(j)
                    wait_w(slot)

                    @pl.when(j < 7)
                    def _():
                        wcopy(wqa, wcol(j + 1), 1 - slot, DM).start()

                    @pl.when(j == 7)
                    def _():
                        wcopy(woa, 0, 0, W).start()

                    rotate(dot(x[rows, :], wbuf[slot]), 0, Q, first, j * TN)

            kv_wait(0, (h,))
            attention(first, 2)

            def then_a():
                @pl.when(h == 0)
                def _():
                    wcopy(wqa, 0, 0, DM).start()

                @pl.when(h == 1)
                def _():
                    then()

            def pre_a():
                @pl.when(h == 1)
                def _():
                    pre()

            out_proj(LA, 0, woa, then_a, pre_a, rows, h == 0)

    def layer_a(i, mid, then, pre):
        with jax.named_scope("x_a"):
            for c in x_from_hid(i):
                c.wait()

        kv_out = pltpu.make_async_copy(kv_own, kvh.at[i], kvo_sem)

        def finish(j, slot):
            kv = j < 2
            col = jnp.where(kv, OWN_KV + j * TN, (j - 2) * TN)
            rotate(acc.at[slot], jnp.where(j == 1, 1, 0), jnp.where(kv, K, Q), 0, col)

        with jax.named_scope("qkv_a"):

            @pl.loop(0, N_QKV)
            def _(j):
                slot = parity(j)
                wait_w(slot)

                @pl.when(j == 0)
                def _():
                    wcopy(wva, 0, 1, DM).start()

                @pl.when((j >= 1) & (j + 1 < N_QKV))
                def _():
                    wcopy(wqa, wcol(j - 1), 1 - slot, DM).start()

                @pl.when(j + 1 == N_QKV)
                def _():
                    wcopy(woa, 0, 0, W).start()

                @pl.when(j == 3)
                def _():
                    kv_out.wait()
                    for h in range(2):
                        kv_sends(i, h, lambda c: c.start())

                finish(jnp.maximum(j - 1, 0), 1 - slot)
                acc[slot] = dot(x[...], wbuf[slot])

                @pl.when(j == 2)
                def _():
                    kv_out.start()

                mid(j)

            finish(N_QKV - 1, 1)

        kv_wait(i, range(2))
        attention(0, N_SEQ)
        out_proj(LA, i, woa, then, pre, pl.ds(0, ROWS), True)

    def key_decay(h):
        back = lax.broadcasted_iota(jnp.int32, (TOK, HD), 0).astype(F32) - (TOK - 1.0)
        return jnp.exp(slopes[h] * back)

    def state_of(g, b, hh, kd):
        rows = blk(b)
        col = hcol(g, hh)
        k = (kvq[K, rows, col].astype(F32) * kd).astype(BF)
        return dot(k, kvq[V, rows, col], TN_DIMS)

    def block_decay(h):
        return jnp.exp(jnp.full((8, HD), -float(TOK), F32) * slopes[h])[0:1, :]

    def st_store(i, g, slot):
        return pltpu.make_async_copy(stg.at[slot], sth.at[i, g], sto_sem.at[slot])

    def st_load(i, g, slot):
        return pltpu.make_async_copy(str_.at[i, g], pst.at[slot], stl_sem.at[slot])

    def next_state(g):
        slot = parity(g)
        for hh in range(4):
            kd = key_decay(4 * g + hh)
            bd = block_decay(4 * g + hh)
            for b in range(N_SEQ):
                stg[slot, b * 4 + hh] = state_of(g, b, hh, kd) + bd * pst[slot, b * 4 + hh]

    def local_state(i, g):
        slot = parity(g)

        @pl.when(is1)
        def _():
            st_load(i, g, slot).wait()

        @pl.when(is0)
        def _():
            for hh in range(N_SEQ):
                kd = key_decay(4 * g + hh)
                for b in range(N_SEQ):
                    stg[slot, b * 4 + hh] = state_of(g, b, hh, kd)

        @pl.when(is1)
        def _():
            for hh in range(N_SEQ):
                kd = key_decay(4 * g + hh)
                bd = block_decay(4 * g + hh)
                for b in range(N_SEQ):
                    stg[slot, b * 4 + hh] = state_of(g, b, hh, kd) + bd * pst[slot, b * 4 + hh]

        st_store(i, g, slot).start()

    def st_send_on(i, g):
        st_store(i, g, parity(g)).wait()
        st_copy(i, g).start()

    def layer_b(i, mid, then, pre):
        with jax.named_scope("x_b"):
            for c in x_from_h1(i):
                c.wait()

        def finish(j, a):
            kv = j < 16
            dst = jnp.where(kv, parity(j), Q)
            kvq[dst, :, pl.ds(wcol(jnp.where(kv, j // 2, j - 16)), TN)] = (a * sigmoid(a)).astype(BF)

        with jax.named_scope("qkv_b"):
            @pl.loop(0, 24)
            def _(j):
                slot = parity(j)
                wait_w(slot)
                issue_b(j + 1, 1 - slot)
                e = j - jnp.where(is0, 0, 2)
                busy = (cp <= 1) & (e >= 1) & (e <= 16)
                g = e // 2

                @pl.when(busy & (parity(e) == 0))
                def _():
                    st_send_on(i, g - 1)

                @pl.when(busy & (parity(e) == 1) & is1)
                def _():
                    st_copy(i, g).wait_recv()
                    st_load(i, g, parity(g)).start()

                finish(j, dot(x[...], wbuf[slot]))

                @pl.when(busy & (parity(e) == 1))
                def _():
                    local_state(i, g)

                mid(j)

        with jax.named_scope("gate"):

            @pl.loop(0, 8)
            def _(j):
                slot = parity(j)
                wait_w(slot)

                @pl.when(j + 1 < 8)
                def _():
                    issue_b(25 + j, 1 - slot)

                @pl.when(j == 7)
                def _():
                    wcopy(wol, 0, 0, W).start()

                @pl.when(is2)
                def _():
                    st_copy(i, j).wait_recv()
                    st_load(i, j, slot).start()

                gbuf[:, pl.ds(wcol(j), TN)] = sigmoid(dot(x[...], wbuf[slot]))

                @pl.when(is2)
                def _():
                    st_load(i, j, slot).wait()
                    next_state(j)
                    st_store(i, j, slot).start()

                    @pl.when(j >= 1)
                    def _():
                        st_send_on(i, j - 1)

        with jax.named_scope("lin"):

            @pl.when(is2)
            def _():
                st_send_on(i, N_G - 1)

            ss[...] = jnp.zeros_like(ss)

            def fetch(g):
                @pl.when(is3)
                def _():
                    st_copy(i, g).wait_recv()

                @pl.when(cp >= 1)
                def _():
                    st_load(i, g, parity(g)).start()

            @pl.when(is0)
            def _():
                pst[...] = jnp.zeros_like(pst)

            fetch(0)

            @pl.loop(0, N_G)
            def _(g):
                slot = parity(g)

                @pl.when(g + 1 < N_G)
                def _():
                    fetch(g + 1)

                for hh in range(4):
                    lam = slopes[4 * g + hh]
                    row = lax.broadcasted_iota(jnp.int32, (TOK, HD), 0).astype(F32)
                    lane = lax.broadcasted_iota(jnp.int32, (TOK, HD), 1).astype(F32)
                    gap = row - lane
                    wtab[hh, 0] = jnp.where(gap >= 0, jnp.exp(-lam * jnp.maximum(gap, 0.0)), 0.0)
                    wtab[hh, 1] = jnp.exp(-lam * (row + 1.0))

                @pl.when(cp >= 1)
                def _():
                    st_load(i, g, slot).wait()

                @pl.loop(0, 2)
                def _(half):
                    pairs = [(half * 2 + z, hh) for z in range(2) for hh in range(4)]
                    at = [(blk(b), hcol(g, hh)) for b, hh in pairs]
                    qs = [kvq[Q, r, c] for r, c in at]
                    inner = [dot(q, kvq[K, r, c], NT_DIMS) for q, (r, c) in zip(qs, at)]
                    prior = [dot(q, pst[slot, b * 4 + hh].astype(BF)) for q, (b, hh) in zip(qs, pairs)]
                    o = [
                        dot((s * wtab[hh, 0]).astype(BF), kvq[V, r, c]) + p * wtab[hh, 1]
                        for s, p, (r, c), (b, hh) in zip(inner, prior, at, pairs)
                    ]
                    for v, (r, c) in zip(o, at):
                        u[r, c] = (v * ginner[0:1, c] * gbuf[r, c]).astype(BF)
                    for z in range(2):
                        ss[at[4 * z][0], :] += sum(v * v for v in o[4 * z : 4 * z + 4])

            sums = [jnp.sum(ss[blk(b), :].T, axis=0, keepdims=True) for b in range(N_SEQ)]
            ssx[i] = jnp.concatenate(sums + sums, axis=0)

        def then_ss():
            ss_copy(i).start()
            pre()

        out_proj(LB, i, wol, then, then_ss, pl.ds(0, ROWS), True)

    wcopy(wka, 0, 0, DM).start()
    start_x_a(0)
    rope_in = pltpu.make_async_copy(rope_hbm.at[cp], rope.at[0], kvo_sem)
    rope_in.start()
    gains[0:1, :] = gain_a[...]
    gains[1:2, :] = gain_b[...]
    rope[1, 0] = jnp.ones((TOK, HD), F32)
    rope[1, 1] = jnp.zeros((TOK, HD), F32)
    rope[1, 2] = jnp.zeros((TOK, HD), F32)
    rope_in.wait()
    pl.semaphore_wait(bar, 4)

    @pl.loop(0, 7)
    def _(s):
        @pl.when((s < 3) | (s == 4))
        def _():
            def mid_a(j):
                @pl.when((s == 1) & (j == 3))
                def _():
                    norm(LA, 0)

            def then_a():
                @pl.when(s < 2)
                def _():
                    wcopy(wka, 0, 0, DM).start()

                @pl.when(s >= 2)
                def _():
                    wcopy(wkl, 0, 0, DM).start()

            def pre_a():
                @pl.when(s < 2)
                def _():
                    start_x_a(s + 1)

                @pl.when(s >= 2)
                def _():
                    start_x_b(jnp.where(s == 2, 0, 1))

            @pl.when(s == 0)
            def _():
                layer_a_first(then_a, pre_a)

            @pl.when(s > 0)
            def _():
                layer_a(jnp.where(s < 3, s, 3), mid_a, then_a, pre_a)

        @pl.when(s == 2)
        def _():
            norm(LA, 1)

        @pl.when(s >= 3)
        def _():
            def mid_b(j):
                now = jnp.where(s == 4, 3, jnp.where(s == 6, 19, 15))

                @pl.when(j == now)
                def _():
                    norm(jnp.where(s == 3, LA, LB), jnp.where(s == 3, 2, s - 4))

            def then_b():
                @pl.when(s == 3)
                def _():
                    wcopy(wka, 0, 0, DM).start()

                @pl.when((s > 3) & (s < 6))
                def _():
                    wcopy(wkl, 0, 0, DM).start()

            def pre_b():
                @pl.when(s == 3)
                def _():
                    start_x_a(3)

                @pl.when((s > 3) & (s < 6))
                def _():
                    start_x_b(s - 2)

            layer_b(s - 3, mid_b, then_b, pre_b)

        @pl.when(s == 4)
        def _():
            norm(LA, 3)

    norm(LB, 3, end=True)

    for i in range(N_CH):
        for n in range(2):
            rs_copy(n, i, 0, DM).wait_send()
            if n == LA or i < N_CH - 1:
                ag_copy(n, i, 0, OWN).wait_send()
        if i < N_CH - 1:
            ag_wait_recv(LB, i)
        ss_copy(i).wait_send()

        for h in range(2):
            kv_sends(i, h, lambda c: c.wait_send())

            @pl.when(is2)
            def _(i=i, h=h):
                kv_copy(i, h, 0, False, 3, 1).wait_send()

            @pl.when(is3)
            def _(i=i, h=h):
                kv_copy(i, h, 1, False, 2, 0).wait_send()

        @pl.when(cp <= 2)
        def _(i=i):
            @pl.loop(0, 8)
            def _(g):
                st_copy(i, g).wait_send()


def assemble(rows, last, res, buf, in_sem, out_sem):
    tp = lax.axis_index("tp")
    n = 2 * N_CH - 1

    def block(k):
        half = jnp.where(k < N_CH, tp, 1 - tp)
        return pl.ds(mo((half * N_CH + lax.rem(k, N_CH)) * OWN, OWN), OWN)

    def load(k):
        src = last if k == N_CH - 1 else rows.at[block(k)]
        return pltpu.make_async_copy(src, buf.at[k % N_CH], in_sem.at[k % N_CH])

    def store(k):
        return pltpu.make_async_copy(buf.at[k % N_CH], res.at[block(k)], out_sem.at[k % N_CH])

    for k in range(N_CH):
        load(k).start()
    for k in range(n):
        load(k).wait()
        store(k).start()
        if k >= 1 and k + N_CH - 1 < n:
            store(k - 1).wait()
            load(k + N_CH - 1).start()
    for k in range(n - N_CH, n):
        store(k).wait()


def solution(mesh):
    n_cp = mesh.shape["cp"]
    table = rope_tables(n_cp)
    any_ = pl.BlockSpec(memory_space=pl.ANY)
    smem = pl.BlockSpec(memory_space=pltpu.SMEM)
    vmem = pl.BlockSpec(memory_space=pltpu.VMEM)
    dma = pltpu.SemaphoreType.DMA
    two = (2,)

    def body(hidden, alphas, wqa, wka, wva, woa, gain_attn, wql, wkl, wvl, wgl, slopes, gain_inner, wol, gain_lin):
        shape = hidden.shape
        hid = hidden.reshape(shape[0] * shape[1], shape[2])
        sds = jax.ShapeDtypeStruct
        outs = (
            sds(hid.shape, BF),
            sds((OWN, DM), BF),
            sds((2, N_CH, ROWS, DM), BF),
            sds((2, N_CH, OWN, DM), BF),
            sds((N_CH, OWN, DM), BF),
            sds((N_CH, OWN, DM), BF),
            sds((N_CH, ROWS, KVW), BF),
            sds((N_CH, 3, ROWS, KVW), BF),
            sds((N_CH, N_G, 16, HD, HD), F32),
            sds((N_CH, N_G, 16, HD, HD), F32),
        )
        scratch = [
            pltpu.VMEM((2, DM, TN), BF),
            pltpu.VMEM((ROWS, DM), BF),
            pltpu.VMEM((3, ROWS, W), BF),
            pltpu.VMEM((ROWS, W), F32),
            pltpu.VMEM((ROWS, W), BF),
            pltpu.VMEM((2, ROWS, TN), F32),
            pltpu.VMEM((2, ROWS, TN), BF),
            pltpu.VMEM((2, 16, HD, HD), F32),
            pltpu.VMEM((2, 16, HD, HD), F32),
            pltpu.VMEM((N_BUF, RB, DM), BF),
            pltpu.VMEM((N_BUF, RB, DM), BF),
            pltpu.VMEM((N_BUF, RB, DM), BF),
            pltpu.VMEM((N_BUF, RB, DM), BF),
            pltpu.VMEM((ROWS, HD), F32),
            pltpu.VMEM((OWN, HD), F32),
            pltpu.VMEM((2, 3, TOK, HD), F32),
            pltpu.VMEM((N_CH, 8, HD), F32),
            pltpu.VMEM((N_CH, 8, HD), F32),
            pltpu.VMEM((4, 2, TOK, HD), F32),
            pltpu.VMEM((2, DM), F32),
            dma(two), dma(two), dma(two), dma(()), dma((3, 2)), dma(two), dma(two), dma((N_BUF, 3)), dma((N_BUF,)),
            dma((2, N_CH)), dma((2, N_CH)), dma((2, N_CH)), dma((2, N_CH)), dma((N_CH, 2, 2)), dma((N_CH, 2, 3)), dma((N_CH, N_G)), dma((N_CH, N_G)),
            dma((N_CH,)), dma((N_CH,)),
        ]
        res = pl.pallas_call(
            kernel,
            out_shape=outs,
            in_specs=[any_] * 11 + [smem, smem, vmem, vmem, vmem],
            out_specs=tuple(any_ for _ in outs),
            scratch_shapes=scratch,
            compiler_params=pltpu.CompilerParams(
                collective_id=0, has_side_effects=True, vmem_limit_bytes=VMEM_BYTES
            ),
            name="layers",
        )(
            hid, wqa, wka, wva, woa, wql, wkl, wvl, wgl, wol, jnp.asarray(table), alphas, slopes, gain_attn.reshape(1, -1),
            gain_lin.reshape(1, -1), gain_inner.reshape(1, -1),
        )
        got = lax.ppermute(res[1], "tp", [(0, 1), (1, 0)])
        rows = pl.pallas_call(
            assemble,
            out_shape=sds(hid.shape, BF),
            in_specs=[any_, any_],
            out_specs=any_,
            scratch_shapes=[pltpu.VMEM((N_CH, OWN, DM), BF), dma((N_CH,)), dma((N_CH,))],
            compiler_params=pltpu.CompilerParams(vmem_limit_bytes=VMEM_BYTES),
            cost_estimate=pl.CostEstimate(flops=10**11, bytes_accessed=2 * hid.size * 2, transcendentals=0),
            name="assemble",
        )(res[0], res[1])
        row = ((1 - lax.axis_index("tp")) * N_CH + N_CH - 1) * OWN
        return lax.dynamic_update_slice(rows, got, (row, 0)).reshape(shape)

    act = P("dp", "cp", None)
    rep = P()
    col = P(None, "tp")
    row = P("tp", None)
    vec = P("tp")
    in_specs = (act, rep, col, col, col, row, rep, col, col, col, col, vec, vec, row, rep)
    return jax.shard_map(body, mesh=mesh, in_specs=in_specs, out_specs=act, check_vma=False)
```

```python
import math

import jax
import jax.numpy as jnp
import numpy as np
from jax import lax
from jax.experimental import pallas as pl
from jax.experimental.pallas import tpu as pltpu
from jax.sharding import PartitionSpec as P

MESH = pl.DeviceIdType.MESH
F32 = jnp.float32
BF = jnp.bfloat16
ROPE_BASE = 10000000.0
EPS = 1e-5

VMEM_BYTES = 67043328
TOK = 128
HD = 128
TN = 512
DM = 6144
W = 4096
KVW = 1024
OWN_KV = W - KVW
N_SEQ = 4
N_CH = 4
N_CP = 4
N_G = 8
ROWS = N_SEQ * TOK
OWN = ROWS // 2
RB = 32
N_RB = OWN // RB
N_QKV = (KVW + W) // TN
N_WO = DM // TN
N_PART = 4
N_BUF = 4
LA, LB = 0, 1
K, V, Q = 0, 1, 2
NT_DIMS = (((1,), (1,)), ((), ()))
TN_DIMS = (((0,), (0,)), ((), ()))


def rope_tables(n_cp):
    half = HD // 4
    inv = ROPE_BASE ** (-np.arange(half, dtype=np.float64) * 2.0 / (2 * half))
    pos = np.arange(n_cp * TOK, dtype=np.float64)
    ang = pos[:, None] * inv[None, :]
    tab = np.zeros((3, n_cp * TOK, HD), np.float32)
    tab[0] = 1.0
    tab[0, :, :half] = np.cos(ang)
    tab[0, :, half : 2 * half] = np.cos(ang)
    tab[1, :, :half] = -np.sin(ang)
    tab[2, :, half : 2 * half] = np.sin(ang)
    return np.ascontiguousarray(tab.reshape(3, n_cp, TOK, HD).transpose(1, 0, 2, 3))


def mo(v, m):
    return pl.multiple_of(v, m)


def parity(j):
    return lax.rem(j, 2)


def blk(b):
    return pl.ds(mo(b * TOK, TOK), TOK)


def hcol(g, hh):
    return pl.ds(mo((4 * g + hh) * HD, HD), HD)


def dot(a, b, dims=(((1,), (0,)), ((), ()))):
    return lax.dot_general(a, b, dims, preferred_element_type=F32)


def sigmoid(z):
    return 1.0 / (1.0 + jnp.exp(-z))


def kernel(
    hid, wqa, wka, wva, woa, wql, wkl, wvl, wgl, wol, rope_hbm, alphas, slopes, gain_a, gain_b, ginner,
    out, last, pt, prec, h1own, h1oth, kvh, kvr, sth, str_,
    wbuf, x, kvq, gbuf, u, acc, ost, stg, pst, nb_p, nb_r, nb_h, nout, ss, rsb, rope, ssx, ssr, wtab, gains,
    w_sem, x_sem, o_sem, kvo_sem, kvl_sem, sto_sem, stl_sem, nl_sem, no_sem,
    rs_send, rs_recv, ag_send, ag_recv, kv_send, kv_recv, st_send, st_recv, ss_send, ss_recv,
):
    cp = lax.axis_index("cp")
    tp = lax.axis_index("tp")
    mate = 1 - tp
    is0, is1, is2, is3 = (cp == c for c in range(N_CP))

    bar = pltpu.get_barrier_semaphore()
    pl.semaphore_signal(bar, inc=1, device_id={"tp": mate}, device_id_type=MESH)
    for d in range(1, 4):
        pl.semaphore_signal(bar, inc=1, device_id={"cp": lax.rem(cp + d, 4)}, device_id_type=MESH)

    def wcopy(src, col, slot, row, rows):
        span = pl.ds(row, rows)
        return pltpu.make_async_copy(src.at[span, pl.ds(col, TN)], wbuf.at[slot, span], w_sem.at[slot])

    def wstart(src, col, slot):
        part = src.shape[0] // N_PART
        for p in range(N_PART):
            wcopy(src, col, slot, p * part, part).start()

    def wfirst(src):
        wstart(src, 0, 0)

    def wcol(j):
        return mo(j * TN, TN)

    def issue_b(j, slot):
        kv = j < 16
        for cond, w, tile in (
            (kv & (parity(j) == 0), wkl, j // 2),
            (kv & (parity(j) == 1), wvl, j // 2),
            ((j >= 16) & (j < 24), wql, j - 16),
            (j >= 24, wgl, j - 24),
        ):

            @pl.when(cond)
            def _(w=w, tile=tile):
                wstart(w, wcol(tile), slot)

    def wait_w(slot, rows=DM):
        wcopy(wqa if rows == DM else woa, 0, slot, 0, rows).wait()

    def own_row(i):
        return mo((tp * 8 + 2 * i) * TOK, TOK)

    def oth_row(i):
        return mo((mate * 8 + 2 * i) * TOK, TOK)

    def x_copies(top, bot):
        return (
            pltpu.make_async_copy(top, x.at[pl.ds(0, OWN)], x_sem.at[0]),
            pltpu.make_async_copy(bot, x.at[pl.ds(OWN, OWN)], x_sem.at[1]),
        )

    def x_from_hid(i):
        return x_copies(hid.at[pl.ds(own_row(i), OWN)], hid.at[pl.ds(oth_row(i), OWN)])

    def x_from_h1(i):
        return x_copies(h1own.at[i], h1oth.at[i])

    def start_x_a(i):
        for c in x_from_hid(i):
            c.start()

    def start_x_b(i):
        ag_wait_recv(LA, i)
        for c in x_from_h1(i):
            c.start()

    def rs_copy(n, i, col, width):
        return pltpu.make_async_remote_copy(
            src_ref=pt.at[n, i, pl.ds(OWN, OWN), pl.ds(col, width)],
            dst_ref=prec.at[n, i, :, pl.ds(col, width)],
            send_sem=rs_send.at[n, i],
            recv_sem=rs_recv.at[n, i],
            device_id={"tp": mate},
            device_id_type=MESH,
        )

    def ag_copy(n, i, row, rows):
        if n == 0:
            src = h1own.at[i, pl.ds(row, rows)]
            dst = h1oth.at[i, pl.ds(row, rows)]
        else:
            src = out.at[pl.ds(mo(own_row(i) + row, RB), rows)]
            dst = src
        return pltpu.make_async_remote_copy(
            src_ref=src,
            dst_ref=dst,
            send_sem=ag_send.at[n, i],
            recv_sem=ag_recv.at[n, i],
            device_id={"tp": mate},
            device_id_type=MESH,
        )

    def ag_wait_recv(n, i):
        if n == 0:
            ag_copy(0, i, 0, OWN).wait_recv()
        else:
            oth = out.at[pl.ds(oth_row(i), OWN)]
            pltpu.make_async_remote_copy(
                src_ref=oth,
                dst_ref=oth,
                send_sem=ag_send.at[n, i],
                recv_sem=ag_recv.at[n, i],
                device_id={"tp": mate},
                device_id_type=MESH,
            ).wait_recv()

    def half_rows(h):
        return pl.ds(mo(OWN * (1 - h), OWN), OWN)

    def kv_copy(i, h, src, own, dst_cp, send):
        rows = half_rows(h)
        return pltpu.make_async_remote_copy(
            src_ref=kvh.at[i, rows] if own else kvr.at[i, src, rows],
            dst_ref=kvr.at[i, src, rows],
            send_sem=kv_send.at[i, h, send],
            recv_sem=kv_recv.at[i, h, src],
            device_id={"cp": dst_cp},
            device_id_type=MESH,
        )

    def kv_sends(i, h, go):
        @pl.when(is0)
        def _():
            go(kv_copy(i, h, 0, True, 2, 0))
            go(kv_copy(i, h, 0, True, 1, 1))

        @pl.when(is1)
        def _():
            go(kv_copy(i, h, 1, True, 3, 0))

        @pl.when(is2)
        def _():
            go(kv_copy(i, h, 2, True, 3, 0))

    def st_copy(i, g):
        return pltpu.make_async_remote_copy(
            src_ref=sth.at[i, g],
            dst_ref=str_.at[i, g],
            send_sem=st_send.at[i, g],
            recv_sem=st_recv.at[i, g],
            device_id={"cp": lax.rem(cp + 1, 4)},
            device_id_type=MESH,
        )

    def ss_copy(i):
        return pltpu.make_async_remote_copy(
            src_ref=ssx.at[i],
            dst_ref=ssr.at[i],
            send_sem=ss_send.at[i],
            recv_sem=ss_recv.at[i],
            device_id={"tp": mate},
            device_id_type=MESH,
        )

    def norm_loads(n, i, r, start):
        slot = lax.rem(r, N_BUF)
        rows = pl.ds(mo(r * RB, RB), RB)
        copies = [
            pltpu.make_async_copy(pt.at[n, i, rows], nb_p.at[slot], nl_sem.at[slot, 0]),
            pltpu.make_async_copy(prec.at[n, i, rows], nb_r.at[slot], nl_sem.at[slot, 1]),
        ]
        res_a = hid.at[pl.ds(mo(own_row(i) + r * RB, RB), RB)]
        res_b = h1own.at[i, rows]
        for layer, res in ((LA, res_a), (LB, res_b)):

            @pl.when(n == layer)
            def _(res=res):
                c = pltpu.make_async_copy(res, nb_h.at[slot], nl_sem.at[slot, 2])
                c.start() if start else c.wait()

        for c in copies:
            c.start() if start else c.wait()

    def norm_begin(n, i):
        with jax.named_scope("norm_wait"):
            rs_copy(n, i, 0, DM).wait_recv()

            @pl.when(n == LB)
            def _():
                ss_copy(i).wait_recv()
                for b in range(2):
                    whole = ssx[i, b : b + 1, :] + ssr[i, b + 2 : b + 3, :]
                    inv = lax.rsqrt(whole / float(2 * W) + EPS)
                    rsb[blk(b), :] = jnp.broadcast_to(inv, (TOK, TOK)).T

            @pl.when(n == LA)
            def _():
                rsb[...] = jnp.ones_like(rsb)

            for r in range(N_BUF - 1):
                norm_loads(n, i, r, True)

    def norm_ready(n, i, r):
        @pl.when(r + N_BUF - 1 < N_RB)
        def _():
            norm_loads(n, i, r + N_BUF - 1, True)

        norm_loads(n, i, r, False)

    def norm_rows(n, r):
        slot = lax.rem(r, N_BUF)
        alpha = alphas[n]
        for q in range(RB // 16):
            rows = slice(q * 16, (q + 1) * 16)
            both = nb_p[slot, rows, :].astype(F32) + nb_r[slot, rows, :].astype(F32)
            both = both * rsb[pl.ds(mo(r * RB + q * 16, 16), 16), 0:1]
            h = alpha * nb_h[slot, rows, :].astype(F32) + both
            inv = lax.rsqrt(jnp.mean(h * h, axis=-1, keepdims=True) + EPS)
            nout[slot, rows, :] = (h * inv * gains[pl.ds(n, 1), :]).astype(BF)

    def norm_store(n, i, r, start, end):
        slot = lax.rem(r, N_BUF)
        if end:
            c = pltpu.make_async_copy(nout.at[slot], last.at[pl.ds(mo(r * RB, RB), RB)], no_sem.at[slot])
            c.start() if start else c.wait()
            return
        dst_a = h1own.at[i, pl.ds(mo(r * RB, RB), RB)]
        dst_b = out.at[pl.ds(mo(own_row(i) + r * RB, RB), RB)]
        for layer, dst in ((LA, dst_a), (LB, dst_b)):

            @pl.when(n == layer)
            def _(layer=layer, dst=dst):
                c = pltpu.make_async_copy(nout.at[slot], dst, no_sem.at[slot])
                if start:
                    c.start()
                else:
                    c.wait()
                    ag_copy(layer, i, mo(r * RB, RB), RB).start()

    def norm_out(n, i, r, end):
        @pl.when(r >= 2)
        def _():
            norm_store(n, i, r - 2, False, end)

        norm_store(n, i, r, True, end)

    def norm_end(n, i, end):
        for r in range(N_RB - 2, N_RB):
            norm_store(n, i, r, False, end)

    def norm(n, i, end=False):
        norm_begin(n, i)
        with jax.named_scope("norm"):

            @pl.loop(0, N_RB)
            def _(r):
                norm_ready(n, i, r)
                norm_rows(n, r)
                norm_out(n, i, r, end)

            norm_end(n, i, end)

    def out_proj(n, i, wo, then, pre, rows, send):
        def put(j, slot):
            size = pl.ds(0, rows.size)
            return pltpu.make_async_copy(ost.at[slot, size], pt.at[n, i, rows, pl.ds(wcol(j), TN)], o_sem.at[slot])

        def send_on(j, slot):
            put(j, slot).wait()

            @pl.when(send)
            def _():
                rs_copy(n, i, wcol(j), TN).start()

        with jax.named_scope("out_proj"):

            @pl.loop(0, N_WO)
            def _(j):
                slot = parity(j)
                wait_w(slot, W)

                @pl.when(j + 1 < N_WO)
                def _():
                    wstart(wo, wcol(j + 1), 1 - slot)

                @pl.when(j == N_WO - 1)
                def _():
                    then()

                @pl.when(j == 8)
                def _():
                    pre()

                ost[slot, 0 : rows.size, :] = dot(u[rows, :], wbuf[slot, 0:W, :]).astype(BF)

                @pl.when(j >= 1)
                def _():
                    send_on(j - 1, 1 - slot)

                put(j, slot).start()

            send_on(N_WO - 1, 1)

    def rotate(a, kind, dst, row, col):
        for b in range(a.shape[0] // TOK):
            for h in range(TN // HD):
                v = a[b * TOK : (b + 1) * TOK, h * HD : (h + 1) * HD]
                v = v * rope[kind, 0] + pltpu.roll(v, HD - 32, 1) * rope[kind, 1] + pltpu.roll(v, 32, 1) * rope[kind, 2]
                kvq[dst, pl.ds(mo(row + b * TOK, TOK), TOK), pl.ds(mo(col + h * HD, HD), HD)] = v.astype(BF)

    def kv_wait(i, halves):
        def got(h, src):
            kv_copy(i, h, src, False, 0, 0).wait_recv()

        def fetch(c, h):
            rows = half_rows(h)
            dst = kvq.at[K, rows, pl.ds(c * KVW, KVW)]
            return pltpu.make_async_copy(kvr.at[i, c, rows], dst, kvl_sem.at[c, h])

        with jax.named_scope("kv_wait"):
            for h in halves:

                @pl.when(is2)
                def _(h=h):
                    got(h, 0)
                    kv_copy(i, h, 0, False, 3, 1).start()

                @pl.when(is3)
                def _(h=h):
                    got(h, 1)
                    kv_copy(i, h, 1, False, 2, 0).start()

            for h in halves:

                @pl.when(is1)
                def _(h=h):
                    got(h, 0)

                @pl.when(is2)
                def _(h=h):
                    got(h, 1)

                @pl.when(is3)
                def _(h=h):
                    got(h, 2)
                    got(h, 0)

            for go in (lambda c: c.start(), lambda c: c.wait()):
                for c in range(N_CP - 1):

                    @pl.when(cp > c)
                    def _(c=c, go=go):
                        for h in halves:
                            go(fetch(c, h))

    def attention(first, count):
        scale = math.log2(math.e) / math.sqrt(HD)
        with jax.named_scope("attn"):
            for c in range(N_CP):

                @pl.when(cp == c)
                def _(c=c):
                    cols = [OWN_KV] + [b * KVW for b in range(c)]

                    @pl.loop(0, 4 * count)
                    def _(t):
                        g = lax.rem(t, 4)
                        seq = pl.ds(mo(first + t // 4 * TOK, TOK), TOK)
                        ks = [kvq[K, seq, pl.ds(mo(o + g * HD, HD), HD)] for o in cols]
                        vs = [kvq[K, seq, pl.ds(mo(o + TN + g * HD, HD), HD)] for o in cols]
                        keys = jnp.concatenate(ks, axis=0) if c else ks[0]
                        vals = jnp.concatenate(vs, axis=0) if c else vs[0]
                        row = lax.rem(lax.broadcasted_iota(jnp.int32, (2 * TOK, TOK), 0), TOK)
                        causal = lax.broadcasted_iota(jnp.int32, (2 * TOK, TOK), 1) <= row

                        def heads(p):
                            return [pl.ds(mo((g * 8 + 2 * p + z) * HD, HD), HD) for z in range(2)]

                        scores = []
                        for p in range(4):
                            qs = jnp.concatenate([kvq[Q, seq, o] for o in heads(p)], axis=0)
                            scores.append(dot(qs, keys, NT_DIMS))
                        for p in range(4):
                            s = scores[p]
                            own = jnp.where(causal, s[:, :TOK], -jnp.inf)
                            s = jnp.concatenate([own, s[:, TOK:]], axis=1) if c else own
                            m = jnp.max(s, axis=1, keepdims=True)
                            e = jnp.exp2((s - m) * scale)
                            o = dot(e.astype(BF), vals) * (1.0 / jnp.sum(e, axis=1, keepdims=True))
                            for z in range(2):
                                u[seq, heads(p)[z]] = o[z * TOK : (z + 1) * TOK].astype(BF)

    kv_own = kvq.at[K, :, pl.ds(OWN_KV, KVW)]

    def layer_a_first(then, pre):
        with jax.named_scope("x_a"):
            for c in x_from_hid(0):
                c.wait()

        with jax.named_scope("kv_a"):

            @pl.loop(0, 2)
            def _(j):
                wait_w(j)

                @pl.when(j == 0)
                def _():
                    wstart(wva, 0, 1)

                @pl.when(j == 1)
                def _():
                    wfirst(wqa)

                rotate(dot(x[...], wbuf[j]), j, K, 0, OWN_KV + j * TN)

            kv_out = pltpu.make_async_copy(kv_own, kvh.at[0], kvo_sem)
            kv_out.start()
            kv_out.wait()
            for h in range(2):
                kv_sends(0, h, lambda c: c.start())

        @pl.loop(0, 2)
        def _(h):
            rows = half_rows(h)
            first = OWN * (1 - h)

            with jax.named_scope("q_a"):

                @pl.loop(0, 8)
                def _(j):
                    slot = parity(j)
                    wait_w(slot)

                    @pl.when(j < 7)
                    def _():
                        wstart(wqa, wcol(j + 1), 1 - slot)

                    @pl.when(j == 7)
                    def _():
                        wfirst(woa)

                    rotate(dot(x[rows, :], wbuf[slot]), 0, Q, first, j * TN)

            kv_wait(0, (h,))
            attention(first, 2)

            def then_a():
                @pl.when(h == 0)
                def _():
                    wfirst(wqa)

                @pl.when(h == 1)
                def _():
                    then()

            def pre_a():
                @pl.when(h == 1)
                def _():
                    pre()

            out_proj(LA, 0, woa, then_a, pre_a, rows, h == 0)

    def layer_a(i, mid, then, pre):
        with jax.named_scope("x_a"):
            for c in x_from_hid(i):
                c.wait()

        kv_out = pltpu.make_async_copy(kv_own, kvh.at[i], kvo_sem)

        def finish(j, slot):
            kv = j < 2
            col = jnp.where(kv, OWN_KV + j * TN, (j - 2) * TN)
            rotate(acc.at[slot], jnp.where(j == 1, 1, 0), jnp.where(kv, K, Q), 0, col)

        with jax.named_scope("qkv_a"):

            @pl.loop(0, N_QKV)
            def _(j):
                slot = parity(j)
                wait_w(slot)

                @pl.when(j == 0)
                def _():
                    wstart(wva, 0, 1)

                @pl.when((j >= 1) & (j + 1 < N_QKV))
                def _():
                    wstart(wqa, wcol(j - 1), 1 - slot)

                @pl.when(j + 1 == N_QKV)
                def _():
                    wfirst(woa)

                @pl.when(j == 3)
                def _():
                    kv_out.wait()
                    for h in range(2):
                        kv_sends(i, h, lambda c: c.start())

                finish(jnp.maximum(j - 1, 0), 1 - slot)
                acc[slot] = dot(x[...], wbuf[slot])

                @pl.when(j == 2)
                def _():
                    kv_out.start()

                mid(j)

            finish(N_QKV - 1, 1)

        kv_wait(i, range(2))
        attention(0, N_SEQ)
        out_proj(LA, i, woa, then, pre, pl.ds(0, ROWS), True)

    def key_decay(h):
        back = lax.broadcasted_iota(jnp.int32, (TOK, HD), 0).astype(F32) - (TOK - 1.0)
        return jnp.exp(slopes[h] * back)

    def state_of(g, b, hh, kd):
        rows = blk(b)
        col = hcol(g, hh)
        k = (kvq[K, rows, col].astype(F32) * kd).astype(BF)
        return dot(k, kvq[V, rows, col], TN_DIMS)

    def block_decay(h):
        return jnp.exp(jnp.full((8, HD), -float(TOK), F32) * slopes[h])[0:1, :]

    def st_store(i, g, slot):
        return pltpu.make_async_copy(stg.at[slot], sth.at[i, g], sto_sem.at[slot])

    def st_load(i, g, slot):
        return pltpu.make_async_copy(str_.at[i, g], pst.at[slot], stl_sem.at[slot])

    def next_state(g):
        slot = parity(g)
        for hh in range(4):
            kd = key_decay(4 * g + hh)
            bd = block_decay(4 * g + hh)
            for b in range(N_SEQ):
                stg[slot, b * 4 + hh] = state_of(g, b, hh, kd) + bd * pst[slot, b * 4 + hh]

    def local_state(i, g):
        slot = parity(g)

        @pl.when(is1)
        def _():
            st_load(i, g, slot).wait()

        @pl.when(is0)
        def _():
            for hh in range(N_SEQ):
                kd = key_decay(4 * g + hh)
                for b in range(N_SEQ):
                    stg[slot, b * 4 + hh] = state_of(g, b, hh, kd)

        @pl.when(is1)
        def _():
            for hh in range(N_SEQ):
                kd = key_decay(4 * g + hh)
                bd = block_decay(4 * g + hh)
                for b in range(N_SEQ):
                    stg[slot, b * 4 + hh] = state_of(g, b, hh, kd) + bd * pst[slot, b * 4 + hh]

        st_store(i, g, slot).start()

    def st_send_on(i, g):
        st_store(i, g, parity(g)).wait()
        st_copy(i, g).start()

    def layer_b(i, mid, then, pre):
        with jax.named_scope("x_b"):
            for c in x_from_h1(i):
                c.wait()

        def finish(j, a):
            kv = j < 16
            dst = jnp.where(kv, parity(j), Q)
            kvq[dst, :, pl.ds(wcol(jnp.where(kv, j // 2, j - 16)), TN)] = (a * sigmoid(a)).astype(BF)

        with jax.named_scope("qkv_b"):
            @pl.loop(0, 24)
            def _(j):
                slot = parity(j)
                wait_w(slot)
                issue_b(j + 1, 1 - slot)
                e = j - jnp.where(is0, 0, 2)
                busy = (cp <= 1) & (e >= 1) & (e <= 16)
                g = e // 2

                @pl.when(busy & (parity(e) == 1) & is1)
                def _():
                    st_copy(i, g).wait_recv()
                    st_load(i, g, parity(g)).start()

                finish(j, dot(x[...], wbuf[slot]))

                @pl.when(busy & (parity(e) == 0))
                def _():
                    st_send_on(i, g - 1)

                @pl.when(busy & (parity(e) == 1))
                def _():
                    local_state(i, g)

                mid(j)

        with jax.named_scope("gate"):

            @pl.loop(0, 8)
            def _(j):
                slot = parity(j)
                wait_w(slot)

                @pl.when(j + 1 < 8)
                def _():
                    issue_b(25 + j, 1 - slot)

                @pl.when(j == 7)
                def _():
                    wfirst(wol)

                @pl.when(is2)
                def _():
                    st_copy(i, j).wait_recv()
                    st_load(i, j, slot).start()

                gbuf[:, pl.ds(wcol(j), TN)] = sigmoid(dot(x[...], wbuf[slot]))

                @pl.when(is2)
                def _():
                    st_load(i, j, slot).wait()
                    next_state(j)
                    st_store(i, j, slot).start()

                    @pl.when(j >= 1)
                    def _():
                        st_send_on(i, j - 1)

        with jax.named_scope("lin"):

            @pl.when(is2)
            def _():
                st_send_on(i, N_G - 1)

            ss[...] = jnp.zeros_like(ss)

            def fetch(g):
                @pl.when(is3)
                def _():
                    st_copy(i, g).wait_recv()

                @pl.when(cp >= 1)
                def _():
                    st_load(i, g, parity(g)).start()

            @pl.when(is0)
            def _():
                pst[...] = jnp.zeros_like(pst)

            fetch(0)

            @pl.loop(0, N_G)
            def _(g):
                slot = parity(g)

                @pl.when(g + 1 < N_G)
                def _():
                    fetch(g + 1)

                for hh in range(4):
                    lam = slopes[4 * g + hh]
                    row = lax.broadcasted_iota(jnp.int32, (TOK, HD), 0).astype(F32)
                    lane = lax.broadcasted_iota(jnp.int32, (TOK, HD), 1).astype(F32)
                    gap = row - lane
                    wtab[hh, 0] = jnp.where(gap >= 0, jnp.exp(-lam * jnp.maximum(gap, 0.0)), 0.0)
                    wtab[hh, 1] = jnp.exp(-lam * (row + 1.0))

                @pl.when(cp >= 1)
                def _():
                    st_load(i, g, slot).wait()

                @pl.loop(0, 2)
                def _(half):
                    pairs = [(half * 2 + z, hh) for z in range(2) for hh in range(4)]
                    at = [(blk(b), hcol(g, hh)) for b, hh in pairs]
                    qs = [kvq[Q, r, c] for r, c in at]
                    inner = [dot(q, kvq[K, r, c], NT_DIMS) for q, (r, c) in zip(qs, at)]
                    prior = [dot(q, pst[slot, b * 4 + hh].astype(BF)) for q, (b, hh) in zip(qs, pairs)]
                    o = [
                        dot((s * wtab[hh, 0]).astype(BF), kvq[V, r, c]) + p * wtab[hh, 1]
                        for s, p, (r, c), (b, hh) in zip(inner, prior, at, pairs)
                    ]
                    for v, (r, c) in zip(o, at):
                        u[r, c] = (v * ginner[0:1, c] * gbuf[r, c]).astype(BF)
                    for z in range(2):
                        ss[at[4 * z][0], :] += sum(v * v for v in o[4 * z : 4 * z + 4])

            sums = [jnp.sum(ss[blk(b), :].T, axis=0, keepdims=True) for b in range(N_SEQ)]
            ssx[i] = jnp.concatenate(sums + sums, axis=0)

        def then_ss():
            ss_copy(i).start()
            pre()

        out_proj(LB, i, wol, then, then_ss, pl.ds(0, ROWS), True)

    wfirst(wka)
    start_x_a(0)
    rope_in = pltpu.make_async_copy(rope_hbm.at[cp], rope.at[0], kvo_sem)
    rope_in.start()
    gains[0:1, :] = gain_a[...]
    gains[1:2, :] = gain_b[...]
    rope[1, 0] = jnp.ones((TOK, HD), F32)
    rope[1, 1] = jnp.zeros((TOK, HD), F32)
    rope[1, 2] = jnp.zeros((TOK, HD), F32)
    rope_in.wait()
    pl.semaphore_wait(bar, 4)

    @pl.loop(0, 7)
    def _(s):
        @pl.when((s < 3) | (s == 4))
        def _():
            def mid_a(j):
                @pl.when((s == 1) & (j == 3))
                def _():
                    norm(LA, 0)

            def then_a():
                @pl.when(s < 2)
                def _():
                    wfirst(wka)

                @pl.when(s >= 2)
                def _():
                    wfirst(wkl)

            def pre_a():
                @pl.when(s < 2)
                def _():
                    start_x_a(s + 1)

                @pl.when(s >= 2)
                def _():
                    start_x_b(jnp.where(s == 2, 0, 1))

            @pl.when(s == 0)
            def _():
                layer_a_first(then_a, pre_a)

            @pl.when(s > 0)
            def _():
                layer_a(jnp.where(s < 3, s, 3), mid_a, then_a, pre_a)

        @pl.when(s == 2)
        def _():
            norm(LA, 1)

        @pl.when(s >= 3)
        def _():
            def mid_b(j):
                now = jnp.where(s == 4, 3, jnp.where(s == 6, 19, 15))

                @pl.when(j == now)
                def _():
                    norm(jnp.where(s == 3, LA, LB), jnp.where(s == 3, 2, s - 4))

            def then_b():
                @pl.when(s == 3)
                def _():
                    wfirst(wka)

                @pl.when((s > 3) & (s < 6))
                def _():
                    wfirst(wkl)

            def pre_b():
                @pl.when(s == 3)
                def _():
                    start_x_a(3)

                @pl.when((s > 3) & (s < 6))
                def _():
                    start_x_b(s - 2)

            layer_b(s - 3, mid_b, then_b, pre_b)

        @pl.when(s == 4)
        def _():
            norm(LA, 3)

    norm(LB, 3, end=True)

    for i in range(N_CH):
        for n in range(2):
            rs_copy(n, i, 0, DM).wait_send()
            if n == LA or i < N_CH - 1:
                ag_copy(n, i, 0, OWN).wait_send()
        if i < N_CH - 1:
            ag_wait_recv(LB, i)
        ss_copy(i).wait_send()

        for h in range(2):
            kv_sends(i, h, lambda c: c.wait_send())

            @pl.when(is2)
            def _(i=i, h=h):
                kv_copy(i, h, 0, False, 3, 1).wait_send()

            @pl.when(is3)
            def _(i=i, h=h):
                kv_copy(i, h, 1, False, 2, 0).wait_send()

        @pl.when(cp <= 2)
        def _(i=i):
            @pl.loop(0, 8)
            def _(g):
                st_copy(i, g).wait_send()


def assemble(rows, last, res, buf, in_sem, out_sem):
    tp = lax.axis_index("tp")
    n = 2 * N_CH - 1

    def block(k):
        half = jnp.where(k < N_CH, tp, 1 - tp)
        return pl.ds(mo((half * N_CH + lax.rem(k, N_CH)) * OWN, OWN), OWN)

    def load(k):
        src = last if k == N_CH - 1 else rows.at[block(k)]
        return pltpu.make_async_copy(src, buf.at[k % N_CH], in_sem.at[k % N_CH])

    def store(k):
        return pltpu.make_async_copy(buf.at[k % N_CH], res.at[block(k)], out_sem.at[k % N_CH])

    for k in range(N_CH):
        load(k).start()
    for k in range(n):
        load(k).wait()
        store(k).start()
        if k >= 1 and k + N_CH - 1 < n:
            store(k - 1).wait()
            load(k + N_CH - 1).start()
    for k in range(n - N_CH, n):
        store(k).wait()


def solution(mesh):
    n_cp = mesh.shape["cp"]
    table = rope_tables(n_cp)
    any_ = pl.BlockSpec(memory_space=pl.ANY)
    smem = pl.BlockSpec(memory_space=pltpu.SMEM)
    vmem = pl.BlockSpec(memory_space=pltpu.VMEM)
    dma = pltpu.SemaphoreType.DMA
    two = (2,)

    def body(hidden, alphas, wqa, wka, wva, woa, gain_attn, wql, wkl, wvl, wgl, slopes, gain_inner, wol, gain_lin):
        shape = hidden.shape
        hid = hidden.reshape(shape[0] * shape[1], shape[2])
        sds = jax.ShapeDtypeStruct
        outs = (
            sds(hid.shape, BF),
            sds((OWN, DM), BF),
            sds((2, N_CH, ROWS, DM), BF),
            sds((2, N_CH, OWN, DM), BF),
            sds((N_CH, OWN, DM), BF),
            sds((N_CH, OWN, DM), BF),
            sds((N_CH, ROWS, KVW), BF),
            sds((N_CH, 3, ROWS, KVW), BF),
            sds((N_CH, N_G, 16, HD, HD), F32),
            sds((N_CH, N_G, 16, HD, HD), F32),
        )
        scratch = [
            pltpu.VMEM((2, DM, TN), BF),
            pltpu.VMEM((ROWS, DM), BF),
            pltpu.VMEM((3, ROWS, W), BF),
            pltpu.VMEM((ROWS, W), F32),
            pltpu.VMEM((ROWS, W), BF),
            pltpu.VMEM((2, ROWS, TN), F32),
            pltpu.VMEM((2, ROWS, TN), BF),
            pltpu.VMEM((2, 16, HD, HD), F32),
            pltpu.VMEM((2, 16, HD, HD), F32),
            pltpu.VMEM((N_BUF, RB, DM), BF),
            pltpu.VMEM((N_BUF, RB, DM), BF),
            pltpu.VMEM((N_BUF, RB, DM), BF),
            pltpu.VMEM((N_BUF, RB, DM), BF),
            pltpu.VMEM((ROWS, HD), F32),
            pltpu.VMEM((OWN, HD), F32),
            pltpu.VMEM((2, 3, TOK, HD), F32),
            pltpu.VMEM((N_CH, 8, HD), F32),
            pltpu.VMEM((N_CH, 8, HD), F32),
            pltpu.VMEM((4, 2, TOK, HD), F32),
            pltpu.VMEM((2, DM), F32),
            dma(two), dma(two), dma(two), dma(()), dma((3, 2)), dma(two), dma(two), dma((N_BUF, 3)), dma((N_BUF,)),
            dma((2, N_CH)), dma((2, N_CH)), dma((2, N_CH)), dma((2, N_CH)), dma((N_CH, 2, 2)), dma((N_CH, 2, 3)), dma((N_CH, N_G)), dma((N_CH, N_G)),
            dma((N_CH,)), dma((N_CH,)),
        ]
        res = pl.pallas_call(
            kernel,
            out_shape=outs,
            in_specs=[any_] * 11 + [smem, smem, vmem, vmem, vmem],
            out_specs=tuple(any_ for _ in outs),
            scratch_shapes=scratch,
            compiler_params=pltpu.CompilerParams(
                collective_id=0, has_side_effects=True, vmem_limit_bytes=VMEM_BYTES
            ),
            name="layers",
        )(
            hid, wqa, wka, wva, woa, wql, wkl, wvl, wgl, wol, jnp.asarray(table), alphas, slopes, gain_attn.reshape(1, -1),
            gain_lin.reshape(1, -1), gain_inner.reshape(1, -1),
        )
        got = lax.ppermute(res[1], "tp", [(0, 1), (1, 0)])
        rows = pl.pallas_call(
            assemble,
            out_shape=sds(hid.shape, BF),
            in_specs=[any_, any_],
            out_specs=any_,
            scratch_shapes=[pltpu.VMEM((N_CH, OWN, DM), BF), dma((N_CH,)), dma((N_CH,))],
            compiler_params=pltpu.CompilerParams(vmem_limit_bytes=VMEM_BYTES),
            cost_estimate=pl.CostEstimate(flops=10**11, bytes_accessed=2 * hid.size * 2, transcendentals=0),
            name="assemble",
        )(res[0], res[1])
        row = ((1 - lax.axis_index("tp")) * N_CH + N_CH - 1) * OWN
        return lax.dynamic_update_slice(rows, got, (row, 0)).reshape(shape)

    act = P("dp", "cp", None)
    rep = P()
    col = P(None, "tp")
    row = P("tp", None)
    vec = P("tp")
    in_specs = (act, rep, col, col, col, row, rep, col, col, col, col, vec, vec, row, rep)
    return jax.shard_map(body, mesh=mesh, in_specs=in_specs, out_specs=act, check_vma=False)
```

```python
import math

import jax
import jax.numpy as jnp
import numpy as np
from jax import lax
from jax.experimental import pallas as pl
from jax.experimental.pallas import tpu as pltpu
from jax.sharding import PartitionSpec as P

MESH = pl.DeviceIdType.MESH
F32 = jnp.float32
BF = jnp.bfloat16
ROPE_BASE = 10000000.0
EPS = 1e-5

VMEM_BYTES = 67043328
TOK = 128
HD = 128
TN = 512
DM = 6144
W = 4096
KVW = 1024
OWN_KV = W - KVW
N_SEQ = 4
N_CH = 4
N_CP = 4
N_G = 8
ROWS = N_SEQ * TOK
OWN = ROWS // 2
RB = 32
N_RB = OWN // RB
N_QKV = (KVW + W) // TN
N_WO = DM // TN
N_BUF = 4
LA, LB = 0, 1
K, V, Q = 0, 1, 2
NT_DIMS = (((1,), (1,)), ((), ()))
TN_DIMS = (((0,), (0,)), ((), ()))


def rope_tables(n_cp):
    half = HD // 4
    inv = ROPE_BASE ** (-np.arange(half, dtype=np.float64) * 2.0 / (2 * half))
    pos = np.arange(n_cp * TOK, dtype=np.float64)
    ang = pos[:, None] * inv[None, :]
    tab = np.zeros((3, n_cp * TOK, HD), np.float32)
    tab[0] = 1.0
    tab[0, :, :half] = np.cos(ang)
    tab[0, :, half : 2 * half] = np.cos(ang)
    tab[1, :, :half] = -np.sin(ang)
    tab[2, :, half : 2 * half] = np.sin(ang)
    return np.ascontiguousarray(tab.reshape(3, n_cp, TOK, HD).transpose(1, 0, 2, 3))


def mo(v, m):
    return pl.multiple_of(v, m)


def parity(j):
    return lax.rem(j, 2)


def blk(b):
    return pl.ds(mo(b * TOK, TOK), TOK)


def hcol(g, hh):
    return pl.ds(mo((4 * g + hh) * HD, HD), HD)


def dot(a, b, dims=(((1,), (0,)), ((), ()))):
    return lax.dot_general(a, b, dims, preferred_element_type=F32)


def sigmoid(z):
    return 1.0 / (1.0 + jnp.exp(-z))


def kernel(
    hid, wqa, wka, wva, woa, wql, wkl, wvl, wgl, wol, rope_hbm, alphas, slopes, gain_a, gain_b, ginner,
    out, last, pt, prec, h1own, h1oth, kvh, kvr, sth, str_,
    wbuf, x, kvq, gbuf, u, acc, ost, stg, pst, nb_p, nb_r, nb_h, nout, ss, rsb, rope, ssx, ssr, wtab, gains,
    w_sem, x_sem, o_sem, kvo_sem, kvl_sem, sto_sem, stl_sem, nl_sem, no_sem,
    rs_send, rs_recv, ag_send, ag_recv, kv_send, kv_recv, st_send, st_recv, ss_send, ss_recv,
):
    cp = lax.axis_index("cp")
    tp = lax.axis_index("tp")
    mate = 1 - tp
    is0, is1, is2, is3 = (cp == c for c in range(N_CP))

    bar = pltpu.get_barrier_semaphore()
    pl.semaphore_signal(bar, inc=1, device_id={"tp": mate}, device_id_type=MESH)
    for d in range(1, 4):
        pl.semaphore_signal(bar, inc=1, device_id={"cp": lax.rem(cp + d, 4)}, device_id_type=MESH)

    def wtile(src, col, slot):
        rows = pl.ds(0, src.shape[0])
        return pltpu.make_async_copy(src.at[:, pl.ds(col, TN)], wbuf.at[slot, rows], w_sem.at[slot])

    def wstart(src, j):
        wtile(src, wcol(j), parity(j)).start()

    def wcol(j):
        return mo(j * TN, TN)

    def issue_a(t):
        for n, w in enumerate((wka, wva)):

            @pl.when(t == n)
            def _(n=n, w=w):
                wtile(w, 0, n).start()

    def issue_b(j):
        kv = j < 16
        for cond, w, tile in (
            (kv & (parity(j) == 0), wkl, j // 2),
            (kv & (parity(j) == 1), wvl, j // 2),
            ((j >= 16) & (j < 24), wql, j - 16),
            (j >= 24, wgl, j - 24),
        ):

            @pl.when(cond)
            def _(w=w, tile=tile):
                wtile(w, wcol(tile), parity(j)).start()

    def wait_w(slot, src=wqa):
        wtile(src, 0, slot).wait()

    def fetch_next(j, count, go, then):
        @pl.when(j + 2 < count)
        def _():
            go(j + 2)

        @pl.when(j + 2 >= count)
        def _():
            then(j + 2 - count)

    def own_row(i):
        return mo((tp * 8 + 2 * i) * TOK, TOK)

    def oth_row(i):
        return mo((mate * 8 + 2 * i) * TOK, TOK)

    def x_copies(top, bot):
        return (
            pltpu.make_async_copy(top, x.at[pl.ds(0, OWN)], x_sem.at[0]),
            pltpu.make_async_copy(bot, x.at[pl.ds(OWN, OWN)], x_sem.at[1]),
        )

    def x_from_hid(i):
        return x_copies(hid.at[pl.ds(own_row(i), OWN)], hid.at[pl.ds(oth_row(i), OWN)])

    def x_from_h1(i):
        return x_copies(h1own.at[i], h1oth.at[i])

    def start_x_a(i):
        for c in x_from_hid(i):
            c.start()

    def start_x_b(i):
        ag_wait_recv(LA, i)
        for c in x_from_h1(i):
            c.start()

    def rs_copy(n, i, col, width):
        return pltpu.make_async_remote_copy(
            src_ref=pt.at[n, i, pl.ds(OWN, OWN), pl.ds(col, width)],
            dst_ref=prec.at[n, i, :, pl.ds(col, width)],
            send_sem=rs_send.at[n, i],
            recv_sem=rs_recv.at[n, i],
            device_id={"tp": mate},
            device_id_type=MESH,
        )

    def ag_copy(n, i, row, rows):
        if n == 0:
            src = h1own.at[i, pl.ds(row, rows)]
            dst = h1oth.at[i, pl.ds(row, rows)]
        else:
            src = out.at[pl.ds(mo(own_row(i) + row, RB), rows)]
            dst = src
        return pltpu.make_async_remote_copy(
            src_ref=src,
            dst_ref=dst,
            send_sem=ag_send.at[n, i],
            recv_sem=ag_recv.at[n, i],
            device_id={"tp": mate},
            device_id_type=MESH,
        )

    def ag_wait_recv(n, i):
        if n == 0:
            ag_copy(0, i, 0, OWN).wait_recv()
        else:
            oth = out.at[pl.ds(oth_row(i), OWN)]
            pltpu.make_async_remote_copy(
                src_ref=oth,
                dst_ref=oth,
                send_sem=ag_send.at[n, i],
                recv_sem=ag_recv.at[n, i],
                device_id={"tp": mate},
                device_id_type=MESH,
            ).wait_recv()

    def half_rows(h):
        return pl.ds(mo(OWN * (1 - h), OWN), OWN)

    def kv_copy(i, h, src, own, dst_cp, send):
        rows = half_rows(h)
        return pltpu.make_async_remote_copy(
            src_ref=kvh.at[i, rows] if own else kvr.at[i, src, rows],
            dst_ref=kvr.at[i, src, rows],
            send_sem=kv_send.at[i, h, send],
            recv_sem=kv_recv.at[i, h, src],
            device_id={"cp": dst_cp},
            device_id_type=MESH,
        )

    def kv_sends(i, h, go):
        @pl.when(is0)
        def _():
            go(kv_copy(i, h, 0, True, 2, 0))
            go(kv_copy(i, h, 0, True, 1, 1))

        @pl.when(is1)
        def _():
            go(kv_copy(i, h, 1, True, 3, 0))

        @pl.when(is2)
        def _():
            go(kv_copy(i, h, 2, True, 3, 0))

    def st_copy(i, g):
        return pltpu.make_async_remote_copy(
            src_ref=sth.at[i, g],
            dst_ref=str_.at[i, g],
            send_sem=st_send.at[i, g],
            recv_sem=st_recv.at[i, g],
            device_id={"cp": lax.rem(cp + 1, 4)},
            device_id_type=MESH,
        )

    def ss_copy(i):
        return pltpu.make_async_remote_copy(
            src_ref=ssx.at[i],
            dst_ref=ssr.at[i],
            send_sem=ss_send.at[i],
            recv_sem=ss_recv.at[i],
            device_id={"tp": mate},
            device_id_type=MESH,
        )

    def norm_loads(n, i, r, start):
        slot = lax.rem(r, N_BUF)
        rows = pl.ds(mo(r * RB, RB), RB)
        copies = [
            pltpu.make_async_copy(pt.at[n, i, rows], nb_p.at[slot], nl_sem.at[slot, 0]),
            pltpu.make_async_copy(prec.at[n, i, rows], nb_r.at[slot], nl_sem.at[slot, 1]),
        ]
        res_a = hid.at[pl.ds(mo(own_row(i) + r * RB, RB), RB)]
        res_b = h1own.at[i, rows]
        for layer, res in ((LA, res_a), (LB, res_b)):

            @pl.when(n == layer)
            def _(res=res):
                c = pltpu.make_async_copy(res, nb_h.at[slot], nl_sem.at[slot, 2])
                c.start() if start else c.wait()

        for c in copies:
            c.start() if start else c.wait()

    def norm_begin(n, i):
        with jax.named_scope("norm_wait"):
            rs_copy(n, i, 0, DM).wait_recv()

            @pl.when(n == LB)
            def _():
                ss_copy(i).wait_recv()
                for b in range(2):
                    whole = ssx[i, b : b + 1, :] + ssr[i, b + 2 : b + 3, :]
                    inv = lax.rsqrt(whole / float(2 * W) + EPS)
                    rsb[blk(b), :] = jnp.broadcast_to(inv, (TOK, TOK)).T

            @pl.when(n == LA)
            def _():
                rsb[...] = jnp.ones_like(rsb)

            for r in range(N_BUF - 1):
                norm_loads(n, i, r, True)

    def norm_ready(n, i, r):
        @pl.when(r + N_BUF - 1 < N_RB)
        def _():
            norm_loads(n, i, r + N_BUF - 1, True)

        norm_loads(n, i, r, False)

    def norm_rows(n, r):
        slot = lax.rem(r, N_BUF)
        alpha = alphas[n]
        for q in range(RB // 16):
            rows = slice(q * 16, (q + 1) * 16)
            both = nb_p[slot, rows, :].astype(F32) + nb_r[slot, rows, :].astype(F32)
            both = both * rsb[pl.ds(mo(r * RB + q * 16, 16), 16), 0:1]
            h = alpha * nb_h[slot, rows, :].astype(F32) + both
            inv = lax.rsqrt(jnp.mean(h * h, axis=-1, keepdims=True) + EPS)
            nout[slot, rows, :] = (h * inv * gains[pl.ds(n, 1), :]).astype(BF)

    def norm_store(n, i, r, start, end):
        slot = lax.rem(r, N_BUF)
        if end:
            c = pltpu.make_async_copy(nout.at[slot], last.at[pl.ds(mo(r * RB, RB), RB)], no_sem.at[slot])
            c.start() if start else c.wait()
            return
        dst_a = h1own.at[i, pl.ds(mo(r * RB, RB), RB)]
        dst_b = out.at[pl.ds(mo(own_row(i) + r * RB, RB), RB)]
        for layer, dst in ((LA, dst_a), (LB, dst_b)):

            @pl.when(n == layer)
            def _(layer=layer, dst=dst):
                c = pltpu.make_async_copy(nout.at[slot], dst, no_sem.at[slot])
                if start:
                    c.start()
                else:
                    c.wait()
                    ag_copy(layer, i, mo(r * RB, RB), RB).start()

    def norm_out(n, i, r, end):
        @pl.when(r >= 2)
        def _():
            norm_store(n, i, r - 2, False, end)

        norm_store(n, i, r, True, end)

    def norm_end(n, i, end):
        for r in range(N_RB - 2, N_RB):
            norm_store(n, i, r, False, end)

    def norm(n, i, end=False):
        norm_begin(n, i)
        with jax.named_scope("norm"):

            @pl.loop(0, N_RB)
            def _(r):
                norm_ready(n, i, r)
                norm_rows(n, r)
                norm_out(n, i, r, end)

            norm_end(n, i, end)

    def out_proj(n, i, wo, then, pre, rows, send):
        def put(j, slot):
            size = pl.ds(0, rows.size)
            return pltpu.make_async_copy(ost.at[slot, size], pt.at[n, i, rows, pl.ds(wcol(j), TN)], o_sem.at[slot])

        def send_on(j, slot):
            put(j, slot).wait()

            @pl.when(send)
            def _():
                rs_copy(n, i, wcol(j), TN).start()

        with jax.named_scope("out_proj"):

            @pl.loop(0, N_WO)
            def _(j):
                slot = parity(j)
                wait_w(slot, wo)

                @pl.when(j == 8)
                def _():
                    pre()

                ost[slot, 0 : rows.size, :] = dot(u[rows, :], wbuf[slot, 0:W, :]).astype(BF)
                fetch_next(j, N_WO, lambda t: wstart(wo, t), then)

                @pl.when(j >= 1)
                def _():
                    send_on(j - 1, 1 - slot)

                put(j, slot).start()

            send_on(N_WO - 1, 1)

    def rotate(a, kind, dst, row, col):
        for b in range(a.shape[0] // TOK):
            for h in range(TN // HD):
                v = a[b * TOK : (b + 1) * TOK, h * HD : (h + 1) * HD]
                v = v * rope[kind, 0] + pltpu.roll(v, HD - 32, 1) * rope[kind, 1] + pltpu.roll(v, 32, 1) * rope[kind, 2]
                kvq[dst, pl.ds(mo(row + b * TOK, TOK), TOK), pl.ds(mo(col + h * HD, HD), HD)] = v.astype(BF)

    def kv_wait(i, halves):
        def got(h, src):
            kv_copy(i, h, src, False, 0, 0).wait_recv()

        def fetch(c, h):
            rows = half_rows(h)
            dst = kvq.at[K, rows, pl.ds(c * KVW, KVW)]
            return pltpu.make_async_copy(kvr.at[i, c, rows], dst, kvl_sem.at[c, h])

        with jax.named_scope("kv_wait"):
            for h in halves:

                @pl.when(is2)
                def _(h=h):
                    got(h, 0)
                    kv_copy(i, h, 0, False, 3, 1).start()

                @pl.when(is3)
                def _(h=h):
                    got(h, 1)
                    kv_copy(i, h, 1, False, 2, 0).start()

            for h in halves:

                @pl.when(is1)
                def _(h=h):
                    got(h, 0)

                @pl.when(is2)
                def _(h=h):
                    got(h, 1)

                @pl.when(is3)
                def _(h=h):
                    got(h, 2)
                    got(h, 0)

            for go in (lambda c: c.start(), lambda c: c.wait()):
                for c in range(N_CP - 1):

                    @pl.when(cp > c)
                    def _(c=c, go=go):
                        for h in halves:
                            go(fetch(c, h))

    def attention(first, count):
        scale = math.log2(math.e) / math.sqrt(HD)
        with jax.named_scope("attn"):
            for c in range(N_CP):

                @pl.when(cp == c)
                def _(c=c):
                    cols = [OWN_KV] + [b * KVW for b in range(c)]

                    @pl.loop(0, 4 * count)
                    def _(t):
                        g = lax.rem(t, 4)
                        seq = pl.ds(mo(first + t // 4 * TOK, TOK), TOK)
                        ks = [kvq[K, seq, pl.ds(mo(o + g * HD, HD), HD)] for o in cols]
                        vs = [kvq[K, seq, pl.ds(mo(o + TN + g * HD, HD), HD)] for o in cols]
                        keys = jnp.concatenate(ks, axis=0) if c else ks[0]
                        vals = jnp.concatenate(vs, axis=0) if c else vs[0]
                        row = lax.rem(lax.broadcasted_iota(jnp.int32, (2 * TOK, TOK), 0), TOK)
                        causal = lax.broadcasted_iota(jnp.int32, (2 * TOK, TOK), 1) <= row

                        def heads(p):
                            return [pl.ds(mo((g * 8 + 2 * p + z) * HD, HD), HD) for z in range(2)]

                        scores = []
                        for p in range(4):
                            qs = jnp.concatenate([kvq[Q, seq, o] for o in heads(p)], axis=0)
                            scores.append(dot(qs, keys, NT_DIMS))
                        for p in range(4):
                            s = scores[p]
                            own = jnp.where(causal, s[:, :TOK], -jnp.inf)
                            s = jnp.concatenate([own, s[:, TOK:]], axis=1) if c else own
                            m = jnp.max(s, axis=1, keepdims=True)
                            e = jnp.exp2((s - m) * scale)
                            o = dot(e.astype(BF), vals) * (1.0 / jnp.sum(e, axis=1, keepdims=True))
                            for z in range(2):
                                u[seq, heads(p)[z]] = o[z * TOK : (z + 1) * TOK].astype(BF)

    kv_own = kvq.at[K, :, pl.ds(OWN_KV, KVW)]

    def layer_a_first(then, pre):
        with jax.named_scope("x_a"):
            for c in x_from_hid(0):
                c.wait()

        with jax.named_scope("kv_a"):

            @pl.loop(0, 2)
            def _(j):
                wait_w(j)
                rotate(dot(x[...], wbuf[j]), j, K, 0, OWN_KV + j * TN)
                wstart(wqa, j)

            kv_out = pltpu.make_async_copy(kv_own, kvh.at[0], kvo_sem)
            kv_out.start()
            kv_out.wait()
            for h in range(2):
                kv_sends(0, h, lambda c: c.start())

        @pl.loop(0, 2)
        def _(h):
            rows = half_rows(h)
            first = OWN * (1 - h)

            with jax.named_scope("q_a"):

                @pl.loop(0, 8)
                def _(j):
                    slot = parity(j)
                    wait_w(slot)
                    rotate(dot(x[rows, :], wbuf[slot]), 0, Q, first, j * TN)
                    fetch_next(j, 8, lambda t: wstart(wqa, t), lambda t: wstart(woa, t))

            kv_wait(0, (h,))
            attention(first, 2)

            def then_a(t):
                @pl.when(h == 0)
                def _():
                    wstart(wqa, t)

                @pl.when(h == 1)
                def _():
                    then(t)

            def pre_a():
                @pl.when(h == 1)
                def _():
                    pre()

            out_proj(LA, 0, woa, then_a, pre_a, rows, h == 0)

    def layer_a(i, mid, then, pre):
        with jax.named_scope("x_a"):
            for c in x_from_hid(i):
                c.wait()

        kv_out = pltpu.make_async_copy(kv_own, kvh.at[i], kvo_sem)

        def finish(j, slot):
            kv = j < 2
            col = jnp.where(kv, OWN_KV + j * TN, (j - 2) * TN)
            rotate(acc.at[slot], jnp.where(j == 1, 1, 0), jnp.where(kv, K, Q), 0, col)

        with jax.named_scope("qkv_a"):

            @pl.loop(0, N_QKV)
            def _(j):
                slot = parity(j)
                wait_w(slot)

                @pl.when(j == 3)
                def _():
                    kv_out.wait()
                    for h in range(2):
                        kv_sends(i, h, lambda c: c.start())

                finish(jnp.maximum(j - 1, 0), 1 - slot)
                acc[slot] = dot(x[...], wbuf[slot])
                fetch_next(j, N_QKV, lambda t: wstart(wqa, t - 2), lambda t: wstart(woa, t))

                @pl.when(j == 2)
                def _():
                    kv_out.start()

                mid(j)

            finish(N_QKV - 1, 1)

        kv_wait(i, range(2))
        attention(0, N_SEQ)
        out_proj(LA, i, woa, then, pre, pl.ds(0, ROWS), True)

    def key_decay(h):
        back = lax.broadcasted_iota(jnp.int32, (TOK, HD), 0).astype(F32) - (TOK - 1.0)
        return jnp.exp(slopes[h] * back)

    def state_of(g, b, hh, kd):
        rows = blk(b)
        col = hcol(g, hh)
        k = (kvq[K, rows, col].astype(F32) * kd).astype(BF)
        return dot(k, kvq[V, rows, col], TN_DIMS)

    def block_decay(h):
        return jnp.exp(jnp.full((8, HD), -float(TOK), F32) * slopes[h])[0:1, :]

    def st_store(i, g, slot):
        return pltpu.make_async_copy(stg.at[slot], sth.at[i, g], sto_sem.at[slot])

    def st_load(i, g, slot):
        return pltpu.make_async_copy(str_.at[i, g], pst.at[slot], stl_sem.at[slot])

    def next_state(g):
        slot = parity(g)
        for hh in range(4):
            kd = key_decay(4 * g + hh)
            bd = block_decay(4 * g + hh)
            for b in range(N_SEQ):
                stg[slot, b * 4 + hh] = state_of(g, b, hh, kd) + bd * pst[slot, b * 4 + hh]

    def local_state(i, g):
        slot = parity(g)

        @pl.when(is1)
        def _():
            st_load(i, g, slot).wait()

        @pl.when(is0)
        def _():
            for hh in range(N_SEQ):
                kd = key_decay(4 * g + hh)
                for b in range(N_SEQ):
                    stg[slot, b * 4 + hh] = state_of(g, b, hh, kd)

        @pl.when(is1)
        def _():
            for hh in range(N_SEQ):
                kd = key_decay(4 * g + hh)
                bd = block_decay(4 * g + hh)
                for b in range(N_SEQ):
                    stg[slot, b * 4 + hh] = state_of(g, b, hh, kd) + bd * pst[slot, b * 4 + hh]

        st_store(i, g, slot).start()

    def st_send_on(i, g):
        st_store(i, g, parity(g)).wait()
        st_copy(i, g).start()

    def layer_b(i, mid, then, pre):
        with jax.named_scope("x_b"):
            for c in x_from_h1(i):
                c.wait()

        def finish(j, a):
            kv = j < 16
            dst = jnp.where(kv, parity(j), Q)
            kvq[dst, :, pl.ds(wcol(jnp.where(kv, j // 2, j - 16)), TN)] = (a * sigmoid(a)).astype(BF)

        with jax.named_scope("qkv_b"):
            @pl.loop(0, 24)
            def _(j):
                slot = parity(j)
                wait_w(slot)
                e = j - jnp.where(is0, 0, 2)
                busy = (cp <= 1) & (e >= 1) & (e <= 16)
                g = e // 2

                @pl.when(busy & (parity(e) == 1) & is1)
                def _():
                    st_copy(i, g).wait_recv()
                    st_load(i, g, parity(g)).start()

                finish(j, dot(x[...], wbuf[slot]))
                issue_b(j + 2)

                @pl.when(busy & (parity(e) == 0))
                def _():
                    st_send_on(i, g - 1)

                @pl.when(busy & (parity(e) == 1))
                def _():
                    local_state(i, g)

                mid(j)

        with jax.named_scope("gate"):

            @pl.loop(0, 8)
            def _(j):
                slot = parity(j)
                wait_w(slot)

                @pl.when(is2)
                def _():
                    st_copy(i, j).wait_recv()
                    st_load(i, j, slot).start()

                gbuf[:, pl.ds(wcol(j), TN)] = sigmoid(dot(x[...], wbuf[slot]))
                fetch_next(j, 8, lambda t: issue_b(t + 24), lambda t: wstart(wol, t))

                @pl.when(is2)
                def _():
                    st_load(i, j, slot).wait()
                    next_state(j)
                    st_store(i, j, slot).start()

                    @pl.when(j >= 1)
                    def _():
                        st_send_on(i, j - 1)

        with jax.named_scope("lin"):

            @pl.when(is2)
            def _():
                st_send_on(i, N_G - 1)

            ss[...] = jnp.zeros_like(ss)

            def fetch(g):
                @pl.when(is3)
                def _():
                    st_copy(i, g).wait_recv()

                @pl.when(cp >= 1)
                def _():
                    st_load(i, g, parity(g)).start()

            @pl.when(is0)
            def _():
                pst[...] = jnp.zeros_like(pst)

            fetch(0)

            @pl.loop(0, N_G)
            def _(g):
                slot = parity(g)

                @pl.when(g + 1 < N_G)
                def _():
                    fetch(g + 1)

                for hh in range(4):
                    lam = slopes[4 * g + hh]
                    row = lax.broadcasted_iota(jnp.int32, (TOK, HD), 0).astype(F32)
                    lane = lax.broadcasted_iota(jnp.int32, (TOK, HD), 1).astype(F32)
                    gap = row - lane
                    wtab[hh, 0] = jnp.where(gap >= 0, jnp.exp(-lam * jnp.maximum(gap, 0.0)), 0.0)
                    wtab[hh, 1] = jnp.exp(-lam * (row + 1.0))

                @pl.when(cp >= 1)
                def _():
                    st_load(i, g, slot).wait()

                @pl.loop(0, 2)
                def _(half):
                    pairs = [(half * 2 + z, hh) for z in range(2) for hh in range(4)]
                    at = [(blk(b), hcol(g, hh)) for b, hh in pairs]
                    qs = [kvq[Q, r, c] for r, c in at]
                    inner = [dot(q, kvq[K, r, c], NT_DIMS) for q, (r, c) in zip(qs, at)]
                    prior = [dot(q, pst[slot, b * 4 + hh].astype(BF)) for q, (b, hh) in zip(qs, pairs)]
                    o = [
                        dot((s * wtab[hh, 0]).astype(BF), kvq[V, r, c]) + p * wtab[hh, 1]
                        for s, p, (r, c), (b, hh) in zip(inner, prior, at, pairs)
                    ]
                    for v, (r, c) in zip(o, at):
                        u[r, c] = (v * ginner[0:1, c] * gbuf[r, c]).astype(BF)
                    for z in range(2):
                        ss[at[4 * z][0], :] += sum(v * v for v in o[4 * z : 4 * z + 4])

            sums = [jnp.sum(ss[blk(b), :].T, axis=0, keepdims=True) for b in range(N_SEQ)]
            ssx[i] = jnp.concatenate(sums + sums, axis=0)

        def then_ss():
            ss_copy(i).start()
            pre()

        out_proj(LB, i, wol, then, then_ss, pl.ds(0, ROWS), True)

    wtile(wka, 0, 0).start()
    start_x_a(0)
    wtile(wva, 0, 1).start()
    rope_in = pltpu.make_async_copy(rope_hbm.at[cp], rope.at[0], kvo_sem)
    rope_in.start()
    gains[0:1, :] = gain_a[...]
    gains[1:2, :] = gain_b[...]
    rope[1, 0] = jnp.ones((TOK, HD), F32)
    rope[1, 1] = jnp.zeros((TOK, HD), F32)
    rope[1, 2] = jnp.zeros((TOK, HD), F32)
    rope_in.wait()
    pl.semaphore_wait(bar, 4)

    @pl.loop(0, 7)
    def _(s):
        @pl.when((s < 3) | (s == 4))
        def _():
            def mid_a(j):
                @pl.when((s == 1) & (j == 3))
                def _():
                    norm(LA, 0)

            def then_a(t):
                @pl.when(s < 2)
                def _():
                    issue_a(t)

                @pl.when(s >= 2)
                def _():
                    issue_b(t)

            def pre_a():
                @pl.when(s < 2)
                def _():
                    start_x_a(s + 1)

                @pl.when(s >= 2)
                def _():
                    start_x_b(jnp.where(s == 2, 0, 1))

            @pl.when(s == 0)
            def _():
                layer_a_first(then_a, pre_a)

            @pl.when(s > 0)
            def _():
                layer_a(jnp.where(s < 3, s, 3), mid_a, then_a, pre_a)

        @pl.when(s == 2)
        def _():
            norm(LA, 1)

        @pl.when(s >= 3)
        def _():
            def mid_b(j):
                now = jnp.where(s == 4, 3, jnp.where(s == 6, 19, 15))

                @pl.when(j == now)
                def _():
                    norm(jnp.where(s == 3, LA, LB), jnp.where(s == 3, 2, s - 4))

            def then_b(t):
                @pl.when(s == 3)
                def _():
                    issue_a(t)

                @pl.when((s > 3) & (s < 6))
                def _():
                    issue_b(t)

            def pre_b():
                @pl.when(s == 3)
                def _():
                    start_x_a(3)

                @pl.when((s > 3) & (s < 6))
                def _():
                    start_x_b(s - 2)

            layer_b(s - 3, mid_b, then_b, pre_b)

        @pl.when(s == 4)
        def _():
            norm(LA, 3)

    norm(LB, 3, end=True)

    for i in range(N_CH):
        for n in range(2):
            rs_copy(n, i, 0, DM).wait_send()
            if n == LA or i < N_CH - 1:
                ag_copy(n, i, 0, OWN).wait_send()
        if i < N_CH - 1:
            ag_wait_recv(LB, i)
        ss_copy(i).wait_send()

        for h in range(2):
            kv_sends(i, h, lambda c: c.wait_send())

            @pl.when(is2)
            def _(i=i, h=h):
                kv_copy(i, h, 0, False, 3, 1).wait_send()

            @pl.when(is3)
            def _(i=i, h=h):
                kv_copy(i, h, 1, False, 2, 0).wait_send()

        @pl.when(cp <= 2)
        def _(i=i):
            @pl.loop(0, 8)
            def _(g):
                st_copy(i, g).wait_send()


def assemble(rows, last, res, buf, in_sem, out_sem):
    tp = lax.axis_index("tp")
    n = 2 * N_CH - 1

    def block(k):
        half = jnp.where(k < N_CH, tp, 1 - tp)
        return pl.ds(mo((half * N_CH + lax.rem(k, N_CH)) * OWN, OWN), OWN)

    def load(k):
        src = last if k == N_CH - 1 else rows.at[block(k)]
        return pltpu.make_async_copy(src, buf.at[k % N_CH], in_sem.at[k % N_CH])

    def store(k):
        return pltpu.make_async_copy(buf.at[k % N_CH], res.at[block(k)], out_sem.at[k % N_CH])

    for k in range(N_CH):
        load(k).start()
    for k in range(n):
        load(k).wait()
        store(k).start()
        if k >= 1 and k + N_CH - 1 < n:
            store(k - 1).wait()
            load(k + N_CH - 1).start()
    for k in range(n - N_CH, n):
        store(k).wait()


def solution(mesh):
    n_cp = mesh.shape["cp"]
    table = rope_tables(n_cp)
    any_ = pl.BlockSpec(memory_space=pl.ANY)
    smem = pl.BlockSpec(memory_space=pltpu.SMEM)
    vmem = pl.BlockSpec(memory_space=pltpu.VMEM)
    dma = pltpu.SemaphoreType.DMA
    two = (2,)

    def body(hidden, alphas, wqa, wka, wva, woa, gain_attn, wql, wkl, wvl, wgl, slopes, gain_inner, wol, gain_lin):
        shape = hidden.shape
        hid = hidden.reshape(shape[0] * shape[1], shape[2])
        sds = jax.ShapeDtypeStruct
        outs = (
            sds(hid.shape, BF),
            sds((OWN, DM), BF),
            sds((2, N_CH, ROWS, DM), BF),
            sds((2, N_CH, OWN, DM), BF),
            sds((N_CH, OWN, DM), BF),
            sds((N_CH, OWN, DM), BF),
            sds((N_CH, ROWS, KVW), BF),
            sds((N_CH, 3, ROWS, KVW), BF),
            sds((N_CH, N_G, 16, HD, HD), F32),
            sds((N_CH, N_G, 16, HD, HD), F32),
        )
        scratch = [
            pltpu.VMEM((2, DM, TN), BF),
            pltpu.VMEM((ROWS, DM), BF),
            pltpu.VMEM((3, ROWS, W), BF),
            pltpu.VMEM((ROWS, W), F32),
            pltpu.VMEM((ROWS, W), BF),
            pltpu.VMEM((2, ROWS, TN), F32),
            pltpu.VMEM((2, ROWS, TN), BF),
            pltpu.VMEM((2, 16, HD, HD), F32),
            pltpu.VMEM((2, 16, HD, HD), F32),
            pltpu.VMEM((N_BUF, RB, DM), BF),
            pltpu.VMEM((N_BUF, RB, DM), BF),
            pltpu.VMEM((N_BUF, RB, DM), BF),
            pltpu.VMEM((N_BUF, RB, DM), BF),
            pltpu.VMEM((ROWS, HD), F32),
            pltpu.VMEM((OWN, HD), F32),
            pltpu.VMEM((2, 3, TOK, HD), F32),
            pltpu.VMEM((N_CH, 8, HD), F32),
            pltpu.VMEM((N_CH, 8, HD), F32),
            pltpu.VMEM((4, 2, TOK, HD), F32),
            pltpu.VMEM((2, DM), F32),
            dma(two), dma(two), dma(two), dma(()), dma((3, 2)), dma(two), dma(two), dma((N_BUF, 3)), dma((N_BUF,)),
            dma((2, N_CH)), dma((2, N_CH)), dma((2, N_CH)), dma((2, N_CH)), dma((N_CH, 2, 2)), dma((N_CH, 2, 3)), dma((N_CH, N_G)), dma((N_CH, N_G)),
            dma((N_CH,)), dma((N_CH,)),
        ]
        res = pl.pallas_call(
            kernel,
            out_shape=outs,
            in_specs=[any_] * 11 + [smem, smem, vmem, vmem, vmem],
            out_specs=tuple(any_ for _ in outs),
            scratch_shapes=scratch,
            compiler_params=pltpu.CompilerParams(
                collective_id=0, has_side_effects=True, vmem_limit_bytes=VMEM_BYTES
            ),
            name="layers",
        )(
            hid, wqa, wka, wva, woa, wql, wkl, wvl, wgl, wol, jnp.asarray(table), alphas, slopes, gain_attn.reshape(1, -1),
            gain_lin.reshape(1, -1), gain_inner.reshape(1, -1),
        )
        got = lax.ppermute(res[1], "tp", [(0, 1), (1, 0)])
        rows = pl.pallas_call(
            assemble,
            out_shape=sds(hid.shape, BF),
            in_specs=[any_, any_],
            out_specs=any_,
            scratch_shapes=[pltpu.VMEM((N_CH, OWN, DM), BF), dma((N_CH,)), dma((N_CH,))],
            compiler_params=pltpu.CompilerParams(vmem_limit_bytes=VMEM_BYTES),
            cost_estimate=pl.CostEstimate(flops=10**11, bytes_accessed=2 * hid.size * 2, transcendentals=0),
            name="assemble",
        )(res[0], res[1])
        row = ((1 - lax.axis_index("tp")) * N_CH + N_CH - 1) * OWN
        return lax.dynamic_update_slice(rows, got, (row, 0)).reshape(shape)

    act = P("dp", "cp", None)
    rep = P()
    col = P(None, "tp")
    row = P("tp", None)
    vec = P("tp")
    in_specs = (act, rep, col, col, col, row, rep, col, col, col, col, vec, vec, row, rep)
    return jax.shard_map(body, mesh=mesh, in_specs=in_specs, out_specs=act, check_vma=False)
```

```python
import math

import jax
import jax.numpy as jnp
import numpy as np
from jax import lax
from jax.experimental import pallas as pl
from jax.experimental.pallas import tpu as pltpu
from jax.sharding import PartitionSpec as P

MESH = pl.DeviceIdType.MESH
F32 = jnp.float32
BF = jnp.bfloat16
ROPE_BASE = 10000000.0
EPS = 1e-5

VMEM_BYTES = 67043328
TOK = 128
HD = 128
TN = 512
DM = 6144
W = 4096
KVW = 1024
OWN_KV = W - KVW
N_SEQ = 4
N_CH = 4
N_CP = 4
N_G = 8
ROWS = N_SEQ * TOK
OWN = ROWS // 2
RB = 32
N_RB = OWN // RB
N_QKV = (KVW + W) // TN
N_WO = DM // TN
N_BUF = 4
LA, LB = 0, 1
K, V, Q = 0, 1, 2
NT_DIMS = (((1,), (1,)), ((), ()))
TN_DIMS = (((0,), (0,)), ((), ()))


def rope_tables(n_cp):
    half = HD // 4
    inv = ROPE_BASE ** (-np.arange(half, dtype=np.float64) * 2.0 / (2 * half))
    pos = np.arange(n_cp * TOK, dtype=np.float64)
    ang = pos[:, None] * inv[None, :]
    tab = np.zeros((3, n_cp * TOK, HD), np.float32)
    tab[0] = 1.0
    tab[0, :, :half] = np.cos(ang)
    tab[0, :, half : 2 * half] = np.cos(ang)
    tab[1, :, :half] = -np.sin(ang)
    tab[2, :, half : 2 * half] = np.sin(ang)
    return np.ascontiguousarray(tab.reshape(3, n_cp, TOK, HD).transpose(1, 0, 2, 3))


def mo(v, m):
    return pl.multiple_of(v, m)


def parity(j):
    return lax.rem(j, 2)


def blk(b):
    return pl.ds(mo(b * TOK, TOK), TOK)


def hcol(g, hh):
    return pl.ds(mo((4 * g + hh) * HD, HD), HD)


def dot(a, b, dims=(((1,), (0,)), ((), ()))):
    return lax.dot_general(a, b, dims, preferred_element_type=F32)


def sigmoid(z):
    return 1.0 / (1.0 + jnp.exp(-z))


def kernel(
    hid, wqa, wka, wva, woa, wql, wkl, wvl, wgl, wol, rope_hbm, alphas, slopes, gain_a, gain_b, ginner,
    out, last, pt, prec, h1own, h1oth, kvh, kvr, sth, str_,
    wbuf, x, kvq, gbuf, u, acc, ost, stg, pst, nb_p, nb_r, nb_h, nout, ss, rsb, rope, ssx, ssr, wtab, gains,
    w_sem, x_sem, o_sem, kvo_sem, kvl_sem, sto_sem, stl_sem, nl_sem, no_sem,
    rs_send, rs_recv, ag_send, ag_recv, kv_send, kv_recv, st_send, st_recv, ss_send, ss_recv,
):
    cp = lax.axis_index("cp")
    tp = lax.axis_index("tp")
    mate = 1 - tp
    is0, is1, is2, is3 = (cp == c for c in range(N_CP))

    bar = pltpu.get_barrier_semaphore()
    pl.semaphore_signal(bar, inc=1, device_id={"tp": mate}, device_id_type=MESH)
    for d in range(1, 4):
        pl.semaphore_signal(bar, inc=1, device_id={"cp": lax.rem(cp + d, 4)}, device_id_type=MESH)

    def wtile(src, col, slot):
        rows = pl.ds(0, src.shape[0])
        return pltpu.make_async_copy(src.at[:, pl.ds(col, TN)], wbuf.at[slot, rows], w_sem.at[slot])

    def wstart(src, j):
        wtile(src, wcol(j), parity(j)).start()

    def wcol(j):
        return mo(j * TN, TN)

    def issue_b(j):
        kv = j < 16
        for cond, w, tile in (
            (kv & (parity(j) == 0), wkl, j // 2),
            (kv & (parity(j) == 1), wvl, j // 2),
            ((j >= 16) & (j < 24), wql, j - 16),
            (j >= 24, wgl, j - 24),
        ):

            @pl.when(cond)
            def _(w=w, tile=tile):
                wtile(w, wcol(tile), parity(j)).start()

    def wait_w(slot, src=wqa):
        wtile(src, 0, slot).wait()

    def fetch_next(j, count, go, then):
        @pl.when(j + 1 < count)
        def _():
            go(j + 1)

        @pl.when(j + 1 >= count)
        def _():
            then()

    def own_row(i):
        return mo((tp * 8 + 2 * i) * TOK, TOK)

    def oth_row(i):
        return mo((mate * 8 + 2 * i) * TOK, TOK)

    def x_copies(top, bot):
        return (
            pltpu.make_async_copy(top, x.at[pl.ds(0, OWN)], x_sem.at[0]),
            pltpu.make_async_copy(bot, x.at[pl.ds(OWN, OWN)], x_sem.at[1]),
        )

    def x_from_hid(i):
        return x_copies(hid.at[pl.ds(own_row(i), OWN)], hid.at[pl.ds(oth_row(i), OWN)])

    def x_from_h1(i):
        return x_copies(h1own.at[i], h1oth.at[i])

    def start_x_a(i):
        for c in x_from_hid(i):
            c.start()

    def start_x_b(i):
        ag_wait_recv(LA, i)
        for c in x_from_h1(i):
            c.start()

    def rs_copy(n, i, col, width):
        return pltpu.make_async_remote_copy(
            src_ref=pt.at[n, i, pl.ds(OWN, OWN), pl.ds(col, width)],
            dst_ref=prec.at[n, i, :, pl.ds(col, width)],
            send_sem=rs_send.at[n, i],
            recv_sem=rs_recv.at[n, i],
            device_id={"tp": mate},
            device_id_type=MESH,
        )

    def ag_copy(n, i, row, rows):
        if n == 0:
            src = h1own.at[i, pl.ds(row, rows)]
            dst = h1oth.at[i, pl.ds(row, rows)]
        else:
            src = out.at[pl.ds(mo(own_row(i) + row, RB), rows)]
            dst = src
        return pltpu.make_async_remote_copy(
            src_ref=src,
            dst_ref=dst,
            send_sem=ag_send.at[n, i],
            recv_sem=ag_recv.at[n, i],
            device_id={"tp": mate},
            device_id_type=MESH,
        )

    def ag_wait_recv(n, i):
        if n == 0:
            ag_copy(0, i, 0, OWN).wait_recv()
        else:
            oth = out.at[pl.ds(oth_row(i), OWN)]
            pltpu.make_async_remote_copy(
                src_ref=oth,
                dst_ref=oth,
                send_sem=ag_send.at[n, i],
                recv_sem=ag_recv.at[n, i],
                device_id={"tp": mate},
                device_id_type=MESH,
            ).wait_recv()

    def kv_copy(i, n, src, own, dst_cp, send):
        cols = pl.ds(n * TN, TN)
        return pltpu.make_async_remote_copy(
            src_ref=kvh.at[i, :, cols] if own else kvr.at[i, src, :, cols],
            dst_ref=kvr.at[i, src, :, cols],
            send_sem=kv_send.at[i, n, send],
            recv_sem=kv_recv.at[i, n, src],
            device_id={"cp": dst_cp},
            device_id_type=MESH,
        )

    def kv_sends(i, h, go):
        @pl.when(is0)
        def _():
            go(kv_copy(i, h, 0, True, 2, 0))
            go(kv_copy(i, h, 0, True, 1, 1))

        @pl.when(is1)
        def _():
            go(kv_copy(i, h, 1, True, 3, 0))

        @pl.when(is2)
        def _():
            go(kv_copy(i, h, 2, True, 3, 0))

    def st_copy(i, g):
        return pltpu.make_async_remote_copy(
            src_ref=sth.at[i, g],
            dst_ref=str_.at[i, g],
            send_sem=st_send.at[i, g],
            recv_sem=st_recv.at[i, g],
            device_id={"cp": lax.rem(cp + 1, 4)},
            device_id_type=MESH,
        )

    def ss_copy(i):
        return pltpu.make_async_remote_copy(
            src_ref=ssx.at[i],
            dst_ref=ssr.at[i],
            send_sem=ss_send.at[i],
            recv_sem=ss_recv.at[i],
            device_id={"tp": mate},
            device_id_type=MESH,
        )

    def norm_loads(n, i, r, start):
        slot = lax.rem(r, N_BUF)
        rows = pl.ds(mo(r * RB, RB), RB)
        copies = [
            pltpu.make_async_copy(pt.at[n, i, rows], nb_p.at[slot], nl_sem.at[slot, 0]),
            pltpu.make_async_copy(prec.at[n, i, rows], nb_r.at[slot], nl_sem.at[slot, 1]),
        ]
        res_a = hid.at[pl.ds(mo(own_row(i) + r * RB, RB), RB)]
        res_b = h1own.at[i, rows]
        for layer, res in ((LA, res_a), (LB, res_b)):

            @pl.when(n == layer)
            def _(res=res):
                c = pltpu.make_async_copy(res, nb_h.at[slot], nl_sem.at[slot, 2])
                c.start() if start else c.wait()

        for c in copies:
            c.start() if start else c.wait()

    def norm_begin(n, i):
        with jax.named_scope("norm_wait"):
            rs_copy(n, i, 0, DM).wait_recv()

            @pl.when(n == LB)
            def _():
                ss_copy(i).wait_recv()
                for b in range(2):
                    whole = ssx[i, b : b + 1, :] + ssr[i, b + 2 : b + 3, :]
                    inv = lax.rsqrt(whole / float(2 * W) + EPS)
                    rsb[blk(b), :] = jnp.broadcast_to(inv, (TOK, TOK)).T

            @pl.when(n == LA)
            def _():
                rsb[...] = jnp.ones_like(rsb)

            for r in range(N_BUF - 1):
                norm_loads(n, i, r, True)

    def norm_ready(n, i, r):
        @pl.when(r + N_BUF - 1 < N_RB)
        def _():
            norm_loads(n, i, r + N_BUF - 1, True)

        norm_loads(n, i, r, False)

    def norm_rows(n, r):
        slot = lax.rem(r, N_BUF)
        alpha = alphas[n]
        for q in range(RB // 16):
            rows = slice(q * 16, (q + 1) * 16)
            both = nb_p[slot, rows, :].astype(F32) + nb_r[slot, rows, :].astype(F32)
            both = both * rsb[pl.ds(mo(r * RB + q * 16, 16), 16), 0:1]
            h = alpha * nb_h[slot, rows, :].astype(F32) + both
            inv = lax.rsqrt(jnp.mean(h * h, axis=-1, keepdims=True) + EPS)
            nout[slot, rows, :] = (h * inv * gains[pl.ds(n, 1), :]).astype(BF)

    def norm_store(n, i, r, start, end):
        slot = lax.rem(r, N_BUF)
        if end:
            c = pltpu.make_async_copy(nout.at[slot], last.at[pl.ds(mo(r * RB, RB), RB)], no_sem.at[slot])
            c.start() if start else c.wait()
            return
        dst_a = h1own.at[i, pl.ds(mo(r * RB, RB), RB)]
        dst_b = out.at[pl.ds(mo(own_row(i) + r * RB, RB), RB)]
        for layer, dst in ((LA, dst_a), (LB, dst_b)):

            @pl.when(n == layer)
            def _(layer=layer, dst=dst):
                c = pltpu.make_async_copy(nout.at[slot], dst, no_sem.at[slot])
                if start:
                    c.start()
                else:
                    c.wait()
                    ag_copy(layer, i, mo(r * RB, RB), RB).start()

    def norm_out(n, i, r, end):
        @pl.when(r >= 2)
        def _():
            norm_store(n, i, r - 2, False, end)

        norm_store(n, i, r, True, end)

    def norm_end(n, i, end):
        for r in range(N_RB - 2, N_RB):
            norm_store(n, i, r, False, end)

    def norm(n, i, end=False):
        norm_begin(n, i)
        with jax.named_scope("norm"):

            @pl.loop(0, N_RB)
            def _(r):
                norm_ready(n, i, r)
                norm_rows(n, r)
                norm_out(n, i, r, end)

            norm_end(n, i, end)

    def out_proj(n, i, wo, then, pre, rows, send):
        def put(j, slot):
            size = pl.ds(0, rows.size)
            return pltpu.make_async_copy(ost.at[slot, size], pt.at[n, i, rows, pl.ds(wcol(j), TN)], o_sem.at[slot])

        def send_on(j, slot):
            put(j, slot).wait()

            @pl.when(send)
            def _():
                rs_copy(n, i, wcol(j), TN).start()

        with jax.named_scope("out_proj"):
            wtile(wo, TN, 1).start()

            @pl.loop(0, N_WO)
            def _(j):
                slot = parity(j)
                wait_w(slot, wo)

                @pl.when(j == 8)
                def _():
                    pre()

                ost[slot, 0 : rows.size, :] = dot(u[rows, :], wbuf[slot, 0:W, :]).astype(BF)

                @pl.when(j + 2 < N_WO)
                def _():
                    wstart(wo, j + 2)

                @pl.when(j + 2 == N_WO)
                def _():
                    then()

                @pl.when(j >= 1)
                def _():
                    send_on(j - 1, 1 - slot)

                put(j, slot).start()

            send_on(N_WO - 1, 1)

    def rotate(a, kind, dst, row, col):
        for b in range(a.shape[0] // TOK):
            for h in range(TN // HD):
                v = a[b * TOK : (b + 1) * TOK, h * HD : (h + 1) * HD]
                v = v * rope[kind, 0] + pltpu.roll(v, HD - 32, 1) * rope[kind, 1] + pltpu.roll(v, 32, 1) * rope[kind, 2]
                kvq[dst, pl.ds(mo(row + b * TOK, TOK), TOK), pl.ds(mo(col + h * HD, HD), HD)] = v.astype(BF)

    def kv_wait(i):
        def got(n, src):
            kv_copy(i, n, src, False, 0, 0).wait_recv()

        def fetch(c):
            return pltpu.make_async_copy(kvr.at[i, c], kvq.at[K, :, pl.ds(c * KVW, KVW)], kvl_sem.at[c])

        with jax.named_scope("kv_wait"):
            for n in range(2):

                @pl.when(is2)
                def _(n=n):
                    got(n, 0)
                    kv_copy(i, n, 0, False, 3, 1).start()

                @pl.when(is3)
                def _(n=n):
                    got(n, 1)
                    kv_copy(i, n, 1, False, 2, 0).start()

            for n in range(2):

                @pl.when(is1)
                def _(n=n):
                    got(n, 0)

                @pl.when(is2)
                def _(n=n):
                    got(n, 1)

                @pl.when(is3)
                def _(n=n):
                    got(n, 2)
                    got(n, 0)

            for go in (lambda c: c.start(), lambda c: c.wait()):
                for c in range(N_CP - 1):

                    @pl.when(cp > c)
                    def _(c=c, go=go):
                        go(fetch(c))

    def attention(first, count):
        scale = math.log2(math.e) / math.sqrt(HD)
        with jax.named_scope("attn"):
            for c in range(N_CP):

                @pl.when(cp == c)
                def _(c=c):
                    cols = [OWN_KV] + [b * KVW for b in range(c)]

                    @pl.loop(0, 4 * count)
                    def _(t):
                        g = lax.rem(t, 4)
                        seq = pl.ds(mo(first + t // 4 * TOK, TOK), TOK)
                        ks = [kvq[K, seq, pl.ds(mo(o + g * HD, HD), HD)] for o in cols]
                        vs = [kvq[K, seq, pl.ds(mo(o + TN + g * HD, HD), HD)] for o in cols]
                        keys = jnp.concatenate(ks, axis=0) if c else ks[0]
                        vals = jnp.concatenate(vs, axis=0) if c else vs[0]
                        row = lax.rem(lax.broadcasted_iota(jnp.int32, (2 * TOK, TOK), 0), TOK)
                        causal = lax.broadcasted_iota(jnp.int32, (2 * TOK, TOK), 1) <= row

                        def heads(p):
                            return [pl.ds(mo((g * 8 + 2 * p + z) * HD, HD), HD) for z in range(2)]

                        scores = []
                        for p in range(4):
                            qs = jnp.concatenate([kvq[Q, seq, o] for o in heads(p)], axis=0)
                            scores.append(dot(qs, keys, NT_DIMS))
                        for p in range(4):
                            s = scores[p]
                            own = jnp.where(causal, s[:, :TOK], -jnp.inf)
                            s = jnp.concatenate([own, s[:, TOK:]], axis=1) if c else own
                            m = jnp.max(s, axis=1, keepdims=True)
                            e = jnp.exp2((s - m) * scale)
                            o = dot(e.astype(BF), vals) * (1.0 / jnp.sum(e, axis=1, keepdims=True))
                            for z in range(2):
                                u[seq, heads(p)[z]] = o[z * TOK : (z + 1) * TOK].astype(BF)

    def layer_a(i, mid, then, pre):
        with jax.named_scope("x_a"):
            for c in x_from_hid(i):
                c.wait()

        def kv_out(n):
            cols = pl.ds(n * TN, TN)
            return pltpu.make_async_copy(kvq.at[K, :, pl.ds(OWN_KV + n * TN, TN)], kvh.at[i, :, cols], kvo_sem.at[n])

        def finish(j, slot):
            kv = j < 2
            col = jnp.where(kv, OWN_KV + j * TN, (j - 2) * TN)
            rotate(acc.at[slot], jnp.where(j == 1, 1, 0), jnp.where(kv, K, Q), 0, col)

        with jax.named_scope("qkv_a"):

            @pl.loop(0, N_QKV)
            def _(j):
                slot = parity(j)
                wait_w(slot)

                @pl.when(j == 0)
                def _():
                    wtile(wva, 0, 1).start()

                @pl.when(j >= 1)
                def _():
                    fetch_next(j, N_QKV, lambda t: wstart(wqa, t - 2), lambda: wtile(woa, 0, 0).start())

                for n in range(2):

                    @pl.when(j == n + 2)
                    def _(n=n):
                        kv_out(n).wait()
                        kv_sends(i, n, lambda c: c.start())

                finish(jnp.maximum(j - 1, 0), 1 - slot)
                acc[slot] = dot(x[...], wbuf[slot])

                for n in range(2):

                    @pl.when(j == n + 1)
                    def _(n=n):
                        kv_out(n).start()

                mid(j)

            finish(N_QKV - 1, 1)

        kv_wait(i)

        @pl.when(i > 0)
        def _():
            attention(0, N_SEQ)
            out_proj(LA, i, woa, then, pre, pl.ds(0, ROWS), True)

        @pl.when(i == 0)
        def _():
            @pl.loop(0, 2)
            def _(h):
                first = mo(OWN * (1 - h), OWN)
                attention(first, 2)

                def then_a():
                    @pl.when(h == 0)
                    def _():
                        wtile(woa, 0, 0).start()

                    @pl.when(h == 1)
                    def _():
                        then()

                def pre_a():
                    @pl.when(h == 1)
                    def _():
                        pre()

                out_proj(LA, 0, woa, then_a, pre_a, pl.ds(first, OWN), h == 0)

    def key_decay(h):
        back = lax.broadcasted_iota(jnp.int32, (TOK, HD), 0).astype(F32) - (TOK - 1.0)
        return jnp.exp(slopes[h] * back)

    def state_of(g, b, hh, kd):
        rows = blk(b)
        col = hcol(g, hh)
        k = (kvq[K, rows, col].astype(F32) * kd).astype(BF)
        return dot(k, kvq[V, rows, col], TN_DIMS)

    def block_decay(h):
        return jnp.exp(jnp.full((8, HD), -float(TOK), F32) * slopes[h])[0:1, :]

    def st_store(i, g, slot):
        return pltpu.make_async_copy(stg.at[slot], sth.at[i, g], sto_sem.at[slot])

    def st_load(i, g, slot):
        return pltpu.make_async_copy(str_.at[i, g], pst.at[slot], stl_sem.at[slot])

    def next_state(g):
        slot = parity(g)
        for hh in range(4):
            kd = key_decay(4 * g + hh)
            bd = block_decay(4 * g + hh)
            new = [state_of(g, b, hh, kd) for b in range(N_SEQ)]
            for b in range(N_SEQ):
                stg[slot, b * 4 + hh] = new[b] + bd * pst[slot, b * 4 + hh]

    def local_state(i, g):
        slot = parity(g)

        @pl.when(is1)
        def _():
            st_load(i, g, slot).wait()

        @pl.when(is0)
        def _():
            for hh in range(N_SEQ):
                kd = key_decay(4 * g + hh)
                for b in range(N_SEQ):
                    stg[slot, b * 4 + hh] = state_of(g, b, hh, kd)

        @pl.when(is1)
        def _():
            for hh in range(N_SEQ):
                kd = key_decay(4 * g + hh)
                bd = block_decay(4 * g + hh)
                for b in range(N_SEQ):
                    stg[slot, b * 4 + hh] = state_of(g, b, hh, kd) + bd * pst[slot, b * 4 + hh]

        st_store(i, g, slot).start()

    def st_send_on(i, g):
        st_store(i, g, parity(g)).wait()
        st_copy(i, g).start()

    def layer_b(i, mid, then, pre):
        with jax.named_scope("x_b"):
            for c in x_from_h1(i):
                c.wait()

        def finish(j, a):
            kv = j < 16
            dst = jnp.where(kv, parity(j), Q)
            kvq[dst, :, pl.ds(wcol(jnp.where(kv, j // 2, j - 16)), TN)] = (a * sigmoid(a)).astype(BF)

        with jax.named_scope("qkv_b"):
            @pl.loop(0, 24)
            def _(j):
                slot = parity(j)
                wait_w(slot)
                issue_b(j + 1)

                e = j - jnp.where(is0, 0, 2)
                busy = (cp <= 1) & (e >= 1) & (e <= 16)
                g = e // 2

                @pl.when(busy & (parity(e) == 1) & is1)
                def _():
                    st_copy(i, g).wait_recv()
                    st_load(i, g, parity(g)).start()

                finish(j, dot(x[...], wbuf[slot]))

                @pl.when(busy & (parity(e) == 0))
                def _():
                    st_send_on(i, g - 1)

                @pl.when(busy & (parity(e) == 1))
                def _():
                    local_state(i, g)

                mid(j)

        with jax.named_scope("gate"):

            @pl.loop(0, 8)
            def _(j):
                slot = parity(j)
                wait_w(slot)
                fetch_next(j, 8, lambda t: issue_b(t + 24), lambda: wtile(wol, 0, 0).start())

                @pl.when(is2)
                def _():
                    st_copy(i, j).wait_recv()
                    st_load(i, j, slot).start()

                gbuf[:, pl.ds(wcol(j), TN)] = sigmoid(dot(x[...], wbuf[slot]))

                @pl.when(is2)
                def _():
                    st_load(i, j, slot).wait()
                    next_state(j)
                    st_store(i, j, slot).start()

                    @pl.when(j >= 1)
                    def _():
                        st_send_on(i, j - 1)

        with jax.named_scope("lin"):

            @pl.when(is2)
            def _():
                st_send_on(i, N_G - 1)

            ss[...] = jnp.zeros_like(ss)

            def fetch(g):
                @pl.when(is3)
                def _():
                    st_copy(i, g).wait_recv()

                @pl.when(cp >= 1)
                def _():
                    st_load(i, g, parity(g)).start()

            @pl.when(is0)
            def _():
                pst[...] = jnp.zeros_like(pst)

            fetch(0)

            @pl.loop(0, N_G)
            def _(g):
                slot = parity(g)

                @pl.when(g + 1 < N_G)
                def _():
                    fetch(g + 1)

                for hh in range(4):
                    lam = slopes[4 * g + hh]
                    row = lax.broadcasted_iota(jnp.int32, (TOK, HD), 0).astype(F32)
                    lane = lax.broadcasted_iota(jnp.int32, (TOK, HD), 1).astype(F32)
                    gap = row - lane
                    wtab[hh, 0] = jnp.where(gap >= 0, jnp.exp(-lam * jnp.maximum(gap, 0.0)), 0.0)
                    wtab[hh, 1] = jnp.exp(-lam * (row + 1.0))

                @pl.when(cp >= 1)
                def _():
                    st_load(i, g, slot).wait()

                @pl.loop(0, 2)
                def _(half):
                    pairs = [(half * 2 + z, hh) for z in range(2) for hh in range(4)]
                    at = [(blk(b), hcol(g, hh)) for b, hh in pairs]
                    qs = [kvq[Q, r, c] for r, c in at]
                    inner = [dot(q, kvq[K, r, c], NT_DIMS) for q, (r, c) in zip(qs, at)]
                    prior = [dot(q, pst[slot, b * 4 + hh].astype(BF)) for q, (b, hh) in zip(qs, pairs)]
                    o = [
                        dot((s * wtab[hh, 0]).astype(BF), kvq[V, r, c]) + p * wtab[hh, 1]
                        for s, p, (r, c), (b, hh) in zip(inner, prior, at, pairs)
                    ]
                    for v, (r, c) in zip(o, at):
                        u[r, c] = (v * ginner[0:1, c] * gbuf[r, c]).astype(BF)
                    for z in range(2):
                        ss[at[4 * z][0], :] += sum(v * v for v in o[4 * z : 4 * z + 4])

            sums = [jnp.sum(ss[blk(b), :].T, axis=0, keepdims=True) for b in range(N_SEQ)]
            ssx[i] = jnp.concatenate(sums + sums, axis=0)

        def then_ss():
            ss_copy(i).start()
            pre()

        out_proj(LB, i, wol, then, then_ss, pl.ds(0, ROWS), True)

    wtile(wka, 0, 0).start()
    start_x_a(0)
    rope_in = pltpu.make_async_copy(rope_hbm.at[cp], rope.at[0], kvo_sem.at[0])
    rope_in.start()
    gains[0:1, :] = gain_a[...]
    gains[1:2, :] = gain_b[...]
    rope[1, 0] = jnp.ones((TOK, HD), F32)
    rope[1, 1] = jnp.zeros((TOK, HD), F32)
    rope[1, 2] = jnp.zeros((TOK, HD), F32)
    rope_in.wait()
    pl.semaphore_wait(bar, 4)

    @pl.loop(0, 7)
    def _(s):
        @pl.when((s < 3) | (s == 4))
        def _():
            def mid_a(j):
                @pl.when((s == 1) & (j == 5))
                def _():
                    norm(LA, 0)

            def then_a():
                @pl.when(s < 2)
                def _():
                    wtile(wka, 0, 0).start()

                @pl.when(s >= 2)
                def _():
                    wtile(wkl, 0, 0).start()

            def pre_a():
                @pl.when(s < 2)
                def _():
                    start_x_a(s + 1)

                @pl.when(s >= 2)
                def _():
                    start_x_b(jnp.where(s == 2, 0, 1))

            layer_a(jnp.where(s < 3, s, 3), mid_a, then_a, pre_a)

        @pl.when(s == 2)
        def _():
            norm(LA, 1)

        @pl.when(s >= 3)
        def _():
            def mid_b(j):
                now = jnp.where(s == 4, 3, jnp.where(s == 6, 19, 15))

                @pl.when(j == now)
                def _():
                    norm(jnp.where(s == 3, LA, LB), jnp.where(s == 3, 2, s - 4))

            def then_b():
                @pl.when(s == 3)
                def _():
                    wtile(wka, 0, 0).start()

                @pl.when((s > 3) & (s < 6))
                def _():
                    wtile(wkl, 0, 0).start()

            def pre_b():
                @pl.when(s == 3)
                def _():
                    start_x_a(3)

                @pl.when((s > 3) & (s < 6))
                def _():
                    start_x_b(s - 2)

            layer_b(s - 3, mid_b, then_b, pre_b)

        @pl.when(s == 4)
        def _():
            norm(LA, 3)

    norm(LB, 3, end=True)

    for i in range(N_CH):
        for n in range(2):
            rs_copy(n, i, 0, DM).wait_send()
            if n == LA or i < N_CH - 1:
                ag_copy(n, i, 0, OWN).wait_send()
        if i < N_CH - 1:
            ag_wait_recv(LB, i)
        ss_copy(i).wait_send()

        for h in range(2):
            kv_sends(i, h, lambda c: c.wait_send())

            @pl.when(is2)
            def _(i=i, h=h):
                kv_copy(i, h, 0, False, 3, 1).wait_send()

            @pl.when(is3)
            def _(i=i, h=h):
                kv_copy(i, h, 1, False, 2, 0).wait_send()

        @pl.when(cp <= 2)
        def _(i=i):
            @pl.loop(0, 8)
            def _(g):
                st_copy(i, g).wait_send()


def assemble(rows, last, res, buf, in_sem, out_sem):
    tp = lax.axis_index("tp")
    n = 2 * N_CH - 1

    def block(k):
        half = jnp.where(k < N_CH, tp, 1 - tp)
        return pl.ds(mo((half * N_CH + lax.rem(k, N_CH)) * OWN, OWN), OWN)

    def load(k):
        src = last if k == N_CH - 1 else rows.at[block(k)]
        return pltpu.make_async_copy(src, buf.at[k % N_CH], in_sem.at[k % N_CH])

    def store(k):
        return pltpu.make_async_copy(buf.at[k % N_CH], res.at[block(k)], out_sem.at[k % N_CH])

    for k in range(N_CH):
        load(k).start()
    for k in range(n):
        load(k).wait()
        store(k).start()
        if k >= 1 and k + N_CH - 1 < n:
            store(k - 1).wait()
            load(k + N_CH - 1).start()
    for k in range(n - N_CH, n):
        store(k).wait()


def solution(mesh):
    n_cp = mesh.shape["cp"]
    table = rope_tables(n_cp)
    any_ = pl.BlockSpec(memory_space=pl.ANY)
    smem = pl.BlockSpec(memory_space=pltpu.SMEM)
    vmem = pl.BlockSpec(memory_space=pltpu.VMEM)
    dma = pltpu.SemaphoreType.DMA
    two = (2,)

    def body(hidden, alphas, wqa, wka, wva, woa, gain_attn, wql, wkl, wvl, wgl, slopes, gain_inner, wol, gain_lin):
        shape = hidden.shape
        hid = hidden.reshape(shape[0] * shape[1], shape[2])
        sds = jax.ShapeDtypeStruct
        outs = (
            sds(hid.shape, BF),
            sds((OWN, DM), BF),
            sds((2, N_CH, ROWS, DM), BF),
            sds((2, N_CH, OWN, DM), BF),
            sds((N_CH, OWN, DM), BF),
            sds((N_CH, OWN, DM), BF),
            sds((N_CH, ROWS, KVW), BF),
            sds((N_CH, 3, ROWS, KVW), BF),
            sds((N_CH, N_G, 16, HD, HD), F32),
            sds((N_CH, N_G, 16, HD, HD), F32),
        )
        scratch = [
            pltpu.VMEM((2, DM, TN), BF),
            pltpu.VMEM((ROWS, DM), BF),
            pltpu.VMEM((3, ROWS, W), BF),
            pltpu.VMEM((ROWS, W), F32),
            pltpu.VMEM((ROWS, W), BF),
            pltpu.VMEM((2, ROWS, TN), F32),
            pltpu.VMEM((2, ROWS, TN), BF),
            pltpu.VMEM((2, 16, HD, HD), F32),
            pltpu.VMEM((2, 16, HD, HD), F32),
            pltpu.VMEM((N_BUF, RB, DM), BF),
            pltpu.VMEM((N_BUF, RB, DM), BF),
            pltpu.VMEM((N_BUF, RB, DM), BF),
            pltpu.VMEM((N_BUF, RB, DM), BF),
            pltpu.VMEM((ROWS, HD), F32),
            pltpu.VMEM((OWN, HD), F32),
            pltpu.VMEM((2, 3, TOK, HD), F32),
            pltpu.VMEM((N_CH, 8, HD), F32),
            pltpu.VMEM((N_CH, 8, HD), F32),
            pltpu.VMEM((4, 2, TOK, HD), F32),
            pltpu.VMEM((2, DM), F32),
            dma(two), dma(two), dma(two), dma(two), dma((3,)), dma(two), dma(two), dma((N_BUF, 3)), dma((N_BUF,)),
            dma((2, N_CH)), dma((2, N_CH)), dma((2, N_CH)), dma((2, N_CH)), dma((N_CH, 2, 2)), dma((N_CH, 2, 3)), dma((N_CH, N_G)), dma((N_CH, N_G)),
            dma((N_CH,)), dma((N_CH,)),
        ]
        res = pl.pallas_call(
            kernel,
            out_shape=outs,
            in_specs=[any_] * 11 + [smem, smem, vmem, vmem, vmem],
            out_specs=tuple(any_ for _ in outs),
            scratch_shapes=scratch,
            compiler_params=pltpu.CompilerParams(
                collective_id=0, has_side_effects=True, vmem_limit_bytes=VMEM_BYTES
            ),
            name="layers",
        )(
            hid, wqa, wka, wva, woa, wql, wkl, wvl, wgl, wol, jnp.asarray(table), alphas, slopes, gain_attn.reshape(1, -1),
            gain_lin.reshape(1, -1), gain_inner.reshape(1, -1),
        )
        got = lax.ppermute(res[1], "tp", [(0, 1), (1, 0)])
        rows = pl.pallas_call(
            assemble,
            out_shape=sds(hid.shape, BF),
            in_specs=[any_, any_],
            out_specs=any_,
            scratch_shapes=[pltpu.VMEM((N_CH, OWN, DM), BF), dma((N_CH,)), dma((N_CH,))],
            compiler_params=pltpu.CompilerParams(vmem_limit_bytes=VMEM_BYTES),
            cost_estimate=pl.CostEstimate(flops=10**11, bytes_accessed=2 * hid.size * 2, transcendentals=0),
            name="assemble",
        )(res[0], res[1])
        row = ((1 - lax.axis_index("tp")) * N_CH + N_CH - 1) * OWN
        return lax.dynamic_update_slice(rows, got, (row, 0)).reshape(shape)

    act = P("dp", "cp", None)
    rep = P()
    col = P(None, "tp")
    row = P("tp", None)
    vec = P("tp")
    in_specs = (act, rep, col, col, col, row, rep, col, col, col, col, vec, vec, row, rep)
    return jax.shard_map(body, mesh=mesh, in_specs=in_specs, out_specs=act, check_vma=False)
```

```python
import math

import jax
import jax.numpy as jnp
import numpy as np
from jax import lax
from jax.experimental import pallas as pl
from jax.experimental.pallas import tpu as pltpu
from jax.sharding import PartitionSpec as P

MESH = pl.DeviceIdType.MESH
F32 = jnp.float32
BF = jnp.bfloat16
ROPE_BASE = 10000000.0
EPS = 1e-5

VMEM_BYTES = 67043328
TOK = 128
HD = 128
TN = 512
DM = 6144
W = 4096
KVW = 1024
OWN_KV = W - KVW
N_SEQ = 4
N_CH = 4
N_CP = 4
N_G = 8
ROWS = N_SEQ * TOK
OWN = ROWS // 2
RB = 32
N_RB = OWN // RB
R_IN = N_RB - 2
IN_ROWS = R_IN * RB
LAST = OWN - IN_ROWS
N_QKV = (KVW + W) // TN
N_WO = DM // TN
N_BUF = 4
LA, LB = 0, 1
K, V, Q = 0, 1, 2
NT_DIMS = (((1,), (1,)), ((), ()))
TN_DIMS = (((0,), (0,)), ((), ()))


def rope_tables(n_cp):
    half = HD // 4
    inv = ROPE_BASE ** (-np.arange(half, dtype=np.float64) * 2.0 / (2 * half))
    pos = np.arange(n_cp * TOK, dtype=np.float64)
    ang = pos[:, None] * inv[None, :]
    tab = np.zeros((3, n_cp * TOK, HD), np.float32)
    tab[0] = 1.0
    tab[0, :, :half] = np.cos(ang)
    tab[0, :, half : 2 * half] = np.cos(ang)
    tab[1, :, :half] = -np.sin(ang)
    tab[2, :, half : 2 * half] = np.sin(ang)
    return np.ascontiguousarray(tab.reshape(3, n_cp, TOK, HD).transpose(1, 0, 2, 3))


def mo(v, m):
    return pl.multiple_of(v, m)


def parity(j):
    return lax.rem(j, 2)


def blk(b):
    return pl.ds(mo(b * TOK, TOK), TOK)


def hcol(g, hh):
    return pl.ds(mo((4 * g + hh) * HD, HD), HD)


def dot(a, b, dims=(((1,), (0,)), ((), ()))):
    return lax.dot_general(a, b, dims, preferred_element_type=F32)


def sigmoid(z):
    return 1.0 / (1.0 + jnp.exp(-z))


def kernel(
    hid, wqa, wka, wva, woa, wql, wkl, wvl, wgl, wol, rope_hbm, alphas, slopes, gain_a, gain_b, ginner,
    out, last, pt, prec, h1own, h1oth, kvh, kvr, sth, str_,
    wbuf, x, kvq, gbuf, u, acc, ost, stg, pst, nb_p, nb_r, nb_h, nout, ss, rsb, rope, ssx, ssr, wtab, gains,
    w_sem, x_sem, o_sem, kvo_sem, kvl_sem, sto_sem, stl_sem, nl_sem, no_sem,
    rs_send, rs_recv, ag_send, ag_recv, kv_send, kv_recv, st_send, st_recv, ss_send, ss_recv,
):
    cp = lax.axis_index("cp")
    tp = lax.axis_index("tp")
    mate = 1 - tp
    is0, is1, is2, is3 = (cp == c for c in range(N_CP))

    bar = pltpu.get_barrier_semaphore()
    pl.semaphore_signal(bar, inc=1, device_id={"tp": mate}, device_id_type=MESH)
    for d in range(1, 4):
        pl.semaphore_signal(bar, inc=1, device_id={"cp": lax.rem(cp + d, 4)}, device_id_type=MESH)

    def wtile(src, col, slot):
        rows = pl.ds(0, src.shape[0])
        return pltpu.make_async_copy(src.at[:, pl.ds(col, TN)], wbuf.at[slot, rows], w_sem.at[slot])

    def wstart(src, j):
        wtile(src, wcol(j), parity(j)).start()

    def wcol(j):
        return mo(j * TN, TN)

    def issue_b(j):
        kv = j < 16
        for cond, w, tile in (
            (kv & (parity(j) == 0), wkl, j // 2),
            (kv & (parity(j) == 1), wvl, j // 2),
            ((j >= 16) & (j < 24), wql, j - 16),
            (j >= 24, wgl, j - 24),
        ):

            @pl.when(cond)
            def _(w=w, tile=tile):
                wtile(w, wcol(tile), parity(j)).start()

    def wait_w(slot, src=wqa):
        wtile(src, 0, slot).wait()

    def fetch_next(j, count, go, then):
        @pl.when(j + 1 < count)
        def _():
            go(j + 1)

        @pl.when(j + 1 >= count)
        def _():
            then()

    def own_row(i):
        return mo((tp * 8 + 2 * i) * TOK, TOK)

    def oth_row(i):
        return mo((mate * 8 + 2 * i) * TOK, TOK)

    def x_copies(top, bot):
        return (
            pltpu.make_async_copy(top, x.at[pl.ds(0, OWN)], x_sem.at[0]),
            pltpu.make_async_copy(bot, x.at[pl.ds(OWN, OWN)], x_sem.at[1]),
        )

    def x_from_hid(i):
        return x_copies(hid.at[pl.ds(own_row(i), OWN)], hid.at[pl.ds(oth_row(i), OWN)])

    def x_from_h1(i):
        return x_copies(h1own.at[i], h1oth.at[i])

    def start_x_a(i):
        for c in x_from_hid(i):
            c.start()

    def start_x_b(i):
        ag_wait_recv(LA, i)
        for c in x_from_h1(i):
            c.start()

    def rs_copy(n, i, col, width):
        return pltpu.make_async_remote_copy(
            src_ref=pt.at[n, i, pl.ds(OWN, OWN), pl.ds(col, width)],
            dst_ref=prec.at[n, i, :, pl.ds(col, width)],
            send_sem=rs_send.at[n, i],
            recv_sem=rs_recv.at[n, i],
            device_id={"tp": mate},
            device_id_type=MESH,
        )

    def ag_copy(n, i, row, rows):
        if n == 0:
            src = h1own.at[i, pl.ds(row, rows)]
            dst = h1oth.at[i, pl.ds(row, rows)]
        else:
            src = out.at[pl.ds(mo(own_row(i) + row, RB), rows)]
            dst = src
        return pltpu.make_async_remote_copy(
            src_ref=src,
            dst_ref=dst,
            send_sem=ag_send.at[n, i],
            recv_sem=ag_recv.at[n, i],
            device_id={"tp": mate},
            device_id_type=MESH,
        )

    def ag_wait_recv(n, i, rows=OWN):
        if n == 0:
            ag_copy(0, i, 0, rows).wait_recv()
        else:
            oth = out.at[pl.ds(oth_row(i), rows)]
            pltpu.make_async_remote_copy(
                src_ref=oth,
                dst_ref=oth,
                send_sem=ag_send.at[n, i],
                recv_sem=ag_recv.at[n, i],
                device_id={"tp": mate},
                device_id_type=MESH,
            ).wait_recv()

    def half_rows(h):
        return pl.ds(mo(OWN * (1 - h), OWN), OWN)

    def kv_copy(i, n, h, src, own, dst_cp, send):
        at = half_rows(h), pl.ds(n * TN, TN)
        return pltpu.make_async_remote_copy(
            src_ref=kvh.at[i, *at] if own else kvr.at[i, src, *at],
            dst_ref=kvr.at[i, src, *at],
            send_sem=kv_send.at[i, n, h, send],
            recv_sem=kv_recv.at[i, n, h, src],
            device_id={"cp": dst_cp},
            device_id_type=MESH,
        )

    def kv_sends(i, n, go):
        for h in range(2):

            @pl.when(is0)
            def _(h=h):
                go(kv_copy(i, n, h, 0, True, 2, 0))
                go(kv_copy(i, n, h, 0, True, 1, 1))

            @pl.when(is1)
            def _(h=h):
                go(kv_copy(i, n, h, 1, True, 3, 0))

            @pl.when(is2)
            def _(h=h):
                go(kv_copy(i, n, h, 2, True, 3, 0))

    def st_copy(i, g):
        return pltpu.make_async_remote_copy(
            src_ref=sth.at[i, g],
            dst_ref=str_.at[i, g],
            send_sem=st_send.at[i, g],
            recv_sem=st_recv.at[i, g],
            device_id={"cp": lax.rem(cp + 1, 4)},
            device_id_type=MESH,
        )

    def ss_copy(i):
        return pltpu.make_async_remote_copy(
            src_ref=ssx.at[i],
            dst_ref=ssr.at[i],
            send_sem=ss_send.at[i],
            recv_sem=ss_recv.at[i],
            device_id={"tp": mate},
            device_id_type=MESH,
        )

    def norm_loads(n, i, r, start):
        slot = lax.rem(r, N_BUF)
        rows = pl.ds(mo(r * RB, RB), RB)
        copies = [
            pltpu.make_async_copy(pt.at[n, i, rows], nb_p.at[slot], nl_sem.at[slot, 0]),
            pltpu.make_async_copy(prec.at[n, i, rows], nb_r.at[slot], nl_sem.at[slot, 1]),
        ]
        res_a = hid.at[pl.ds(mo(own_row(i) + r * RB, RB), RB)]
        res_b = h1own.at[i, rows]
        for layer, res in ((LA, res_a), (LB, res_b)):

            @pl.when(n == layer)
            def _(res=res):
                c = pltpu.make_async_copy(res, nb_h.at[slot], nl_sem.at[slot, 2])
                c.start() if start else c.wait()

        for c in copies:
            c.start() if start else c.wait()

    def norm_begin(n, i):
        with jax.named_scope("norm_wait"):
            rs_copy(n, i, 0, DM).wait_recv()

            @pl.when(n == LB)
            def _():
                ss_copy(i).wait_recv()
                for b in range(2):
                    whole = ssx[i, b : b + 1, :] + ssr[i, b + 2 : b + 3, :]
                    inv = lax.rsqrt(whole / float(2 * W) + EPS)
                    rsb[blk(b), :] = jnp.broadcast_to(inv, (TOK, TOK)).T

            @pl.when(n == LA)
            def _():
                rsb[...] = jnp.ones_like(rsb)

            for r in range(N_BUF - 1):
                norm_loads(n, i, r, True)

    def norm_ready(n, i, r):
        @pl.when(r + N_BUF - 1 < N_RB)
        def _():
            norm_loads(n, i, r + N_BUF - 1, True)

        norm_loads(n, i, r, False)

    def norm_rows(n, r):
        slot = lax.rem(r, N_BUF)
        alpha = alphas[n]
        for q in range(RB // 16):
            rows = slice(q * 16, (q + 1) * 16)
            both = nb_p[slot, rows, :].astype(F32) + nb_r[slot, rows, :].astype(F32)
            both = both * rsb[pl.ds(mo(r * RB + q * 16, 16), 16), 0:1]
            h = alpha * nb_h[slot, rows, :].astype(F32) + both
            inv = lax.rsqrt(jnp.mean(h * h, axis=-1, keepdims=True) + EPS)
            nout[slot, rows, :] = (h * inv * gains[pl.ds(n, 1), :]).astype(BF)

    def norm_store(n, i, r, start, end):
        slot = lax.rem(r, N_BUF)
        dst_a = h1own.at[i, pl.ds(mo(r * RB, RB), RB)]
        dst_b = out.at[pl.ds(mo(own_row(i) + r * RB, RB), RB)]
        inside = r < R_IN if end else True
        if end:

            @pl.when(r >= R_IN)
            def _():
                c = pltpu.make_async_copy(nout.at[slot], last.at[pl.ds(mo((r - R_IN) * RB, RB), RB)], no_sem.at[slot])
                c.start() if start else c.wait()

        for layer, dst in ((LA, dst_a), (LB, dst_b)):

            @pl.when((n == layer) & inside)
            def _(layer=layer, dst=dst):
                c = pltpu.make_async_copy(nout.at[slot], dst, no_sem.at[slot])
                if start:
                    c.start()
                else:
                    c.wait()
                    ag_copy(layer, i, mo(r * RB, RB), RB).start()

    def norm_out(n, i, r, end):
        @pl.when(r >= 2)
        def _():
            norm_store(n, i, r - 2, False, end)

        norm_store(n, i, r, True, end)

    def norm_end(n, i, end):
        for r in range(N_RB - 2, N_RB):
            norm_store(n, i, r, False, end)

    def norm(n, i, end=False):
        norm_begin(n, i)
        with jax.named_scope("norm"):

            @pl.loop(0, N_RB)
            def _(r):
                norm_ready(n, i, r)
                norm_rows(n, r)
                norm_out(n, i, r, end)

            norm_end(n, i, end)

    def out_proj(n, i, wo, then, pre, rows, send):
        def put(j, slot):
            size = pl.ds(0, rows.size)
            return pltpu.make_async_copy(ost.at[slot, size], pt.at[n, i, rows, pl.ds(wcol(j), TN)], o_sem.at[slot])

        def send_on(j, slot):
            put(j, slot).wait()

            @pl.when(send)
            def _():
                rs_copy(n, i, wcol(j), TN).start()

        with jax.named_scope("out_proj"):
            wtile(wo, TN, 1).start()

            @pl.loop(0, N_WO)
            def _(j):
                slot = parity(j)
                wait_w(slot, wo)

                @pl.when(j == 8)
                def _():
                    pre()

                ost[slot, 0 : rows.size, :] = dot(u[rows, :], wbuf[slot, 0:W, :]).astype(BF)

                @pl.when(j + 2 < N_WO)
                def _():
                    wstart(wo, j + 2)

                @pl.when(j + 2 == N_WO)
                def _():
                    then()

                @pl.when(j >= 1)
                def _():
                    send_on(j - 1, 1 - slot)

                put(j, slot).start()

            send_on(N_WO - 1, 1)

    def rotate(a, kind, dst, row, col):
        for b in range(a.shape[0] // TOK):
            for h in range(TN // HD):
                v = a[b * TOK : (b + 1) * TOK, h * HD : (h + 1) * HD]
                v = v * rope[kind, 0] + pltpu.roll(v, HD - 32, 1) * rope[kind, 1] + pltpu.roll(v, 32, 1) * rope[kind, 2]
                kvq[dst, pl.ds(mo(row + b * TOK, TOK), TOK), pl.ds(mo(col + h * HD, HD), HD)] = v.astype(BF)

    def kv_wait(i, halves):
        parts = [(n, h) for h in halves for n in range(2)]

        def got(n, h, src):
            kv_copy(i, n, h, src, False, 0, 0).wait_recv()

        def fetch(c, h):
            rows = half_rows(h)
            dst = kvq.at[K, rows, pl.ds(c * KVW, KVW)]
            return pltpu.make_async_copy(kvr.at[i, c, rows], dst, kvl_sem.at[c, h])

        with jax.named_scope("kv_wait"):
            for n, h in parts:

                @pl.when(is2)
                def _(n=n, h=h):
                    got(n, h, 0)
                    kv_copy(i, n, h, 0, False, 3, 1).start()

                @pl.when(is3)
                def _(n=n, h=h):
                    got(n, h, 1)
                    kv_copy(i, n, h, 1, False, 2, 0).start()

            for n, h in parts:

                @pl.when(is1)
                def _(n=n, h=h):
                    got(n, h, 0)

                @pl.when(is2)
                def _(n=n, h=h):
                    got(n, h, 1)

                @pl.when(is3)
                def _(n=n, h=h):
                    got(n, h, 2)
                    got(n, h, 0)

            for go in (lambda c: c.start(), lambda c: c.wait()):
                for c in range(N_CP - 1):

                    @pl.when(cp > c)
                    def _(c=c, go=go):
                        for h in halves:
                            go(fetch(c, h))

    def attention(first, count):
        scale = math.log2(math.e) / math.sqrt(HD)
        with jax.named_scope("attn"):
            for c in range(N_CP):

                @pl.when(cp == c)
                def _(c=c):
                    cols = [OWN_KV] + [b * KVW for b in range(c)]

                    @pl.loop(0, 4 * count)
                    def _(t):
                        g = lax.rem(t, 4)
                        seq = pl.ds(mo(first + t // 4 * TOK, TOK), TOK)
                        ks = [kvq[K, seq, pl.ds(mo(o + g * HD, HD), HD)] for o in cols]
                        vs = [kvq[K, seq, pl.ds(mo(o + TN + g * HD, HD), HD)] for o in cols]
                        keys = jnp.concatenate(ks, axis=0) if c else ks[0]
                        vals = jnp.concatenate(vs, axis=0) if c else vs[0]
                        row = lax.rem(lax.broadcasted_iota(jnp.int32, (2 * TOK, TOK), 0), TOK)
                        causal = lax.broadcasted_iota(jnp.int32, (2 * TOK, TOK), 1) <= row

                        def heads(p):
                            return [pl.ds(mo((g * 8 + 2 * p + z) * HD, HD), HD) for z in range(2)]

                        scores = []
                        for p in range(4):
                            qs = jnp.concatenate([kvq[Q, seq, o] for o in heads(p)], axis=0)
                            scores.append(dot(qs, keys, NT_DIMS))
                        for p in range(4):
                            s = scores[p]
                            own = jnp.where(causal, s[:, :TOK], -jnp.inf)
                            s = jnp.concatenate([own, s[:, TOK:]], axis=1) if c else own
                            m = jnp.max(s, axis=1, keepdims=True)
                            e = jnp.exp2((s - m) * scale)
                            o = dot(e.astype(BF), vals) * (1.0 / jnp.sum(e, axis=1, keepdims=True))
                            for z in range(2):
                                u[seq, heads(p)[z]] = o[z * TOK : (z + 1) * TOK].astype(BF)

    def layer_a(i, mid, then, pre):
        with jax.named_scope("x_a"):
            for c in x_from_hid(i):
                c.wait()

        def kv_out(n):
            cols = pl.ds(n * TN, TN)
            return pltpu.make_async_copy(kvq.at[K, :, pl.ds(OWN_KV + n * TN, TN)], kvh.at[i, :, cols], kvo_sem.at[n])

        def finish(j, slot):
            kv = j < 2
            col = jnp.where(kv, OWN_KV + j * TN, (j - 2) * TN)
            rotate(acc.at[slot], jnp.where(j == 1, 1, 0), jnp.where(kv, K, Q), 0, col)

        with jax.named_scope("qkv_a"):

            @pl.loop(0, N_QKV)
            def _(j):
                slot = parity(j)
                wait_w(slot)

                @pl.when(j == 0)
                def _():
                    wtile(wva, 0, 1).start()

                @pl.when(j >= 1)
                def _():
                    fetch_next(j, N_QKV, lambda t: wstart(wqa, t - 2), lambda: wtile(woa, 0, 0).start())

                for n in range(2):

                    @pl.when(j == n + 2)
                    def _(n=n):
                        kv_out(n).wait()
                        kv_sends(i, n, lambda c: c.start())

                finish(jnp.maximum(j - 1, 0), 1 - slot)
                acc[slot] = dot(x[...], wbuf[slot])

                for n in range(2):

                    @pl.when(j == n + 1)
                    def _(n=n):
                        kv_out(n).start()

                mid(j)

            finish(N_QKV - 1, 1)

        @pl.when(i > 0)
        def _():
            kv_wait(i, range(2))
            attention(0, N_SEQ)
            out_proj(LA, i, woa, then, pre, pl.ds(0, ROWS), True)

        @pl.when(i == 0)
        def _():
            @pl.loop(0, 2)
            def _(h):
                first = mo(OWN * (1 - h), OWN)
                kv_wait(0, (h,))
                attention(first, 2)

                def then_a():
                    @pl.when(h == 0)
                    def _():
                        wtile(woa, 0, 0).start()

                    @pl.when(h == 1)
                    def _():
                        then()

                def pre_a():
                    @pl.when(h == 1)
                    def _():
                        pre()

                out_proj(LA, 0, woa, then_a, pre_a, pl.ds(first, OWN), h == 0)

    def key_decay(h):
        back = lax.broadcasted_iota(jnp.int32, (TOK, HD), 0).astype(F32) - (TOK - 1.0)
        return jnp.exp(slopes[h] * back)

    def state_of(g, b, hh, kd):
        rows = blk(b)
        col = hcol(g, hh)
        k = (kvq[K, rows, col].astype(F32) * kd).astype(BF)
        return dot(k, kvq[V, rows, col], TN_DIMS)

    def block_decay(h):
        return jnp.exp(jnp.full((8, HD), -float(TOK), F32) * slopes[h])[0:1, :]

    def st_store(i, g, slot):
        return pltpu.make_async_copy(stg.at[slot], sth.at[i, g], sto_sem.at[slot])

    def st_load(i, g, slot):
        return pltpu.make_async_copy(str_.at[i, g], pst.at[slot], stl_sem.at[slot])

    def next_state(g):
        slot = parity(g)
        for hh in range(4):
            kd = key_decay(4 * g + hh)
            bd = block_decay(4 * g + hh)
            new = [state_of(g, b, hh, kd) for b in range(N_SEQ)]
            for b in range(N_SEQ):
                stg[slot, b * 4 + hh] = new[b] + bd * pst[slot, b * 4 + hh]

    def local_state(i, g):
        slot = parity(g)

        @pl.when(is1)
        def _():
            st_load(i, g, slot).wait()

        @pl.when(is0)
        def _():
            for hh in range(N_SEQ):
                kd = key_decay(4 * g + hh)
                for b in range(N_SEQ):
                    stg[slot, b * 4 + hh] = state_of(g, b, hh, kd)

        @pl.when(is1)
        def _():
            for hh in range(N_SEQ):
                kd = key_decay(4 * g + hh)
                bd = block_decay(4 * g + hh)
                for b in range(N_SEQ):
                    stg[slot, b * 4 + hh] = state_of(g, b, hh, kd) + bd * pst[slot, b * 4 + hh]

        st_store(i, g, slot).start()

    def st_send_on(i, g):
        st_store(i, g, parity(g)).wait()
        st_copy(i, g).start()

    def layer_b(i, mid, then, pre):
        with jax.named_scope("x_b"):
            for c in x_from_h1(i):
                c.wait()

        def finish(j, a):
            kv = j < 16
            dst = jnp.where(kv, parity(j), Q)
            kvq[dst, :, pl.ds(wcol(jnp.where(kv, j // 2, j - 16)), TN)] = (a * sigmoid(a)).astype(BF)

        with jax.named_scope("qkv_b"):
            @pl.loop(0, 24)
            def _(j):
                slot = parity(j)
                wait_w(slot)
                issue_b(j + 1)

                e = j - jnp.where(is0, 0, 2)
                busy = (cp <= 1) & (e >= 1) & (e <= 16)
                g = e // 2

                @pl.when(busy & (parity(e) == 1) & is1)
                def _():
                    st_copy(i, g).wait_recv()
                    st_load(i, g, parity(g)).start()

                finish(j, dot(x[...], wbuf[slot]))

                @pl.when(busy & (parity(e) == 0))
                def _():
                    st_send_on(i, g - 1)

                @pl.when(busy & (parity(e) == 1))
                def _():
                    local_state(i, g)

                mid(j)

        with jax.named_scope("gate"):

            @pl.loop(0, 8)
            def _(j):
                slot = parity(j)
                wait_w(slot)
                fetch_next(j, 8, lambda t: issue_b(t + 24), lambda: wtile(wol, 0, 0).start())

                @pl.when(is2)
                def _():
                    st_copy(i, j).wait_recv()
                    st_load(i, j, slot).start()

                gbuf[:, pl.ds(wcol(j), TN)] = sigmoid(dot(x[...], wbuf[slot]))

                @pl.when(is2)
                def _():
                    st_load(i, j, slot).wait()
                    next_state(j)
                    st_store(i, j, slot).start()

                    @pl.when(j >= 1)
                    def _():
                        st_send_on(i, j - 1)

        with jax.named_scope("lin"):

            @pl.when(is2)
            def _():
                st_send_on(i, N_G - 1)

            ss[...] = jnp.zeros_like(ss)

            def fetch(g):
                @pl.when(is3)
                def _():
                    st_copy(i, g).wait_recv()

                @pl.when(cp >= 1)
                def _():
                    st_load(i, g, parity(g)).start()

            @pl.when(is0)
            def _():
                pst[...] = jnp.zeros_like(pst)

            fetch(0)

            @pl.loop(0, N_G)
            def _(g):
                slot = parity(g)

                @pl.when(g + 1 < N_G)
                def _():
                    fetch(g + 1)

                for hh in range(4):
                    lam = slopes[4 * g + hh]
                    row = lax.broadcasted_iota(jnp.int32, (TOK, HD), 0).astype(F32)
                    lane = lax.broadcasted_iota(jnp.int32, (TOK, HD), 1).astype(F32)
                    gap = row - lane
                    wtab[hh, 0] = jnp.where(gap >= 0, jnp.exp(-lam * jnp.maximum(gap, 0.0)), 0.0)
                    wtab[hh, 1] = jnp.exp(-lam * (row + 1.0))

                @pl.when(cp >= 1)
                def _():
                    st_load(i, g, slot).wait()

                @pl.loop(0, 2)
                def _(half):
                    pairs = [(half * 2 + z, hh) for z in range(2) for hh in range(4)]
                    at = [(blk(b), hcol(g, hh)) for b, hh in pairs]
                    qs = [kvq[Q, r, c] for r, c in at]
                    inner = [dot(q, kvq[K, r, c], NT_DIMS) for q, (r, c) in zip(qs, at)]
                    prior = [dot(q, pst[slot, b * 4 + hh].astype(BF)) for q, (b, hh) in zip(qs, pairs)]
                    o = [
                        dot((s * wtab[hh, 0]).astype(BF), kvq[V, r, c]) + p * wtab[hh, 1]
                        for s, p, (r, c), (b, hh) in zip(inner, prior, at, pairs)
                    ]
                    for v, (r, c) in zip(o, at):
                        u[r, c] = (v * ginner[0:1, c] * gbuf[r, c]).astype(BF)
                    for z in range(2):
                        ss[at[4 * z][0], :] += sum(v * v for v in o[4 * z : 4 * z + 4])

            sums = [jnp.sum(ss[blk(b), :].T, axis=0, keepdims=True) for b in range(N_SEQ)]
            ssx[i] = jnp.concatenate(sums + sums, axis=0)

        def then_ss():
            ss_copy(i).start()
            pre()

        out_proj(LB, i, wol, then, then_ss, pl.ds(0, ROWS), True)

    wtile(wka, 0, 0).start()
    start_x_a(0)
    rope_in = pltpu.make_async_copy(rope_hbm.at[cp], rope.at[0], kvo_sem.at[0])
    rope_in.start()
    gains[0:1, :] = gain_a[...]
    gains[1:2, :] = gain_b[...]
    rope[1, 0] = jnp.ones((TOK, HD), F32)
    rope[1, 1] = jnp.zeros((TOK, HD), F32)
    rope[1, 2] = jnp.zeros((TOK, HD), F32)
    rope_in.wait()
    pl.semaphore_wait(bar, 4)

    @pl.loop(0, 7)
    def _(s):
        @pl.when((s < 3) | (s == 4))
        def _():
            def mid_a(j):
                @pl.when((s == 1) & (j == 4))
                def _():
                    norm(LA, 0)

            def then_a():
                @pl.when(s < 2)
                def _():
                    wtile(wka, 0, 0).start()

                @pl.when(s >= 2)
                def _():
                    wtile(wkl, 0, 0).start()

            def pre_a():
                @pl.when(s < 2)
                def _():
                    start_x_a(s + 1)

                @pl.when(s >= 2)
                def _():
                    start_x_b(jnp.where(s == 2, 0, 1))

            layer_a(jnp.where(s < 3, s, 3), mid_a, then_a, pre_a)

        @pl.when(s == 2)
        def _():
            norm(LA, 1)

        @pl.when(s >= 3)
        def _():
            def mid_b(j):
                now = jnp.where(s == 4, 3, jnp.where(s == 6, 19, 15))

                @pl.when(j == now)
                def _():
                    norm(jnp.where(s == 3, LA, LB), jnp.where(s == 3, 2, s - 4))

            def then_b():
                @pl.when(s == 3)
                def _():
                    wtile(wka, 0, 0).start()

                @pl.when((s > 3) & (s < 6))
                def _():
                    wtile(wkl, 0, 0).start()

            def pre_b():
                @pl.when(s == 3)
                def _():
                    start_x_a(3)

                @pl.when((s > 3) & (s < 6))
                def _():
                    start_x_b(s - 2)

            layer_b(s - 3, mid_b, then_b, pre_b)

        @pl.when(s == 4)
        def _():
            norm(LA, 3)

    norm(LB, 3, end=True)

    for i in range(N_CH):
        for n in range(2):
            rs_copy(n, i, 0, DM).wait_send()
            rows = IN_ROWS if n == LB and i == N_CH - 1 else OWN
            ag_copy(n, i, 0, rows).wait_send()
        ag_wait_recv(LB, i, rows)
        ss_copy(i).wait_send()

        for n in range(2):
            kv_sends(i, n, lambda c: c.wait_send())
            for h in range(2):

                @pl.when(is2)
                def _(i=i, n=n, h=h):
                    kv_copy(i, n, h, 0, False, 3, 1).wait_send()

                @pl.when(is3)
                def _(i=i, n=n, h=h):
                    kv_copy(i, n, h, 1, False, 2, 0).wait_send()

        @pl.when(cp <= 2)
        def _(i=i):
            @pl.loop(0, 8)
            def _(g):
                st_copy(i, g).wait_send()


def assemble(rows, last, res, buf, in_sem, out_sem):
    tp = lax.axis_index("tp")
    parts = [(own, k, IN_ROWS if k == N_CH - 1 else OWN, False) for own in (True, False) for k in range(N_CH)]
    parts.append((True, N_CH - 1, LAST, True))

    def place(p):
        own, k, size, end = parts[p]
        first = ((tp if own else 1 - tp) * N_CH + k) * OWN + (IN_ROWS if end else 0)
        return pl.ds(mo(first, LAST), size), buf.at[p % N_CH, pl.ds(0, size)], last if end else None

    def load(p):
        at, mid, src = place(p)
        return pltpu.make_async_copy(rows.at[at] if src is None else src, mid, in_sem.at[p % N_CH])

    def store(p):
        at, mid, _ = place(p)
        return pltpu.make_async_copy(mid, res.at[at], out_sem.at[p % N_CH])

    for p in range(N_CH):
        load(p).start()
    for p in range(len(parts)):
        load(p).wait()
        store(p).start()
        if p >= 1 and p + N_CH - 1 < len(parts):
            store(p - 1).wait()
            load(p + N_CH - 1).start()
    for p in range(len(parts) - N_CH, len(parts)):
        store(p).wait()


def solution(mesh):
    n_cp = mesh.shape["cp"]
    table = rope_tables(n_cp)
    any_ = pl.BlockSpec(memory_space=pl.ANY)
    smem = pl.BlockSpec(memory_space=pltpu.SMEM)
    vmem = pl.BlockSpec(memory_space=pltpu.VMEM)
    dma = pltpu.SemaphoreType.DMA
    two = (2,)

    def body(hidden, alphas, wqa, wka, wva, woa, gain_attn, wql, wkl, wvl, wgl, slopes, gain_inner, wol, gain_lin):
        shape = hidden.shape
        hid = hidden.reshape(shape[0] * shape[1], shape[2])
        sds = jax.ShapeDtypeStruct
        outs = (
            sds(hid.shape, BF),
            sds((LAST, DM), BF),
            sds((2, N_CH, ROWS, DM), BF),
            sds((2, N_CH, OWN, DM), BF),
            sds((N_CH, OWN, DM), BF),
            sds((N_CH, OWN, DM), BF),
            sds((N_CH, ROWS, KVW), BF),
            sds((N_CH, 3, ROWS, KVW), BF),
            sds((N_CH, N_G, 16, HD, HD), F32),
            sds((N_CH, N_G, 16, HD, HD), F32),
        )
        scratch = [
            pltpu.VMEM((2, DM, TN), BF),
            pltpu.VMEM((ROWS, DM), BF),
            pltpu.VMEM((3, ROWS, W), BF),
            pltpu.VMEM((ROWS, W), F32),
            pltpu.VMEM((ROWS, W), BF),
            pltpu.VMEM((2, ROWS, TN), F32),
            pltpu.VMEM((2, ROWS, TN), BF),
            pltpu.VMEM((2, 16, HD, HD), F32),
            pltpu.VMEM((2, 16, HD, HD), F32),
            pltpu.VMEM((N_BUF, RB, DM), BF),
            pltpu.VMEM((N_BUF, RB, DM), BF),
            pltpu.VMEM((N_BUF, RB, DM), BF),
            pltpu.VMEM((N_BUF, RB, DM), BF),
            pltpu.VMEM((ROWS, HD), F32),
            pltpu.VMEM((OWN, HD), F32),
            pltpu.VMEM((2, 3, TOK, HD), F32),
            pltpu.VMEM((N_CH, 8, HD), F32),
            pltpu.VMEM((N_CH, 8, HD), F32),
            pltpu.VMEM((4, 2, TOK, HD), F32),
            pltpu.VMEM((2, DM), F32),
            dma(two), dma(two), dma(two), dma(two), dma((3, 2)), dma(two), dma(two), dma((N_BUF, 3)), dma((N_BUF,)),
            dma((2, N_CH)), dma((2, N_CH)), dma((2, N_CH)), dma((2, N_CH)), dma((N_CH, 2, 2, 2)), dma((N_CH, 2, 2, 3)), dma((N_CH, N_G)), dma((N_CH, N_G)),
            dma((N_CH,)), dma((N_CH,)),
        ]
        res = pl.pallas_call(
            kernel,
            out_shape=outs,
            in_specs=[any_] * 11 + [smem, smem, vmem, vmem, vmem],
            out_specs=tuple(any_ for _ in outs),
            scratch_shapes=scratch,
            compiler_params=pltpu.CompilerParams(
                collective_id=0, has_side_effects=True, vmem_limit_bytes=VMEM_BYTES
            ),
            name="layers",
        )(
            hid, wqa, wka, wva, woa, wql, wkl, wvl, wgl, wol, jnp.asarray(table), alphas, slopes, gain_attn.reshape(1, -1),
            gain_lin.reshape(1, -1), gain_inner.reshape(1, -1),
        )
        got = lax.ppermute(res[1], "tp", [(0, 1), (1, 0)])
        rows = pl.pallas_call(
            assemble,
            out_shape=sds(hid.shape, BF),
            in_specs=[any_, any_],
            out_specs=any_,
            scratch_shapes=[pltpu.VMEM((N_CH, OWN, DM), BF), dma((N_CH,)), dma((N_CH,))],
            compiler_params=pltpu.CompilerParams(vmem_limit_bytes=VMEM_BYTES),
            cost_estimate=pl.CostEstimate(flops=10**11, bytes_accessed=2 * hid.size * 2, transcendentals=0),
            name="assemble",
        )(res[0], res[1])
        row = ((1 - lax.axis_index("tp")) * N_CH + N_CH - 1) * OWN + IN_ROWS
        return lax.dynamic_update_slice(rows, got, (row, 0)).reshape(shape)

    act = P("dp", "cp", None)
    rep = P()
    col = P(None, "tp")
    row = P("tp", None)
    vec = P("tp")
    in_specs = (act, rep, col, col, col, row, rep, col, col, col, col, vec, vec, row, rep)
    return jax.shard_map(body, mesh=mesh, in_specs=in_specs, out_specs=act, check_vma=False)
```

```python
import math

import jax
import jax.numpy as jnp
import numpy as np
from jax import lax
from jax.experimental import pallas as pl
from jax.experimental.pallas import tpu as pltpu
from jax.sharding import PartitionSpec as P

MESH = pl.DeviceIdType.MESH
F32 = jnp.float32
BF = jnp.bfloat16
ROPE_BASE = 10000000.0
EPS = 1e-5

VMEM_BYTES = 67043328
TOK = 128
HD = 128
TN = 512
DM = 6144
W = 4096
KVW = 1024
OWN_KV = W - KVW
N_SEQ = 4
N_CH = 4
N_CP = 4
N_G = 8
ROWS = N_SEQ * TOK
OWN = ROWS // 2
RB = 32
N_RB = OWN // RB
R_IN = N_RB - 2
IN_ROWS = R_IN * RB
LAST = OWN - IN_ROWS
N_Q = W // TN
N_QKV = KVW // TN + N_Q
N_WO = DM // TN
N_BUF = 4
LA, LB = 0, 1
PAIR = range(2)
K, V, Q = 0, 1, 2
NT_DIMS = (((1,), (1,)), ((), ()))
TN_DIMS = (((0,), (0,)), ((), ()))


def rope_tables(n_cp):
    half = HD // 4
    inv = ROPE_BASE ** (-np.arange(half, dtype=np.float64) * 2.0 / (2 * half))
    pos = np.arange(n_cp * TOK, dtype=np.float64)
    ang = pos[:, None] * inv[None, :]
    tab = np.zeros((3, n_cp * TOK, HD), np.float32)
    tab[0] = 1.0
    tab[0, :, :half] = np.cos(ang)
    tab[0, :, half : 2 * half] = np.cos(ang)
    tab[1, :, :half] = -np.sin(ang)
    tab[2, :, half : 2 * half] = np.sin(ang)
    return np.ascontiguousarray(tab.reshape(3, n_cp, TOK, HD).transpose(1, 0, 2, 3))


def mo(v, m):
    return pl.multiple_of(v, m)


def parity(j):
    return lax.rem(j, 2)


def blk(b):
    return pl.ds(mo(b * TOK, TOK), TOK)


def hcol(g, hh):
    return pl.ds(mo((4 * g + hh) * HD, HD), HD)


def dot(a, b, dims=(((1,), (0,)), ((), ()))):
    return lax.dot_general(a, b, dims, preferred_element_type=F32)


def sigmoid(z):
    return 1.0 / (1.0 + jnp.exp(-z))


def kernel(
    hid, wqa, wka, wva, woa, wql, wkl, wvl, wgl, wol, rope_hbm, alphas, slopes, gain_a, gain_b, ginner,
    out, last, pt, prec, h1own, h1oth, kvh, kvr, sth, str_,
    wbuf, x, kvq, gbuf, u, acc, ost, stg, pst, nb_p, nb_r, nb_h, nout, ss, rsb, rope, ssx, ssr, wtab, gains,
    w_sem, x_sem, o_sem, kvo_sem, kvl_sem, sto_sem, stl_sem, nl_sem, no_sem,
    rs_send, rs_recv, ag_send, ag_recv, kv_send, kv_recv, st_send, st_recv, ss_send, ss_recv,
):
    cp = lax.axis_index("cp")
    tp = lax.axis_index("tp")
    mate = 1 - tp
    is0, is1, is2, is3 = (cp == c for c in range(N_CP))

    bar = pltpu.get_barrier_semaphore()
    pl.semaphore_signal(bar, inc=1, device_id={"tp": mate}, device_id_type=MESH)
    for d in range(1, 4):
        pl.semaphore_signal(bar, inc=1, device_id={"cp": lax.rem(cp + d, 4)}, device_id_type=MESH)

    def wtile(src, col, slot):
        rows = pl.ds(0, src.shape[0])
        return pltpu.make_async_copy(src.at[:, pl.ds(col, TN)], wbuf.at[slot, rows], w_sem.at[slot])

    def wstart(src, j):
        wtile(src, wcol(j), parity(j)).start()

    def wcol(j):
        return mo(j * TN, TN)

    def issue_b(j):
        kv = j < 16
        for cond, w, tile in (
            (kv & (parity(j) == 0), wkl, j // 2),
            (kv & (parity(j) == 1), wvl, j // 2),
            ((j >= 16) & (j < 24), wql, j - 16),
            (j >= 24, wgl, j - 24),
        ):

            @pl.when(cond)
            def _(w=w, tile=tile):
                wtile(w, wcol(tile), parity(j)).start()

    def wait_w(slot, src=wqa):
        wtile(src, 0, slot).wait()

    def fetch_next(j, count, go, then):
        @pl.when(j + 1 < count)
        def _():
            go(j + 1)

        @pl.when(j + 1 >= count)
        def _():
            then()

    def own_row(i):
        return mo((tp * 8 + 2 * i) * TOK, TOK)

    def oth_row(i):
        return mo((mate * 8 + 2 * i) * TOK, TOK)

    def x_copies(top, bot):
        return (
            pltpu.make_async_copy(top, x.at[pl.ds(0, OWN)], x_sem.at[0]),
            pltpu.make_async_copy(bot, x.at[pl.ds(OWN, OWN)], x_sem.at[1]),
        )

    def x_from_hid(i):
        return x_copies(hid.at[pl.ds(own_row(i), OWN)], hid.at[pl.ds(oth_row(i), OWN)])

    def x_from_h1(i):
        return x_copies(h1own.at[i], h1oth.at[i])

    def start_x_a(i):
        for c in x_from_hid(i):
            c.start()

    def start_x_b(i):
        ag_wait_recv(LA, i)
        for c in x_from_h1(i):
            c.start()

    def rs_copy(n, i, col, width):
        return pltpu.make_async_remote_copy(
            src_ref=pt.at[n, i, pl.ds(OWN, OWN), pl.ds(col, width)],
            dst_ref=prec.at[n, i, :, pl.ds(col, width)],
            send_sem=rs_send.at[n, i],
            recv_sem=rs_recv.at[n, i],
            device_id={"tp": mate},
            device_id_type=MESH,
        )

    def ag_copy(n, i, row, rows):
        if n == 0:
            src = h1own.at[i, pl.ds(row, rows)]
            dst = h1oth.at[i, pl.ds(row, rows)]
        else:
            src = out.at[pl.ds(mo(own_row(i) + row, RB), rows)]
            dst = src
        return pltpu.make_async_remote_copy(
            src_ref=src,
            dst_ref=dst,
            send_sem=ag_send.at[n, i],
            recv_sem=ag_recv.at[n, i],
            device_id={"tp": mate},
            device_id_type=MESH,
        )

    def ag_wait_recv(n, i, rows=OWN):
        if n == 0:
            ag_copy(0, i, 0, rows).wait_recv()
        else:
            oth = out.at[pl.ds(oth_row(i), rows)]
            pltpu.make_async_remote_copy(
                src_ref=oth,
                dst_ref=oth,
                send_sem=ag_send.at[n, i],
                recv_sem=ag_recv.at[n, i],
                device_id={"tp": mate},
                device_id_type=MESH,
            ).wait_recv()

    def half_rows(h):
        return pl.ds(mo(OWN * (1 - h), OWN), OWN)

    def kv_copy(i, n, h, src, own, dst_cp, send):
        at = half_rows(h), pl.ds(n * TN, TN)
        return pltpu.make_async_remote_copy(
            src_ref=kvh.at[i, *at] if own else kvr.at[i, src, *at],
            dst_ref=kvr.at[i, src, *at],
            send_sem=kv_send.at[i, n, h, send],
            recv_sem=kv_recv.at[i, n, h, src],
            device_id={"cp": dst_cp},
            device_id_type=MESH,
        )

    def kv_sends(i, n, go):
        for h in PAIR:

            @pl.when(is0)
            def _(h=h):
                go(kv_copy(i, n, h, 0, True, 2, 0))
                go(kv_copy(i, n, h, 0, True, 1, 1))

            @pl.when(is1)
            def _(h=h):
                go(kv_copy(i, n, h, 1, True, 3, 0))

            @pl.when(is2)
            def _(h=h):
                go(kv_copy(i, n, h, 2, True, 3, 0))

    def st_copy(i, g):
        return pltpu.make_async_remote_copy(
            src_ref=sth.at[i, g],
            dst_ref=str_.at[i, g],
            send_sem=st_send.at[i, g],
            recv_sem=st_recv.at[i, g],
            device_id={"cp": lax.rem(cp + 1, 4)},
            device_id_type=MESH,
        )

    def ss_copy(i):
        return pltpu.make_async_remote_copy(
            src_ref=ssx.at[i],
            dst_ref=ssr.at[i],
            send_sem=ss_send.at[i],
            recv_sem=ss_recv.at[i],
            device_id={"tp": mate},
            device_id_type=MESH,
        )

    def norm_loads(n, i, r, start):
        slot = lax.rem(r, N_BUF)
        rows = pl.ds(mo(r * RB, RB), RB)
        copies = [
            pltpu.make_async_copy(pt.at[n, i, rows], nb_p.at[slot], nl_sem.at[slot, 0]),
            pltpu.make_async_copy(prec.at[n, i, rows], nb_r.at[slot], nl_sem.at[slot, 1]),
        ]
        res_a = hid.at[pl.ds(mo(own_row(i) + r * RB, RB), RB)]
        res_b = h1own.at[i, rows]
        for layer, res in ((LA, res_a), (LB, res_b)):

            @pl.when(n == layer)
            def _(res=res):
                c = pltpu.make_async_copy(res, nb_h.at[slot], nl_sem.at[slot, 2])
                c.start() if start else c.wait()

        for c in copies:
            c.start() if start else c.wait()

    def norm_begin(n, i):
        with jax.named_scope("norm_wait"):
            rs_copy(n, i, 0, DM).wait_recv()

            @pl.when(n == LB)
            def _():
                ss_copy(i).wait_recv()
                for b in PAIR:
                    whole = ssx[i, b : b + 1, :] + ssr[i, b + 2 : b + 3, :]
                    inv = lax.rsqrt(whole / float(2 * W) + EPS)
                    rsb[blk(b), :] = jnp.broadcast_to(inv, (TOK, TOK)).T

            @pl.when(n == LA)
            def _():
                rsb[...] = jnp.ones_like(rsb)

            for r in range(N_BUF - 1):
                norm_loads(n, i, r, True)

    def norm_ready(n, i, r):
        @pl.when(r + N_BUF - 1 < N_RB)
        def _():
            norm_loads(n, i, r + N_BUF - 1, True)

        norm_loads(n, i, r, False)

    def norm_rows(n, r):
        slot = lax.rem(r, N_BUF)
        alpha = alphas[n]
        for q in range(RB // 16):
            rows = slice(q * 16, (q + 1) * 16)
            both = nb_p[slot, rows, :].astype(F32) + nb_r[slot, rows, :].astype(F32)
            both = both * rsb[pl.ds(mo(r * RB + q * 16, 16), 16), 0:1]
            h = alpha * nb_h[slot, rows, :].astype(F32) + both
            inv = lax.rsqrt(jnp.mean(h * h, axis=-1, keepdims=True) + EPS)
            nout[slot, rows, :] = (h * inv * gains[pl.ds(n, 1), :]).astype(BF)

    def norm_store(n, i, r, start, end):
        slot = lax.rem(r, N_BUF)
        dst_a = h1own.at[i, pl.ds(mo(r * RB, RB), RB)]
        dst_b = out.at[pl.ds(mo(own_row(i) + r * RB, RB), RB)]
        inside = r < R_IN if end else True
        if end:

            @pl.when(r >= R_IN)
            def _():
                c = pltpu.make_async_copy(nout.at[slot], last.at[pl.ds(mo((r - R_IN) * RB, RB), RB)], no_sem.at[slot])
                c.start() if start else c.wait()

        for layer, dst in ((LA, dst_a), (LB, dst_b)):

            @pl.when((n == layer) & inside)
            def _(layer=layer, dst=dst):
                c = pltpu.make_async_copy(nout.at[slot], dst, no_sem.at[slot])
                if start:
                    c.start()
                else:
                    c.wait()
                    ag_copy(layer, i, mo(r * RB, RB), RB).start()

    def norm_out(n, i, r, end):
        @pl.when(r >= 2)
        def _():
            norm_store(n, i, r - 2, False, end)

        norm_store(n, i, r, True, end)

    def norm_end(n, i, end):
        for r in range(N_RB - 2, N_RB):
            norm_store(n, i, r, False, end)

    def norm(n, i, end=False):
        norm_begin(n, i)
        with jax.named_scope("norm"):

            @pl.loop(0, N_RB)
            def _(r):
                norm_ready(n, i, r)
                norm_rows(n, r)
                norm_out(n, i, r, end)

            norm_end(n, i, end)

    def out_proj(n, i, wo, then, pre, rows, send):
        def put(j, slot):
            size = pl.ds(0, rows.size)
            return pltpu.make_async_copy(ost.at[slot, size], pt.at[n, i, rows, pl.ds(wcol(j), TN)], o_sem.at[slot])

        def send_on(j, slot):
            put(j, slot).wait()

            @pl.when(send)
            def _():
                rs_copy(n, i, wcol(j), TN).start()

        with jax.named_scope("out_proj"):
            wtile(wo, TN, 1).start()

            @pl.loop(0, N_WO)
            def _(j):
                slot = parity(j)
                wait_w(slot, wo)

                @pl.when(j == 8)
                def _():
                    pre()

                ost[slot, 0 : rows.size, :] = dot(u[rows, :], wbuf[slot, 0:W, :]).astype(BF)

                @pl.when(j + 2 < N_WO)
                def _():
                    wstart(wo, j + 2)

                @pl.when(j + 2 == N_WO)
                def _():
                    then()

                @pl.when(j >= 1)
                def _():
                    send_on(j - 1, 1 - slot)

                put(j, slot).start()

            send_on(N_WO - 1, 1)

    def rotate(a, kind, dst, row, col):
        for b in range(a.shape[0] // TOK):
            for h in range(TN // HD):
                v = a[b * TOK : (b + 1) * TOK, h * HD : (h + 1) * HD]
                v = v * rope[kind, 0] + pltpu.roll(v, HD - 32, 1) * rope[kind, 1] + pltpu.roll(v, 32, 1) * rope[kind, 2]
                kvq[dst, pl.ds(mo(row + b * TOK, TOK), TOK), pl.ds(mo(col + h * HD, HD), HD)] = v.astype(BF)

    def kv_wait(i, halves):
        parts = [(n, h) for h in halves for n in PAIR]

        def got(n, h, src):
            kv_copy(i, n, h, src, False, 0, 0).wait_recv()

        def fetch(c, h):
            rows = half_rows(h)
            dst = kvq.at[K, rows, pl.ds(c * KVW, KVW)]
            return pltpu.make_async_copy(kvr.at[i, c, rows], dst, kvl_sem.at[c, h])

        with jax.named_scope("kv_wait"):
            for n, h in parts:

                @pl.when(is2)
                def _(n=n, h=h):
                    got(n, h, 0)
                    kv_copy(i, n, h, 0, False, 3, 1).start()

                @pl.when(is3)
                def _(n=n, h=h):
                    got(n, h, 1)
                    kv_copy(i, n, h, 1, False, 2, 0).start()

            for n, h in parts:

                @pl.when(is1)
                def _(n=n, h=h):
                    got(n, h, 0)

                @pl.when(is2)
                def _(n=n, h=h):
                    got(n, h, 1)

                @pl.when(is3)
                def _(n=n, h=h):
                    got(n, h, 2)
                    got(n, h, 0)

            for go in (lambda c: c.start(), lambda c: c.wait()):
                for c in range(N_CP - 1):

                    @pl.when(cp > c)
                    def _(c=c, go=go):
                        for h in halves:
                            go(fetch(c, h))

    def attention(first, count):
        scale = math.log2(math.e) / math.sqrt(HD)
        with jax.named_scope("attn"):
            for c in range(N_CP):

                @pl.when(cp == c)
                def _(c=c):
                    cols = [OWN_KV] + [b * KVW for b in range(c)]

                    @pl.loop(0, 4 * count)
                    def _(t):
                        g = lax.rem(t, 4)
                        seq = pl.ds(mo(first + t // 4 * TOK, TOK), TOK)
                        ks = [kvq[K, seq, pl.ds(mo(o + g * HD, HD), HD)] for o in cols]
                        vs = [kvq[K, seq, pl.ds(mo(o + TN + g * HD, HD), HD)] for o in cols]
                        keys = jnp.concatenate(ks, axis=0) if c else ks[0]
                        vals = jnp.concatenate(vs, axis=0) if c else vs[0]
                        row = lax.rem(lax.broadcasted_iota(jnp.int32, (2 * TOK, TOK), 0), TOK)
                        causal = lax.broadcasted_iota(jnp.int32, (2 * TOK, TOK), 1) <= row

                        def heads(p):
                            return [pl.ds(mo((g * 8 + 2 * p + z) * HD, HD), HD) for z in PAIR]

                        scores = []
                        for p in range(4):
                            qs = jnp.concatenate([kvq[Q, seq, o] for o in heads(p)], axis=0)
                            scores.append(dot(qs, keys, NT_DIMS))
                        for p in range(4):
                            s = scores[p]
                            own = jnp.where(causal, s[:, :TOK], -jnp.inf)
                            s = jnp.concatenate([own, s[:, TOK:]], axis=1) if c else own
                            m = jnp.max(s, axis=1, keepdims=True)
                            e = jnp.exp2((s - m) * scale)
                            o = dot(e.astype(BF), vals) * (1.0 / jnp.sum(e, axis=1, keepdims=True))
                            for z in PAIR:
                                u[seq, heads(p)[z]] = o[z * TOK : (z + 1) * TOK].astype(BF)

    def layer_a(i, then, pre):
        with jax.named_scope("x_a"):
            for c in x_from_hid(i):
                c.wait()

        def kv_out(n):
            cols = pl.ds(n * TN, TN)
            return pltpu.make_async_copy(kvq.at[K, :, pl.ds(OWN_KV + n * TN, TN)], kvh.at[i, :, cols], kvo_sem.at[n])

        def finish(j, slot):
            kv = j < 2
            col = jnp.where(kv, OWN_KV + j * TN, (j - 2) * TN)
            rotate(acc.at[slot], jnp.where(j == 1, 1, 0), jnp.where(kv, K, Q), 0, col)

        with jax.named_scope("qkv_a"):

            @pl.loop(0, jnp.where(i == 0, 2, N_QKV))
            def _(j):
                slot = parity(j)
                wait_w(slot)

                @pl.when(j == 0)
                def _():
                    wtile(wva, 0, 1).start()

                @pl.when(j >= 1)
                def _():
                    fetch_next(j, N_QKV, lambda t: wstart(wqa, t - 2), lambda: wtile(woa, 0, 0).start())

                for n in PAIR:

                    @pl.when(j == n + 2)
                    def _(n=n):
                        kv_out(n).wait()
                        kv_sends(i, n, lambda c: c.start())

                finish(jnp.maximum(j - 1, 0), 1 - slot)
                acc[slot] = dot(x[...], wbuf[slot])

                for n in PAIR:

                    @pl.when(j == n + 1)
                    def _(n=n):
                        kv_out(n).start()

            finish(jnp.where(i == 0, 1, N_QKV - 1), 1)

        @pl.when(i > 0)
        def _():
            kv_wait(i, PAIR)
            attention(0, N_SEQ)
            out_proj(LA, i, woa, then, pre, pl.ds(0, ROWS), True)

        @pl.when(i == 0)
        def _():
            kv_out(0).wait()
            kv_out(1).start()
            kv_sends(0, 0, lambda c: c.start())
            kv_out(1).wait()
            kv_sends(0, 1, lambda c: c.start())

            @pl.loop(0, 2)
            def _(h):
                first = mo(OWN * (1 - h), OWN)
                wtile(wqa, TN, 1).start()
                with jax.named_scope("q_a"):

                    @pl.loop(0, N_Q)
                    def _(j):
                        slot = parity(j)
                        wait_w(slot)
                        rotate(dot(x[pl.ds(first, OWN), :], wbuf[slot]), 0, Q, first, j * TN)

                        @pl.when(j + 2 < N_Q)
                        def _():
                            wstart(wqa, j + 2)

                        @pl.when(j + 2 == N_Q)
                        def _():
                            wtile(woa, 0, 0).start()

                kv_wait(0, (h,))
                attention(first, 2)

                def then_a():
                    @pl.when(h == 0)
                    def _():
                        wtile(wqa, 0, 0).start()

                    @pl.when(h == 1)
                    def _():
                        then()

                def pre_a():
                    @pl.when(h == 1)
                    def _():
                        pre()

                out_proj(LA, 0, woa, then_a, pre_a, pl.ds(first, OWN), h == 0)

    def key_decay(h):
        back = lax.broadcasted_iota(jnp.int32, (TOK, HD), 0).astype(F32) - (TOK - 1.0)
        return jnp.exp(slopes[h] * back)

    def state_of(g, b, hh, kd):
        rows = blk(b)
        col = hcol(g, hh)
        k = (kvq[K, rows, col].astype(F32) * kd).astype(BF)
        return dot(k, kvq[V, rows, col], TN_DIMS)

    def block_decay(h):
        return jnp.exp(jnp.full((8, HD), -float(TOK), F32) * slopes[h])[0:1, :]

    def st_store(i, g, slot):
        return pltpu.make_async_copy(stg.at[slot], sth.at[i, g], sto_sem.at[slot])

    def st_load(i, g, slot):
        return pltpu.make_async_copy(str_.at[i, g], pst.at[slot], stl_sem.at[slot])

    def next_state(g):
        slot = parity(g)
        for hh in range(4):
            kd = key_decay(4 * g + hh)
            bd = block_decay(4 * g + hh)
            new = [state_of(g, b, hh, kd) for b in range(N_SEQ)]
            for b in range(N_SEQ):
                stg[slot, b * 4 + hh] = new[b] + bd * pst[slot, b * 4 + hh]

    def local_state(i, g):
        slot = parity(g)

        @pl.when(is1)
        def _():
            st_load(i, g, slot).wait()

        @pl.when(is0)
        def _():
            for hh in range(N_SEQ):
                kd = key_decay(4 * g + hh)
                for b in range(N_SEQ):
                    stg[slot, b * 4 + hh] = state_of(g, b, hh, kd)

        @pl.when(is1)
        def _():
            for hh in range(N_SEQ):
                kd = key_decay(4 * g + hh)
                bd = block_decay(4 * g + hh)
                for b in range(N_SEQ):
                    stg[slot, b * 4 + hh] = state_of(g, b, hh, kd) + bd * pst[slot, b * 4 + hh]

        st_store(i, g, slot).start()

    def st_send_on(i, g):
        st_store(i, g, parity(g)).wait()
        st_copy(i, g).start()

    def layer_b(i, mid, then, pre):
        with jax.named_scope("x_b"):
            for c in x_from_h1(i):
                c.wait()

        def finish(j, a):
            kv = j < 16
            dst = jnp.where(kv, parity(j), Q)
            kvq[dst, :, pl.ds(wcol(jnp.where(kv, j // 2, j - 16)), TN)] = (a * sigmoid(a)).astype(BF)

        with jax.named_scope("qkv_b"):
            @pl.loop(0, 24)
            def _(j):
                slot = parity(j)
                wait_w(slot)
                issue_b(j + 1)

                e = j - jnp.where(is0, 0, 2)
                busy = (cp <= 1) & (e >= 1) & (e <= 16)
                g = e // 2

                @pl.when(busy & (parity(e) == 1) & is1)
                def _():
                    st_copy(i, g).wait_recv()
                    st_load(i, g, parity(g)).start()

                finish(j, dot(x[...], wbuf[slot]))

                @pl.when(busy & (parity(e) == 0))
                def _():
                    st_send_on(i, g - 1)

                @pl.when(busy & (parity(e) == 1))
                def _():
                    local_state(i, g)

                mid(j)

        with jax.named_scope("gate"):

            @pl.loop(0, 8)
            def _(j):
                slot = parity(j)
                wait_w(slot)
                fetch_next(j, 8, lambda t: issue_b(t + 24), lambda: wtile(wol, 0, 0).start())

                @pl.when(is2)
                def _():
                    st_copy(i, j).wait_recv()
                    st_load(i, j, slot).start()

                gbuf[:, pl.ds(wcol(j), TN)] = sigmoid(dot(x[...], wbuf[slot]))

                @pl.when(is2)
                def _():
                    st_load(i, j, slot).wait()
                    next_state(j)
                    st_store(i, j, slot).start()

                    @pl.when(j >= 1)
                    def _():
                        st_send_on(i, j - 1)

        with jax.named_scope("lin"):

            @pl.when(is2)
            def _():
                st_send_on(i, N_G - 1)

            ss[...] = jnp.zeros_like(ss)

            def fetch(g):
                @pl.when(is3)
                def _():
                    st_copy(i, g).wait_recv()

                @pl.when(cp >= 1)
                def _():
                    st_load(i, g, parity(g)).start()

            @pl.when(is0)
            def _():
                pst[...] = jnp.zeros_like(pst)

            fetch(0)

            @pl.loop(0, N_G)
            def _(g):
                slot = parity(g)

                @pl.when(g + 1 < N_G)
                def _():
                    fetch(g + 1)

                for hh in range(4):
                    lam = slopes[4 * g + hh]
                    row = lax.broadcasted_iota(jnp.int32, (TOK, HD), 0).astype(F32)
                    lane = lax.broadcasted_iota(jnp.int32, (TOK, HD), 1).astype(F32)
                    gap = row - lane
                    wtab[hh, 0] = jnp.where(gap >= 0, jnp.exp(-lam * jnp.maximum(gap, 0.0)), 0.0)
                    wtab[hh, 1] = jnp.exp(-lam * (row + 1.0))

                @pl.when(cp >= 1)
                def _():
                    st_load(i, g, slot).wait()

                @pl.loop(0, 2)
                def _(half):
                    pairs = [(half * 2 + z, hh) for z in PAIR for hh in range(4)]
                    at = [(blk(b), hcol(g, hh)) for b, hh in pairs]
                    qs = [kvq[Q, r, c] for r, c in at]
                    inner = [dot(q, kvq[K, r, c], NT_DIMS) for q, (r, c) in zip(qs, at)]
                    prior = [dot(q, pst[slot, b * 4 + hh].astype(BF)) for q, (b, hh) in zip(qs, pairs)]
                    o = [
                        dot((s * wtab[hh, 0]).astype(BF), kvq[V, r, c]) + p * wtab[hh, 1]
                        for s, p, (r, c), (b, hh) in zip(inner, prior, at, pairs)
                    ]
                    for v, (r, c) in zip(o, at):
                        u[r, c] = (v * ginner[0:1, c] * gbuf[r, c]).astype(BF)
                    for z in PAIR:
                        ss[at[4 * z][0], :] += sum(v * v for v in o[4 * z : 4 * z + 4])

            sums = [jnp.sum(ss[blk(b), :].T, axis=0, keepdims=True) for b in range(N_SEQ)]
            ssx[i] = jnp.concatenate(sums + sums, axis=0)

        def then_ss():
            ss_copy(i).start()
            pre()

        out_proj(LB, i, wol, then, then_ss, pl.ds(0, ROWS), True)

    wtile(wka, 0, 0).start()
    start_x_a(0)
    rope_in = pltpu.make_async_copy(rope_hbm.at[cp], rope.at[0], kvo_sem.at[0])
    rope_in.start()
    gains[0:1, :] = gain_a[...]
    gains[1:2, :] = gain_b[...]
    rope[1, 0] = jnp.ones((TOK, HD), F32)
    rope[1, 1] = jnp.zeros((TOK, HD), F32)
    rope[1, 2] = jnp.zeros((TOK, HD), F32)
    rope_in.wait()
    pl.semaphore_wait(bar, 4)

    @pl.loop(0, 7)
    def _(s):
        @pl.when((s < 3) | (s == 4))
        def _():
            def then_a():
                @pl.when(s < 2)
                def _():
                    wtile(wka, 0, 0).start()

                @pl.when(s >= 2)
                def _():
                    wtile(wkl, 0, 0).start()

            def pre_a():
                @pl.when(s < 2)
                def _():
                    start_x_a(s + 1)

                @pl.when(s >= 2)
                def _():
                    start_x_b(jnp.where(s == 2, 0, 1))

            layer_a(jnp.where(s < 3, s, 3), then_a, pre_a)

        @pl.when((s == 0) | (s == 2))
        def _():
            norm(LA, s // 2)

        @pl.when(s >= 3)
        def _():
            def mid_b(j):
                now = jnp.where(s == 4, 3, jnp.where(s == 6, 19, 15))

                @pl.when(j == now)
                def _():
                    norm(jnp.where(s == 3, LA, LB), jnp.where(s == 3, 2, s - 4))

            def then_b():
                @pl.when(s == 3)
                def _():
                    wtile(wka, 0, 0).start()

                @pl.when((s > 3) & (s < 6))
                def _():
                    wtile(wkl, 0, 0).start()

            def pre_b():
                @pl.when(s == 3)
                def _():
                    start_x_a(3)

                @pl.when((s > 3) & (s < 6))
                def _():
                    start_x_b(s - 2)

            layer_b(s - 3, mid_b, then_b, pre_b)

        @pl.when(s == 4)
        def _():
            norm(LA, 3)

    norm(LB, 3, end=True)

    for i in range(N_CH):
        for n in PAIR:
            rs_copy(n, i, 0, DM).wait_send()
            rows = IN_ROWS if n == LB and i == N_CH - 1 else OWN
            ag_copy(n, i, 0, rows).wait_send()
        ag_wait_recv(LB, i, rows)
        ss_copy(i).wait_send()

        for n in PAIR:
            kv_sends(i, n, lambda c: c.wait_send())
            for h in PAIR:

                @pl.when(is2)
                def _(i=i, n=n, h=h):
                    kv_copy(i, n, h, 0, False, 3, 1).wait_send()

                @pl.when(is3)
                def _(i=i, n=n, h=h):
                    kv_copy(i, n, h, 1, False, 2, 0).wait_send()

        @pl.when(cp <= 2)
        def _(i=i):
            @pl.loop(0, 8)
            def _(g):
                st_copy(i, g).wait_send()


def assemble(rows, last, res, buf, in_sem, out_sem):
    tp = lax.axis_index("tp")
    parts = [(own, k, IN_ROWS if k == N_CH - 1 else OWN, False) for own in (True, False) for k in range(N_CH)]
    parts.append((True, N_CH - 1, LAST, True))

    def place(p):
        own, k, size, end = parts[p]
        first = ((tp if own else 1 - tp) * N_CH + k) * OWN + (IN_ROWS if end else 0)
        return pl.ds(mo(first, LAST), size), buf.at[p % N_CH, pl.ds(0, size)], last if end else None

    def load(p):
        at, mid, src = place(p)
        return pltpu.make_async_copy(rows.at[at] if src is None else src, mid, in_sem.at[p % N_CH])

    def store(p):
        at, mid, _ = place(p)
        return pltpu.make_async_copy(mid, res.at[at], out_sem.at[p % N_CH])

    for p in range(N_CH):
        load(p).start()
    for p in range(len(parts)):
        load(p).wait()
        store(p).start()
        if p >= 1 and p + N_CH - 1 < len(parts):
            store(p - 1).wait()
            load(p + N_CH - 1).start()
    for p in range(len(parts) - N_CH, len(parts)):
        store(p).wait()


def solution(mesh):
    n_cp = mesh.shape["cp"]
    table = rope_tables(n_cp)
    any_ = pl.BlockSpec(memory_space=pl.ANY)
    smem = pl.BlockSpec(memory_space=pltpu.SMEM)
    vmem = pl.BlockSpec(memory_space=pltpu.VMEM)
    dma = pltpu.SemaphoreType.DMA
    two = (2,)

    def body(hidden, alphas, wqa, wka, wva, woa, gain_attn, wql, wkl, wvl, wgl, slopes, gain_inner, wol, gain_lin):
        shape = hidden.shape
        hid = hidden.reshape(shape[0] * shape[1], shape[2])
        sds = jax.ShapeDtypeStruct
        outs = (
            sds(hid.shape, BF),
            sds((LAST, DM), BF),
            sds((2, N_CH, ROWS, DM), BF),
            sds((2, N_CH, OWN, DM), BF),
            sds((N_CH, OWN, DM), BF),
            sds((N_CH, OWN, DM), BF),
            sds((N_CH, ROWS, KVW), BF),
            sds((N_CH, 3, ROWS, KVW), BF),
            sds((N_CH, N_G, 16, HD, HD), F32),
            sds((N_CH, N_G, 16, HD, HD), F32),
        )
        scratch = [
            pltpu.VMEM((2, DM, TN), BF),
            pltpu.VMEM((ROWS, DM), BF),
            pltpu.VMEM((3, ROWS, W), BF),
            pltpu.VMEM((ROWS, W), F32),
            pltpu.VMEM((ROWS, W), BF),
            pltpu.VMEM((2, ROWS, TN), F32),
            pltpu.VMEM((2, ROWS, TN), BF),
            pltpu.VMEM((2, 16, HD, HD), F32),
            pltpu.VMEM((2, 16, HD, HD), F32),
            pltpu.VMEM((N_BUF, RB, DM), BF),
            pltpu.VMEM((N_BUF, RB, DM), BF),
            pltpu.VMEM((N_BUF, RB, DM), BF),
            pltpu.VMEM((N_BUF, RB, DM), BF),
            pltpu.VMEM((ROWS, HD), F32),
            pltpu.VMEM((OWN, HD), F32),
            pltpu.VMEM((2, 3, TOK, HD), F32),
            pltpu.VMEM((N_CH, 8, HD), F32),
            pltpu.VMEM((N_CH, 8, HD), F32),
            pltpu.VMEM((4, 2, TOK, HD), F32),
            pltpu.VMEM((2, DM), F32),
            dma(two), dma(two), dma(two), dma(two), dma((3, 2)), dma(two), dma(two), dma((N_BUF, 3)), dma((N_BUF,)),
            dma((2, N_CH)), dma((2, N_CH)), dma((2, N_CH)), dma((2, N_CH)), dma((N_CH, 2, 2, 2)), dma((N_CH, 2, 2, 3)), dma((N_CH, N_G)), dma((N_CH, N_G)),
            dma((N_CH,)), dma((N_CH,)),
        ]
        res = pl.pallas_call(
            kernel,
            out_shape=outs,
            in_specs=[any_] * 11 + [smem, smem, vmem, vmem, vmem],
            out_specs=tuple(any_ for _ in outs),
            scratch_shapes=scratch,
            compiler_params=pltpu.CompilerParams(
                collective_id=0, has_side_effects=True, vmem_limit_bytes=VMEM_BYTES
            ),
            name="layers",
        )(
            hid, wqa, wka, wva, woa, wql, wkl, wvl, wgl, wol, jnp.asarray(table), alphas, slopes, gain_attn.reshape(1, -1),
            gain_lin.reshape(1, -1), gain_inner.reshape(1, -1),
        )
        got = lax.ppermute(res[1], "tp", [(0, 1), (1, 0)])
        rows = pl.pallas_call(
            assemble,
            out_shape=sds(hid.shape, BF),
            in_specs=[any_, any_],
            out_specs=any_,
            scratch_shapes=[pltpu.VMEM((N_CH, OWN, DM), BF), dma((N_CH,)), dma((N_CH,))],
            compiler_params=pltpu.CompilerParams(vmem_limit_bytes=VMEM_BYTES),
            cost_estimate=pl.CostEstimate(flops=10**11, bytes_accessed=2 * hid.size * 2, transcendentals=0),
            name="assemble",
        )(res[0], res[1])
        row = ((1 - lax.axis_index("tp")) * N_CH + N_CH - 1) * OWN + IN_ROWS
        return lax.dynamic_update_slice(rows, got, (row, 0)).reshape(shape)

    act = P("dp", "cp", None)
    rep = P()
    col = P(None, "tp")
    row = P("tp", None)
    vec = P("tp")
    in_specs = (act, rep, col, col, col, row, rep, col, col, col, col, vec, vec, row, rep)
    return jax.shard_map(body, mesh=mesh, in_specs=in_specs, out_specs=act, check_vma=False)
```

```python
import math

import jax
import jax.numpy as jnp
import numpy as np
from jax import lax
from jax.experimental import pallas as pl
from jax.experimental.pallas import tpu as pltpu
from jax.sharding import PartitionSpec as P

MESH = pl.DeviceIdType.MESH
F32 = jnp.float32
BF = jnp.bfloat16
ROPE_BASE = 10000000.0
EPS = 1e-5

VMEM_BYTES = 67043328
TOK = 128
HD = 128
TN = 512
DM = 6144
W = 4096
KVW = 1024
OWN_KV = W - KVW
N_SEQ = 4
N_CH = 4
N_CP = 4
N_G = 8
ROWS = N_SEQ * TOK
OWN = ROWS // 2
RB = 32
N_RB = OWN // RB
R_IN = N_RB - 2
IN_ROWS = R_IN * RB
LAST = OWN - IN_ROWS
N_QKV = (KVW + W) // TN
N_WO = DM // TN
N_BUF = 4
LA, LB = 0, 1
PAIR = range(2)
K, V, Q = 0, 1, 2
NT_DIMS = (((1,), (1,)), ((), ()))
TN_DIMS = (((0,), (0,)), ((), ()))


def rope_tables(n_cp):
    half = HD // 4
    inv = ROPE_BASE ** (-np.arange(half, dtype=np.float64) * 2.0 / (2 * half))
    pos = np.arange(n_cp * TOK, dtype=np.float64)
    ang = pos[:, None] * inv[None, :]
    tab = np.zeros((3, n_cp * TOK, HD), np.float32)
    tab[0] = 1.0
    tab[0, :, :half] = np.cos(ang)
    tab[0, :, half : 2 * half] = np.cos(ang)
    tab[1, :, :half] = -np.sin(ang)
    tab[2, :, half : 2 * half] = np.sin(ang)
    return np.ascontiguousarray(tab.reshape(3, n_cp, TOK, HD).transpose(1, 0, 2, 3))


def mo(v, m):
    return pl.multiple_of(v, m)


def parity(j):
    return lax.rem(j, 2)


def blk(b):
    return pl.ds(mo(b * TOK, TOK), TOK)


def hcol(g, hh):
    return pl.ds(mo((4 * g + hh) * HD, HD), HD)


def dot(a, b, dims=(((1,), (0,)), ((), ()))):
    return lax.dot_general(a, b, dims, preferred_element_type=F32)


def sigmoid(z):
    return 1.0 / (1.0 + jnp.exp(-z))


def kernel(
    hid, wqa, wka, wva, woa, wql, wkl, wvl, wgl, wol, rope_hbm, alphas, slopes, gain_a, gain_b, ginner,
    out, last, pt, prec, h1own, h1oth, kvh, kvr, sth, str_,
    wbuf, x, kvq, gbuf, u, acc, ost, stg, pst, nb_p, nb_r, nb_h, nout, ss, rsb, rope, ssx, ssr, wtab, gains,
    w_sem, x_sem, o_sem, kvo_sem, kvl_sem, sto_sem, stl_sem, nl_sem, no_sem,
    rs_send, rs_recv, ag_send, ag_recv, kv_send, kv_recv, st_send, st_recv, ss_send, ss_recv,
):
    cp = lax.axis_index("cp")
    tp = lax.axis_index("tp")
    mate = 1 - tp
    is0, is1, is2, is3 = (cp == c for c in range(N_CP))

    bar = pltpu.get_barrier_semaphore()
    pl.semaphore_signal(bar, inc=1, device_id={"tp": mate}, device_id_type=MESH)
    for d in range(1, 4):
        pl.semaphore_signal(bar, inc=1, device_id={"cp": lax.rem(cp + d, 4)}, device_id_type=MESH)

    def wtile(src, col, slot):
        rows = pl.ds(0, src.shape[0])
        return pltpu.make_async_copy(src.at[:, pl.ds(col, TN)], wbuf.at[slot, rows], w_sem.at[slot])

    def wstart(src, j):
        wtile(src, wcol(j), parity(j)).start()

    def wcol(j):
        return mo(j * TN, TN)

    def issue_b(j):
        kv = j < 16
        for cond, w, tile in (
            (kv & (parity(j) == 0), wkl, j // 2),
            (kv & (parity(j) == 1), wvl, j // 2),
            ((j >= 16) & (j < 24), wql, j - 16),
            (j >= 24, wgl, j - 24),
        ):

            @pl.when(cond)
            def _(w=w, tile=tile):
                wtile(w, wcol(tile), parity(j)).start()

    def wait_w(slot, src=wqa):
        wtile(src, 0, slot).wait()

    def fetch_next(j, count, go, then):
        @pl.when(j + 1 < count)
        def _():
            go(j + 1)

        @pl.when(j + 1 >= count)
        def _():
            then()

    def own_row(i):
        return mo((tp * 8 + 2 * i) * TOK, TOK)

    def oth_row(i):
        return mo((mate * 8 + 2 * i) * TOK, TOK)

    def x_copies(top, bot):
        return (
            pltpu.make_async_copy(top, x.at[pl.ds(0, OWN)], x_sem.at[0]),
            pltpu.make_async_copy(bot, x.at[pl.ds(OWN, OWN)], x_sem.at[1]),
        )

    def x_from_hid(i):
        return x_copies(hid.at[pl.ds(own_row(i), OWN)], hid.at[pl.ds(oth_row(i), OWN)])

    def x_from_h1(i):
        return x_copies(h1own.at[i], h1oth.at[i])

    def start_x_a(i):
        for c in x_from_hid(i):
            c.start()

    def start_x_b(i):
        ag_wait_recv(LA, i)
        for c in x_from_h1(i):
            c.start()

    def rs_copy(n, i, col, width):
        return pltpu.make_async_remote_copy(
            src_ref=pt.at[n, i, pl.ds(OWN, OWN), pl.ds(col, width)],
            dst_ref=prec.at[n, i, :, pl.ds(col, width)],
            send_sem=rs_send.at[n, i],
            recv_sem=rs_recv.at[n, i],
            device_id={"tp": mate},
            device_id_type=MESH,
        )

    def ag_copy(n, i, row, rows):
        if n == 0:
            src = h1own.at[i, pl.ds(row, rows)]
            dst = h1oth.at[i, pl.ds(row, rows)]
        else:
            src = out.at[pl.ds(mo(own_row(i) + row, RB), rows)]
            dst = src
        return pltpu.make_async_remote_copy(
            src_ref=src,
            dst_ref=dst,
            send_sem=ag_send.at[n, i],
            recv_sem=ag_recv.at[n, i],
            device_id={"tp": mate},
            device_id_type=MESH,
        )

    def ag_wait_recv(n, i, rows=OWN):
        if n == 0:
            ag_copy(0, i, 0, rows).wait_recv()
        else:
            oth = out.at[pl.ds(oth_row(i), rows)]
            pltpu.make_async_remote_copy(
                src_ref=oth,
                dst_ref=oth,
                send_sem=ag_send.at[n, i],
                recv_sem=ag_recv.at[n, i],
                device_id={"tp": mate},
                device_id_type=MESH,
            ).wait_recv()

    def half_rows(h):
        return pl.ds(mo(OWN * (1 - h), OWN), OWN)

    def kv_copy(i, n, h, src, own, dst_cp, send):
        at = half_rows(h), pl.ds(n * TN, TN)
        return pltpu.make_async_remote_copy(
            src_ref=kvh.at[i, *at] if own else kvr.at[i, src, *at],
            dst_ref=kvr.at[i, src, *at],
            send_sem=kv_send.at[i, n, h, send],
            recv_sem=kv_recv.at[i, n, h, src],
            device_id={"cp": dst_cp},
            device_id_type=MESH,
        )

    def kv_sends(i, n, go):
        for h in PAIR:

            @pl.when(is0)
            def _(h=h):
                go(kv_copy(i, n, h, 0, True, 2, 0))
                go(kv_copy(i, n, h, 0, True, 1, 1))

            @pl.when(is1)
            def _(h=h):
                go(kv_copy(i, n, h, 1, True, 3, 0))

            @pl.when(is2)
            def _(h=h):
                go(kv_copy(i, n, h, 2, True, 3, 0))

    def st_copy(i, g):
        return pltpu.make_async_remote_copy(
            src_ref=sth.at[i, g],
            dst_ref=str_.at[i, g],
            send_sem=st_send.at[i, g],
            recv_sem=st_recv.at[i, g],
            device_id={"cp": lax.rem(cp + 1, 4)},
            device_id_type=MESH,
        )

    def ss_copy(i):
        return pltpu.make_async_remote_copy(
            src_ref=ssx.at[i],
            dst_ref=ssr.at[i],
            send_sem=ss_send.at[i],
            recv_sem=ss_recv.at[i],
            device_id={"tp": mate},
            device_id_type=MESH,
        )

    def norm_loads(n, i, r, start):
        slot = lax.rem(r, N_BUF)
        rows = pl.ds(mo(r * RB, RB), RB)
        copies = [
            pltpu.make_async_copy(pt.at[n, i, rows], nb_p.at[slot], nl_sem.at[slot, 0]),
            pltpu.make_async_copy(prec.at[n, i, rows], nb_r.at[slot], nl_sem.at[slot, 1]),
        ]
        res_a = hid.at[pl.ds(mo(own_row(i) + r * RB, RB), RB)]
        res_b = h1own.at[i, rows]
        for layer, res in ((LA, res_a), (LB, res_b)):

            @pl.when(n == layer)
            def _(res=res):
                c = pltpu.make_async_copy(res, nb_h.at[slot], nl_sem.at[slot, 2])
                c.start() if start else c.wait()

        for c in copies:
            c.start() if start else c.wait()

    def norm_begin(n, i):
        with jax.named_scope("norm_wait"):
            rs_copy(n, i, 0, DM).wait_recv()

            @pl.when(n == LB)
            def _():
                ss_copy(i).wait_recv()
                for b in PAIR:
                    whole = ssx[i, b : b + 1, :] + ssr[i, b + 2 : b + 3, :]
                    inv = lax.rsqrt(whole / float(2 * W) + EPS)
                    rsb[blk(b), :] = jnp.broadcast_to(inv, (TOK, TOK)).T

            @pl.when(n == LA)
            def _():
                rsb[...] = jnp.ones_like(rsb)

            for r in range(N_BUF - 1):
                norm_loads(n, i, r, True)

    def norm_ready(n, i, r):
        @pl.when(r + N_BUF - 1 < N_RB)
        def _():
            norm_loads(n, i, r + N_BUF - 1, True)

        norm_loads(n, i, r, False)

    def norm_rows(n, r):
        slot = lax.rem(r, N_BUF)
        alpha = alphas[n]
        for q in range(RB // 16):
            rows = slice(q * 16, (q + 1) * 16)
            both = nb_p[slot, rows, :].astype(F32) + nb_r[slot, rows, :].astype(F32)
            both = both * rsb[pl.ds(mo(r * RB + q * 16, 16), 16), 0:1]
            h = alpha * nb_h[slot, rows, :].astype(F32) + both
            inv = lax.rsqrt(jnp.mean(h * h, axis=-1, keepdims=True) + EPS)
            nout[slot, rows, :] = (h * inv * gains[pl.ds(n, 1), :]).astype(BF)

    def norm_store(n, i, r, start, end):
        slot = lax.rem(r, N_BUF)
        dst_a = h1own.at[i, pl.ds(mo(r * RB, RB), RB)]
        dst_b = out.at[pl.ds(mo(own_row(i) + r * RB, RB), RB)]
        inside = r < R_IN if end else True
        if end:

            @pl.when(r >= R_IN)
            def _():
                c = pltpu.make_async_copy(nout.at[slot], last.at[pl.ds(mo((r - R_IN) * RB, RB), RB)], no_sem.at[slot])
                c.start() if start else c.wait()

        for layer, dst in ((LA, dst_a), (LB, dst_b)):

            @pl.when((n == layer) & inside)
            def _(layer=layer, dst=dst):
                c = pltpu.make_async_copy(nout.at[slot], dst, no_sem.at[slot])
                if start:
                    c.start()
                else:
                    c.wait()

                    @pl.when((layer == LA) | (i == 0) | end | (r < R_IN))
                    def _():
                        ag_copy(layer, i, mo(r * RB, RB), RB).start()

    def norm_out(n, i, r, end):
        @pl.when(r >= 2)
        def _():
            norm_store(n, i, r - 2, False, end)

        norm_store(n, i, r, True, end)

    def norm_end(n, i, end):
        for r in range(N_RB - 2, N_RB):
            norm_store(n, i, r, False, end)

    def norm(n, i, end=False):
        norm_begin(n, i)
        with jax.named_scope("norm"):

            @pl.loop(0, N_RB)
            def _(r):
                norm_ready(n, i, r)
                norm_rows(n, r)
                norm_out(n, i, r, end)

            norm_end(n, i, end)

    def out_proj(n, i, wo, then, pre, rows, send):
        def put(j, slot):
            size = pl.ds(0, rows.size)
            return pltpu.make_async_copy(ost.at[slot, size], pt.at[n, i, rows, pl.ds(wcol(j), TN)], o_sem.at[slot])

        def send_on(j, slot):
            put(j, slot).wait()

            @pl.when(send)
            def _():
                rs_copy(n, i, wcol(j), TN).start()

        with jax.named_scope("out_proj"):
            wtile(wo, TN, 1).start()

            @pl.loop(0, N_WO)
            def _(j):
                slot = parity(j)
                wait_w(slot, wo)

                @pl.when(j == 8)
                def _():
                    pre()

                ost[slot, 0 : rows.size, :] = dot(u[rows, :], wbuf[slot, 0:W, :]).astype(BF)

                @pl.when(j + 2 < N_WO)
                def _():
                    wstart(wo, j + 2)

                @pl.when(j + 2 == N_WO)
                def _():
                    then()

                @pl.when(j >= 1)
                def _():
                    send_on(j - 1, 1 - slot)

                put(j, slot).start()

            send_on(N_WO - 1, 1)

    def rotate(a, kind, dst, row, col):
        for b in range(a.shape[0] // TOK):
            for h in range(TN // HD):
                v = a[b * TOK : (b + 1) * TOK, h * HD : (h + 1) * HD]
                v = v * rope[kind, 0] + pltpu.roll(v, HD - 32, 1) * rope[kind, 1] + pltpu.roll(v, 32, 1) * rope[kind, 2]
                kvq[dst, pl.ds(mo(row + b * TOK, TOK), TOK), pl.ds(mo(col + h * HD, HD), HD)] = v.astype(BF)

    def kv_forward(i, h):
        for n in PAIR:

            @pl.when(is2)
            def _(n=n):
                kv_copy(i, n, h, 0, False, 3, 1).wait_recv()
                kv_copy(i, n, h, 0, False, 3, 1).start()

            @pl.when(is3)
            def _(n=n):
                kv_copy(i, n, h, 1, False, 2, 0).wait_recv()
                kv_copy(i, n, h, 1, False, 2, 0).start()

    def kv_wait(i, halves):
        parts = [(n, h) for h in halves for n in PAIR]

        def got(n, h, src):
            kv_copy(i, n, h, src, False, 0, 0).wait_recv()

        def fetch(c, h):
            rows = half_rows(h)
            dst = kvq.at[K, rows, pl.ds(c * KVW, KVW)]
            return pltpu.make_async_copy(kvr.at[i, c, rows], dst, kvl_sem.at[c, h])

        with jax.named_scope("kv_wait"):
            for n, h in parts:

                @pl.when(is1)
                def _(n=n, h=h):
                    got(n, h, 0)

                @pl.when(is2)
                def _(n=n, h=h):
                    got(n, h, 1)

                @pl.when(is3)
                def _(n=n, h=h):
                    got(n, h, 2)
                    got(n, h, 0)

            for go in (lambda c: c.start(), lambda c: c.wait()):
                for c in range(N_CP - 1):

                    @pl.when(cp > c)
                    def _(c=c, go=go):
                        for h in halves:
                            go(fetch(c, h))

    def attention(first, count):
        scale = math.log2(math.e) / math.sqrt(HD)
        with jax.named_scope("attn"):
            for c in range(N_CP):

                @pl.when(cp == c)
                def _(c=c):
                    cols = [OWN_KV] + [b * KVW for b in range(c)]

                    @pl.loop(0, 4 * count)
                    def _(t):
                        g = lax.rem(t, 4)
                        seq = pl.ds(mo(first + t // 4 * TOK, TOK), TOK)
                        ks = [kvq[K, seq, pl.ds(mo(o + g * HD, HD), HD)] for o in cols]
                        vs = [kvq[K, seq, pl.ds(mo(o + TN + g * HD, HD), HD)] for o in cols]
                        keys = jnp.concatenate(ks, axis=0) if c else ks[0]
                        vals = jnp.concatenate(vs, axis=0) if c else vs[0]
                        row = lax.rem(lax.broadcasted_iota(jnp.int32, (2 * TOK, TOK), 0), TOK)
                        causal = lax.broadcasted_iota(jnp.int32, (2 * TOK, TOK), 1) <= row

                        def heads(p):
                            return [pl.ds(mo((g * 8 + 2 * p + z) * HD, HD), HD) for z in PAIR]

                        scores = []
                        for p in range(4):
                            qs = jnp.concatenate([kvq[Q, seq, o] for o in heads(p)], axis=0)
                            scores.append(dot(qs, keys, NT_DIMS))
                        for p in range(4):
                            s = scores[p]
                            own = jnp.where(causal, s[:, :TOK], -jnp.inf)
                            s = jnp.concatenate([own, s[:, TOK:]], axis=1) if c else own
                            m = jnp.max(s, axis=1, keepdims=True)
                            e = jnp.exp2((s - m) * scale)
                            o = dot(e.astype(BF), vals) * (1.0 / jnp.sum(e, axis=1, keepdims=True))
                            for z in PAIR:
                                u[seq, heads(p)[z]] = o[z * TOK : (z + 1) * TOK].astype(BF)

    def layer_a(i, mid, then, pre):
        with jax.named_scope("x_a"):
            for c in x_from_hid(i):
                c.wait()

        def kv_out(n):
            cols = pl.ds(n * TN, TN)
            return pltpu.make_async_copy(kvq.at[K, :, pl.ds(OWN_KV + n * TN, TN)], kvh.at[i, :, cols], kvo_sem.at[n])

        def finish(j, slot):
            kv = j < 2
            col = jnp.where(kv, OWN_KV + j * TN, (j - 2) * TN)
            rotate(acc.at[slot], jnp.where(j == 1, 1, 0), jnp.where(kv, K, Q), 0, col)

        with jax.named_scope("qkv_a"):

            @pl.loop(0, N_QKV)
            def _(j):
                slot = parity(j)
                wait_w(slot)

                @pl.when(j == 0)
                def _():
                    wtile(wva, 0, 1).start()

                @pl.when(j >= 1)
                def _():
                    fetch_next(j, N_QKV, lambda t: wstart(wqa, t - 2), lambda: wtile(woa, 0, 0).start())

                for n in PAIR:

                    @pl.when(j == n + 2)
                    def _(n=n):
                        kv_out(n).wait()
                        kv_sends(i, n, lambda c: c.start())

                for h in PAIR:

                    @pl.when(j == N_QKV - 2 + h)
                    def _(h=h):
                        kv_forward(i, h)

                finish(jnp.maximum(j - 1, 0), 1 - slot)
                acc[slot] = dot(x[...], wbuf[slot])

                for n in PAIR:

                    @pl.when(j == n + 1)
                    def _(n=n):
                        kv_out(n).start()

                mid(j)

            finish(N_QKV - 1, 1)

        @pl.when(i > 0)
        def _():
            kv_wait(i, PAIR)
            attention(0, N_SEQ)
            out_proj(LA, i, woa, then, pre, pl.ds(0, ROWS), True)

        @pl.when(i == 0)
        def _():
            @pl.loop(0, 2)
            def _(h):
                first = mo(OWN * (1 - h), OWN)
                kv_wait(0, (h,))
                attention(first, 2)

                def then_a():
                    @pl.when(h == 0)
                    def _():
                        wtile(woa, 0, 0).start()

                    @pl.when(h == 1)
                    def _():
                        then()

                def pre_a():
                    @pl.when(h == 1)
                    def _():
                        pre()

                out_proj(LA, 0, woa, then_a, pre_a, pl.ds(first, OWN), h == 0)

    def key_decay(h):
        back = lax.broadcasted_iota(jnp.int32, (TOK, HD), 0).astype(F32) - (TOK - 1.0)
        return jnp.exp(slopes[h] * back)

    def state_of(g, b, hh, kd):
        rows = blk(b)
        col = hcol(g, hh)
        k = (kvq[K, rows, col].astype(F32) * kd).astype(BF)
        return dot(k, kvq[V, rows, col], TN_DIMS)

    def block_decay(h):
        return jnp.exp(jnp.full((8, HD), -float(TOK), F32) * slopes[h])[0:1, :]

    def st_store(i, g, slot):
        return pltpu.make_async_copy(stg.at[slot], sth.at[i, g], sto_sem.at[slot])

    def st_load(i, g, slot):
        return pltpu.make_async_copy(str_.at[i, g], pst.at[slot], stl_sem.at[slot])

    def next_state(g):
        slot = parity(g)
        for hh in range(4):
            kd = key_decay(4 * g + hh)
            bd = block_decay(4 * g + hh)
            new = [state_of(g, b, hh, kd) for b in range(N_SEQ)]
            for b in range(N_SEQ):
                stg[slot, b * 4 + hh] = new[b] + bd * pst[slot, b * 4 + hh]

    def local_state(i, g):
        slot = parity(g)

        @pl.when(is1)
        def _():
            st_load(i, g, slot).wait()

        @pl.when(is0)
        def _():
            for hh in range(N_SEQ):
                kd = key_decay(4 * g + hh)
                for b in range(N_SEQ):
                    stg[slot, b * 4 + hh] = state_of(g, b, hh, kd)

        @pl.when(is1)
        def _():
            for hh in range(N_SEQ):
                kd = key_decay(4 * g + hh)
                bd = block_decay(4 * g + hh)
                for b in range(N_SEQ):
                    stg[slot, b * 4 + hh] = state_of(g, b, hh, kd) + bd * pst[slot, b * 4 + hh]

        st_store(i, g, slot).start()

    def st_send_on(i, g):
        st_store(i, g, parity(g)).wait()
        st_copy(i, g).start()

    def layer_b(i, mid, then, pre):
        with jax.named_scope("x_b"):
            for c in x_from_h1(i):
                c.wait()

        def finish(j, a):
            kv = j < 16
            dst = jnp.where(kv, parity(j), Q)
            kvq[dst, :, pl.ds(wcol(jnp.where(kv, j // 2, j - 16)), TN)] = (a * sigmoid(a)).astype(BF)

        with jax.named_scope("qkv_b"):
            @pl.loop(0, 24)
            def _(j):
                slot = parity(j)
                wait_w(slot)
                issue_b(j + 1)

                e = j - jnp.where(is0, 0, 2)
                busy = (cp <= 1) & (e >= 1) & (e <= 16)
                g = e // 2

                @pl.when(busy & (parity(e) == 1) & is1)
                def _():
                    st_copy(i, g).wait_recv()
                    st_load(i, g, parity(g)).start()

                finish(j, dot(x[...], wbuf[slot]))

                @pl.when(busy & (parity(e) == 0))
                def _():
                    st_send_on(i, g - 1)

                @pl.when(busy & (parity(e) == 1))
                def _():
                    local_state(i, g)

                mid(j)

        with jax.named_scope("gate"):

            @pl.loop(0, 8)
            def _(j):
                slot = parity(j)
                wait_w(slot)
                fetch_next(j, 8, lambda t: issue_b(t + 24), lambda: wtile(wol, 0, 0).start())

                @pl.when(is2)
                def _():
                    st_copy(i, j).wait_recv()
                    st_load(i, j, slot).start()

                gbuf[:, pl.ds(wcol(j), TN)] = sigmoid(dot(x[...], wbuf[slot]))

                @pl.when(is2)
                def _():
                    st_load(i, j, slot).wait()
                    next_state(j)
                    st_store(i, j, slot).start()

                    @pl.when(j >= 1)
                    def _():
                        st_send_on(i, j - 1)

        with jax.named_scope("lin"):

            @pl.when(is2)
            def _():
                st_send_on(i, N_G - 1)

            ss[...] = jnp.zeros_like(ss)

            def fetch(g):
                @pl.when(is3)
                def _():
                    st_copy(i, g).wait_recv()

                @pl.when(cp >= 1)
                def _():
                    st_load(i, g, parity(g)).start()

            @pl.when(is0)
            def _():
                pst[...] = jnp.zeros_like(pst)

            fetch(0)

            @pl.loop(0, N_G)
            def _(g):
                slot = parity(g)

                @pl.when(g + 1 < N_G)
                def _():
                    fetch(g + 1)

                for hh in range(4):
                    lam = slopes[4 * g + hh]
                    row = lax.broadcasted_iota(jnp.int32, (TOK, HD), 0).astype(F32)
                    lane = lax.broadcasted_iota(jnp.int32, (TOK, HD), 1).astype(F32)
                    gap = row - lane
                    wtab[hh, 0] = jnp.where(gap >= 0, jnp.exp(-lam * jnp.maximum(gap, 0.0)), 0.0)
                    wtab[hh, 1] = jnp.exp(-lam * (row + 1.0))

                @pl.when(cp >= 1)
                def _():
                    st_load(i, g, slot).wait()

                @pl.loop(0, 2)
                def _(half):
                    pairs = [(half * 2 + z, hh) for z in PAIR for hh in range(4)]
                    at = [(blk(b), hcol(g, hh)) for b, hh in pairs]
                    qs = [kvq[Q, r, c] for r, c in at]
                    inner = [dot(q, kvq[K, r, c], NT_DIMS) for q, (r, c) in zip(qs, at)]
                    prior = [dot(q, pst[slot, b * 4 + hh].astype(BF)) for q, (b, hh) in zip(qs, pairs)]
                    o = [
                        dot((s * wtab[hh, 0]).astype(BF), kvq[V, r, c]) + p * wtab[hh, 1]
                        for s, p, (r, c), (b, hh) in zip(inner, prior, at, pairs)
                    ]
                    for v, (r, c) in zip(o, at):
                        u[r, c] = (v * ginner[0:1, c] * gbuf[r, c]).astype(BF)
                    for z in PAIR:
                        ss[at[4 * z][0], :] += sum(v * v for v in o[4 * z : 4 * z + 4])

            sums = [jnp.sum(ss[blk(b), :].T, axis=0, keepdims=True) for b in range(N_SEQ)]
            ssx[i] = jnp.concatenate(sums + sums, axis=0)

        def then_ss():
            ss_copy(i).start()
            pre()

        out_proj(LB, i, wol, then, then_ss, pl.ds(0, ROWS), True)

        @pl.when(i >= 2)
        def _():
            ag_copy(LB, i - 1, IN_ROWS, LAST).start()

    wtile(wka, 0, 0).start()
    start_x_a(0)
    rope_in = pltpu.make_async_copy(rope_hbm.at[cp], rope.at[0], kvo_sem.at[0])
    rope_in.start()
    gains[0:1, :] = gain_a[...]
    gains[1:2, :] = gain_b[...]
    rope[1, 0] = jnp.ones((TOK, HD), F32)
    rope[1, 1] = jnp.zeros((TOK, HD), F32)
    rope[1, 2] = jnp.zeros((TOK, HD), F32)
    rope_in.wait()
    pl.semaphore_wait(bar, 4)

    @pl.loop(0, 7)
    def _(s):
        @pl.when((s < 3) | (s == 4))
        def _():
            def mid_a(j):
                @pl.when((s == 1) & (j == 4))
                def _():
                    norm(LA, 0)

            def then_a():
                @pl.when(s < 2)
                def _():
                    wtile(wka, 0, 0).start()

                @pl.when(s >= 2)
                def _():
                    wtile(wkl, 0, 0).start()

            def pre_a():
                @pl.when(s < 2)
                def _():
                    start_x_a(s + 1)

                @pl.when(s >= 2)
                def _():
                    start_x_b(jnp.where(s == 2, 0, 1))

            layer_a(jnp.where(s < 3, s, 3), mid_a, then_a, pre_a)

        @pl.when(s == 2)
        def _():
            norm(LA, 1)

        @pl.when(s >= 3)
        def _():
            def mid_b(j):
                now = jnp.where(s == 4, 3, jnp.where(s == 6, 19, 15))

                @pl.when(j == now)
                def _():
                    norm(jnp.where(s == 3, LA, LB), jnp.where(s == 3, 2, s - 4))

            def then_b():
                @pl.when(s == 3)
                def _():
                    wtile(wka, 0, 0).start()

                @pl.when((s > 3) & (s < 6))
                def _():
                    wtile(wkl, 0, 0).start()

            def pre_b():
                @pl.when(s == 3)
                def _():
                    start_x_a(3)

                @pl.when((s > 3) & (s < 6))
                def _():
                    start_x_b(s - 2)

            layer_b(s - 3, mid_b, then_b, pre_b)

        @pl.when(s == 4)
        def _():
            norm(LA, 3)

    norm(LB, 3, end=True)

    for i in range(N_CH):
        for n in PAIR:
            rs_copy(n, i, 0, DM).wait_send()
            rows = IN_ROWS if n == LB and i == N_CH - 1 else OWN
            ag_copy(n, i, 0, rows).wait_send()
        ag_wait_recv(LB, i, rows)
        ss_copy(i).wait_send()

        for n in PAIR:
            kv_sends(i, n, lambda c: c.wait_send())
            for h in PAIR:

                @pl.when(is2)
                def _(i=i, n=n, h=h):
                    kv_copy(i, n, h, 0, False, 3, 1).wait_send()

                @pl.when(is3)
                def _(i=i, n=n, h=h):
                    kv_copy(i, n, h, 1, False, 2, 0).wait_send()

        @pl.when(cp <= 2)
        def _(i=i):
            @pl.loop(0, 8)
            def _(g):
                st_copy(i, g).wait_send()


def assemble(rows, last, res, buf, in_sem, out_sem):
    tp = lax.axis_index("tp")
    parts = [(own, k, IN_ROWS if k == N_CH - 1 else OWN, False) for own in (True, False) for k in range(N_CH)]
    parts.append((True, N_CH - 1, LAST, True))

    def place(p):
        own, k, size, end = parts[p]
        first = ((tp if own else 1 - tp) * N_CH + k) * OWN + (IN_ROWS if end else 0)
        return pl.ds(mo(first, LAST), size), buf.at[p % N_CH, pl.ds(0, size)], last if end else None

    def load(p):
        at, mid, src = place(p)
        return pltpu.make_async_copy(rows.at[at] if src is None else src, mid, in_sem.at[p % N_CH])

    def store(p):
        at, mid, _ = place(p)
        return pltpu.make_async_copy(mid, res.at[at], out_sem.at[p % N_CH])

    for p in range(N_CH):
        load(p).start()
    for p in range(len(parts)):
        load(p).wait()
        store(p).start()
        if p >= 1 and p + N_CH - 1 < len(parts):
            store(p - 1).wait()
            load(p + N_CH - 1).start()
    for p in range(len(parts) - N_CH, len(parts)):
        store(p).wait()


def solution(mesh):
    n_cp = mesh.shape["cp"]
    table = rope_tables(n_cp)
    any_ = pl.BlockSpec(memory_space=pl.ANY)
    smem = pl.BlockSpec(memory_space=pltpu.SMEM)
    vmem = pl.BlockSpec(memory_space=pltpu.VMEM)
    dma = pltpu.SemaphoreType.DMA
    two = (2,)

    def body(hidden, alphas, wqa, wka, wva, woa, gain_attn, wql, wkl, wvl, wgl, slopes, gain_inner, wol, gain_lin):
        shape = hidden.shape
        hid = hidden.reshape(shape[0] * shape[1], shape[2])
        sds = jax.ShapeDtypeStruct
        outs = (
            sds(hid.shape, BF),
            sds((LAST, DM), BF),
            sds((2, N_CH, ROWS, DM), BF),
            sds((2, N_CH, OWN, DM), BF),
            sds((N_CH, OWN, DM), BF),
            sds((N_CH, OWN, DM), BF),
            sds((N_CH, ROWS, KVW), BF),
            sds((N_CH, 3, ROWS, KVW), BF),
            sds((N_CH, N_G, 16, HD, HD), F32),
            sds((N_CH, N_G, 16, HD, HD), F32),
        )
        scratch = [
            pltpu.VMEM((2, DM, TN), BF),
            pltpu.VMEM((ROWS, DM), BF),
            pltpu.VMEM((3, ROWS, W), BF),
            pltpu.VMEM((ROWS, W), F32),
            pltpu.VMEM((ROWS, W), BF),
            pltpu.VMEM((2, ROWS, TN), F32),
            pltpu.VMEM((2, ROWS, TN), BF),
            pltpu.VMEM((2, 16, HD, HD), F32),
            pltpu.VMEM((2, 16, HD, HD), F32),
            pltpu.VMEM((N_BUF, RB, DM), BF),
            pltpu.VMEM((N_BUF, RB, DM), BF),
            pltpu.VMEM((N_BUF, RB, DM), BF),
            pltpu.VMEM((N_BUF, RB, DM), BF),
            pltpu.VMEM((ROWS, HD), F32),
            pltpu.VMEM((OWN, HD), F32),
            pltpu.VMEM((2, 3, TOK, HD), F32),
            pltpu.VMEM((N_CH, 8, HD), F32),
            pltpu.VMEM((N_CH, 8, HD), F32),
            pltpu.VMEM((4, 2, TOK, HD), F32),
            pltpu.VMEM((2, DM), F32),
            dma(two), dma(two), dma(two), dma(two), dma((3, 2)), dma(two), dma(two), dma((N_BUF, 3)), dma((N_BUF,)),
            dma((2, N_CH)), dma((2, N_CH)), dma((2, N_CH)), dma((2, N_CH)), dma((N_CH, 2, 2, 2)), dma((N_CH, 2, 2, 3)), dma((N_CH, N_G)), dma((N_CH, N_G)),
            dma((N_CH,)), dma((N_CH,)),
        ]
        res = pl.pallas_call(
            kernel,
            out_shape=outs,
            in_specs=[any_] * 11 + [smem, smem, vmem, vmem, vmem],
            out_specs=tuple(any_ for _ in outs),
            scratch_shapes=scratch,
            compiler_params=pltpu.CompilerParams(
                collective_id=0, has_side_effects=True, vmem_limit_bytes=VMEM_BYTES
            ),
            name="layers",
        )(
            hid, wqa, wka, wva, woa, wql, wkl, wvl, wgl, wol, jnp.asarray(table), alphas, slopes, gain_attn.reshape(1, -1),
            gain_lin.reshape(1, -1), gain_inner.reshape(1, -1),
        )
        got = lax.ppermute(res[1], "tp", [(0, 1), (1, 0)])
        rows = pl.pallas_call(
            assemble,
            out_shape=sds(hid.shape, BF),
            in_specs=[any_, any_],
            out_specs=any_,
            scratch_shapes=[pltpu.VMEM((N_CH, OWN, DM), BF), dma((N_CH,)), dma((N_CH,))],
            compiler_params=pltpu.CompilerParams(vmem_limit_bytes=VMEM_BYTES),
            cost_estimate=pl.CostEstimate(flops=10**11, bytes_accessed=2 * hid.size * 2, transcendentals=0),
            name="assemble",
        )(res[0], res[1])
        row = ((1 - lax.axis_index("tp")) * N_CH + N_CH - 1) * OWN + IN_ROWS
        return lax.dynamic_update_slice(rows, got, (row, 0)).reshape(shape)

    act = P("dp", "cp", None)
    rep = P()
    col = P(None, "tp")
    row = P("tp", None)
    vec = P("tp")
    in_specs = (act, rep, col, col, col, row, rep, col, col, col, col, vec, vec, row, rep)
    return jax.shard_map(body, mesh=mesh, in_specs=in_specs, out_specs=act, check_vma=False)
```

```python
import math

import jax
import jax.numpy as jnp
import numpy as np
from jax import lax
from jax.experimental import pallas as pl
from jax.experimental.pallas import tpu as pltpu
from jax.sharding import PartitionSpec as P

MESH = pl.DeviceIdType.MESH
F32 = jnp.float32
BF = jnp.bfloat16
ROPE_BASE = 10000000.0
EPS = 1e-5

VMEM_BYTES = 67043328
TOK = 128
HD = 128
TN = 512
DM = 6144
W = 4096
KVW = 1024
OWN_KV = W - KVW
N_SEQ = 4
N_CH = 4
N_CP = 4
N_G = 8
ROWS = N_SEQ * TOK
OWN = ROWS // 2
RB = 32
N_RB = OWN // RB
R_IN = N_RB - 2
IN_ROWS = R_IN * RB
N_FIN = 2 * N_CH + 1
LAST = OWN - IN_ROWS
N_QKV = (KVW + W) // TN
N_WO = DM // TN
N_BUF = 4
LA, LB = 0, 1
PAIR = range(2)
K, V, Q = 0, 1, 2
NT_DIMS = (((1,), (1,)), ((), ()))
TN_DIMS = (((0,), (0,)), ((), ()))


def rope_tables(n_cp):
    half = HD // 4
    inv = ROPE_BASE ** (-np.arange(half, dtype=np.float64) * 2.0 / (2 * half))
    pos = np.arange(n_cp * TOK, dtype=np.float64)
    ang = pos[:, None] * inv[None, :]
    tab = np.zeros((3, n_cp * TOK, HD), np.float32)
    tab[0] = 1.0
    tab[0, :, :half] = np.cos(ang)
    tab[0, :, half : 2 * half] = np.cos(ang)
    tab[1, :, :half] = -np.sin(ang)
    tab[2, :, half : 2 * half] = np.sin(ang)
    return np.ascontiguousarray(tab.reshape(3, n_cp, TOK, HD).transpose(1, 0, 2, 3))


def mo(v, m):
    return pl.multiple_of(v, m)


def parity(j):
    return lax.rem(j, 2)


def blk(b):
    return pl.ds(mo(b * TOK, TOK), TOK)


def hcol(g, hh):
    return pl.ds(mo((4 * g + hh) * HD, HD), HD)


def dot(a, b, dims=(((1,), (0,)), ((), ()))):
    return lax.dot_general(a, b, dims, preferred_element_type=F32)


def sigmoid(z):
    return 1.0 / (1.0 + jnp.exp(-z))


def kernel(
    hid, wqa, wka, wva, woa, wql, wkl, wvl, wgl, wol, rope_hbm, alphas, slopes, gain_a, gain_b, ginner,
    out, last, pt, prec, h1own, h1oth, kvh, kvr, sth, str_,
    wbuf, x, kvq, gbuf, u, acc, ost, stg, pst, nb_p, nb_r, nb_h, nout, ss, rsb, rope, ssx, ssr, wtab, gains,
    w_sem, x_sem, o_sem, kvo_sem, kvl_sem, sto_sem, stl_sem, nl_sem, no_sem,
    rs_send, rs_recv, ag_send, ag_recv, kv_send, kv_recv, st_send, st_recv, ss_send, ss_recv,
):
    cp = lax.axis_index("cp")
    tp = lax.axis_index("tp")
    mate = 1 - tp
    is0, is1, is2, is3 = (cp == c for c in range(N_CP))

    bar = pltpu.get_barrier_semaphore()
    pl.semaphore_signal(bar, inc=1, device_id={"tp": mate}, device_id_type=MESH)
    for d in range(1, 4):
        pl.semaphore_signal(bar, inc=1, device_id={"cp": lax.rem(cp + d, 4)}, device_id_type=MESH)

    def wtile(src, col, slot):
        rows = pl.ds(0, src.shape[0])
        return pltpu.make_async_copy(src.at[:, pl.ds(col, TN)], wbuf.at[slot, rows], w_sem.at[slot])

    def wstart(src, j):
        wtile(src, wcol(j), parity(j)).start()

    def wcol(j):
        return mo(j * TN, TN)

    def issue_b(j):
        kv = j < 16
        for cond, w, tile in (
            (kv & (parity(j) == 0), wkl, j // 2),
            (kv & (parity(j) == 1), wvl, j // 2),
            ((j >= 16) & (j < 24), wql, j - 16),
            (j >= 24, wgl, j - 24),
        ):

            @pl.when(cond)
            def _(w=w, tile=tile):
                wtile(w, wcol(tile), parity(j)).start()

    def wait_w(slot, src=wqa):
        wtile(src, 0, slot).wait()

    def fetch_next(j, count, go, then):
        @pl.when(j + 1 < count)
        def _():
            go(j + 1)

        @pl.when(j + 1 >= count)
        def _():
            then()

    def own_row(i):
        return mo((tp * 8 + 2 * i) * TOK, TOK)

    def oth_row(i):
        return mo((mate * 8 + 2 * i) * TOK, TOK)

    def x_copies(top, bot):
        return (
            pltpu.make_async_copy(top, x.at[pl.ds(0, OWN)], x_sem.at[0]),
            pltpu.make_async_copy(bot, x.at[pl.ds(OWN, OWN)], x_sem.at[1]),
        )

    def x_from_hid(i):
        return x_copies(hid.at[pl.ds(own_row(i), OWN)], hid.at[pl.ds(oth_row(i), OWN)])

    def x_from_h1(i):
        return x_copies(h1own.at[i], h1oth.at[i])

    def start_x_a(i):
        for c in x_from_hid(i):
            c.start()

    def start_x_b(i):
        ag_wait_recv(LA, i)
        for c in x_from_h1(i):
            c.start()

    def rs_copy(n, i, col, width):
        return pltpu.make_async_remote_copy(
            src_ref=pt.at[n, i, pl.ds(OWN, OWN), pl.ds(col, width)],
            dst_ref=prec.at[n, i, :, pl.ds(col, width)],
            send_sem=rs_send.at[n, i],
            recv_sem=rs_recv.at[n, i],
            device_id={"tp": mate},
            device_id_type=MESH,
        )

    def ag_copy(n, i, row, rows):
        if n == 0:
            src = h1own.at[i, pl.ds(row, rows)]
            dst = h1oth.at[i, pl.ds(row, rows)]
        else:
            src = out.at[pl.ds(mo(own_row(i) + row, RB), rows)]
            dst = src
        return pltpu.make_async_remote_copy(
            src_ref=src,
            dst_ref=dst,
            send_sem=ag_send.at[n, i],
            recv_sem=ag_recv.at[n, i],
            device_id={"tp": mate},
            device_id_type=MESH,
        )

    def ag_wait_recv(n, i, rows=OWN):
        if n == 0:
            ag_copy(0, i, 0, rows).wait_recv()
        else:
            oth = out.at[pl.ds(oth_row(i), rows)]
            pltpu.make_async_remote_copy(
                src_ref=oth,
                dst_ref=oth,
                send_sem=ag_send.at[n, i],
                recv_sem=ag_recv.at[n, i],
                device_id={"tp": mate},
                device_id_type=MESH,
            ).wait_recv()

    def half_rows(h):
        return pl.ds(mo(OWN * (1 - h), OWN), OWN)

    def kv_copy(i, n, h, src, own, dst_cp, send):
        at = half_rows(h), pl.ds(n * TN, TN)
        return pltpu.make_async_remote_copy(
            src_ref=kvh.at[i, *at] if own else kvr.at[i, src, *at],
            dst_ref=kvr.at[i, src, *at],
            send_sem=kv_send.at[i, n, h, send],
            recv_sem=kv_recv.at[i, n, h, src],
            device_id={"cp": dst_cp},
            device_id_type=MESH,
        )

    def kv_sends(i, n, go):
        for h in PAIR:

            @pl.when(is0)
            def _(h=h):
                go(kv_copy(i, n, h, 0, True, 2, 0))
                go(kv_copy(i, n, h, 0, True, 1, 1))

            @pl.when(is1)
            def _(h=h):
                go(kv_copy(i, n, h, 1, True, 3, 0))

            @pl.when(is2)
            def _(h=h):
                go(kv_copy(i, n, h, 2, True, 3, 0))

    def st_copy(i, g):
        return pltpu.make_async_remote_copy(
            src_ref=sth.at[i, g],
            dst_ref=str_.at[i, g],
            send_sem=st_send.at[i, g],
            recv_sem=st_recv.at[i, g],
            device_id={"cp": lax.rem(cp + 1, 4)},
            device_id_type=MESH,
        )

    def ss_copy(i):
        return pltpu.make_async_remote_copy(
            src_ref=ssx.at[i],
            dst_ref=ssr.at[i],
            send_sem=ss_send.at[i],
            recv_sem=ss_recv.at[i],
            device_id={"tp": mate},
            device_id_type=MESH,
        )

    def norm_loads(n, i, r, start):
        slot = lax.rem(r, N_BUF)
        rows = pl.ds(mo(r * RB, RB), RB)
        copies = [
            pltpu.make_async_copy(pt.at[n, i, rows], nb_p.at[slot], nl_sem.at[slot, 0]),
            pltpu.make_async_copy(prec.at[n, i, rows], nb_r.at[slot], nl_sem.at[slot, 1]),
        ]
        res_a = hid.at[pl.ds(mo(own_row(i) + r * RB, RB), RB)]
        res_b = h1own.at[i, rows]
        for layer, res in ((LA, res_a), (LB, res_b)):

            @pl.when(n == layer)
            def _(res=res):
                c = pltpu.make_async_copy(res, nb_h.at[slot], nl_sem.at[slot, 2])
                c.start() if start else c.wait()

        for c in copies:
            c.start() if start else c.wait()

    def norm_begin(n, i):
        with jax.named_scope("norm_wait"):
            rs_copy(n, i, 0, DM).wait_recv()

            @pl.when(n == LB)
            def _():
                ss_copy(i).wait_recv()
                for b in PAIR:
                    whole = ssx[i, b : b + 1, :] + ssr[i, b + 2 : b + 3, :]
                    inv = lax.rsqrt(whole / float(2 * W) + EPS)
                    rsb[blk(b), :] = jnp.broadcast_to(inv, (TOK, TOK)).T

            @pl.when(n == LA)
            def _():
                rsb[...] = jnp.ones_like(rsb)

            for r in range(N_BUF - 1):
                norm_loads(n, i, r, True)

    def norm_ready(n, i, r):
        @pl.when(r + N_BUF - 1 < N_RB)
        def _():
            norm_loads(n, i, r + N_BUF - 1, True)

        norm_loads(n, i, r, False)

    def norm_rows(n, r):
        slot = lax.rem(r, N_BUF)
        alpha = alphas[n]
        for q in range(RB // 16):
            rows = slice(q * 16, (q + 1) * 16)
            both = nb_p[slot, rows, :].astype(F32) + nb_r[slot, rows, :].astype(F32)
            both = both * rsb[pl.ds(mo(r * RB + q * 16, 16), 16), 0:1]
            h = alpha * nb_h[slot, rows, :].astype(F32) + both
            inv = lax.rsqrt(jnp.mean(h * h, axis=-1, keepdims=True) + EPS)
            nout[slot, rows, :] = (h * inv * gains[pl.ds(n, 1), :]).astype(BF)

    def norm_store(n, i, r, start, end):
        slot = lax.rem(r, N_BUF)
        dst_a = h1own.at[i, pl.ds(mo(r * RB, RB), RB)]
        dst_b = out.at[pl.ds(mo(own_row(i) + r * RB, RB), RB)]
        inside = r < R_IN if end else True
        if end:

            @pl.when(r >= R_IN)
            def _():
                c = pltpu.make_async_copy(nout.at[slot], last.at[pl.ds(mo((r - R_IN) * RB, RB), RB)], no_sem.at[slot])
                c.start() if start else c.wait()

        for layer, dst in ((LA, dst_a), (LB, dst_b)):

            @pl.when((n == layer) & inside)
            def _(layer=layer, dst=dst):
                c = pltpu.make_async_copy(nout.at[slot], dst, no_sem.at[slot])
                if start:
                    c.start()
                else:
                    c.wait()

                    @pl.when((layer == LA) | (i == 0) | end | (r < R_IN))
                    def _():
                        ag_copy(layer, i, mo(r * RB, RB), RB).start()

    def norm_out(n, i, r, end):
        @pl.when(r >= 2)
        def _():
            norm_store(n, i, r - 2, False, end)

        norm_store(n, i, r, True, end)

    def norm_end(n, i, end):
        for r in range(N_RB - 2, N_RB):
            norm_store(n, i, r, False, end)

    def norm_run(n, i, end=False):
        with jax.named_scope("norm"):

            @pl.loop(0, N_RB)
            def _(r):
                norm_ready(n, i, r)
                norm_rows(n, r)
                norm_out(n, i, r, end)

            norm_end(n, i, end)

    def norm(n, i, end=False):
        norm_begin(n, i)
        norm_run(n, i, end)

    def out_proj(n, i, wo, then, pre, rows, send):
        def put(j, slot):
            size = pl.ds(0, rows.size)
            return pltpu.make_async_copy(ost.at[slot, size], pt.at[n, i, rows, pl.ds(wcol(j), TN)], o_sem.at[slot])

        def send_on(j, slot):
            put(j, slot).wait()

            @pl.when(send)
            def _():
                rs_copy(n, i, wcol(j), TN).start()

        with jax.named_scope("out_proj"):
            wtile(wo, TN, 1).start()

            @pl.loop(0, N_WO)
            def _(j):
                slot = parity(j)
                wait_w(slot, wo)

                @pl.when(j == 8)
                def _():
                    pre()

                ost[slot, 0 : rows.size, :] = dot(u[rows, :], wbuf[slot, 0:W, :]).astype(BF)

                @pl.when(j + 2 < N_WO)
                def _():
                    wstart(wo, j + 2)

                @pl.when(j + 2 == N_WO)
                def _():
                    then()

                @pl.when(j >= 1)
                def _():
                    send_on(j - 1, 1 - slot)

                put(j, slot).start()

            send_on(N_WO - 1, 1)

    def rotate(a, kind, dst, row, col):
        for b in range(a.shape[0] // TOK):
            for h in range(TN // HD):
                v = a[b * TOK : (b + 1) * TOK, h * HD : (h + 1) * HD]
                v = v * rope[kind, 0] + pltpu.roll(v, HD - 32, 1) * rope[kind, 1] + pltpu.roll(v, 32, 1) * rope[kind, 2]
                kvq[dst, pl.ds(mo(row + b * TOK, TOK), TOK), pl.ds(mo(col + h * HD, HD), HD)] = v.astype(BF)

    def kv_forward(i, h):
        for n in PAIR:

            @pl.when(is2)
            def _(n=n):
                kv_copy(i, n, h, 0, False, 3, 1).wait_recv()
                kv_copy(i, n, h, 0, False, 3, 1).start()

            @pl.when(is3)
            def _(n=n):
                kv_copy(i, n, h, 1, False, 2, 0).wait_recv()
                kv_copy(i, n, h, 1, False, 2, 0).start()

    def kv_wait(i, halves):
        parts = [(n, h) for h in halves for n in PAIR]

        def got(n, h, src):
            kv_copy(i, n, h, src, False, 0, 0).wait_recv()

        def fetch(c, h):
            rows = half_rows(h)
            dst = kvq.at[K, rows, pl.ds(c * KVW, KVW)]
            return pltpu.make_async_copy(kvr.at[i, c, rows], dst, kvl_sem.at[c, h])

        with jax.named_scope("kv_wait"):
            for n, h in parts:

                @pl.when(is1)
                def _(n=n, h=h):
                    got(n, h, 0)

                @pl.when(is2)
                def _(n=n, h=h):
                    got(n, h, 1)

                @pl.when(is3)
                def _(n=n, h=h):
                    got(n, h, 2)
                    got(n, h, 0)

            for go in (lambda c: c.start(), lambda c: c.wait()):
                for c in range(N_CP - 1):

                    @pl.when(cp > c)
                    def _(c=c, go=go):
                        for h in halves:
                            go(fetch(c, h))

    def attention(first, count):
        scale = math.log2(math.e) / math.sqrt(HD)
        with jax.named_scope("attn"):
            for c in range(N_CP):

                @pl.when(cp == c)
                def _(c=c):
                    cols = [OWN_KV] + [b * KVW for b in range(c)]

                    @pl.loop(0, 4 * count)
                    def _(t):
                        g = lax.rem(t, 4)
                        seq = pl.ds(mo(first + t // 4 * TOK, TOK), TOK)
                        ks = [kvq[K, seq, pl.ds(mo(o + g * HD, HD), HD)] for o in cols]
                        vs = [kvq[K, seq, pl.ds(mo(o + TN + g * HD, HD), HD)] for o in cols]
                        keys = jnp.concatenate(ks, axis=0) if c else ks[0]
                        vals = jnp.concatenate(vs, axis=0) if c else vs[0]
                        row = lax.rem(lax.broadcasted_iota(jnp.int32, (2 * TOK, TOK), 0), TOK)
                        causal = lax.broadcasted_iota(jnp.int32, (2 * TOK, TOK), 1) <= row

                        def heads(p):
                            return [pl.ds(mo((g * 8 + 2 * p + z) * HD, HD), HD) for z in PAIR]

                        scores = []
                        for p in range(4):
                            qs = jnp.concatenate([kvq[Q, seq, o] for o in heads(p)], axis=0)
                            scores.append(dot(qs, keys, NT_DIMS))
                        for p in range(4):
                            s = scores[p]
                            own = jnp.where(causal, s[:, :TOK], -jnp.inf)
                            s = jnp.concatenate([own, s[:, TOK:]], axis=1) if c else own
                            m = jnp.max(s, axis=1, keepdims=True)
                            e = jnp.exp2((s - m) * scale)
                            o = dot(e.astype(BF), vals) * (1.0 / jnp.sum(e, axis=1, keepdims=True))
                            for z in PAIR:
                                u[seq, heads(p)[z]] = o[z * TOK : (z + 1) * TOK].astype(BF)

    def layer_a(i, mid, then, pre):
        with jax.named_scope("x_a"):
            for c in x_from_hid(i):
                c.wait()

        def kv_out(n):
            cols = pl.ds(n * TN, TN)
            return pltpu.make_async_copy(kvq.at[K, :, pl.ds(OWN_KV + n * TN, TN)], kvh.at[i, :, cols], kvo_sem.at[n])

        def finish(j, slot):
            kv = j < 2
            col = jnp.where(kv, OWN_KV + j * TN, (j - 2) * TN)
            rotate(acc.at[slot], jnp.where(j == 1, 1, 0), jnp.where(kv, K, Q), 0, col)

        with jax.named_scope("qkv_a"):

            @pl.loop(0, N_QKV)
            def _(j):
                slot = parity(j)
                wait_w(slot)

                @pl.when(j == 0)
                def _():
                    wtile(wva, 0, 1).start()

                @pl.when(j >= 1)
                def _():
                    fetch_next(j, N_QKV, lambda t: wstart(wqa, t - 2), lambda: wtile(woa, 0, 0).start())

                for n in PAIR:

                    @pl.when(j == n + 2)
                    def _(n=n):
                        kv_out(n).wait()
                        kv_sends(i, n, lambda c: c.start())

                for h in PAIR:

                    @pl.when(j == N_QKV - 2 + h)
                    def _(h=h):
                        kv_forward(i, h)

                finish(jnp.maximum(j - 1, 0), 1 - slot)
                acc[slot] = dot(x[...], wbuf[slot])

                for n in PAIR:

                    @pl.when(j == n + 1)
                    def _(n=n):
                        kv_out(n).start()

                mid(j)

            finish(N_QKV - 1, 1)

        @pl.when(i > 0)
        def _():
            kv_wait(i, PAIR)
            attention(0, N_SEQ)
            out_proj(LA, i, woa, then, pre, pl.ds(0, ROWS), True)

        @pl.when(i == 0)
        def _():
            @pl.loop(0, 2)
            def _(h):
                first = mo(OWN * (1 - h), OWN)
                kv_wait(0, (h,))
                attention(first, 2)

                def then_a():
                    @pl.when(h == 0)
                    def _():
                        wtile(woa, 0, 0).start()

                    @pl.when(h == 1)
                    def _():
                        then()

                def pre_a():
                    @pl.when(h == 1)
                    def _():
                        pre()

                out_proj(LA, 0, woa, then_a, pre_a, pl.ds(first, OWN), h == 0)

    def key_decay(h):
        back = lax.broadcasted_iota(jnp.int32, (TOK, HD), 0).astype(F32) - (TOK - 1.0)
        return jnp.exp(slopes[h] * back)

    def state_of(g, b, hh, kd):
        rows = blk(b)
        col = hcol(g, hh)
        k = (kvq[K, rows, col].astype(F32) * kd).astype(BF)
        return dot(k, kvq[V, rows, col], TN_DIMS)

    def block_decay(h):
        return jnp.exp(jnp.full((8, HD), -float(TOK), F32) * slopes[h])[0:1, :]

    def st_store(i, g, slot):
        return pltpu.make_async_copy(stg.at[slot], sth.at[i, g], sto_sem.at[slot])

    def st_load(i, g, slot):
        return pltpu.make_async_copy(str_.at[i, g], pst.at[slot], stl_sem.at[slot])

    def next_state(g):
        slot = parity(g)
        for hh in range(4):
            kd = key_decay(4 * g + hh)
            bd = block_decay(4 * g + hh)
            new = [state_of(g, b, hh, kd) for b in range(N_SEQ)]
            for b in range(N_SEQ):
                stg[slot, b * 4 + hh] = new[b] + bd * pst[slot, b * 4 + hh]

    def local_state(i, g):
        slot = parity(g)

        @pl.when(is1)
        def _():
            st_load(i, g, slot).wait()

        @pl.when(is0)
        def _():
            for hh in range(N_SEQ):
                kd = key_decay(4 * g + hh)
                for b in range(N_SEQ):
                    stg[slot, b * 4 + hh] = state_of(g, b, hh, kd)

        @pl.when(is1)
        def _():
            for hh in range(N_SEQ):
                kd = key_decay(4 * g + hh)
                bd = block_decay(4 * g + hh)
                for b in range(N_SEQ):
                    stg[slot, b * 4 + hh] = state_of(g, b, hh, kd) + bd * pst[slot, b * 4 + hh]

        st_store(i, g, slot).start()

    def st_send_on(i, g):
        st_store(i, g, parity(g)).wait()
        st_copy(i, g).start()

    def layer_b(i, mid, then, pre):
        with jax.named_scope("x_b"):
            for c in x_from_h1(i):
                c.wait()

        def finish(j, a):
            kv = j < 16
            dst = jnp.where(kv, parity(j), Q)
            kvq[dst, :, pl.ds(wcol(jnp.where(kv, j // 2, j - 16)), TN)] = (a * sigmoid(a)).astype(BF)

        with jax.named_scope("qkv_b"):
            @pl.loop(0, 24)
            def _(j):
                slot = parity(j)
                wait_w(slot)
                issue_b(j + 1)

                e = j - jnp.where(is0, 0, 2)
                busy = (cp <= 1) & (e >= 1) & (e <= 16)
                g = e // 2

                @pl.when(busy & (parity(e) == 1) & is1)
                def _():
                    st_copy(i, g).wait_recv()
                    st_load(i, g, parity(g)).start()

                mid(j, norm_begin)
                finish(j, dot(x[...], wbuf[slot]))

                @pl.when(busy & (parity(e) == 0))
                def _():
                    st_send_on(i, g - 1)

                @pl.when(busy & (parity(e) == 1))
                def _():
                    local_state(i, g)

                mid(j, norm_run)

        with jax.named_scope("gate"):

            @pl.loop(0, 8)
            def _(j):
                slot = parity(j)
                wait_w(slot)
                fetch_next(j, 8, lambda t: issue_b(t + 24), lambda: wtile(wol, 0, 0).start())

                @pl.when(is2)
                def _():
                    st_copy(i, j).wait_recv()
                    st_load(i, j, slot).start()

                gbuf[:, pl.ds(wcol(j), TN)] = sigmoid(dot(x[...], wbuf[slot]))

                @pl.when(is2)
                def _():
                    st_load(i, j, slot).wait()
                    next_state(j)
                    st_store(i, j, slot).start()

                    @pl.when(j >= 1)
                    def _():
                        st_send_on(i, j - 1)

        with jax.named_scope("lin"):

            @pl.when(is2)
            def _():
                st_send_on(i, N_G - 1)

            ss[...] = jnp.zeros_like(ss)

            def fetch(g):
                @pl.when(is3)
                def _():
                    st_copy(i, g).wait_recv()

                @pl.when(cp >= 1)
                def _():
                    st_load(i, g, parity(g)).start()

            @pl.when(is0)
            def _():
                pst[...] = jnp.zeros_like(pst)

            fetch(0)

            @pl.loop(0, N_G)
            def _(g):
                slot = parity(g)

                @pl.when(g + 1 < N_G)
                def _():
                    fetch(g + 1)

                for hh in range(4):
                    lam = slopes[4 * g + hh]
                    row = lax.broadcasted_iota(jnp.int32, (TOK, HD), 0).astype(F32)
                    lane = lax.broadcasted_iota(jnp.int32, (TOK, HD), 1).astype(F32)
                    gap = row - lane
                    wtab[hh, 0] = jnp.where(gap >= 0, jnp.exp(-lam * jnp.maximum(gap, 0.0)), 0.0)
                    wtab[hh, 1] = jnp.exp(-lam * (row + 1.0))

                @pl.when(cp >= 1)
                def _():
                    st_load(i, g, slot).wait()

                @pl.loop(0, 2)
                def _(half):
                    pairs = [(half * 2 + z, hh) for z in PAIR for hh in range(4)]
                    at = [(blk(b), hcol(g, hh)) for b, hh in pairs]
                    qs = [kvq[Q, r, c] for r, c in at]
                    inner = [dot(q, kvq[K, r, c], NT_DIMS) for q, (r, c) in zip(qs, at)]
                    prior = [dot(q, pst[slot, b * 4 + hh].astype(BF)) for q, (b, hh) in zip(qs, pairs)]
                    o = [
                        dot((s * wtab[hh, 0]).astype(BF), kvq[V, r, c]) + p * wtab[hh, 1]
                        for s, p, (r, c), (b, hh) in zip(inner, prior, at, pairs)
                    ]
                    for v, (r, c) in zip(o, at):
                        u[r, c] = (v * ginner[0:1, c] * gbuf[r, c]).astype(BF)
                    for z in PAIR:
                        ss[at[4 * z][0], :] += sum(v * v for v in o[4 * z : 4 * z + 4])

            sums = [jnp.sum(ss[blk(b), :].T, axis=0, keepdims=True) for b in range(N_SEQ)]
            ssx[i] = jnp.concatenate(sums + sums, axis=0)

        def then_ss():
            ss_copy(i).start()
            pre()

        out_proj(LB, i, wol, then, then_ss, pl.ds(0, ROWS), True)

        @pl.when(i >= 2)
        def _():
            ag_copy(LB, i - 1, IN_ROWS, LAST).start()

    wtile(wka, 0, 0).start()
    start_x_a(0)
    rope_in = pltpu.make_async_copy(rope_hbm.at[cp], rope.at[0], kvo_sem.at[0])
    rope_in.start()
    gains[0:1, :] = gain_a[...]
    gains[1:2, :] = gain_b[...]
    rope[1, 0] = jnp.ones((TOK, HD), F32)
    rope[1, 1] = jnp.zeros((TOK, HD), F32)
    rope[1, 2] = jnp.zeros((TOK, HD), F32)
    rope_in.wait()
    pl.semaphore_wait(bar, 4)

    @pl.loop(0, 7)
    def _(s):
        @pl.when((s < 3) | (s == 4))
        def _():
            def mid_a(j):
                @pl.when((s == 1) & (j == 4))
                def _():
                    norm(LA, 0)

            def then_a():
                @pl.when(s < 2)
                def _():
                    wtile(wka, 0, 0).start()

                @pl.when(s >= 2)
                def _():
                    wtile(wkl, 0, 0).start()

            def pre_a():
                @pl.when(s < 2)
                def _():
                    start_x_a(s + 1)

                @pl.when(s >= 2)
                def _():
                    start_x_b(jnp.where(s == 2, 0, 1))

            layer_a(jnp.where(s < 3, s, 3), mid_a, then_a, pre_a)

        @pl.when(s == 2)
        def _():
            norm(LA, 1)

        @pl.when(s >= 3)
        def _():
            def mid_b(j, go):
                now = jnp.where(s == 4, 4, jnp.where(s == 6, 19, 15))

                @pl.when(j == now)
                def _():
                    go(jnp.where(s == 3, LA, LB), jnp.where(s == 3, 2, s - 4))

            def then_b():
                @pl.when(s == 3)
                def _():
                    wtile(wka, 0, 0).start()

                @pl.when((s > 3) & (s < 6))
                def _():
                    wtile(wkl, 0, 0).start()

            def pre_b():
                @pl.when(s == 3)
                def _():
                    start_x_a(3)

                @pl.when((s > 3) & (s < 6))
                def _():
                    start_x_b(s - 2)

            layer_b(s - 3, mid_b, then_b, pre_b)

        @pl.when(s == 4)
        def _():
            norm(LA, 3)

    norm(LB, 3, end=True)

    for i in range(N_CH):
        for n in PAIR:
            rs_copy(n, i, 0, DM).wait_send()
            rows = IN_ROWS if n == LB and i == N_CH - 1 else OWN
            ag_copy(n, i, 0, rows).wait_send()
        ag_wait_recv(LB, i, rows)
        ss_copy(i).wait_send()

        for n in PAIR:
            kv_sends(i, n, lambda c: c.wait_send())
            for h in PAIR:

                @pl.when(is2)
                def _(i=i, n=n, h=h):
                    kv_copy(i, n, h, 0, False, 3, 1).wait_send()

                @pl.when(is3)
                def _(i=i, n=n, h=h):
                    kv_copy(i, n, h, 1, False, 2, 0).wait_send()

        @pl.when(cp <= 2)
        def _(i=i):
            @pl.loop(0, 8)
            def _(g):
                st_copy(i, g).wait_send()


def assemble(rows, last, res, buf, in_sem, out_sem):
    tp = lax.axis_index("tp")
    parts = [(own, k, IN_ROWS if k == N_CH - 1 else OWN, False) for own in (True, False) for k in range(N_CH)]
    parts.append((True, N_CH - 1, LAST, True))

    def place(p):
        own, k, size, end = parts[p]
        first = ((tp if own else 1 - tp) * N_CH + k) * OWN + (IN_ROWS if end else 0)
        return pl.ds(mo(first, LAST), size), buf.at[p, pl.ds(0, size)], last if end else None

    def load(p):
        at, mid, src = place(p)
        return pltpu.make_async_copy(rows.at[at] if src is None else src, mid, in_sem.at[p])

    def store(p):
        at, mid, _ = place(p)
        return pltpu.make_async_copy(mid, res.at[at], out_sem.at[p])

    for p in range(N_FIN):
        load(p).start()
    for p in range(N_FIN):
        load(p).wait()
        store(p).start()
    for p in range(N_FIN):
        store(p).wait()


def solution(mesh):
    n_cp = mesh.shape["cp"]
    table = rope_tables(n_cp)
    any_ = pl.BlockSpec(memory_space=pl.ANY)
    smem = pl.BlockSpec(memory_space=pltpu.SMEM)
    vmem = pl.BlockSpec(memory_space=pltpu.VMEM)
    dma = pltpu.SemaphoreType.DMA
    two = (2,)

    def body(hidden, alphas, wqa, wka, wva, woa, gain_attn, wql, wkl, wvl, wgl, slopes, gain_inner, wol, gain_lin):
        shape = hidden.shape
        hid = hidden.reshape(shape[0] * shape[1], shape[2])
        sds = jax.ShapeDtypeStruct
        outs = (
            sds(hid.shape, BF),
            sds((LAST, DM), BF),
            sds((2, N_CH, ROWS, DM), BF),
            sds((2, N_CH, OWN, DM), BF),
            sds((N_CH, OWN, DM), BF),
            sds((N_CH, OWN, DM), BF),
            sds((N_CH, ROWS, KVW), BF),
            sds((N_CH, 3, ROWS, KVW), BF),
            sds((N_CH, N_G, 16, HD, HD), F32),
            sds((N_CH, N_G, 16, HD, HD), F32),
        )
        scratch = [
            pltpu.VMEM((2, DM, TN), BF),
            pltpu.VMEM((ROWS, DM), BF),
            pltpu.VMEM((3, ROWS, W), BF),
            pltpu.VMEM((ROWS, W), F32),
            pltpu.VMEM((ROWS, W), BF),
            pltpu.VMEM((2, ROWS, TN), F32),
            pltpu.VMEM((2, ROWS, TN), BF),
            pltpu.VMEM((2, 16, HD, HD), F32),
            pltpu.VMEM((2, 16, HD, HD), F32),
            pltpu.VMEM((N_BUF, RB, DM), BF),
            pltpu.VMEM((N_BUF, RB, DM), BF),
            pltpu.VMEM((N_BUF, RB, DM), BF),
            pltpu.VMEM((N_BUF, RB, DM), BF),
            pltpu.VMEM((ROWS, HD), F32),
            pltpu.VMEM((OWN, HD), F32),
            pltpu.VMEM((2, 3, TOK, HD), F32),
            pltpu.VMEM((N_CH, 8, HD), F32),
            pltpu.VMEM((N_CH, 8, HD), F32),
            pltpu.VMEM((4, 2, TOK, HD), F32),
            pltpu.VMEM((2, DM), F32),
            dma(two), dma(two), dma(two), dma(two), dma((3, 2)), dma(two), dma(two), dma((N_BUF, 3)), dma((N_BUF,)),
            dma((2, N_CH)), dma((2, N_CH)), dma((2, N_CH)), dma((2, N_CH)), dma((N_CH, 2, 2, 2)), dma((N_CH, 2, 2, 3)), dma((N_CH, N_G)), dma((N_CH, N_G)),
            dma((N_CH,)), dma((N_CH,)),
        ]
        res = pl.pallas_call(
            kernel,
            out_shape=outs,
            in_specs=[any_] * 11 + [smem, smem, vmem, vmem, vmem],
            out_specs=tuple(any_ for _ in outs),
            scratch_shapes=scratch,
            compiler_params=pltpu.CompilerParams(
                collective_id=0, has_side_effects=True, vmem_limit_bytes=VMEM_BYTES
            ),
            name="layers",
        )(
            hid, wqa, wka, wva, woa, wql, wkl, wvl, wgl, wol, jnp.asarray(table), alphas, slopes, gain_attn.reshape(1, -1),
            gain_lin.reshape(1, -1), gain_inner.reshape(1, -1),
        )
        got = lax.ppermute(res[1], "tp", [(0, 1), (1, 0)])
        rows = pl.pallas_call(
            assemble,
            out_shape=sds(hid.shape, BF),
            in_specs=[any_, any_],
            out_specs=any_,
            scratch_shapes=[pltpu.VMEM((N_FIN, OWN, DM), BF), dma((N_FIN,)), dma((N_FIN,))],
            compiler_params=pltpu.CompilerParams(vmem_limit_bytes=VMEM_BYTES),
            cost_estimate=pl.CostEstimate(flops=10**11, bytes_accessed=2 * hid.size * 2, transcendentals=0),
            name="assemble",
        )(res[0], res[1])
        row = ((1 - lax.axis_index("tp")) * N_CH + N_CH - 1) * OWN + IN_ROWS
        return lax.dynamic_update_slice(rows, got, (row, 0)).reshape(shape)

    act = P("dp", "cp", None)
    rep = P()
    col = P(None, "tp")
    row = P("tp", None)
    vec = P("tp")
    in_specs = (act, rep, col, col, col, row, rep, col, col, col, col, vec, vec, row, rep)
    return jax.shard_map(body, mesh=mesh, in_specs=in_specs, out_specs=act, check_vma=False)
```

```python
import math

import jax
import jax.numpy as jnp
import numpy as np
from jax import lax
from jax.experimental import pallas as pl
from jax.experimental.pallas import tpu as pltpu
from jax.sharding import PartitionSpec as P

MESH = pl.DeviceIdType.MESH
F32 = jnp.float32
BF = jnp.bfloat16
ROPE_BASE = 10000000.0
EPS = 1e-5

VMEM_BYTES = 67043328
TOK = 128
HD = 128
TN = 512
DM = 6144
W = 4096
KVW = 1024
OWN_KV = W - KVW
N_SEQ = 4
N_CH = 4
N_CP = 4
N_G = 8
ROWS = N_SEQ * TOK
OWN = ROWS // 2
RB = 32
N_RB = OWN // RB
R_IN = N_RB - 2
IN_ROWS = R_IN * RB
N_FIN = 2 * N_CH + 1
LAST = OWN - IN_ROWS
N_QKV = (KVW + W) // TN
N_WO = DM // TN
N_BUF = 4
LA, LB = 0, 1
PAIR = range(2)
K, V, Q = 0, 1, 2
NT_DIMS = (((1,), (1,)), ((), ()))
TN_DIMS = (((0,), (0,)), ((), ()))


def rope_tables(n_cp):
    half = HD // 4
    inv = ROPE_BASE ** (-np.arange(half, dtype=np.float64) * 2.0 / (2 * half))
    pos = np.arange(n_cp * TOK, dtype=np.float64)
    ang = pos[:, None] * inv[None, :]
    tab = np.zeros((3, n_cp * TOK, HD), np.float32)
    tab[0] = 1.0
    tab[0, :, :half] = np.cos(ang)
    tab[0, :, half : 2 * half] = np.cos(ang)
    tab[1, :, :half] = -np.sin(ang)
    tab[2, :, half : 2 * half] = np.sin(ang)
    return np.ascontiguousarray(tab.reshape(3, n_cp, TOK, HD).transpose(1, 0, 2, 3))


def mo(v, m):
    return pl.multiple_of(v, m)


def upto(n):
    return pl.loop(0, n)


def parity(j):
    return lax.rem(j, 2)


def blk(b):
    return pl.ds(mo(b * TOK, TOK), TOK)


def hcol(g, hh):
    return pl.ds(mo((4 * g + hh) * HD, HD), HD)


def dot(a, b, dims=(((1,), (0,)), ((), ()))):
    return lax.dot_general(a, b, dims, preferred_element_type=F32)


def sigmoid(z):
    return 1.0 / (1.0 + jnp.exp(-z))


def kernel(
    hid, wqa, wka, wva, woa, wql, wkl, wvl, wgl, wol, rope_hbm, alphas, slopes, gain_a, gain_b, ginner,
    out, last, pt, prec, h1own, h1oth, kvh, kvr, sth, str_,
    wbuf, x, kvq, gbuf, u, acc, ost, stg, pst, nb_p, nb_r, nb_h, nout, ss, rsb, rope, ssx, ssr, wtab, gains,
    w_sem, x_sem, o_sem, kvo_sem, kvl_sem, sto_sem, stl_sem, nl_sem, no_sem,
    rs_send, rs_recv, ag_send, ag_recv, kv_send, kv_recv, st_send, st_recv, ss_send, ss_recv,
):
    cp = lax.axis_index("cp")
    tp = lax.axis_index("tp")
    mate = 1 - tp
    is0, is1, is2, is3 = (cp == c for c in range(N_CP))

    bar = pltpu.get_barrier_semaphore()
    pl.semaphore_signal(bar, inc=1, device_id={"tp": mate}, device_id_type=MESH)
    for d in range(1, 4):
        pl.semaphore_signal(bar, inc=1, device_id={"cp": lax.rem(cp + d, 4)}, device_id_type=MESH)

    def wtile(src, col, slot):
        rows = pl.ds(0, src.shape[0])
        return pltpu.make_async_copy(src.at[:, pl.ds(col, TN)], wbuf.at[slot, rows], w_sem.at[slot])

    def wstart(src, j):
        wtile(src, wcol(j), parity(j)).start()

    def wcol(j):
        return mo(j * TN, TN)

    def issue_b(j):
        kv = j < 16
        for cond, w, tile in (
            (kv & (parity(j) == 0), wkl, j // 2),
            (kv & (parity(j) == 1), wvl, j // 2),
            ((j >= 16) & (j < 24), wql, j - 16),
            (j >= 24, wgl, j - 24),
        ):

            @pl.when(cond)
            def _(w=w, tile=tile):
                wtile(w, wcol(tile), parity(j)).start()

    def wait_w(slot, src=wqa):
        wtile(src, 0, slot).wait()

    def fetch_next(j, count, go, then):
        @pl.when(j + 1 < count)
        def _():
            go(j + 1)

        @pl.when(j + 1 >= count)
        def _():
            then()

    def own_row(i):
        return mo((tp * 8 + 2 * i) * TOK, TOK)

    def oth_row(i):
        return mo((mate * 8 + 2 * i) * TOK, TOK)

    def x_copies(top, bot):
        return (
            pltpu.make_async_copy(top, x.at[pl.ds(0, OWN)], x_sem.at[0]),
            pltpu.make_async_copy(bot, x.at[pl.ds(OWN, OWN)], x_sem.at[1]),
        )

    def x_from_hid(i):
        return x_copies(hid.at[pl.ds(own_row(i), OWN)], hid.at[pl.ds(oth_row(i), OWN)])

    def x_from_h1(i):
        return x_copies(h1own.at[i], h1oth.at[i])

    def start_x_a(i):
        for c in x_from_hid(i):
            c.start()

    def start_x_b(i):
        ag_wait_recv(LA, i)
        for c in x_from_h1(i):
            c.start()

    def rs_copy(n, i, col, width, part=0, row=0, rows=OWN):
        return pltpu.make_async_remote_copy(
            src_ref=pt.at[n, i, pl.ds(OWN + row, rows), pl.ds(col, width)],
            dst_ref=prec.at[n, i, pl.ds(row, rows), pl.ds(col, width)],
            send_sem=rs_send.at[n, i, part],
            recv_sem=rs_recv.at[n, i, part],
            device_id={"tp": mate},
            device_id_type=MESH,
        )

    def ag_copy(n, i, row, rows):
        if n == 0:
            src = h1own.at[i, pl.ds(row, rows)]
            dst = h1oth.at[i, pl.ds(row, rows)]
        else:
            src = out.at[pl.ds(mo(own_row(i) + row, RB), rows)]
            dst = src
        return pltpu.make_async_remote_copy(
            src_ref=src,
            dst_ref=dst,
            send_sem=ag_send.at[n, i],
            recv_sem=ag_recv.at[n, i],
            device_id={"tp": mate},
            device_id_type=MESH,
        )

    def ag_wait_recv(n, i, rows=OWN):
        if n == 0:
            ag_copy(0, i, 0, rows).wait_recv()
        else:
            oth = out.at[pl.ds(oth_row(i), rows)]
            pltpu.make_async_remote_copy(
                src_ref=oth,
                dst_ref=oth,
                send_sem=ag_send.at[n, i],
                recv_sem=ag_recv.at[n, i],
                device_id={"tp": mate},
                device_id_type=MESH,
            ).wait_recv()

    def half_rows(h):
        return pl.ds(mo(OWN * (1 - h), OWN), OWN)

    def kv_copy(i, n, h, src, own, dst_cp, send):
        at = half_rows(h), pl.ds(n * TN, TN)
        return pltpu.make_async_remote_copy(
            src_ref=kvh.at[i, *at] if own else kvr.at[i, src, *at],
            dst_ref=kvr.at[i, src, *at],
            send_sem=kv_send.at[i, n, h, send],
            recv_sem=kv_recv.at[i, n, h, src],
            device_id={"cp": dst_cp},
            device_id_type=MESH,
        )

    def kv_sends(i, n, go):
        for h in PAIR:

            @pl.when(is0)
            def _(h=h):
                go(kv_copy(i, n, h, 0, True, 2, 0))
                go(kv_copy(i, n, h, 0, True, 1, 1))

            @pl.when(is1)
            def _(h=h):
                go(kv_copy(i, n, h, 1, True, 3, 0))

            @pl.when(is2)
            def _(h=h):
                go(kv_copy(i, n, h, 2, True, 3, 0))

    def st_copy(i, g):
        return pltpu.make_async_remote_copy(
            src_ref=sth.at[i, g],
            dst_ref=str_.at[i, g],
            send_sem=st_send.at[i, g],
            recv_sem=st_recv.at[i, g],
            device_id={"cp": lax.rem(cp + 1, 4)},
            device_id_type=MESH,
        )

    def ss_copy(i):
        return pltpu.make_async_remote_copy(
            src_ref=ssx.at[i],
            dst_ref=ssr.at[i],
            send_sem=ss_send.at[i],
            recv_sem=ss_recv.at[i],
            device_id={"tp": mate},
            device_id_type=MESH,
        )

    def norm_loads(n, i, r, start):
        slot = lax.rem(r, N_BUF)
        rows = pl.ds(mo(r * RB, RB), RB)
        copies = [
            pltpu.make_async_copy(pt.at[n, i, rows], nb_p.at[slot], nl_sem.at[slot, 0]),
            pltpu.make_async_copy(prec.at[n, i, rows], nb_r.at[slot], nl_sem.at[slot, 1]),
        ]
        res_a = hid.at[pl.ds(mo(own_row(i) + r * RB, RB), RB)]
        res_b = h1own.at[i, rows]
        for layer, res in ((LA, res_a), (LB, res_b)):

            @pl.when(n == layer)
            def _(res=res):
                c = pltpu.make_async_copy(res, nb_h.at[slot], nl_sem.at[slot, 2])
                c.start() if start else c.wait()

        for c in copies:
            c.start() if start else c.wait()

    def norm_begin(n, i, got=None, lo=0):
        with jax.named_scope("norm_wait"):
            (got or rs_copy(n, i, 0, DM)).wait_recv()

            @pl.when(n == LB)
            def _():
                ss_copy(i).wait_recv()
                for b in PAIR:
                    whole = ssx[i, b : b + 1, :] + ssr[i, b + 2 : b + 3, :]
                    inv = lax.rsqrt(whole / float(2 * W) + EPS)
                    rsb[blk(b), :] = jnp.broadcast_to(inv, (TOK, TOK)).T

            @pl.when(n == LA)
            def _():
                rsb[...] = jnp.ones_like(rsb)

            for r in range(lo, lo + N_BUF - 1):
                norm_loads(n, i, r, True)

    def norm_ready(n, i, r, hi):
        @pl.when(r + N_BUF - 1 < hi)
        def _():
            norm_loads(n, i, r + N_BUF - 1, True)

        norm_loads(n, i, r, False)

    def norm_rows(n, r):
        slot = lax.rem(r, N_BUF)
        alpha = alphas[n]
        for q in range(RB // 16):
            rows = slice(q * 16, (q + 1) * 16)
            both = nb_p[slot, rows, :].astype(F32) + nb_r[slot, rows, :].astype(F32)
            both = both * rsb[pl.ds(mo(r * RB + q * 16, 16), 16), 0:1]
            h = alpha * nb_h[slot, rows, :].astype(F32) + both
            inv = lax.rsqrt(jnp.mean(h * h, axis=-1, keepdims=True) + EPS)
            nout[slot, rows, :] = (h * inv * gains[pl.ds(n, 1), :]).astype(BF)

    def norm_store(n, i, r, start, end):
        slot = lax.rem(r, N_BUF)
        dst_a = h1own.at[i, pl.ds(mo(r * RB, RB), RB)]
        dst_b = out.at[pl.ds(mo(own_row(i) + r * RB, RB), RB)]
        inside = r < R_IN if end else True
        if end:

            @pl.when(r >= R_IN)
            def _():
                c = pltpu.make_async_copy(nout.at[slot], last.at[pl.ds(mo((r - R_IN) * RB, RB), RB)], no_sem.at[slot])
                c.start() if start else c.wait()

        for layer, dst in ((LA, dst_a), (LB, dst_b)):

            @pl.when((n == layer) & inside)
            def _(layer=layer, dst=dst):
                c = pltpu.make_async_copy(nout.at[slot], dst, no_sem.at[slot])
                if start:
                    c.start()
                else:
                    c.wait()

                    @pl.when((layer == LA) | (i == 0) | end | (r < R_IN))
                    def _():
                        ag_copy(layer, i, mo(r * RB, RB), RB).start()

    def norm_out(n, i, r, lo, end):
        @pl.when(r >= lo + 2)
        def _():
            norm_store(n, i, r - 2, False, end)

        norm_store(n, i, r, True, end)

    def norm_run(n, i, end=False, lo=0, hi=N_RB):
        with jax.named_scope("norm"):

            @pl.loop(lo, hi)
            def _(r):
                norm_ready(n, i, r, hi)
                norm_rows(n, r)
                norm_out(n, i, r, lo, end)

            for r in range(hi - 2, hi):
                norm_store(n, i, r, False, end)

    def norm(n, i, end=False):
        norm_begin(n, i)
        norm_run(n, i, end)

    def norm_seq(b):
        lo = b * TOK // RB
        norm_begin(LA, 0, rs_copy(LA, 0, 0, DM, b, b * TOK, TOK), lo)
        norm_run(LA, 0, False, lo, lo + TOK // RB)

    def out_proj(n, i, wo, then, pre, rows, send, sent=OWN):
        def put(j, slot):
            size = pl.ds(0, rows.size)
            return pltpu.make_async_copy(ost.at[slot, size], pt.at[n, i, rows, pl.ds(wcol(j), TN)], o_sem.at[slot])

        def send_on(j, slot):
            put(j, slot).wait()

            @pl.when(send)
            def _():
                rs_copy(n, i, wcol(j), TN, 0, 0, sent).start()

        with jax.named_scope("out_proj"):
            wtile(wo, TN, 1).start()

            @upto(N_WO)
            def _(j):
                slot = parity(j)
                wait_w(slot, wo)

                @pl.when(j == 8)
                def _():
                    pre()

                ost[slot, 0 : rows.size, :] = dot(u[rows, :], wbuf[slot, 0:W, :]).astype(BF)

                @pl.when(j + 2 < N_WO)
                def _():
                    wstart(wo, j + 2)

                @pl.when(j + 2 == N_WO)
                def _():
                    then()

                @pl.when(j >= 1)
                def _():
                    send_on(j - 1, 1 - slot)

                put(j, slot).start()

            send_on(N_WO - 1, 1)

    def rotate(a, kind, dst, row, col):
        for b in range(a.shape[0] // TOK):
            for h in range(TN // HD):
                v = a[b * TOK : (b + 1) * TOK, h * HD : (h + 1) * HD]
                v = v * rope[kind, 0] + pltpu.roll(v, HD - 32, 1) * rope[kind, 1] + pltpu.roll(v, 32, 1) * rope[kind, 2]
                kvq[dst, pl.ds(mo(row + b * TOK, TOK), TOK), pl.ds(mo(col + h * HD, HD), HD)] = v.astype(BF)

    def kv_forward(i, h):
        for n in PAIR:

            @pl.when(is2)
            def _(n=n):
                kv_copy(i, n, h, 0, False, 3, 1).wait_recv()
                kv_copy(i, n, h, 0, False, 3, 1).start()

            @pl.when(is3)
            def _(n=n):
                kv_copy(i, n, h, 1, False, 2, 0).wait_recv()
                kv_copy(i, n, h, 1, False, 2, 0).start()

    def kv_wait(i, halves):
        parts = [(n, h) for h in halves for n in PAIR]

        def got(n, h, src):
            kv_copy(i, n, h, src, False, 0, 0).wait_recv()

        def fetch(c, h):
            rows = half_rows(h)
            dst = kvq.at[K, rows, pl.ds(c * KVW, KVW)]
            return pltpu.make_async_copy(kvr.at[i, c, rows], dst, kvl_sem.at[c, h])

        with jax.named_scope("kv_wait"):
            for n, h in parts:

                @pl.when(is1)
                def _(n=n, h=h):
                    got(n, h, 0)

                @pl.when(is2)
                def _(n=n, h=h):
                    got(n, h, 1)

                @pl.when(is3)
                def _(n=n, h=h):
                    got(n, h, 2)
                    got(n, h, 0)

            for go in (lambda c: c.start(), lambda c: c.wait()):
                for c in range(N_CP - 1):

                    @pl.when(cp > c)
                    def _(c=c, go=go):
                        for h in halves:
                            go(fetch(c, h))

    def attention(first, count):
        scale = math.log2(math.e) / math.sqrt(HD)
        with jax.named_scope("attn"):
            for c in range(N_CP):

                @pl.when(cp == c)
                def _(c=c):
                    cols = [OWN_KV] + [b * KVW for b in range(c)]

                    @upto(4 * count)
                    def _(t):
                        g = lax.rem(t, 4)
                        seq = pl.ds(mo(first + t // 4 * TOK, TOK), TOK)
                        ks = [kvq[K, seq, pl.ds(mo(o + g * HD, HD), HD)] for o in cols]
                        vs = [kvq[K, seq, pl.ds(mo(o + TN + g * HD, HD), HD)] for o in cols]
                        keys = jnp.concatenate(ks, axis=0) if c else ks[0]
                        vals = jnp.concatenate(vs, axis=0) if c else vs[0]
                        row = lax.rem(lax.broadcasted_iota(jnp.int32, (2 * TOK, TOK), 0), TOK)
                        causal = lax.broadcasted_iota(jnp.int32, (2 * TOK, TOK), 1) <= row

                        def heads(p):
                            return [pl.ds(mo((g * 8 + 2 * p + z) * HD, HD), HD) for z in PAIR]

                        scores = []
                        for p in range(4):
                            qs = jnp.concatenate([kvq[Q, seq, o] for o in heads(p)], axis=0)
                            scores.append(dot(qs, keys, NT_DIMS))
                        for p in range(4):
                            s = scores[p]
                            own = jnp.where(causal, s[:, :TOK], -jnp.inf)
                            s = jnp.concatenate([own, s[:, TOK:]], axis=1) if c else own
                            m = jnp.max(s, axis=1, keepdims=True)
                            e = jnp.exp2((s - m) * scale)
                            o = dot(e.astype(BF), vals) * (1.0 / jnp.sum(e, axis=1, keepdims=True))
                            for z in PAIR:
                                u[seq, heads(p)[z]] = o[z * TOK : (z + 1) * TOK].astype(BF)

    def layer_a(i, mid, then, pre):
        with jax.named_scope("x_a"):
            for c in x_from_hid(i):
                c.wait()

        def kv_out(n):
            cols = pl.ds(n * TN, TN)
            return pltpu.make_async_copy(kvq.at[K, :, pl.ds(OWN_KV + n * TN, TN)], kvh.at[i, :, cols], kvo_sem.at[n])

        def finish(j, slot):
            kv = j < 2
            col = jnp.where(kv, OWN_KV + j * TN, (j - 2) * TN)
            rotate(acc.at[slot], jnp.where(j == 1, 1, 0), jnp.where(kv, K, Q), 0, col)

        with jax.named_scope("qkv_a"):

            @upto(N_QKV)
            def _(j):
                slot = parity(j)
                wait_w(slot)

                @pl.when(j == 0)
                def _():
                    wtile(wva, 0, 1).start()

                @pl.when(j >= 1)
                def _():
                    fetch_next(j, N_QKV, lambda t: wstart(wqa, t - 2), lambda: wtile(woa, 0, 0).start())

                for n in PAIR:

                    @pl.when(j == n + 2)
                    def _(n=n):
                        kv_out(n).wait()
                        kv_sends(i, n, lambda c: c.start())

                for h in PAIR:

                    @pl.when(j == N_QKV - 2 + h)
                    def _(h=h):
                        kv_forward(i, h)

                finish(jnp.maximum(j - 1, 0), 1 - slot)
                acc[slot] = dot(x[...], wbuf[slot])

                for n in PAIR:

                    @pl.when(j == n + 1)
                    def _(n=n):
                        kv_out(n).start()

                mid(j)

            finish(N_QKV - 1, 1)

        @pl.when(i > 0)
        def _():
            kv_wait(i, PAIR)
            attention(0, N_SEQ)
            out_proj(LA, i, woa, then, pre, pl.ds(0, ROWS), True)

        @pl.when(i == 0)
        def _():
            @upto(2)
            def _(h):
                first = mo(OWN * (1 - h), OWN)
                kv_wait(0, (h,))
                attention(first, 2)

                def then_a():
                    @pl.when(h == 0)
                    def _():
                        wtile(woa, 0, 0).start()

                    @pl.when(h == 1)
                    def _():
                        then()

                def pre_a():
                    @pl.when(h == 1)
                    def _():
                        pre()

                out_proj(LA, 0, woa, then_a, pre_a, pl.ds(first, OWN), h == 0, TOK)

                @pl.when(h == 0)
                def _():
                    rs_copy(LA, 0, 0, DM, 1, TOK, TOK).start()

    def key_decay(h):
        back = lax.broadcasted_iota(jnp.int32, (TOK, HD), 0).astype(F32) - (TOK - 1.0)
        return jnp.exp(slopes[h] * back)

    def state_of(g, b, hh, kd):
        rows = blk(b)
        col = hcol(g, hh)
        k = (kvq[K, rows, col].astype(F32) * kd).astype(BF)
        return dot(k, kvq[V, rows, col], TN_DIMS)

    def block_decay(h):
        return jnp.exp(jnp.full((8, HD), -float(TOK), F32) * slopes[h])[0:1, :]

    def st_store(i, g, slot):
        return pltpu.make_async_copy(stg.at[slot], sth.at[i, g], sto_sem.at[slot])

    def st_load(i, g, slot):
        return pltpu.make_async_copy(str_.at[i, g], pst.at[slot], stl_sem.at[slot])

    def next_state(g):
        slot = parity(g)
        for hh in range(4):
            kd = key_decay(4 * g + hh)
            bd = block_decay(4 * g + hh)
            new = [state_of(g, b, hh, kd) for b in range(N_SEQ)]
            for b in range(N_SEQ):
                stg[slot, b * 4 + hh] = new[b] + bd * pst[slot, b * 4 + hh]

    def local_state(i, g):
        slot = parity(g)

        @pl.when(is1)
        def _():
            st_load(i, g, slot).wait()

        @pl.when(is0)
        def _():
            for hh in range(N_SEQ):
                kd = key_decay(4 * g + hh)
                for b in range(N_SEQ):
                    stg[slot, b * 4 + hh] = state_of(g, b, hh, kd)

        @pl.when(is1)
        def _():
            for hh in range(N_SEQ):
                kd = key_decay(4 * g + hh)
                bd = block_decay(4 * g + hh)
                for b in range(N_SEQ):
                    stg[slot, b * 4 + hh] = state_of(g, b, hh, kd) + bd * pst[slot, b * 4 + hh]

        st_store(i, g, slot).start()

    def st_send_on(i, g):
        st_store(i, g, parity(g)).wait()
        st_copy(i, g).start()

    def layer_b(i, mid, then, pre):
        with jax.named_scope("x_b"):
            for c in x_from_h1(i):
                c.wait()

        def finish(j, a):
            kv = j < 16
            dst = jnp.where(kv, parity(j), Q)
            kvq[dst, :, pl.ds(wcol(jnp.where(kv, j // 2, j - 16)), TN)] = (a * sigmoid(a)).astype(BF)

        with jax.named_scope("qkv_b"):
            @upto(24)
            def _(j):
                slot = parity(j)
                wait_w(slot)
                issue_b(j + 1)

                e = j - jnp.where(is0, 0, 2)
                busy = (cp <= 1) & (e >= 1) & (e <= 16)
                g = e // 2

                @pl.when(busy & (parity(e) == 1) & is1)
                def _():
                    st_copy(i, g).wait_recv()
                    st_load(i, g, parity(g)).start()

                mid(j, norm_begin)
                finish(j, dot(x[...], wbuf[slot]))

                @pl.when(busy & (parity(e) == 0))
                def _():
                    st_send_on(i, g - 1)

                @pl.when(busy & (parity(e) == 1))
                def _():
                    local_state(i, g)

                mid(j, norm_run)

        with jax.named_scope("gate"):

            @upto(8)
            def _(j):
                slot = parity(j)
                wait_w(slot)
                fetch_next(j, 8, lambda t: issue_b(t + 24), lambda: wtile(wol, 0, 0).start())

                @pl.when(is2)
                def _():
                    st_copy(i, j).wait_recv()
                    st_load(i, j, slot).start()

                gbuf[:, pl.ds(wcol(j), TN)] = sigmoid(dot(x[...], wbuf[slot]))

                @pl.when(is2)
                def _():
                    st_load(i, j, slot).wait()
                    next_state(j)
                    st_store(i, j, slot).start()

                    @pl.when(j >= 1)
                    def _():
                        st_send_on(i, j - 1)

        with jax.named_scope("lin"):

            @pl.when(is2)
            def _():
                st_send_on(i, N_G - 1)

            ss[...] = jnp.zeros_like(ss)

            def fetch(g):
                @pl.when(is3)
                def _():
                    st_copy(i, g).wait_recv()

                @pl.when(cp >= 1)
                def _():
                    st_load(i, g, parity(g)).start()

            @pl.when(is0)
            def _():
                pst[...] = jnp.zeros_like(pst)

            fetch(0)

            @upto(N_G)
            def _(g):
                slot = parity(g)

                @pl.when(g + 1 < N_G)
                def _():
                    fetch(g + 1)

                for hh in range(4):
                    lam = slopes[4 * g + hh]
                    row = lax.broadcasted_iota(jnp.int32, (TOK, HD), 0).astype(F32)
                    lane = lax.broadcasted_iota(jnp.int32, (TOK, HD), 1).astype(F32)
                    gap = row - lane
                    wtab[hh, 0] = jnp.where(gap >= 0, jnp.exp(-lam * jnp.maximum(gap, 0.0)), 0.0)
                    wtab[hh, 1] = jnp.exp(-lam * (row + 1.0))

                @pl.when(cp >= 1)
                def _():
                    st_load(i, g, slot).wait()

                @upto(2)
                def _(half):
                    pairs = [(half * 2 + z, hh) for z in PAIR for hh in range(4)]
                    at = [(blk(b), hcol(g, hh)) for b, hh in pairs]
                    qs = [kvq[Q, r, c] for r, c in at]
                    inner = [dot(q, kvq[K, r, c], NT_DIMS) for q, (r, c) in zip(qs, at)]
                    prior = [dot(q, pst[slot, b * 4 + hh].astype(BF)) for q, (b, hh) in zip(qs, pairs)]
                    o = [
                        dot((s * wtab[hh, 0]).astype(BF), kvq[V, r, c]) + p * wtab[hh, 1]
                        for s, p, (r, c), (b, hh) in zip(inner, prior, at, pairs)
                    ]
                    for v, (r, c) in zip(o, at):
                        u[r, c] = (v * ginner[0:1, c] * gbuf[r, c]).astype(BF)
                    for z in PAIR:
                        ss[at[4 * z][0], :] += sum(v * v for v in o[4 * z : 4 * z + 4])

            sums = [jnp.sum(ss[blk(b), :].T, axis=0, keepdims=True) for b in range(N_SEQ)]
            ssx[i] = jnp.concatenate(sums + sums, axis=0)

        def then_ss():
            ss_copy(i).start()
            pre()

        out_proj(LB, i, wol, then, then_ss, pl.ds(0, ROWS), True)

        @pl.when(i >= 2)
        def _():
            ag_copy(LB, i - 1, IN_ROWS, LAST).start()

    wtile(wka, 0, 0).start()
    start_x_a(0)
    rope_in = pltpu.make_async_copy(rope_hbm.at[cp], rope.at[0], kvo_sem.at[0])
    rope_in.start()
    gains[0:1, :] = gain_a[...]
    gains[1:2, :] = gain_b[...]
    rope[1, 0] = jnp.ones((TOK, HD), F32)
    rope[1, 1] = jnp.zeros((TOK, HD), F32)
    rope[1, 2] = jnp.zeros((TOK, HD), F32)
    rope_in.wait()
    pl.semaphore_wait(bar, 4)

    @upto(7)
    def _(s):
        @pl.when((s < 3) | (s == 4))
        def _():
            def mid_a(j):
                for b in PAIR:

                    @pl.when((s == 1) & (j == 4 * b))
                    def _(b=b):
                        norm_seq(b)

            def then_a():
                @pl.when(s < 2)
                def _():
                    wtile(wka, 0, 0).start()

                @pl.when(s >= 2)
                def _():
                    wtile(wkl, 0, 0).start()

            def pre_a():
                @pl.when(s < 2)
                def _():
                    start_x_a(s + 1)

                @pl.when(s >= 2)
                def _():
                    start_x_b(jnp.where(s == 2, 0, 1))

            layer_a(jnp.where(s < 3, s, 3), mid_a, then_a, pre_a)

        @pl.when(s == 2)
        def _():
            norm(LA, 1)

        @pl.when(s >= 3)
        def _():
            def mid_b(j, go):
                now = jnp.where(s == 4, 4, jnp.where(s == 6, 19, 15))

                @pl.when(j == now)
                def _():
                    go(jnp.where(s == 3, LA, LB), jnp.where(s == 3, 2, s - 4))

            def then_b():
                @pl.when(s == 3)
                def _():
                    wtile(wka, 0, 0).start()

                @pl.when((s > 3) & (s < 6))
                def _():
                    wtile(wkl, 0, 0).start()

            def pre_b():
                @pl.when(s == 3)
                def _():
                    start_x_a(3)

                @pl.when((s > 3) & (s < 6))
                def _():
                    start_x_b(s - 2)

            layer_b(s - 3, mid_b, then_b, pre_b)

        @pl.when(s == 4)
        def _():
            norm(LA, 3)

    norm(LB, 3, end=True)

    for i in range(N_CH):
        for n in PAIR:
            if n == LA and i == 0:
                for b in PAIR:
                    rs_copy(n, i, 0, DM, b, b * TOK, TOK).wait_send()
            else:
                rs_copy(n, i, 0, DM).wait_send()
            rows = IN_ROWS if n == LB and i == N_CH - 1 else OWN
            ag_copy(n, i, 0, rows).wait_send()
        ag_wait_recv(LB, i, rows)
        ss_copy(i).wait_send()

        for n in PAIR:
            kv_sends(i, n, lambda c: c.wait_send())
            for h in PAIR:

                @pl.when(is2)
                def _(i=i, n=n, h=h):
                    kv_copy(i, n, h, 0, False, 3, 1).wait_send()

                @pl.when(is3)
                def _(i=i, n=n, h=h):
                    kv_copy(i, n, h, 1, False, 2, 0).wait_send()

        @pl.when(cp <= 2)
        def _(i=i):
            @upto(8)
            def _(g):
                st_copy(i, g).wait_send()


def assemble(rows, last, res, buf, in_sem, out_sem):
    tp = lax.axis_index("tp")
    parts = [(own, k, IN_ROWS if k == N_CH - 1 else OWN, False) for own in (True, False) for k in range(N_CH)]
    parts.append((True, N_CH - 1, LAST, True))

    def place(p):
        own, k, size, end = parts[p]
        first = ((tp if own else 1 - tp) * N_CH + k) * OWN + (IN_ROWS if end else 0)
        return pl.ds(mo(first, LAST), size), buf.at[p, pl.ds(0, size)], last if end else None

    def load(p):
        at, mid, src = place(p)
        return pltpu.make_async_copy(rows.at[at] if src is None else src, mid, in_sem.at[p])

    def store(p):
        at, mid, _ = place(p)
        return pltpu.make_async_copy(mid, res.at[at], out_sem.at[p])

    for p in range(N_FIN):
        load(p).start()
    for p in range(N_FIN):
        load(p).wait()
        store(p).start()
    for p in range(N_FIN):
        store(p).wait()


def solution(mesh):
    n_cp = mesh.shape["cp"]
    table = rope_tables(n_cp)
    any_ = pl.BlockSpec(memory_space=pl.ANY)
    smem = pl.BlockSpec(memory_space=pltpu.SMEM)
    vmem = pl.BlockSpec(memory_space=pltpu.VMEM)
    dma = pltpu.SemaphoreType.DMA
    two = (2,)

    def body(hidden, alphas, wqa, wka, wva, woa, gain_attn, wql, wkl, wvl, wgl, slopes, gain_inner, wol, gain_lin):
        shape = hidden.shape
        hid = hidden.reshape(shape[0] * shape[1], shape[2])
        sds = jax.ShapeDtypeStruct
        outs = (
            sds(hid.shape, BF),
            sds((LAST, DM), BF),
            sds((2, N_CH, ROWS, DM), BF),
            sds((2, N_CH, OWN, DM), BF),
            sds((N_CH, OWN, DM), BF),
            sds((N_CH, OWN, DM), BF),
            sds((N_CH, ROWS, KVW), BF),
            sds((N_CH, 3, ROWS, KVW), BF),
            sds((N_CH, N_G, 16, HD, HD), F32),
            sds((N_CH, N_G, 16, HD, HD), F32),
        )
        scratch = [
            pltpu.VMEM((2, DM, TN), BF),
            pltpu.VMEM((ROWS, DM), BF),
            pltpu.VMEM((3, ROWS, W), BF),
            pltpu.VMEM((ROWS, W), F32),
            pltpu.VMEM((ROWS, W), BF),
            pltpu.VMEM((2, ROWS, TN), F32),
            pltpu.VMEM((2, ROWS, TN), BF),
            pltpu.VMEM((2, 16, HD, HD), F32),
            pltpu.VMEM((2, 16, HD, HD), F32),
            pltpu.VMEM((N_BUF, RB, DM), BF),
            pltpu.VMEM((N_BUF, RB, DM), BF),
            pltpu.VMEM((N_BUF, RB, DM), BF),
            pltpu.VMEM((N_BUF, RB, DM), BF),
            pltpu.VMEM((ROWS, HD), F32),
            pltpu.VMEM((OWN, HD), F32),
            pltpu.VMEM((2, 3, TOK, HD), F32),
            pltpu.VMEM((N_CH, 8, HD), F32),
            pltpu.VMEM((N_CH, 8, HD), F32),
            pltpu.VMEM((4, 2, TOK, HD), F32),
            pltpu.VMEM((2, DM), F32),
            dma(two), dma(two), dma(two), dma(two), dma((3, 2)), dma(two), dma(two), dma((N_BUF, 3)), dma((N_BUF,)),
            dma((2, N_CH, 2)), dma((2, N_CH, 2)), dma((2, N_CH)), dma((2, N_CH)), dma((N_CH, 2, 2, 2)), dma((N_CH, 2, 2, 3)), dma((N_CH, N_G)), dma((N_CH, N_G)),
            dma((N_CH,)), dma((N_CH,)),
        ]
        res = pl.pallas_call(
            kernel,
            out_shape=outs,
            in_specs=[any_] * 11 + [smem, smem, vmem, vmem, vmem],
            out_specs=tuple(any_ for _ in outs),
            scratch_shapes=scratch,
            compiler_params=pltpu.CompilerParams(
                collective_id=0, has_side_effects=True, vmem_limit_bytes=VMEM_BYTES
            ),
            name="layers",
        )(
            hid, wqa, wka, wva, woa, wql, wkl, wvl, wgl, wol, jnp.asarray(table), alphas, slopes, gain_attn.reshape(1, -1),
            gain_lin.reshape(1, -1), gain_inner.reshape(1, -1),
        )
        got = lax.ppermute(res[1], "tp", [(0, 1), (1, 0)])
        rows = pl.pallas_call(
            assemble,
            out_shape=sds(hid.shape, BF),
            in_specs=[any_, any_],
            out_specs=any_,
            scratch_shapes=[pltpu.VMEM((N_FIN, OWN, DM), BF), dma((N_FIN,)), dma((N_FIN,))],
            compiler_params=pltpu.CompilerParams(vmem_limit_bytes=VMEM_BYTES),
            cost_estimate=pl.CostEstimate(flops=10**11, bytes_accessed=2 * hid.size * 2, transcendentals=0),
            name="assemble",
        )(res[0], res[1])
        row = ((1 - lax.axis_index("tp")) * N_CH + N_CH - 1) * OWN + IN_ROWS
        return lax.dynamic_update_slice(rows, got, (row, 0)).reshape(shape)

    act = P("dp", "cp", None)
    rep = P()
    col = P(None, "tp")
    row = P("tp", None)
    vec = P("tp")
    in_specs = (act, rep, col, col, col, row, rep, col, col, col, col, vec, vec, row, rep)
    return jax.shard_map(body, mesh=mesh, in_specs=in_specs, out_specs=act, check_vma=False)
```
